32 devices in a mesh: z: 4 (over z), y: 2 (over y), x: 4 (over x, core).
Axes of the slice: x: 2, y: 2, z: 4, core: 2. Of those that a mesh axis runs over, the one named last changes fastest.
Arguments:
- atom_pos: float32 [23328, 3], P(('z', 'y', 'x'))
- atom_vel: float32 [23328, 3], P(('z', 'y', 'x'))
- atom_frc: float32 [23328, 3], P(('z', 'y', 'x'))
- atom_id: int32 [23328], P(('z', 'y', 'x'))
- atom_ok: int32 [23328], P(('z', 'y', 'x'))
- brick_side: float32 [], replicated
Outputs:
- output 1: float32 [23328, 3], P(('z', 'y', 'x'))
- output 2: float32 [23328, 3], P(('z', 'y', 'x'))
- output 3: float32 [23328, 3], P(('z', 'y', 'x'))
- output 4: int32 [23328], P(('z', 'y', 'x'))
- output 5: int32 [23328], P(('z', 'y', 'x'))
- output 6: float32 [], replicated
All inputs are finite; a program needn't handle non-finite values.
Results may differ from the reference program's by a relative error of at most 0.001.
Values sent between devices are 32-bit elements.
A program may use at most 1 GiB of HBM per device.

```python
import jax
import jax.numpy as jnp
from jax import lax

NZ = 4
NY = 2
NX = 4
GRID = 8
RHO_E4 = 9600
CAP = 729

DEVICES = NZ * NY * NX
SITES = DEVICES * GRID * GRID * GRID
MOVE_MAX = max(1, CAP // 100)
PLANE = (GRID - 1) * (GRID - 1)
SITE_SHAPE = (NZ, NY, NX, GRID, GRID, GRID)
VEC_SHAPE = (NZ, NY, NX, GRID, GRID, GRID, 3)
DT = 0.005
RC = 2.5
UCUT = 4.0 * (RC ** -12 - RC ** -6)
UPC = -48.0 * RC ** -13 + 24.0 * RC ** -7


def place_atoms(base_key, spacing, jitter, free_disp, prev_force):
    sub_keys = jax.random.split(base_key, 8)
    brick_vec = jnp.stack([lax.broadcasted_iota(jnp.int32, SITE_SHAPE, 2), lax.broadcasted_iota(jnp.int32, SITE_SHAPE, 1), lax.broadcasted_iota(jnp.int32, SITE_SHAPE, 0)], axis=-1)
    site_vec = jnp.stack([lax.broadcasted_iota(jnp.int32, SITE_SHAPE, 5), lax.broadcasted_iota(jnp.int32, SITE_SHAPE, 4), lax.broadcasted_iota(jnp.int32, SITE_SHAPE, 3)], axis=-1)
    dims_int = jnp.array([NX, NY, NZ], jnp.int32)
    on_face = site_vec == 0
    face_count = jnp.sum(on_face.astype(jnp.int32), axis=-1, keepdims=True)
    side_sign = 2 * jax.random.randint(sub_keys[0], VEC_SHAPE, 0, 2) - 1
    plane_perm = jax.random.permutation(sub_keys[1], jnp.broadcast_to(jnp.arange(PLANE), (NZ, NY, NX, 3, PLANE)), axis=-1, independent=True)
    inner_k = jnp.maximum(site_vec - 1, 0)
    plane_idx = jnp.stack([inner_k[..., (axis_d + 1) % 3] * (GRID - 1) + inner_k[..., (axis_d + 2) % 3] for axis_d in range(3)], axis=-1)
    plane_rank = jnp.take_along_axis(jnp.broadcast_to(plane_perm[:, :, :, None, None, None, :, :], VEC_SHAPE + (PLANE,)), plane_idx[..., None], axis=-1)[..., 0]
    down_count = jax.random.randint(sub_keys[2], (NZ, NY, NX, 3), 0, MOVE_MAX + 1)[:, :, :, None, None, None, :]
    up_count = jax.random.randint(sub_keys[3], (NZ, NY, NX, 3), 0, MOVE_MAX + 1).at[0, 0, 0, 0].set(MOVE_MAX)[:, :, :, None, None, None, :]
    plane_site = on_face & (face_count == 1)
    go_down = plane_site & (plane_rank < down_count)
    go_up = plane_site & (plane_rank >= down_count) & (plane_rank < down_count + up_count)
    edge_flag = (face_count == 2) & jnp.logical_not(on_face[..., 2:3]) & (site_vec[..., 2:3] == 1)
    corner_flag = face_count == 3
    crossing = go_down | go_up | (on_face & (edge_flag | corner_flag))
    side_sign = jnp.where(go_down, -1, jnp.where(go_up, 1, side_sign))
    pre_side = jnp.where(crossing, -side_sign, side_sign)
    pre_brick = jnp.mod(brick_vec + jnp.where(on_face & (pre_side < 0), -1, 0), dims_int)
    pre_dev = (pre_brick[..., 2] * NY + pre_brick[..., 1]) * NX + pre_brick[..., 0]
    fill_pct = jax.random.randint(sub_keys[4], (NZ, NY, NX, 1, 1, 1), 50, 101)
    occupied = (jax.random.randint(sub_keys[5], SITE_SHAPE, 0, 100) < fill_pct) | jnp.any(crossing, axis=-1)
    atom_ids = jax.random.permutation(sub_keys[6], SITES).astype(jnp.int32).reshape(SITE_SHAPE)
    near_gaps = jax.random.uniform(sub_keys[7], VEC_SHAPE + (2,), jnp.float32, 0.002, 0.006)
    face_gap = near_gaps[..., 0]
    cross_gap = near_gaps[..., 1]
    sign_f = side_sign.astype(jnp.float32)
    lattice = (brick_vec * GRID + site_vec).astype(jnp.float32) * spacing
    post_pos = lattice + jnp.where(on_face, sign_f * face_gap, jitter * spacing)
    displace = jnp.where(on_face, jnp.where(crossing, sign_f * (face_gap + cross_gap), 0.5 * sign_f * face_gap), free_disp)
    box_len = spacing * GRID * dims_int.astype(jnp.float32)
    start_pos = jnp.mod(post_pos - displace, box_len)
    start_vel = displace / DT - (0.5 * DT) * prev_force
    flat_ok = occupied.reshape(SITES)
    flat_dev = pre_dev.reshape(SITES)
    sort_key = jnp.where(flat_ok, flat_dev * SITES + atom_ids.reshape(SITES), DEVICES * SITES)
    sort_order = jnp.argsort(sort_key)
    counts = jax.ops.segment_sum(flat_ok.astype(jnp.int32), flat_dev, num_segments=DEVICES)
    first_row = jnp.cumsum(counts) - counts
    sorted_dev = flat_dev[sort_order]
    dest_row = jnp.where(flat_ok[sort_order], sorted_dev * CAP + jnp.arange(SITES) - first_row[sorted_dev], DEVICES * CAP)

    def spread(values):
        tail_dims = values.shape[6:]
        flat_vals = values.reshape((SITES,) + tail_dims)[sort_order]
        return jnp.zeros((DEVICES * CAP,) + tail_dims, values.dtype).at[dest_row].set(flat_vals, mode="drop")

    return {"atom_pos": spread(start_pos), "atom_vel": spread(start_vel), "atom_frc": spread(prev_force), "atom_id": spread(atom_ids), "atom_ok": spread(occupied.astype(jnp.int32)), "brick_side": spacing * GRID}


def setup_inputs(seed: int = 0) -> dict:
    value_keys = jax.random.split(jax.random.key(seed + 1), 4)
    spacing = (RHO_E4 / 10000.0) ** (-1.0 / 3.0) * (1.0 + 0.01 * jax.random.uniform(value_keys[0], (), jnp.float32, -1.0, 1.0))
    jitter = jax.random.uniform(value_keys[1], VEC_SHAPE, jnp.float32, -0.05, 0.05)
    free_disp = jax.random.uniform(value_keys[2], VEC_SHAPE, jnp.float32, -0.01, 0.01)
    prev_force = 40.0 * jax.random.normal(value_keys[3], VEC_SHAPE, jnp.float32)
    return place_atoms(jax.random.key(seed), spacing, jitter, free_disp, prev_force)


def pair_terms(own_pos, own_ok, other_pos, other_ok, box_len):
    delta_r = own_pos[..., :, None, :] - other_pos[..., None, :, :]
    delta_r = delta_r - box_len * jnp.floor(delta_r / box_len + 0.5)
    dist_sq = jnp.sum(delta_r * delta_r, axis=-1)
    in_range = own_ok[..., :, None] & other_ok[..., None, :] & (dist_sq < RC * RC) & (dist_sq > 0.01)
    safe_sq = jnp.where(in_range, dist_sq, 1.0)
    inv_r2 = 1.0 / safe_sq
    inv_r6 = inv_r2 * inv_r2 * inv_r2
    radius = jnp.sqrt(safe_sq)
    f_scale = jnp.where(in_range, (48.0 * inv_r6 * inv_r6 - 24.0 * inv_r6) * inv_r2 + UPC / radius, 0.0)
    pair_energy = jnp.where(in_range, 4.0 * (inv_r6 * inv_r6 - inv_r6) - UCUT - (radius - RC) * UPC, 0.0)
    force_sum = jnp.sum(f_scale[..., None] * delta_r, axis=-2)
    return force_sum, jnp.sum(pair_energy)


def brick_forces(own_pos, own_ok, other_pos, other_ok, box_len):
    force_sum = jnp.zeros_like(own_pos)
    energy_sum = jnp.zeros((), own_pos.dtype)
    for neighbor in range(other_pos.shape[0]):
        force_part, energy_part = pair_terms(own_pos, own_ok, other_pos[neighbor], other_ok[neighbor], box_len)
        force_sum = force_sum + force_part
        energy_sum = energy_sum + energy_part
    return force_sum, energy_sum


def reference(atom_pos, atom_vel, atom_frc, atom_id, atom_ok, brick_side):
    dims_int = jnp.array([NX, NY, NZ], jnp.int32)
    box_len = brick_side * dims_int.astype(jnp.float32)
    owned = atom_ok > 0
    half_v = atom_vel + (0.5 * DT) * atom_frc
    moved = jnp.mod(atom_pos + DT * half_v, box_len)
    new_cell = jnp.clip(jnp.floor(moved / brick_side).astype(jnp.int32), 0, dims_int - 1)
    dest_dev = (new_cell[:, 2] * NY + new_cell[:, 1]) * NX + new_cell[:, 0]
    sort_key = jnp.where(owned, dest_dev * SITES + atom_id, DEVICES * SITES)
    sort_order = jnp.argsort(sort_key)
    counts = jax.ops.segment_sum(owned.astype(jnp.int32), dest_dev, num_segments=DEVICES)
    first_row = jnp.cumsum(counts) - counts
    sorted_dev = dest_dev[sort_order]
    dest_row = jnp.where(owned[sort_order], sorted_dev * CAP + jnp.arange(DEVICES * CAP) - first_row[sorted_dev], DEVICES * CAP)

    def spread(values):
        return jnp.zeros_like(values).at[dest_row].set(values[sort_order], mode="drop")

    new_pos = spread(moved)
    new_half = spread(half_v)
    new_id = spread(atom_id)
    new_ok = spread(atom_ok)
    grid_pos = new_pos.reshape(NZ, NY, NX, CAP, 3)
    grid_ok = (new_ok > 0).reshape(NZ, NY, NX, CAP)
    steps_z = range(-1, 2) if NZ > 2 else range(0, 2)
    steps_y = range(-1, 2) if NY > 2 else range(0, 2)
    steps_x = range(-1, 2) if NX > 2 else range(0, 2)
    shell_list = [(shift_z, shift_y, shift_x) for shift_z in steps_z for shift_y in steps_y for shift_x in steps_x]
    other_pos = jnp.stack([jnp.roll(grid_pos, (-shift_zyx[0], -shift_zyx[1], -shift_zyx[2]), axis=(0, 1, 2)) for shift_zyx in shell_list], axis=3)
    other_ok = jnp.stack([jnp.roll(grid_ok, (-shift_zyx[0], -shift_zyx[1], -shift_zyx[2]), axis=(0, 1, 2)) for shift_zyx in shell_list], axis=3)
    n_shell = len(shell_list)
    force_grid, energy_grid = lax.map(lambda packed: brick_forces(packed[0], packed[1], packed[2], packed[3], box_len), (grid_pos.reshape(DEVICES, CAP, 3), grid_ok.reshape(DEVICES, CAP), other_pos.reshape(DEVICES, n_shell, CAP, 3), other_ok.reshape(DEVICES, n_shell, CAP)))
    new_force = force_grid.reshape(DEVICES * CAP, 3)
    ok_f = (new_ok > 0).astype(new_pos.dtype)[:, None]
    new_vel = (new_half + (0.5 * DT) * new_force) * ok_f
    energy = 0.5 * jnp.sum(energy_grid)
    return new_pos, new_vel, new_force, new_id, new_ok, energy
```

```python
import functools

import jax
import jax.numpy as jnp
from jax import lax
from jax.experimental import pallas as pl
from jax.experimental.pallas import tpu as pltpu
from jax.sharding import PartitionSpec as P

DT = 0.005
RC = 2.5
FAR = 1.0e6
UCUT = 4.0 * (RC ** -12 - RC ** -6)
UPC = -48.0 * RC ** -13 + 24.0 * RC ** -7
MESH_AXES = ("z", "y", "x")
DIRS = [(dx, dy, dz) for dz in (-1, 0, 1) for dy in (-1, 0, 1) for dx in (-1, 0, 1) if (dx, dy, dz) != (0, 0, 0)]
NEAR = RC + 1.0e-3
PACK = 8
L = 128
F32 = jnp.float32
BF16 = jnp.bfloat16
I32 = jnp.int32
NT = (((1,), (1,)), ((), ()))
NN = (((1,), (0,)), ((), ()))


def order_of(d):
    if d[2] == 0:
        return 1 if d[1] != 0 else 2
    return 2 if (d[1] == 0 and d[0] != 0) else 0


def range_of(d):
    cx, cy, cz = [(1, 0, 2)[c] for c in (d[0], d[1], d[2])]
    kind = order_of(d)
    if kind == 0:
        if d[0] == 0 and d[1] == 0:
            return cz * 9, cz * 9 + 9
        if d[0] == 0:
            return cz * 9 + cy * 3, cz * 9 + cy * 3 + 3
        return cz * 9 + cy * 3 + cx, cz * 9 + cy * 3 + cx + 1
    if kind == 1:
        if d[0] == 0:
            return cy * 9, cy * 9 + 9
        return cy * 9 + cx * 3, cy * 9 + cx * 3 + 3
    if d[2] == 0:
        return cx * 9, cx * 9 + 9
    return cx * 9 + cz * 3, cx * 9 + cz * 3 + 3


def split3(x):
    hi = x.astype(BF16)
    rest = x - hi.astype(F32)
    mid = rest.astype(BF16)
    low = (rest - mid.astype(F32)).astype(BF16)
    return hi, mid, low


def onehot_rows(dest, base, count):
    rows = lax.broadcasted_iota(I32, (count, dest.shape[1]), 0) + base
    return jnp.where(rows == dest, 1.0, 0.0).astype(BF16)


def scatter_lanes(data, dest, slots):
    rows = data.shape[0]
    parts = jnp.concatenate(split3(data), axis=0)
    out = []
    for base in range(0, slots, 256):
        hot = onehot_rows(dest, base, min(256, slots - base))
        got = lax.dot_general(parts, hot, NT, preferred_element_type=F32)
        out.append(got[0:rows] + got[rows:2 * rows] + got[2 * rows:3 * rows])
    return jnp.concatenate(out, axis=1)


def class_places(code, with_before):
    width = code.shape[1]
    tiles = width // L
    cls = lax.broadcasted_iota(I32, (32, width), 0)
    member = jnp.where(cls == code, 1.0, 0.0)
    member_b = member.astype(BF16)
    stacked = jnp.concatenate([member_b[:, t * L:(t + 1) * L] for t in range(tiles)], axis=0)
    row_i = lax.broadcasted_iota(I32, (L, 256), 0)
    col_i = lax.broadcasted_iota(I32, (L, 256), 1)
    tri = jnp.where((row_i < col_i) | (col_i >= L), 1.0, 0.0).astype(BF16)
    pre = lax.dot_general(stacked, tri, NN, preferred_element_type=F32)
    carry = jnp.zeros((32, L), F32)
    if with_before:
        before_b = jnp.where(code < cls, 1.0, 0.0).astype(BF16)
        before_s = before_b[:, 0:L]
        tot = None
        ones = jnp.ones((L, L), BF16)
        for t in range(tiles):
            part = lax.dot_general(before_b[:, t * L:(t + 1) * L], ones, NN, preferred_element_type=F32)
            tot = part if tot is None else tot + part
        before = tot
        carry = before
    else:
        before = None
    places = []
    for t in range(tiles):
        within = pre[32 * t:32 * t + 32, 0:L] + carry
        places.append(jnp.sum(member[:, t * L:(t + 1) * L] * within, axis=0, keepdims=True))
        carry = carry + pre[32 * t:32 * t + 32, L:256]
    return jnp.concatenate(places, axis=1), before


def pad_lanes(x, width):
    return jnp.concatenate([x, jnp.zeros((x.shape[0], width - x.shape[1]), x.dtype)], axis=1)


def exchange_kernel(sizes, peers, slots, pos_ref, vel_ref, frc_ref, id_ref, ok_ref, side_ref, srt_ref, gh_ref, pkt, rcv, out3, psend, precv, gsend, grecv):
    size_x, size_y, size_z = sizes
    me = (lax.axis_index("x"), lax.axis_index("y"), lax.axis_index("z"))

    def device_at(offset):
        return (lax.rem(me[2] + offset[2], size_z), lax.rem(me[1] + offset[1], size_y), lax.rem(me[0] + offset[0], size_x))

    barrier = pltpu.get_barrier_semaphore()
    for offset in peers:
        pl.semaphore_signal(barrier, inc=1, device_id=device_at(offset), device_id_type=pl.DeviceIdType.MESH)

    n = pos_ref.shape[1]
    side = side_ref[0, 0]
    owned = pad_lanes(ok_ref[...], slots) > 0
    half = vel_ref[...] + (0.5 * DT) * frc_ref[...]
    free = pos_ref[...] + DT * half
    half = pad_lanes(half, slots)
    free = pad_lanes(free, slots)
    ids = pad_lanes(id_ref[...], slots)
    code = jnp.zeros((1, slots), I32)
    moved = []
    low_side = []
    for axis in range(3):
        low = me[axis].astype(F32) * side
        high = (me[axis] + 1).astype(F32) * side
        box = side * float(sizes[axis])
        u = free[axis:axis + 1]
        step = jnp.where(u >= high, 1, 0) - jnp.where(u < low, 1, 0)
        code = code + (step + 1) * (1, 3, 9)[axis]
        moved.append(jnp.where(u < 0.0, u + box, jnp.where(u >= box, u - box, u)))
        low_side.append(low)
    code = jnp.where(owned, code, 31)
    id_hi = (ids >> 16).astype(F32)
    id_lo = (ids & 65535).astype(F32)
    okf = jnp.where(owned, 1.0, 0.0)
    data = jnp.concatenate(moved + [half, id_hi, id_lo, okf, jnp.zeros((7, slots), F32)], axis=0)

    place, _ = class_places(code, False)
    leaving = owned & (code != 13)
    target = jnp.where(leaving, (code - jnp.where(code > 13, 1, 0)) * PACK + place.astype(I32), -1)
    hot = onehot_rows(target, 0, 26 * PACK)
    parts = split3(data)
    got = lax.dot_general(hot, parts[0], NT, preferred_element_type=F32)
    got = got + lax.dot_general(hot, parts[1], NT, preferred_element_type=F32)
    got = got + lax.dot_general(hot, parts[2], NT, preferred_element_type=F32)
    pkt[...] = jnp.concatenate([got, jnp.zeros((26 * PACK, 112), F32)], axis=1)

    pl.semaphore_wait(barrier, len(peers))
    copies = []
    for index, d in enumerate(DIRS):
        offset = (d[0] % size_x, d[1] % size_y, d[2] % size_z)
        copy = pltpu.make_async_remote_copy(
            src_ref=pkt.at[pl.ds(index * PACK, PACK)], dst_ref=rcv.at[pl.ds(index * PACK, PACK)],
            send_sem=psend.at[index], recv_sem=precv.at[index],
            device_id=device_at(offset), device_id_type=pl.DeviceIdType.MESH)
        copy.start()
        copies.append(copy)
    staying = code == 13
    stay_f = jnp.where(staying, 1.0, 0.0)
    for copy in copies:
        copy.wait_recv()

    came = jnp.concatenate([rcv[...], jnp.zeros((256 - 26 * PACK, L), F32)], axis=0)
    came_t = jnp.transpose(came)[0:16]
    valid = jnp.concatenate([staying, came_t[8:9] > 0.5], axis=1)
    cand = jnp.concatenate([data, came_t], axis=1)
    bins = []
    for axis in range(3):
        loc = cand[axis:axis + 1] - low_side[axis]
        bins.append(jnp.where(loc < NEAR, 0, jnp.where(loc > side - NEAR, 2, 1)))
    cx, cy, cz = bins
    orders = [cz * 9 + cy * 3 + cx, cy * 9 + cx * 3 + cz, cx * 9 + cz * 3 + cy]
    lane = lax.broadcasted_iota(I32, (1, slots), 1).astype(F32)
    eye = lax.broadcasted_iota(I32, (32, L), 0) == lax.broadcasted_iota(I32, (32, L), 1)
    cand8 = cand[0:8]
    gcopies = []
    for kind in range(3):
        key = jnp.where(valid, orders[kind], 28)
        place, before = class_places(key, True)
        dest = jnp.where(valid, place.astype(I32), -1)
        arranged = scatter_lanes(cand8, dest, slots)
        total = jnp.concatenate([before[27:28]] * (slots // L), axis=1)
        xyz = jnp.where(lane < total, arranged[0:3], FAR)
        counts = jnp.sum(jnp.where(eye, before, 0.0), axis=0, keepdims=True)
        out3[kind] = jnp.concatenate([xyz, pad_lanes(counts, slots)], axis=0)
        for index, offset in enumerate(peers):
            sign = tuple(0 if c == 0 else 1 for c in offset)
            if order_of(sign) != kind:
                continue
            copy = pltpu.make_async_remote_copy(
                src_ref=out3.at[kind], dst_ref=gh_ref.at[index],
                send_sem=gsend.at[index], recv_sem=grecv.at[index],
                device_id=device_at(offset), device_id_type=pl.DeviceIdType.MESH)
            copy.start()
            gcopies.append(copy)

    arr_ids = came[:, 6:7].astype(I32) * 65536 + came[:, 7:8].astype(I32)
    arr_ok = came[:, 8:9] > 0.5
    row_ids = jnp.concatenate([ids, came_t[6:7].astype(I32) * 65536 + came_t[7:8].astype(I32)], axis=1)
    less = jnp.where((arr_ids < row_ids) & arr_ok, 1.0, 0.0)
    arrivals_below = jnp.sum(less, axis=0, keepdims=True)
    above = jnp.where((arr_ids > row_ids[:, 0:slots]) & staying, 1.0, 0.0).astype(BF16)
    stay_below = lax.dot_general(jnp.ones((16, slots), BF16), above, NT, preferred_element_type=F32)[0:1]
    stay_place, _ = class_places(jnp.where(staying, 0, 31), False)
    rank = jnp.concatenate([stay_place, stay_below], axis=1) + arrivals_below
    dest = jnp.where(valid, rank.astype(I32), -1)
    srt_ref[...] = scatter_lanes(cand, dest, slots)

    for copy in gcopies:
        copy.wait_recv()
    for copy in copies + gcopies:
        copy.wait_send()


def force_kernel(sizes, peers, slots, unroll, srt_ref, gh_ref, offs_ref, side_ref, pos_ref, vel_ref, frc_ref, id_ref, ok_ref, en_ref, rolled, cols, acc):
    size_x, size_y, size_z = sizes
    me = (lax.axis_index("x"), lax.axis_index("y"), lax.axis_index("z"))
    n = pos_ref.shape[1]
    side = side_ref[0, 0]
    tiles = slots // L
    okrow = srt_ref[8:9]
    own = jnp.where(okrow > 0.5, srt_ref[0:3], -FAR)
    count = jnp.sum(okrow).astype(I32)
    wide = side > 2.0 * NEAR

    def put(block, length, start):
        rolled[...] = block

        def one(t, carry):
            tile = rolled[:, pl.ds(pl.multiple_of(t * L, L), L)]
            cols[pl.ds(pl.multiple_of(start + t * L, 8), L), 0:8] = jnp.transpose(tile)
            return carry

        lax.fori_loop(0, (length + 127) // L, one, 0)
        return start + ((length + 7) // 8) * 8

    pad5 = jnp.zeros((5, slots), F32)
    fill = put(jnp.concatenate([jnp.where(okrow > 0.5, srt_ref[0:3], FAR), pad5], axis=0), count, jnp.int32(0))
    for d in DIRS:
        offset = (d[0] % size_x, d[1] % size_y, d[2] % size_z)
        back = ((-offset[0]) % size_x, (-offset[1]) % size_y, (-offset[2]) % size_z)
        index = peers.index(back)
        first, last = range_of(d)
        begin = jnp.where(wide, offs_ref[index, first], 0)
        end = jnp.where(wide, offs_ref[index, last], offs_ref[index, 27])
        shifts = []
        for axis in range(3):
            box = side * float(sizes[axis])
            if d[axis] == 1:
                shifts.append(jnp.where(me[axis] == sizes[axis] - 1, box, 0.0))
            elif d[axis] == -1:
                shifts.append(jnp.where(me[axis] == 0, -box, 0.0))
            else:
                shifts.append(jnp.float32(0.0))
        block = jnp.concatenate([gh_ref[index, a:a + 1] + shifts[a] for a in range(3)] + [pad5], axis=0)
        block = pltpu.roll(block, lax.rem(slots - begin, slots), 1)
        fill = put(block, end - begin, fill)
    cols[pl.ds(pl.multiple_of(fill, 8), 8 * unroll), 0:8] = jnp.full((8 * unroll, 8), FAR, F32)
    steps = (fill // 8 + unroll - 1) // unroll

    def sweep(used):
        ox, oy, oz = [[jnp.broadcast_to(own[a:a + 1, t * L:t * L + L], (8, L)) for t in range(used)] for a in range(3)]

        def body(i, carry):
            fx, fy, fz, en = [list(c) for c in carry]
            for u in range(unroll):
                col = cols[pl.ds(pl.multiple_of((i * unroll + u) * 8, 8), 8), :]
                gx = jnp.broadcast_to(col[:, 0:1], (8, L))
                gy = jnp.broadcast_to(col[:, 1:2], (8, L))
                gz = jnp.broadcast_to(col[:, 2:3], (8, L))
                for t in range(used):
                    dx = ox[t] - gx
                    dy = oy[t] - gy
                    dz = oz[t] - gz
                    d2 = dx * dx + dy * dy + dz * dz
                    near = (d2 < RC * RC) & (d2 > 0.0)
                    inv = lax.rsqrt(d2)
                    inv2 = inv * inv
                    inv6 = inv2 * inv2 * inv2
                    scale = jnp.where(near, (48.0 * inv6 - 24.0) * inv6 * inv2 + UPC * inv, 0.0)
                    pair = jnp.where(near, (4.0 * inv6 - 4.0) * inv6 + (RC * UPC - UCUT) - UPC * (d2 * inv), 0.0)
                    fx[t] = fx[t] + scale * dx
                    fy[t] = fy[t] + scale * dy
                    fz[t] = fz[t] + scale * dz
                    en[t] = en[t] + pair
            return tuple(fx), tuple(fy), tuple(fz), tuple(en)

        zero = tuple(jnp.zeros((8, L), F32) for _ in range(used))
        sums = lax.fori_loop(0, steps, body, (zero,) * 4)
        for a in range(4):
            for t in range(used):
                acc[a:a + 1, t * L:t * L + L] = jnp.sum(sums[a][t], axis=0, keepdims=True)

    acc[...] = jnp.zeros_like(acc)
    need = (count + 127) // L
    for used in range(1, tiles + 1):
        if used <= 3:
            if used == 3:
                pl.when(need <= 3)(functools.partial(sweep, used))
        else:
            pl.when(need == used)(functools.partial(sweep, used))

    force = acc[0:3] * okrow
    pos_ref[...] = srt_ref[0:3, 0:n]
    frc_ref[...] = force[:, 0:n]
    vel_ref[...] = ((srt_ref[3:6] + (0.5 * DT) * force) * okrow)[:, 0:n]
    id_ref[...] = (srt_ref[6:7].astype(I32) * 65536 + srt_ref[7:8].astype(I32))[:, 0:n]
    ok_ref[...] = okrow[:, 0:n].astype(I32)
    en_ref[0, 0] = 0.5 * jnp.sum(acc[3:4] * okrow)


def solution(mesh):
    sizes = (mesh.shape["x"], mesh.shape["y"], mesh.shape["z"])
    peers = sorted({(d[0] % sizes[0], d[1] % sizes[1], d[2] % sizes[2]) for d in DIRS} - {(0, 0, 0)})
    unroll = 2

    def local_step(atom_pos, atom_vel, atom_frc, atom_id, atom_ok, brick_side):
        n = atom_pos.shape[0]
        slots = -(-n // L) * L
        side = jnp.reshape(brick_side, (1, 1))
        vmem = pl.BlockSpec(memory_space=pltpu.VMEM)
        smem = pl.BlockSpec(memory_space=pltpu.SMEM)
        srt, ghosts = pl.pallas_call(
            functools.partial(exchange_kernel, sizes, peers, slots),
            out_shape=(jax.ShapeDtypeStruct((16, slots), F32), jax.ShapeDtypeStruct((len(peers), 4, slots), F32)),
            in_specs=[vmem] * 5 + [smem],
            out_specs=(vmem, vmem),
            scratch_shapes=[
                pltpu.VMEM((26 * PACK, L), F32), pltpu.VMEM((26 * PACK, L), F32), pltpu.VMEM((3, 4, slots), F32),
                pltpu.SemaphoreType.DMA((26,)), pltpu.SemaphoreType.DMA((26,)),
                pltpu.SemaphoreType.DMA((len(peers),)), pltpu.SemaphoreType.DMA((len(peers),)),
            ],
            compiler_params=pltpu.CompilerParams(collective_id=0, has_side_effects=True, vmem_limit_bytes=40 * 2 ** 20),
            name="exchange",
        )(atom_pos.T, atom_vel.T, atom_frc.T, atom_id[None, :], atom_ok[None, :], side)
        offs = ghosts[:, 3, 0:32].astype(I32)
        out_f = jax.ShapeDtypeStruct((3, n), F32)
        out_i = jax.ShapeDtypeStruct((1, n), I32)
        new_pos, new_vel, new_frc, new_id, new_ok, energy = pl.pallas_call(
            functools.partial(force_kernel, sizes, peers, slots, unroll),
            out_shape=(out_f, out_f, out_f, out_i, out_i, jax.ShapeDtypeStruct((1, 1), F32)),
            in_specs=[vmem, vmem, smem, smem],
            out_specs=(vmem, vmem, vmem, vmem, vmem, smem),
            scratch_shapes=[pltpu.VMEM((8, slots), F32), pltpu.VMEM((27 * slots + L + 8 * unroll, L), F32), pltpu.VMEM((4, slots), F32)],
            compiler_params=pltpu.CompilerParams(vmem_limit_bytes=40 * 2 ** 20),
            name="forces",
        )(srt, ghosts, offs, side)
        energy = lax.psum(energy[0, 0], MESH_AXES)
        return new_pos.T, new_vel.T, new_frc.T, new_id[0], new_ok[0], energy

    row_spec = P(MESH_AXES, None)
    id_spec = P(MESH_AXES)
    return jax.shard_map(local_step, mesh=mesh, in_specs=(row_spec, row_spec, row_spec, id_spec, id_spec, P()), out_specs=(row_spec, row_spec, row_spec, id_spec, id_spec, P()), check_vma=False)
```

```python
import functools

import jax
import jax.numpy as jnp
from jax import lax
from jax.experimental import pallas as pl
from jax.experimental.pallas import tpu as pltpu
from jax.sharding import PartitionSpec as P

DT = 0.005
RC = 2.5
FAR = 1.0e6
UCUT = 4.0 * (RC ** -12 - RC ** -6)
UPC = -48.0 * RC ** -13 + 24.0 * RC ** -7
MESH_AXES = ("z", "y", "x")
DIRS = [(dx, dy, dz) for dz in (-1, 0, 1) for dy in (-1, 0, 1) for dx in (-1, 0, 1) if (dx, dy, dz) != (0, 0, 0)]
NEAR = RC + 1.0e-3
PACK = 8
L = 128
F32 = jnp.float32
BF16 = jnp.bfloat16
I32 = jnp.int32
NT = (((1,), (1,)), ((), ()))
NN = (((1,), (0,)), ((), ()))


def order_of(d):
    if d[2] == 0:
        return 1 if d[1] != 0 else 2
    return 2 if (d[1] == 0 and d[0] != 0) else 0


def range_of(d):
    cx, cy, cz = [(1, 0, 2)[c] for c in (d[0], d[1], d[2])]
    kind = order_of(d)
    if kind == 0:
        if d[0] == 0 and d[1] == 0:
            return cz * 9, cz * 9 + 9
        if d[0] == 0:
            return cz * 9 + cy * 3, cz * 9 + cy * 3 + 3
        return cz * 9 + cy * 3 + cx, cz * 9 + cy * 3 + cx + 1
    if kind == 1:
        if d[0] == 0:
            return cy * 9, cy * 9 + 9
        return cy * 9 + cx * 3, cy * 9 + cx * 3 + 3
    if d[2] == 0:
        return cx * 9, cx * 9 + 9
    return cx * 9 + cz * 3, cx * 9 + cz * 3 + 3


def split3(x):
    hi = x.astype(BF16)
    rest = x - hi.astype(F32)
    mid = rest.astype(BF16)
    low = (rest - mid.astype(F32)).astype(BF16)
    return hi, mid, low


def onehot_rows(dest, base, count):
    rows = lax.broadcasted_iota(I32, (count, dest.shape[1]), 0) + base
    return jnp.where(rows == dest, 1.0, 0.0).astype(BF16)


def scatter_lanes(data, dest, slots):
    rows = data.shape[0]
    parts = jnp.concatenate(split3(data), axis=0)
    out = []
    for base in range(0, slots, 256):
        hot = onehot_rows(dest, base, min(256, slots - base))
        got = lax.dot_general(parts, hot, NT, preferred_element_type=F32)
        out.append(got[0:rows] + got[rows:2 * rows] + got[2 * rows:3 * rows])
    return jnp.concatenate(out, axis=1)


def class_places(code, with_before):
    width = code.shape[1]
    tiles = width // L
    cls = lax.broadcasted_iota(I32, (32, width), 0)
    member = jnp.where(cls == code, 1.0, 0.0)
    member_b = member.astype(BF16)
    stacked = jnp.concatenate([member_b[:, t * L:(t + 1) * L] for t in range(tiles)], axis=0)
    row_i = lax.broadcasted_iota(I32, (L, 256), 0)
    col_i = lax.broadcasted_iota(I32, (L, 256), 1)
    tri = jnp.where((row_i < col_i) | (col_i >= L), 1.0, 0.0).astype(BF16)
    pre = lax.dot_general(stacked, tri, NN, preferred_element_type=F32)
    carry = jnp.zeros((32, L), F32)
    if with_before:
        before_b = jnp.where(code < cls, 1.0, 0.0).astype(BF16)
        before_s = before_b[:, 0:L]
        tot = None
        ones = jnp.ones((L, L), BF16)
        for t in range(tiles):
            part = lax.dot_general(before_b[:, t * L:(t + 1) * L], ones, NN, preferred_element_type=F32)
            tot = part if tot is None else tot + part
        before = tot
        carry = before
    else:
        before = None
    places = []
    for t in range(tiles):
        within = pre[32 * t:32 * t + 32, 0:L] + carry
        places.append(jnp.sum(member[:, t * L:(t + 1) * L] * within, axis=0, keepdims=True))
        carry = carry + pre[32 * t:32 * t + 32, L:256]
    return jnp.concatenate(places, axis=1), before


def pad_lanes(x, width):
    return jnp.concatenate([x, jnp.zeros((x.shape[0], width - x.shape[1]), x.dtype)], axis=1)


def exchange_kernel(sizes, peers, slots, pos_ref, vel_ref, frc_ref, id_ref, ok_ref, side_ref, srt_ref, gh_ref, pkt, rcv, out3, psend, precv, gsend, grecv):
    size_x, size_y, size_z = sizes
    me = (lax.axis_index("x"), lax.axis_index("y"), lax.axis_index("z"))

    def device_at(offset):
        return (lax.rem(me[2] + offset[2], size_z), lax.rem(me[1] + offset[1], size_y), lax.rem(me[0] + offset[0], size_x))

    barrier = pltpu.get_barrier_semaphore()
    for offset in peers:
        pl.semaphore_signal(barrier, inc=1, device_id=device_at(offset), device_id_type=pl.DeviceIdType.MESH)

    n = pos_ref.shape[1]
    side = side_ref[0, 0]
    owned = pad_lanes(ok_ref[...], slots) > 0
    half = vel_ref[...] + (0.5 * DT) * frc_ref[...]
    free = pos_ref[...] + DT * half
    half = pad_lanes(half, slots)
    free = pad_lanes(free, slots)
    ids = pad_lanes(id_ref[...], slots)
    code = jnp.zeros((1, slots), I32)
    moved = []
    low_side = []
    for axis in range(3):
        low = me[axis].astype(F32) * side
        high = (me[axis] + 1).astype(F32) * side
        box = side * float(sizes[axis])
        u = free[axis:axis + 1]
        step = jnp.where(u >= high, 1, 0) - jnp.where(u < low, 1, 0)
        code = code + (step + 1) * (1, 3, 9)[axis]
        moved.append(jnp.where(u < 0.0, u + box, jnp.where(u >= box, u - box, u)))
        low_side.append(low)
    code = jnp.where(owned, code, 31)
    id_hi = (ids >> 16).astype(F32)
    id_lo = (ids & 65535).astype(F32)
    okf = jnp.where(owned, 1.0, 0.0)
    data = jnp.concatenate(moved + [half, id_hi, id_lo, okf, jnp.zeros((7, slots), F32)], axis=0)

    place, _ = class_places(code, False)
    leaving = owned & (code != 13)
    target = jnp.where(leaving, (code - jnp.where(code > 13, 1, 0)) * PACK + place.astype(I32), -1)
    hot = onehot_rows(target, 0, 26 * PACK)
    parts = split3(data)
    got = lax.dot_general(hot, parts[0], NT, preferred_element_type=F32)
    got = got + lax.dot_general(hot, parts[1], NT, preferred_element_type=F32)
    got = got + lax.dot_general(hot, parts[2], NT, preferred_element_type=F32)
    pkt[...] = jnp.concatenate([got, jnp.zeros((26 * PACK, 112), F32)], axis=1)

    pl.semaphore_wait(barrier, len(peers))
    copies = []
    for index, d in enumerate(DIRS):
        offset = (d[0] % size_x, d[1] % size_y, d[2] % size_z)
        copy = pltpu.make_async_remote_copy(
            src_ref=pkt.at[pl.ds(index * PACK, PACK)], dst_ref=rcv.at[pl.ds(index * PACK, PACK)],
            send_sem=psend.at[index], recv_sem=precv.at[index],
            device_id=device_at(offset), device_id_type=pl.DeviceIdType.MESH)
        copy.start()
        copies.append(copy)
    staying = code == 13
    stay_f = jnp.where(staying, 1.0, 0.0)
    for copy in copies:
        copy.wait_recv()

    came = jnp.concatenate([rcv[...], jnp.zeros((256 - 26 * PACK, L), F32)], axis=0)
    came_t = jnp.transpose(came)[0:16]
    valid = jnp.concatenate([staying, came_t[8:9] > 0.5], axis=1)
    cand = jnp.concatenate([data, came_t], axis=1)
    bins = []
    for axis in range(3):
        loc = cand[axis:axis + 1] - low_side[axis]
        bins.append(jnp.where(loc < NEAR, 0, jnp.where(loc > side - NEAR, 2, 1)))
    cx, cy, cz = bins
    orders = [cz * 9 + cy * 3 + cx, cy * 9 + cx * 3 + cz, cx * 9 + cz * 3 + cy]
    lane = lax.broadcasted_iota(I32, (1, slots), 1).astype(F32)
    eye = lax.broadcasted_iota(I32, (32, L), 0) == lax.broadcasted_iota(I32, (32, L), 1)
    cand8 = cand[0:8]
    gcopies = []
    for kind in range(3):
        key = jnp.where(valid, orders[kind], 28)
        place, before = class_places(key, True)
        dest = jnp.where(valid, place.astype(I32), -1)
        arranged = scatter_lanes(cand8, dest, slots)
        total = jnp.concatenate([before[27:28]] * (slots // L), axis=1)
        xyz = jnp.where(lane < total, arranged[0:3], FAR)
        counts = jnp.sum(jnp.where(eye, before, 0.0), axis=0, keepdims=True)
        out3[kind] = jnp.concatenate([xyz, pad_lanes(counts, slots)], axis=0)
        for index, offset in enumerate(peers):
            sign = tuple(0 if c == 0 else 1 for c in offset)
            if order_of(sign) != kind:
                continue
            copy = pltpu.make_async_remote_copy(
                src_ref=out3.at[kind], dst_ref=gh_ref.at[index],
                send_sem=gsend.at[index], recv_sem=grecv.at[index],
                device_id=device_at(offset), device_id_type=pl.DeviceIdType.MESH)
            copy.start()
            gcopies.append(copy)

    arr_ids = came[:, 6:7].astype(I32) * 65536 + came[:, 7:8].astype(I32)
    arr_ok = came[:, 8:9] > 0.5
    row_ids = jnp.concatenate([ids, came_t[6:7].astype(I32) * 65536 + came_t[7:8].astype(I32)], axis=1)
    less = jnp.where((arr_ids < row_ids) & arr_ok, 1.0, 0.0)
    arrivals_below = jnp.sum(less, axis=0, keepdims=True)
    above = jnp.where((arr_ids > row_ids[:, 0:slots]) & staying, 1.0, 0.0).astype(BF16)
    stay_below = lax.dot_general(jnp.ones((16, slots), BF16), above, NT, preferred_element_type=F32)[0:1]
    stay_place, _ = class_places(jnp.where(staying, 0, 31), False)
    rank = jnp.concatenate([stay_place, stay_below], axis=1) + arrivals_below
    dest = jnp.where(valid, rank.astype(I32), -1)
    srt_ref[...] = scatter_lanes(cand, dest, slots)

    for copy in gcopies:
        copy.wait_recv()
    for copy in copies + gcopies:
        copy.wait_send()


def force_kernel(sizes, peers, slots, unroll, srt_ref, gh_ref, offs_ref, side_ref, pos_ref, vel_ref, frc_ref, id_ref, ok_ref, en_ref, rolled, cols, acc):
    size_x, size_y, size_z = sizes
    me = (lax.axis_index("x"), lax.axis_index("y"), lax.axis_index("z"))
    n = pos_ref.shape[1]
    side = side_ref[0, 0]
    tiles = slots // L
    okrow = srt_ref[8:9]
    own = jnp.where(okrow > 0.5, srt_ref[0:3], -FAR)
    count = jnp.sum(okrow).astype(I32)
    wide = side > 2.0 * NEAR

    def put(block, length, start):
        rolled[...] = block

        def one(t, carry):
            tile = rolled[:, pl.ds(pl.multiple_of(t * L, L), L)]
            cols[pl.ds(pl.multiple_of(start + t * L, 8), L), 0:8] = jnp.transpose(tile)
            return carry

        lax.fori_loop(0, (length + 127) // L, one, 0)
        return start + ((length + 7) // 8) * 8

    pad5 = jnp.zeros((5, slots), F32)
    fill = put(jnp.concatenate([jnp.where(okrow > 0.5, srt_ref[0:3], FAR), pad5], axis=0), count, jnp.int32(0))
    spare = jnp.full((8 * unroll, 8), FAR, F32)
    cols[pl.ds(pl.multiple_of(fill, 8), 8 * unroll), 0:8] = spare
    self_steps = (fill // 8 + unroll - 1) // unroll
    fill = self_steps * (8 * unroll)
    for d in DIRS:
        offset = (d[0] % size_x, d[1] % size_y, d[2] % size_z)
        back = ((-offset[0]) % size_x, (-offset[1]) % size_y, (-offset[2]) % size_z)
        index = peers.index(back)
        first, last = range_of(d)
        begin = jnp.where(wide, offs_ref[index, first], 0)
        end = jnp.where(wide, offs_ref[index, last], offs_ref[index, 27])
        shifts = []
        for axis in range(3):
            box = side * float(sizes[axis])
            if d[axis] == 1:
                shifts.append(jnp.where(me[axis] == sizes[axis] - 1, box, 0.0))
            elif d[axis] == -1:
                shifts.append(jnp.where(me[axis] == 0, -box, 0.0))
            else:
                shifts.append(jnp.float32(0.0))
        block = jnp.concatenate([gh_ref[index, a:a + 1] + shifts[a] for a in range(3)] + [pad5], axis=0)
        block = pltpu.roll(block, lax.rem(slots - begin, slots), 1)
        fill = put(block, end - begin, fill)
    cols[pl.ds(pl.multiple_of(fill, 8), 8 * unroll), 0:8] = spare
    steps = (fill // 8 + unroll - 1) // unroll

    def sweep(used):
        ox, oy, oz = [[jnp.broadcast_to(own[a:a + 1, t * L:t * L + L], (8, L)) for t in range(used)] for a in range(3)]

        def body(with_self, i, carry):
            fx, fy, fz, en = list(carry[0]), list(carry[1]), list(carry[2]), carry[3]
            for u in range(unroll):
                col = cols[pl.ds(pl.multiple_of((i * unroll + u) * 8, 8), 8), :]
                gx, gy, gz = [jnp.broadcast_to(col[:, a:a + 1], (8, L)) for a in range(3)]
                for t in range(used):
                    dx = ox[t] - gx
                    dy = oy[t] - gy
                    dz = oz[t] - gz
                    d2 = dx * dx + dy * dy + dz * dz
                    near = d2 < RC * RC
                    if with_self:
                        near = near & (d2 > 0.0)
                    inv = jnp.where(near, lax.rsqrt(d2), 0.0)
                    s2 = inv * inv
                    s6 = s2 * s2 * s2
                    s12 = s6 * s6
                    p = s12 - s6
                    w = inv * (UPC / 24.0)
                    scale = (p + s12) * s2 + w
                    en = en + ((p + jnp.where(near, 0.25 * (RC * UPC - UCUT), 0.0)) - 6.0 * (w * d2))
                    fx[t] = fx[t] + scale * dx
                    fy[t] = fy[t] + scale * dy
                    fz[t] = fz[t] + scale * dz
            return tuple(fx), tuple(fy), tuple(fz), en

        zero = jnp.zeros((8, L), F32)
        sums = lax.fori_loop(0, self_steps, functools.partial(body, True), ((zero,) * used,) * 3 + (zero,))
        sums = lax.fori_loop(self_steps, steps, functools.partial(body, False), sums)
        for a in range(3):
            for t in range(used):
                acc[a:a + 1, t * L:t * L + L] = 24.0 * jnp.sum(sums[a][t], axis=0, keepdims=True)
        en_ref[...] = 2.0 * jnp.sum(sums[3], axis=0, keepdims=True)

    acc[...] = jnp.zeros_like(acc)
    need = (count + L - 1) // L
    pl.when(need <= 3)(functools.partial(sweep, min(3, tiles)))
    for used in range(4, tiles + 1):
        pl.when(need == used)(functools.partial(sweep, used))

    force = acc[0:3] * okrow
    pos_ref[...] = srt_ref[0:3, 0:n]
    frc_ref[...] = force[:, 0:n]
    vel_ref[...] = ((srt_ref[3:6] + (0.5 * DT) * force) * okrow)[:, 0:n]
    id_ref[...] = (srt_ref[6:7].astype(I32) * 65536 + srt_ref[7:8].astype(I32))[:, 0:n]
    ok_ref[...] = okrow[:, 0:n].astype(I32)


def total_kernel(sizes, part_ref, sum_ref, rows, ssem, rsem):
    size_x, size_y, size_z = sizes
    me = (lax.axis_index("x"), lax.axis_index("y"), lax.axis_index("z"))
    mine = (me[2] * size_y + me[1]) * size_x + me[0]
    others = [(dx, dy, dz) for dz in range(size_z) for dy in range(size_y) for dx in range(size_x) if dx + dy + dz > 0]

    def device_at(offset):
        return (lax.rem(me[2] + offset[2], size_z), lax.rem(me[1] + offset[1], size_y), lax.rem(me[0] + offset[0], size_x))

    barrier = pltpu.get_barrier_semaphore()
    for offset in others:
        pl.semaphore_signal(barrier, inc=1, device_id=device_at(offset), device_id_type=pl.DeviceIdType.MESH)
    rows[pl.ds(mine, 1)] = part_ref[...]
    pl.semaphore_wait(barrier, len(others))
    copies = []
    for index, offset in enumerate(others):
        copy = pltpu.make_async_remote_copy(
            src_ref=part_ref, dst_ref=rows.at[pl.ds(mine, 1)], send_sem=ssem.at[index], recv_sem=rsem.at[index],
            device_id=device_at(offset), device_id_type=pl.DeviceIdType.MESH)
        copy.start()
        copies.append(copy)
    for copy in copies:
        copy.wait_recv()
    sum_ref[0, 0] = jnp.sum(rows[...])
    for copy in copies:
        copy.wait_send()


def solution(mesh):
    sizes = (mesh.shape["x"], mesh.shape["y"], mesh.shape["z"])
    peers = sorted({(d[0] % sizes[0], d[1] % sizes[1], d[2] % sizes[2]) for d in DIRS} - {(0, 0, 0)})
    devices = sizes[0] * sizes[1] * sizes[2]
    unroll = 2

    def local_step(atom_pos, atom_vel, atom_frc, atom_id, atom_ok, brick_side):
        n = atom_pos.shape[0]
        slots = -(-n // L) * L
        side = jnp.reshape(brick_side, (1, 1))
        vmem = pl.BlockSpec(memory_space=pltpu.VMEM)
        smem = pl.BlockSpec(memory_space=pltpu.SMEM)
        srt, ghosts = pl.pallas_call(
            functools.partial(exchange_kernel, sizes, peers, slots),
            out_shape=(jax.ShapeDtypeStruct((16, slots), F32), jax.ShapeDtypeStruct((len(peers), 4, slots), F32)),
            in_specs=[vmem] * 5 + [smem],
            out_specs=(vmem, vmem),
            scratch_shapes=[
                pltpu.VMEM((26 * PACK, L), F32), pltpu.VMEM((26 * PACK, L), F32), pltpu.VMEM((3, 4, slots), F32),
                pltpu.SemaphoreType.DMA((26,)), pltpu.SemaphoreType.DMA((26,)),
                pltpu.SemaphoreType.DMA((len(peers),)), pltpu.SemaphoreType.DMA((len(peers),)),
            ],
            compiler_params=pltpu.CompilerParams(collective_id=0, has_side_effects=True, vmem_limit_bytes=40 * 2 ** 20),
            name="exchange",
        )(atom_pos.T, atom_vel.T, atom_frc.T, atom_id[None, :], atom_ok[None, :], side)
        offs = ghosts[:, 3, 0:32].astype(I32)
        out_f = jax.ShapeDtypeStruct((3, n), F32)
        out_i = jax.ShapeDtypeStruct((1, n), I32)
        new_pos, new_vel, new_frc, new_id, new_ok, energy = pl.pallas_call(
            functools.partial(force_kernel, sizes, peers, slots, unroll),
            out_shape=(out_f, out_f, out_f, out_i, out_i, jax.ShapeDtypeStruct((1, L), F32)),
            in_specs=[vmem, vmem, smem, smem],
            out_specs=(vmem,) * 6,
            scratch_shapes=[pltpu.VMEM((8, slots), F32), pltpu.VMEM((27 * slots + L + 8 * unroll, L), F32), pltpu.VMEM((3, slots), F32)],
            compiler_params=pltpu.CompilerParams(vmem_limit_bytes=40 * 2 ** 20),
            name="forces",
        )(srt, ghosts, offs, side)
        energy = pl.pallas_call(
            functools.partial(total_kernel, sizes),
            out_shape=jax.ShapeDtypeStruct((1, 1), F32),
            in_specs=[vmem],
            out_specs=smem,
            scratch_shapes=[pltpu.VMEM((devices, L), F32), pltpu.SemaphoreType.DMA((devices,)), pltpu.SemaphoreType.DMA((devices,))],
            compiler_params=pltpu.CompilerParams(collective_id=1, has_side_effects=True),
            name="total",
        )(energy)[0, 0]
        return new_pos.T, new_vel.T, new_frc.T, new_id[0], new_ok[0], energy

    row_spec = P(MESH_AXES, None)
    id_spec = P(MESH_AXES)
    return jax.shard_map(local_step, mesh=mesh, in_specs=(row_spec, row_spec, row_spec, id_spec, id_spec, P()), out_specs=(row_spec, row_spec, row_spec, id_spec, id_spec, P()), check_vma=False)
```

```python
import functools

import jax
import jax.numpy as jnp
from jax import lax
from jax.experimental import pallas as pl
from jax.experimental.pallas import tpu as pltpu
from jax.sharding import PartitionSpec as P

DT = 0.005
RC = 2.5
FAR = 1.0e6
UCUT = 4.0 * (RC ** -12 - RC ** -6)
UPC = -48.0 * RC ** -13 + 24.0 * RC ** -7
MESH_AXES = ("z", "y", "x")
DIRS = [(dx, dy, dz) for dz in (-1, 0, 1) for dy in (-1, 0, 1) for dx in (-1, 0, 1) if (dx, dy, dz) != (0, 0, 0)]
NEAR = RC + 1.0e-3
PACK = 8
CHUNK = 4
GROUPS = 4
L = 128
F32 = jnp.float32
BF16 = jnp.bfloat16
I32 = jnp.int32
NT = (((1,), (1,)), ((), ()))
NN = (((1,), (0,)), ((), ()))


def order_of(d):
    if d[2] == 0:
        return 1 if d[1] != 0 else 2
    return 2 if (d[1] == 0 and d[0] != 0) else 0


def range_of(d):
    cx, cy, cz = [(1, 0, 2)[c] for c in (d[0], d[1], d[2])]
    kind = order_of(d)
    if kind == 0:
        if d[0] == 0 and d[1] == 0:
            return cz * 9, cz * 9 + 9
        if d[0] == 0:
            return cz * 9 + cy * 3, cz * 9 + cy * 3 + 3
        return cz * 9 + cy * 3 + cx, cz * 9 + cy * 3 + cx + 1
    if kind == 1:
        if d[0] == 0:
            return cy * 9, cy * 9 + 9
        return cy * 9 + cx * 3, cy * 9 + cx * 3 + 3
    if d[2] == 0:
        return cx * 9, cx * 9 + 9
    return cx * 9 + cz * 3, cx * 9 + cz * 3 + 3


def split3(x):
    hi = x.astype(BF16)
    rest = x - hi.astype(F32)
    mid = rest.astype(BF16)
    low = (rest - mid.astype(F32)).astype(BF16)
    return hi, mid, low


def onehot_rows(dest, base, count):
    rows = lax.broadcasted_iota(I32, (count, dest.shape[1]), 0) + base
    return jnp.where(rows == dest, 1.0, 0.0).astype(BF16)


def scatter_lanes(data, dest, slots):
    rows = data.shape[0]
    parts = jnp.concatenate(split3(data), axis=0)
    out = []
    for base in range(0, slots, 256):
        hot = onehot_rows(dest, base, min(256, slots - base))
        got = lax.dot_general(parts, hot, NT, preferred_element_type=F32)
        out.append(got[0:rows] + got[rows:2 * rows] + got[2 * rows:3 * rows])
    return jnp.concatenate(out, axis=1)


def class_places(code, with_before):
    width = code.shape[1]
    tiles = width // L
    cls = lax.broadcasted_iota(I32, (32, width), 0)
    member = jnp.where(cls == code, 1.0, 0.0)
    member_b = member.astype(BF16)
    stacked = jnp.concatenate([member_b[:, t * L:(t + 1) * L] for t in range(tiles)], axis=0)
    row_i = lax.broadcasted_iota(I32, (L, 256), 0)
    col_i = lax.broadcasted_iota(I32, (L, 256), 1)
    tri = jnp.where((row_i < col_i) | (col_i >= L), 1.0, 0.0).astype(BF16)
    pre = lax.dot_general(stacked, tri, NN, preferred_element_type=F32)
    carry = jnp.zeros((32, L), F32)
    if with_before:
        before_b = jnp.where(code < cls, 1.0, 0.0).astype(BF16)
        before_s = before_b[:, 0:L]
        tot = None
        ones = jnp.ones((L, L), BF16)
        for t in range(tiles):
            part = lax.dot_general(before_b[:, t * L:(t + 1) * L], ones, NN, preferred_element_type=F32)
            tot = part if tot is None else tot + part
        before = tot
        carry = before
    else:
        before = None
    places = []
    for t in range(tiles):
        within = pre[32 * t:32 * t + 32, 0:L] + carry
        places.append(jnp.sum(member[:, t * L:(t + 1) * L] * within, axis=0, keepdims=True))
        carry = carry + pre[32 * t:32 * t + 32, L:256]
    return jnp.concatenate(places, axis=1), before


def pad_lanes(x, width):
    return jnp.concatenate([x, jnp.zeros((x.shape[0], width - x.shape[1]), x.dtype)], axis=1)


def exchange_kernel(sizes, peers, slots, pos_ref, vel_ref, frc_ref, id_ref, ok_ref, side_ref, srt_ref, gh_ref, pkt, rcv, out3, psend, precv, gsend, grecv):
    size_x, size_y, size_z = sizes
    me = (lax.axis_index("x"), lax.axis_index("y"), lax.axis_index("z"))

    def device_at(offset):
        return (lax.rem(me[2] + offset[2], size_z), lax.rem(me[1] + offset[1], size_y), lax.rem(me[0] + offset[0], size_x))

    barrier = pltpu.get_barrier_semaphore()
    for offset in peers:
        pl.semaphore_signal(barrier, inc=1, device_id=device_at(offset), device_id_type=pl.DeviceIdType.MESH)

    n = pos_ref.shape[1]
    side = side_ref[0, 0]
    owned = pad_lanes(ok_ref[...], slots) > 0
    half = vel_ref[...] + (0.5 * DT) * frc_ref[...]
    free = pos_ref[...] + DT * half
    half = pad_lanes(half, slots)
    free = pad_lanes(free, slots)
    ids = pad_lanes(id_ref[...], slots)
    code = jnp.zeros((1, slots), I32)
    moved = []
    low_side = []
    for axis in range(3):
        low = me[axis].astype(F32) * side
        high = (me[axis] + 1).astype(F32) * side
        box = side * float(sizes[axis])
        u = free[axis:axis + 1]
        step = jnp.where(u >= high, 1, 0) - jnp.where(u < low, 1, 0)
        code = code + (step + 1) * (1, 3, 9)[axis]
        moved.append(jnp.where(u < 0.0, u + box, jnp.where(u >= box, u - box, u)))
        low_side.append(low)
    code = jnp.where(owned, code, 31)
    id_hi = (ids >> 16).astype(F32)
    id_lo = (ids & 65535).astype(F32)
    okf = jnp.where(owned, 1.0, 0.0)
    data = jnp.concatenate(moved + [half, id_hi, id_lo, okf, jnp.zeros((7, slots), F32)], axis=0)

    place, _ = class_places(code, False)
    leaving = owned & (code != 13)
    target = jnp.where(leaving, (code - jnp.where(code > 13, 1, 0)) * PACK + place.astype(I32), -1)
    hot = onehot_rows(target, 0, 26 * PACK)
    parts = split3(data)
    got = lax.dot_general(hot, parts[0], NT, preferred_element_type=F32)
    got = got + lax.dot_general(hot, parts[1], NT, preferred_element_type=F32)
    got = got + lax.dot_general(hot, parts[2], NT, preferred_element_type=F32)
    pkt[...] = jnp.concatenate([got, jnp.zeros((26 * PACK, 112), F32)], axis=1)

    pl.semaphore_wait(barrier, len(peers))
    copies = []
    for index, d in enumerate(DIRS):
        offset = (d[0] % size_x, d[1] % size_y, d[2] % size_z)
        copy = pltpu.make_async_remote_copy(
            src_ref=pkt.at[pl.ds(index * PACK, PACK)], dst_ref=rcv.at[pl.ds(index * PACK, PACK)],
            send_sem=psend.at[index], recv_sem=precv.at[index],
            device_id=device_at(offset), device_id_type=pl.DeviceIdType.MESH)
        copy.start()
        copies.append(copy)
    staying = code == 13
    stay_f = jnp.where(staying, 1.0, 0.0)
    for copy in copies:
        copy.wait_recv()

    came = jnp.concatenate([rcv[...], jnp.zeros((256 - 26 * PACK, L), F32)], axis=0)
    came_t = jnp.transpose(came)[0:16]
    valid = jnp.concatenate([staying, came_t[8:9] > 0.5], axis=1)
    cand = jnp.concatenate([data, came_t], axis=1)
    bins = []
    for axis in range(3):
        loc = cand[axis:axis + 1] - low_side[axis]
        bins.append(jnp.where(loc < NEAR, 0, jnp.where(loc > side - NEAR, 2, 1)))
    cx, cy, cz = bins
    orders = [cz * 9 + cy * 3 + cx, cy * 9 + cx * 3 + cz, cx * 9 + cz * 3 + cy]
    lane = lax.broadcasted_iota(I32, (1, slots), 1).astype(F32)
    eye = lax.broadcasted_iota(I32, (32, L), 0) == lax.broadcasted_iota(I32, (32, L), 1)
    cand8 = cand[0:8]
    gcopies = []
    for kind in range(3):
        key = jnp.where(valid, orders[kind], 28)
        place, before = class_places(key, True)
        dest = jnp.where(valid, place.astype(I32), -1)
        arranged = scatter_lanes(cand8, dest, slots)
        total = jnp.concatenate([before[27:28]] * (slots // L), axis=1)
        xyz = jnp.where(lane < total, arranged[0:3], FAR)
        counts = jnp.sum(jnp.where(eye, before, 0.0), axis=0, keepdims=True)
        out3[kind] = jnp.concatenate([xyz, pad_lanes(counts, slots)], axis=0)
        for index, offset in enumerate(peers):
            sign = tuple(0 if c == 0 else 1 for c in offset)
            if order_of(sign) != kind:
                continue
            copy = pltpu.make_async_remote_copy(
                src_ref=out3.at[kind], dst_ref=gh_ref.at[index],
                send_sem=gsend.at[index], recv_sem=grecv.at[index],
                device_id=device_at(offset), device_id_type=pl.DeviceIdType.MESH)
            copy.start()
            gcopies.append(copy)

    arr_ids = came[:, 6:7].astype(I32) * 65536 + came[:, 7:8].astype(I32)
    arr_ok = came[:, 8:9] > 0.5
    row_ids = jnp.concatenate([ids, came_t[6:7].astype(I32) * 65536 + came_t[7:8].astype(I32)], axis=1)
    less = jnp.where((arr_ids < row_ids) & arr_ok, 1.0, 0.0)
    arrivals_below = jnp.sum(less, axis=0, keepdims=True)
    above = jnp.where((arr_ids > row_ids[:, 0:slots]) & staying, 1.0, 0.0).astype(BF16)
    stay_below = lax.dot_general(jnp.ones((16, slots), BF16), above, NT, preferred_element_type=F32)[0:1]
    stay_place, _ = class_places(jnp.where(staying, 0, 31), False)
    rank = jnp.concatenate([stay_place, stay_below], axis=1) + arrivals_below
    dest = jnp.where(valid, rank.astype(I32), -1)
    srt_ref[...] = scatter_lanes(cand, dest, slots)

    for copy in gcopies:
        copy.wait_recv()
    for copy in copies + gcopies:
        copy.wait_send()


def force_kernel(sizes, peers, slots, srt_ref, gh_ref, offs_ref, side_ref, pos_ref, vel_ref, frc_ref, id_ref, ok_ref, en_ref, line, wide_line, own_cols, sums):
    size_x, size_y, size_z = sizes
    me = (lax.axis_index("x"), lax.axis_index("y"), lax.axis_index("z"))
    n = pos_ref.shape[1]
    side = side_ref[0, 0]
    okrow = srt_ref[8:9]
    good = okrow > 0.5
    count = jnp.sum(okrow).astype(I32)
    spread = side > 2.0 * NEAR
    span = slots + L

    parts = [part.astype(F32) for part in split3(jnp.where(good, srt_ref[0:3], -FAR))]
    parts = jnp.concatenate(parts + [jnp.zeros((7, slots), F32)], axis=0)
    row = lax.broadcasted_iota(I32, (16, 3 * L), 0)
    tile = lax.broadcasted_iota(I32, (16, 3 * L), 1) // L
    picks = jnp.where((row == tile) | (row == tile + 3) | (row == tile + 6), 1.0, 0.0).astype(BF16)
    own_cols[...] = lax.dot_general(jnp.transpose(parts).astype(BF16), picks, NN, preferred_element_type=F32)

    pad5 = jnp.zeros((5, slots), F32)
    away = jnp.full((8, L), FAR, F32)
    line[:, 0:span] = jnp.concatenate([jnp.concatenate([jnp.where(good, srt_ref[0:3], FAR), pad5], axis=0), away], axis=1)
    lane = lax.broadcasted_iota(I32, (8, span), 1)
    fill = count
    for d in DIRS:
        offset = (d[0] % size_x, d[1] % size_y, d[2] % size_z)
        back = ((-offset[0]) % size_x, (-offset[1]) % size_y, (-offset[2]) % size_z)
        index = peers.index(back)
        first, last = range_of(d)
        begin = jnp.where(spread, offs_ref[index, first], 0)
        end = jnp.where(spread, offs_ref[index, last], offs_ref[index, 27])
        shifts = []
        for axis in range(3):
            box = side * float(sizes[axis])
            if d[axis] == 1:
                shifts.append(jnp.where(me[axis] == sizes[axis] - 1, box, 0.0))
            elif d[axis] == -1:
                shifts.append(jnp.where(me[axis] == 0, -box, 0.0))
            else:
                shifts.append(jnp.float32(0.0))
        block = jnp.concatenate([gh_ref[index, a:a + 1] + shifts[a] for a in range(3)] + [pad5], axis=0)
        block = jnp.concatenate([block, away], axis=1)
        head = fill & (L - 1)
        base = pl.multiple_of(fill - head, L)
        move = head - begin
        block = pltpu.roll(block, jnp.where(move < 0, move + span, move), 1)
        tail = head + end - begin
        block = jnp.where(lane < tail, block, FAR)
        line[:, pl.ds(base, L)] = jnp.where(lane[:, 0:L] < head, line[:, pl.ds(base, L)], block[:, 0:L])
        line[:, pl.ds(pl.multiple_of(base + L, L), slots)] = block[:, L:]
        fill = fill + (end - begin)
    rest = pl.multiple_of(((fill + L - 1) // L) * L, L)
    line[:, pl.ds(rest, CHUNK * L)] = jnp.full((8, CHUNK * L), FAR, F32)
    self_chunks = (count + CHUNK * L - 1) // (CHUNK * L)
    chunks = (fill + CHUNK * L - 1) // (CHUNK * L)

    def widen(c, carry):
        for t in range(CHUNK):
            place = pl.ds(pl.multiple_of((c * CHUNK + t) * L, L), L)
            tile = line[:, place]
            for a in range(3):
                wide_line[a, :, place] = jnp.broadcast_to(tile[a:a + 1], (8, L))
        return carry

    lax.fori_loop(0, chunks, widen, 0)

    def own_step(q, energy):
        rows = [pl.ds(pl.multiple_of((q * GROUPS + g) * 8, 8), 8) for g in range(GROUPS)]
        own = [[own_cols[rows[g], a * L:a * L + L] for a in range(3)] for g in range(GROUPS)]

        def body(with_self, c, carry):
            force, en = [list(f) for f in carry[0]], carry[1]
            for t in range(CHUNK):
                place = pl.ds(pl.multiple_of((c * CHUNK + t) * L, L), L)
                near_xyz = [wide_line[a, :, place] for a in range(3)]
                for g in range(GROUPS):
                    dx, dy, dz = [own[g][a] - near_xyz[a] for a in range(3)]
                    d2 = dx * dx + dy * dy + dz * dz
                    near = d2 < RC * RC
                    if with_self:
                        near = near & (d2 > 0.0)
                    inv = jnp.where(near, lax.rsqrt(d2), 0.0)
                    s2 = inv * inv
                    s6 = s2 * s2 * s2
                    s12 = s6 * s6
                    p = s12 - s6
                    w = inv * (UPC / 24.0)
                    scale = (p + s12) * s2 + w
                    en = en + ((p + jnp.where(near, 0.25 * (RC * UPC - UCUT), 0.0)) - 6.0 * (w * d2))
                    force[g] = [force[g][0] + scale * dx, force[g][1] + scale * dy, force[g][2] + scale * dz]
            return tuple(tuple(f) for f in force), en

        zero = jnp.zeros((8, L), F32)
        carry = (((zero,) * 3,) * GROUPS, energy)
        carry = lax.fori_loop(0, self_chunks, functools.partial(body, True), carry)
        force, energy = lax.fori_loop(self_chunks, chunks, functools.partial(body, False), carry)
        for g in range(GROUPS):
            for a in range(3):
                sums[a, rows[g], :] = force[g][a]
        return energy

    own_steps = (count + 8 * GROUPS - 1) // (8 * GROUPS)
    energy = lax.fori_loop(0, own_steps, own_step, jnp.zeros((8, L), F32))
    en_ref[...] = 2.0 * jnp.sum(energy, axis=0, keepdims=True)

    col = lax.broadcasted_iota(I32, (L, L), 1)
    total = jnp.zeros((slots, L), F32)
    for a in range(3):
        pick = jnp.where(col == a, 1.0, 0.0).astype(BF16)
        for part in split3(sums[a]):
            total = total + lax.dot_general(part, pick, NN, preferred_element_type=F32)
    force = jnp.where(good, 24.0 * jnp.transpose(total)[0:3], 0.0)
    pos_ref[...] = srt_ref[0:3, 0:n]
    frc_ref[...] = force[:, 0:n]
    vel_ref[...] = (srt_ref[3:6] + (0.5 * DT) * force)[:, 0:n]
    id_ref[...] = (srt_ref[6:7].astype(I32) * 65536 + srt_ref[7:8].astype(I32))[:, 0:n]
    ok_ref[...] = okrow[:, 0:n].astype(I32)


def total_kernel(sizes, part_ref, sum_ref, rows, ssem, rsem):
    size_x, size_y, size_z = sizes
    me = (lax.axis_index("x"), lax.axis_index("y"), lax.axis_index("z"))
    mine = (me[2] * size_y + me[1]) * size_x + me[0]
    others = [(dx, dy, dz) for dz in range(size_z) for dy in range(size_y) for dx in range(size_x) if dx + dy + dz > 0]

    def device_at(offset):
        return (lax.rem(me[2] + offset[2], size_z), lax.rem(me[1] + offset[1], size_y), lax.rem(me[0] + offset[0], size_x))

    barrier = pltpu.get_barrier_semaphore()
    for offset in others:
        pl.semaphore_signal(barrier, inc=1, device_id=device_at(offset), device_id_type=pl.DeviceIdType.MESH)
    rows[pl.ds(mine, 1)] = part_ref[...]
    pl.semaphore_wait(barrier, len(others))
    copies = []
    for index, offset in enumerate(others):
        copy = pltpu.make_async_remote_copy(
            src_ref=part_ref, dst_ref=rows.at[pl.ds(mine, 1)], send_sem=ssem.at[index], recv_sem=rsem.at[index],
            device_id=device_at(offset), device_id_type=pl.DeviceIdType.MESH)
        copy.start()
        copies.append(copy)
    for copy in copies:
        copy.wait_recv()
    sum_ref[0, 0] = jnp.sum(rows[...])
    for copy in copies:
        copy.wait_send()


def solution(mesh):
    sizes = (mesh.shape["x"], mesh.shape["y"], mesh.shape["z"])
    peers = sorted({(d[0] % sizes[0], d[1] % sizes[1], d[2] % sizes[2]) for d in DIRS} - {(0, 0, 0)})
    devices = sizes[0] * sizes[1] * sizes[2]

    def local_step(atom_pos, atom_vel, atom_frc, atom_id, atom_ok, brick_side):
        n = atom_pos.shape[0]
        slots = -(-n // L) * L
        side = jnp.reshape(brick_side, (1, 1))
        vmem = pl.BlockSpec(memory_space=pltpu.VMEM)
        smem = pl.BlockSpec(memory_space=pltpu.SMEM)
        srt, ghosts = pl.pallas_call(
            functools.partial(exchange_kernel, sizes, peers, slots),
            out_shape=(jax.ShapeDtypeStruct((16, slots), F32), jax.ShapeDtypeStruct((len(peers), 4, slots), F32)),
            in_specs=[vmem] * 5 + [smem],
            out_specs=(vmem, vmem),
            scratch_shapes=[
                pltpu.VMEM((26 * PACK, L), F32), pltpu.VMEM((26 * PACK, L), F32), pltpu.VMEM((3, 4, slots), F32),
                pltpu.SemaphoreType.DMA((26,)), pltpu.SemaphoreType.DMA((26,)),
                pltpu.SemaphoreType.DMA((len(peers),)), pltpu.SemaphoreType.DMA((len(peers),)),
            ],
            compiler_params=pltpu.CompilerParams(collective_id=0, has_side_effects=True, vmem_limit_bytes=40 * 2 ** 20),
            name="exchange",
        )(atom_pos.T, atom_vel.T, atom_frc.T, atom_id[None, :], atom_ok[None, :], side)
        offs = ghosts[:, 3, 0:32].astype(I32)
        out_f = jax.ShapeDtypeStruct((3, n), F32)
        out_i = jax.ShapeDtypeStruct((1, n), I32)
        new_pos, new_vel, new_frc, new_id, new_ok, energy = pl.pallas_call(
            functools.partial(force_kernel, sizes, peers, slots),
            out_shape=(out_f, out_f, out_f, out_i, out_i, jax.ShapeDtypeStruct((1, L), F32)),
            in_specs=[vmem, vmem, smem, smem],
            out_specs=(vmem,) * 6,
            scratch_shapes=[pltpu.VMEM((8, 28 * slots + CHUNK * L), F32), pltpu.VMEM((3, 8, 28 * slots + CHUNK * L), F32), pltpu.VMEM((slots, 3 * L), F32), pltpu.VMEM((3, slots, L), F32)],
            compiler_params=pltpu.CompilerParams(vmem_limit_bytes=40 * 2 ** 20),
            name="forces",
        )(srt, ghosts, offs, side)
        energy = pl.pallas_call(
            functools.partial(total_kernel, sizes),
            out_shape=jax.ShapeDtypeStruct((1, 1), F32),
            in_specs=[vmem],
            out_specs=smem,
            scratch_shapes=[pltpu.VMEM((devices, L), F32), pltpu.SemaphoreType.DMA((devices,)), pltpu.SemaphoreType.DMA((devices,))],
            compiler_params=pltpu.CompilerParams(collective_id=1, has_side_effects=True),
            name="total",
        )(energy)[0, 0]
        return new_pos.T, new_vel.T, new_frc.T, new_id[0], new_ok[0], energy

    row_spec = P(MESH_AXES, None)
    id_spec = P(MESH_AXES)
    return jax.shard_map(local_step, mesh=mesh, in_specs=(row_spec, row_spec, row_spec, id_spec, id_spec, P()), out_specs=(row_spec, row_spec, row_spec, id_spec, id_spec, P()), check_vma=False)
```

```python
import functools

import jax
import jax.numpy as jnp
from jax import lax
from jax.experimental import pallas as pl
from jax.experimental.pallas import tpu as pltpu
from jax.sharding import PartitionSpec as P

DT = 0.005
RC = 2.5
FAR = 1.0e6
UCUT = 4.0 * (RC ** -12 - RC ** -6)
UPC = -48.0 * RC ** -13 + 24.0 * RC ** -7
MESH_AXES = ("z", "y", "x")
DIRS = [(dx, dy, dz) for dz in (-1, 0, 1) for dy in (-1, 0, 1) for dx in (-1, 0, 1) if (dx, dy, dz) != (0, 0, 0)]
NEAR = RC + 1.0e-3
PACK = 8
CHUNK = 4
GROUPS = 4
L = 128
F32 = jnp.float32
BF16 = jnp.bfloat16
I32 = jnp.int32
NT = (((1,), (1,)), ((), ()))
NN = (((1,), (0,)), ((), ()))


def order_of(d):
    if d[2] == 0:
        return 1 if d[1] != 0 else 2
    return 2 if (d[1] == 0 and d[0] != 0) else 0


def range_of(d):
    cx, cy, cz = [(1, 0, 2)[c] for c in (d[0], d[1], d[2])]
    kind = order_of(d)
    if kind == 0:
        if d[0] == 0 and d[1] == 0:
            return cz * 9, cz * 9 + 9
        if d[0] == 0:
            return cz * 9 + cy * 3, cz * 9 + cy * 3 + 3
        return cz * 9 + cy * 3 + cx, cz * 9 + cy * 3 + cx + 1
    if kind == 1:
        if d[0] == 0:
            return cy * 9, cy * 9 + 9
        return cy * 9 + cx * 3, cy * 9 + cx * 3 + 3
    if d[2] == 0:
        return cx * 9, cx * 9 + 9
    return cx * 9 + cz * 3, cx * 9 + cz * 3 + 3


def split3(x):
    hi = x.astype(BF16)
    rest = x - hi.astype(F32)
    mid = rest.astype(BF16)
    low = (rest - mid.astype(F32)).astype(BF16)
    return hi, mid, low


def onehot_rows(dest, base, count):
    rows = lax.broadcasted_iota(I32, (count, dest.shape[1]), 0) + base
    return jnp.where(rows == dest, 1.0, 0.0).astype(BF16)


def scatter_lanes(data, dest, slots):
    rows = data.shape[0]
    parts = jnp.concatenate(split3(data), axis=0)
    out = []
    for base in range(0, slots, 256):
        hot = onehot_rows(dest, base, min(256, slots - base))
        got = lax.dot_general(parts, hot, NT, preferred_element_type=F32)
        out.append(got[0:rows] + got[rows:2 * rows] + got[2 * rows:3 * rows])
    return jnp.concatenate(out, axis=1)


def class_places(code, with_before):
    width = code.shape[1]
    tiles = width // L
    cls = lax.broadcasted_iota(I32, (32, width), 0)
    member = jnp.where(cls == code, 1.0, 0.0)
    member_b = member.astype(BF16)
    stacked = jnp.concatenate([member_b[:, t * L:(t + 1) * L] for t in range(tiles)], axis=0)
    row_i = lax.broadcasted_iota(I32, (L, 256), 0)
    col_i = lax.broadcasted_iota(I32, (L, 256), 1)
    tri = jnp.where((row_i < col_i) | (col_i >= L), 1.0, 0.0).astype(BF16)
    pre = lax.dot_general(stacked, tri, NN, preferred_element_type=F32)
    carry = jnp.zeros((32, L), F32)
    if with_before:
        before_b = jnp.where(code < cls, 1.0, 0.0).astype(BF16)
        before_s = before_b[:, 0:L]
        tot = None
        ones = jnp.ones((L, L), BF16)
        for t in range(tiles):
            part = lax.dot_general(before_b[:, t * L:(t + 1) * L], ones, NN, preferred_element_type=F32)
            tot = part if tot is None else tot + part
        before = tot
        carry = before
    else:
        before = None
    places = []
    for t in range(tiles):
        within = pre[32 * t:32 * t + 32, 0:L] + carry
        places.append(jnp.sum(member[:, t * L:(t + 1) * L] * within, axis=0, keepdims=True))
        carry = carry + pre[32 * t:32 * t + 32, L:256]
    return jnp.concatenate(places, axis=1), before


def pad_lanes(x, width):
    return jnp.concatenate([x, jnp.zeros((x.shape[0], width - x.shape[1]), x.dtype)], axis=1)


def exchange_kernel(sizes, peers, slots, pos_hbm, vel_hbm, frc_hbm, id_hbm, ok_hbm, side_ref, srt_ref, gh_ref, pos_ref, vel_ref, frc_ref, id_ref, ok_ref, pkt, rcv, out3, isem, psend, precv, gsend, grecv):
    size_x, size_y, size_z = sizes
    me = (lax.axis_index("x"), lax.axis_index("y"), lax.axis_index("z"))

    def device_at(offset):
        return (lax.rem(me[2] + offset[2], size_z), lax.rem(me[1] + offset[1], size_y), lax.rem(me[0] + offset[0], size_x))

    loads = []
    for index, (src, dst) in enumerate(((ok_hbm, ok_ref), (id_hbm, id_ref), (pos_hbm, pos_ref), (vel_hbm, vel_ref), (frc_hbm, frc_ref))):
        load = pltpu.make_async_copy(src, dst, isem.at[index])
        load.start()
        loads.append(load)
    barrier = pltpu.get_barrier_semaphore()
    for offset in peers:
        pl.semaphore_signal(barrier, inc=1, device_id=device_at(offset), device_id_type=pl.DeviceIdType.MESH)

    n = pos_ref.shape[1]
    side = side_ref[0, 0]
    for load in loads:
        load.wait()
    owned = pad_lanes(jnp.reshape(ok_ref[...], (1, n)), slots) > 0
    half = vel_ref[...] + (0.5 * DT) * frc_ref[...]
    free = pos_ref[...] + DT * half
    half = pad_lanes(half, slots)
    free = pad_lanes(free, slots)
    ids = pad_lanes(jnp.reshape(id_ref[...], (1, n)), slots)
    code = jnp.zeros((1, slots), I32)
    moved = []
    low_side = []
    for axis in range(3):
        low = me[axis].astype(F32) * side
        high = (me[axis] + 1).astype(F32) * side
        box = side * float(sizes[axis])
        u = free[axis:axis + 1]
        step = jnp.where(u >= high, 1, 0) - jnp.where(u < low, 1, 0)
        code = code + (step + 1) * (1, 3, 9)[axis]
        moved.append(jnp.where(u < 0.0, u + box, jnp.where(u >= box, u - box, u)))
        low_side.append(low)
    code = jnp.where(owned, code, 31)
    id_hi = (ids >> 16).astype(F32)
    id_lo = (ids & 65535).astype(F32)
    okf = jnp.where(owned, 1.0, 0.0)
    data = jnp.concatenate(moved + [half, id_hi, id_lo, okf, jnp.zeros((7, slots), F32)], axis=0)

    place, _ = class_places(code, False)
    leaving = owned & (code != 13)
    target = jnp.where(leaving, (code - jnp.where(code > 13, 1, 0)) * PACK + place.astype(I32), -1)
    hot = onehot_rows(target, 0, 26 * PACK)
    parts = split3(data)
    got = lax.dot_general(hot, parts[0], NT, preferred_element_type=F32)
    got = got + lax.dot_general(hot, parts[1], NT, preferred_element_type=F32)
    got = got + lax.dot_general(hot, parts[2], NT, preferred_element_type=F32)
    pkt[...] = jnp.concatenate([got, jnp.zeros((26 * PACK, 112), F32)], axis=1)

    pl.semaphore_wait(barrier, len(peers))
    copies = []
    for index, d in enumerate(DIRS):
        offset = (d[0] % size_x, d[1] % size_y, d[2] % size_z)
        copy = pltpu.make_async_remote_copy(
            src_ref=pkt.at[pl.ds(index * PACK, PACK)], dst_ref=rcv.at[pl.ds(index * PACK, PACK)],
            send_sem=psend.at[index], recv_sem=precv.at[index],
            device_id=device_at(offset), device_id_type=pl.DeviceIdType.MESH)
        copy.start()
        copies.append(copy)
    staying = code == 13
    stay_f = jnp.where(staying, 1.0, 0.0)
    for copy in copies:
        copy.wait_recv()

    came = jnp.concatenate([rcv[...], jnp.zeros((256 - 26 * PACK, L), F32)], axis=0)
    came_t = jnp.transpose(came)[0:16]
    valid = jnp.concatenate([staying, came_t[8:9] > 0.5], axis=1)
    cand = jnp.concatenate([data, came_t], axis=1)
    bins = []
    for axis in range(3):
        loc = cand[axis:axis + 1] - low_side[axis]
        bins.append(jnp.where(loc < NEAR, 0, jnp.where(loc > side - NEAR, 2, 1)))
    cx, cy, cz = bins
    orders = [cz * 9 + cy * 3 + cx, cy * 9 + cx * 3 + cz, cx * 9 + cz * 3 + cy]
    lane = lax.broadcasted_iota(I32, (1, slots), 1).astype(F32)
    eye = lax.broadcasted_iota(I32, (32, L), 0) == lax.broadcasted_iota(I32, (32, L), 1)
    cand8 = cand[0:8]
    gcopies = []
    for kind in range(3):
        key = jnp.where(valid, orders[kind], 28)
        place, before = class_places(key, True)
        dest = jnp.where(valid, place.astype(I32), -1)
        arranged = scatter_lanes(cand8, dest, slots)
        total = jnp.concatenate([before[27:28]] * (slots // L), axis=1)
        xyz = jnp.where(lane < total, arranged[0:3], FAR)
        counts = jnp.sum(jnp.where(eye, before, 0.0), axis=0, keepdims=True)
        out3[kind] = jnp.concatenate([xyz, pad_lanes(counts, slots)], axis=0)
        for index, offset in enumerate(peers):
            sign = tuple(0 if c == 0 else 1 for c in offset)
            if order_of(sign) != kind:
                continue
            copy = pltpu.make_async_remote_copy(
                src_ref=out3.at[kind], dst_ref=gh_ref.at[index],
                send_sem=gsend.at[index], recv_sem=grecv.at[index],
                device_id=device_at(offset), device_id_type=pl.DeviceIdType.MESH)
            copy.start()
            gcopies.append(copy)

    arr_ids = came[:, 6:7].astype(I32) * 65536 + came[:, 7:8].astype(I32)
    arr_ok = came[:, 8:9] > 0.5
    row_ids = jnp.concatenate([ids, came_t[6:7].astype(I32) * 65536 + came_t[7:8].astype(I32)], axis=1)
    less = jnp.where((arr_ids < row_ids) & arr_ok, 1.0, 0.0)
    arrivals_below = jnp.sum(less, axis=0, keepdims=True)
    above = jnp.where((arr_ids > row_ids[:, 0:slots]) & staying, 1.0, 0.0).astype(BF16)
    stay_below = lax.dot_general(jnp.ones((16, slots), BF16), above, NT, preferred_element_type=F32)[0:1]
    stay_place, _ = class_places(jnp.where(staying, 0, 31), False)
    rank = jnp.concatenate([stay_place, stay_below], axis=1) + arrivals_below
    dest = jnp.where(valid, rank.astype(I32), -1)
    srt_ref[...] = scatter_lanes(cand, dest, slots)

    for copy in gcopies:
        copy.wait_recv()
    for copy in copies + gcopies:
        copy.wait_send()


def force_kernel(sizes, peers, slots, srt_ref, gh_ref, offs_ref, side_ref, pos_ref, vel_ref, frc_ref, id_ref, ok_ref, en_ref, line, wide_line, own_cols, sums):
    size_x, size_y, size_z = sizes
    me = (lax.axis_index("x"), lax.axis_index("y"), lax.axis_index("z"))
    n = pos_ref.shape[1]
    side = side_ref[0, 0]
    okrow = srt_ref[8:9]
    good = okrow > 0.5
    count = jnp.sum(okrow).astype(I32)
    spread = side > 2.0 * NEAR
    span = slots + L

    parts = [part.astype(F32) for part in split3(jnp.where(good, srt_ref[0:3], -FAR))]
    parts = jnp.concatenate(parts + [jnp.zeros((7, slots), F32)], axis=0)
    row = lax.broadcasted_iota(I32, (16, 3 * L), 0)
    tile = lax.broadcasted_iota(I32, (16, 3 * L), 1) // L
    picks = jnp.where((row == tile) | (row == tile + 3) | (row == tile + 6), 1.0, 0.0).astype(BF16)
    own_cols[...] = lax.dot_general(jnp.transpose(parts).astype(BF16), picks, NN, preferred_element_type=F32)

    pad5 = jnp.zeros((5, slots), F32)
    away = jnp.full((8, L), FAR, F32)
    line[:, 0:span] = jnp.concatenate([jnp.concatenate([jnp.where(good, srt_ref[0:3], FAR), pad5], axis=0), away], axis=1)
    lane = lax.broadcasted_iota(I32, (8, span), 1)
    fill = count
    for d in DIRS:
        offset = (d[0] % size_x, d[1] % size_y, d[2] % size_z)
        back = ((-offset[0]) % size_x, (-offset[1]) % size_y, (-offset[2]) % size_z)
        index = peers.index(back)
        first, last = range_of(d)
        begin = jnp.where(spread, offs_ref[index, first], 0)
        end = jnp.where(spread, offs_ref[index, last], offs_ref[index, 27])
        shifts = []
        for axis in range(3):
            box = side * float(sizes[axis])
            if d[axis] == 1:
                shifts.append(jnp.where(me[axis] == sizes[axis] - 1, box, 0.0))
            elif d[axis] == -1:
                shifts.append(jnp.where(me[axis] == 0, -box, 0.0))
            else:
                shifts.append(jnp.float32(0.0))
        block = jnp.concatenate([gh_ref[index, a:a + 1] + shifts[a] for a in range(3)] + [pad5], axis=0)
        block = jnp.concatenate([block, away], axis=1)
        head = fill & (L - 1)
        base = pl.multiple_of(fill - head, L)
        move = head - begin
        block = pltpu.roll(block, jnp.where(move < 0, move + span, move), 1)
        tail = head + end - begin
        block = jnp.where(lane < tail, block, FAR)
        line[:, pl.ds(base, L)] = jnp.where(lane[:, 0:L] < head, line[:, pl.ds(base, L)], block[:, 0:L])
        line[:, pl.ds(pl.multiple_of(base + L, L), slots)] = block[:, L:]
        fill = fill + (end - begin)
    rest = pl.multiple_of(((fill + L - 1) // L) * L, L)
    line[:, pl.ds(rest, CHUNK * L)] = jnp.full((8, CHUNK * L), FAR, F32)
    self_chunks = (count + CHUNK * L - 1) // (CHUNK * L)
    chunks = (fill + CHUNK * L - 1) // (CHUNK * L)

    def widen(c, carry):
        for t in range(CHUNK):
            place = pl.ds(pl.multiple_of((c * CHUNK + t) * L, L), L)
            tile = line[:, place]
            for a in range(3):
                wide_line[a, :, place] = jnp.broadcast_to(tile[a:a + 1], (8, L))
        return carry

    lax.fori_loop(0, chunks, widen, 0)

    def own_step(q, energy):
        rows = [pl.ds(pl.multiple_of((q * GROUPS + g) * 8, 8), 8) for g in range(GROUPS)]
        own = [[own_cols[rows[g], a * L:a * L + L] for a in range(3)] for g in range(GROUPS)]

        def body(with_self, c, carry):
            force, en = [list(f) for f in carry[0]], carry[1]
            for t in range(CHUNK):
                place = pl.ds(pl.multiple_of((c * CHUNK + t) * L, L), L)
                near_xyz = [wide_line[a, :, place] for a in range(3)]
                for g in range(GROUPS):
                    dx, dy, dz = [own[g][a] - near_xyz[a] for a in range(3)]
                    d2 = dx * dx + dy * dy + dz * dz
                    near = d2 < RC * RC
                    if with_self:
                        near = near & (d2 > 0.0)
                    inv = jnp.where(near, lax.rsqrt(d2), 0.0)
                    s2 = inv * inv
                    s6 = s2 * s2 * s2
                    s12 = s6 * s6
                    p = s12 - s6
                    w = inv * (UPC / 24.0)
                    scale = (p + s12) * s2 + w
                    en = en + ((p + jnp.where(near, 0.25 * (RC * UPC - UCUT), 0.0)) - 6.0 * (w * d2))
                    force[g] = [force[g][0] + scale * dx, force[g][1] + scale * dy, force[g][2] + scale * dz]
            return tuple(tuple(f) for f in force), en

        zero = jnp.zeros((8, L), F32)
        carry = (((zero,) * 3,) * GROUPS, energy)
        carry = lax.fori_loop(0, self_chunks, functools.partial(body, True), carry)
        force, energy = lax.fori_loop(self_chunks, chunks, functools.partial(body, False), carry)
        for g in range(GROUPS):
            for a in range(3):
                sums[a, rows[g], :] = force[g][a]
        return energy

    own_steps = (count + 8 * GROUPS - 1) // (8 * GROUPS)
    energy = lax.fori_loop(0, own_steps, own_step, jnp.zeros((8, L), F32))
    en_ref[...] = 2.0 * jnp.sum(energy, axis=0, keepdims=True)

    col = lax.broadcasted_iota(I32, (L, L), 1)
    total = jnp.zeros((slots, L), F32)
    for a in range(3):
        pick = jnp.where(col == a, 1.0, 0.0).astype(BF16)
        for part in split3(sums[a]):
            total = total + lax.dot_general(part, pick, NN, preferred_element_type=F32)
    force = jnp.where(good, 24.0 * jnp.transpose(total)[0:3], 0.0)
    pos_ref[...] = srt_ref[0:3, 0:n]
    frc_ref[...] = force[:, 0:n]
    vel_ref[...] = (srt_ref[3:6] + (0.5 * DT) * force)[:, 0:n]
    id_ref[...] = jnp.reshape((srt_ref[6:7].astype(I32) * 65536 + srt_ref[7:8].astype(I32))[:, 0:n], (n,))
    ok_ref[...] = jnp.reshape(okrow[:, 0:n].astype(I32), (n,))


def total_kernel(sizes, part_ref, sum_ref, rows, ssem, rsem):
    size_x, size_y, size_z = sizes
    me = (lax.axis_index("x"), lax.axis_index("y"), lax.axis_index("z"))
    mine = (me[2] * size_y + me[1]) * size_x + me[0]
    others = [(dx, dy, dz) for dz in range(size_z) for dy in range(size_y) for dx in range(size_x) if dx + dy + dz > 0]

    def device_at(offset):
        return (lax.rem(me[2] + offset[2], size_z), lax.rem(me[1] + offset[1], size_y), lax.rem(me[0] + offset[0], size_x))

    barrier = pltpu.get_barrier_semaphore()
    for offset in others:
        pl.semaphore_signal(barrier, inc=1, device_id=device_at(offset), device_id_type=pl.DeviceIdType.MESH)
    rows[pl.ds(mine, 1)] = part_ref[...]
    pl.semaphore_wait(barrier, len(others))
    copies = []
    for index, offset in enumerate(others):
        copy = pltpu.make_async_remote_copy(
            src_ref=part_ref, dst_ref=rows.at[pl.ds(mine, 1)], send_sem=ssem.at[index], recv_sem=rsem.at[index],
            device_id=device_at(offset), device_id_type=pl.DeviceIdType.MESH)
        copy.start()
        copies.append(copy)
    for copy in copies:
        copy.wait_recv()
    sum_ref[0, 0] = jnp.sum(rows[...])
    for copy in copies:
        copy.wait_send()


def solution(mesh):
    sizes = (mesh.shape["x"], mesh.shape["y"], mesh.shape["z"])
    peers = sorted({(d[0] % sizes[0], d[1] % sizes[1], d[2] % sizes[2]) for d in DIRS} - {(0, 0, 0)})
    devices = sizes[0] * sizes[1] * sizes[2]

    def local_step(atom_pos, atom_vel, atom_frc, atom_id, atom_ok, brick_side):
        n = atom_pos.shape[0]
        slots = -(-n // L) * L
        side = jnp.reshape(brick_side, (1, 1))
        vmem = pl.BlockSpec(memory_space=pltpu.VMEM)
        smem = pl.BlockSpec(memory_space=pltpu.SMEM)
        srt, ghosts = pl.pallas_call(
            functools.partial(exchange_kernel, sizes, peers, slots),
            out_shape=(jax.ShapeDtypeStruct((16, slots), F32), jax.ShapeDtypeStruct((len(peers), 4, slots), F32)),
            in_specs=[pl.BlockSpec(memory_space=pltpu.HBM)] * 5 + [smem],
            out_specs=(vmem, vmem),
            scratch_shapes=[
                pltpu.VMEM((3, n), F32), pltpu.VMEM((3, n), F32), pltpu.VMEM((3, n), F32), pltpu.VMEM((n,), I32), pltpu.VMEM((n,), I32),
                pltpu.VMEM((26 * PACK, L), F32), pltpu.VMEM((26 * PACK, L), F32), pltpu.VMEM((3, 4, slots), F32),
                pltpu.SemaphoreType.DMA((5,)), pltpu.SemaphoreType.DMA((26,)), pltpu.SemaphoreType.DMA((26,)),
                pltpu.SemaphoreType.DMA((len(peers),)), pltpu.SemaphoreType.DMA((len(peers),)),
            ],
            compiler_params=pltpu.CompilerParams(collective_id=0, has_side_effects=True, vmem_limit_bytes=40 * 2 ** 20),
            name="exchange",
        )(*[pltpu.with_memory_space_constraint(v, pltpu.HBM) for v in (atom_pos.T, atom_vel.T, atom_frc.T, atom_id, atom_ok)], side)
        offs = ghosts[:, 3, 0:32].astype(I32)
        out_f = jax.ShapeDtypeStruct((3, n), F32)
        out_i = jax.ShapeDtypeStruct((n,), I32)
        new_pos, new_vel, new_frc, new_id, new_ok, energy = pl.pallas_call(
            functools.partial(force_kernel, sizes, peers, slots),
            out_shape=(out_f, out_f, out_f, out_i, out_i, jax.ShapeDtypeStruct((1, L), F32)),
            in_specs=[vmem, vmem, smem, smem],
            out_specs=(vmem,) * 6,
            scratch_shapes=[pltpu.VMEM((8, 28 * slots + CHUNK * L), F32), pltpu.VMEM((3, 8, 28 * slots + CHUNK * L), F32), pltpu.VMEM((slots, 3 * L), F32), pltpu.VMEM((3, slots, L), F32)],
            compiler_params=pltpu.CompilerParams(vmem_limit_bytes=40 * 2 ** 20),
            name="forces",
        )(srt, ghosts, offs, side)
        energy = pl.pallas_call(
            functools.partial(total_kernel, sizes),
            out_shape=jax.ShapeDtypeStruct((1, 1), F32),
            in_specs=[vmem],
            out_specs=smem,
            scratch_shapes=[pltpu.VMEM((devices, L), F32), pltpu.SemaphoreType.DMA((devices,)), pltpu.SemaphoreType.DMA((devices,))],
            compiler_params=pltpu.CompilerParams(collective_id=1, has_side_effects=True),
            name="total",
        )(pltpu.with_memory_space_constraint(energy, pltpu.VMEM))[0, 0]
        return new_pos.T, new_vel.T, new_frc.T, new_id, new_ok, energy

    row_spec = P(MESH_AXES, None)
    id_spec = P(MESH_AXES)
    return jax.shard_map(local_step, mesh=mesh, in_specs=(row_spec, row_spec, row_spec, id_spec, id_spec, P()), out_specs=(row_spec, row_spec, row_spec, id_spec, id_spec, P()), check_vma=False)
```

```python
import functools

import jax
import jax.numpy as jnp
from jax import lax
from jax.experimental import pallas as pl
from jax.experimental.pallas import tpu as pltpu
from jax.sharding import PartitionSpec as P

DT = 0.005
RC = 2.5
FAR = 1.0e6
UCUT = 4.0 * (RC ** -12 - RC ** -6)
UPC = -48.0 * RC ** -13 + 24.0 * RC ** -7
MESH_AXES = ("z", "y", "x")
DIRS = [(dx, dy, dz) for dz in (-1, 0, 1) for dy in (-1, 0, 1) for dx in (-1, 0, 1) if (dx, dy, dz) != (0, 0, 0)]
NEAR = RC + 1.0e-3
PACK = 8
NEW = 256
CHUNK = 4
GROUPS = 4
L = 128
F32 = jnp.float32
BF16 = jnp.bfloat16
I32 = jnp.int32
NT = (((1,), (1,)), ((), ()))
NN = (((1,), (0,)), ((), ()))


def order_of(d):
    if d[2] == 0:
        return 1 if d[1] != 0 else 2
    return 2 if (d[1] == 0 and d[0] != 0) else 0


def range_of(d):
    cx, cy, cz = [(1, 0, 2)[c] for c in (d[0], d[1], d[2])]
    kind = order_of(d)
    if kind == 0:
        if d[0] == 0 and d[1] == 0:
            return cz * 9, cz * 9 + 9
        if d[0] == 0:
            return cz * 9 + cy * 3, cz * 9 + cy * 3 + 3
        return cz * 9 + cy * 3 + cx, cz * 9 + cy * 3 + cx + 1
    if kind == 1:
        if d[0] == 0:
            return cy * 9, cy * 9 + 9
        return cy * 9 + cx * 3, cy * 9 + cx * 3 + 3
    if d[2] == 0:
        return cx * 9, cx * 9 + 9
    return cx * 9 + cz * 3, cx * 9 + cz * 3 + 3


def split3(x):
    hi = x.astype(BF16)
    rest = x - hi.astype(F32)
    mid = rest.astype(BF16)
    low = (rest - mid.astype(F32)).astype(BF16)
    return hi, mid, low


def onehot_rows(dest, base, count):
    rows = lax.broadcasted_iota(I32, (count, dest.shape[1]), 0) + base
    return jnp.where(rows == dest, 1.0, 0.0).astype(BF16)


def scatter_lanes(data, dest, slots):
    rows = data.shape[0]
    parts = jnp.concatenate(split3(data), axis=0)
    out = []
    for base in range(0, slots, 256):
        hot = onehot_rows(dest, base, min(256, slots - base))
        got = lax.dot_general(parts, hot, NT, preferred_element_type=F32)
        out.append(got[0:rows] + got[rows:2 * rows] + got[2 * rows:3 * rows])
    return jnp.concatenate(out, axis=1)


def class_places(code, with_before):
    width = code.shape[1]
    tiles = width // L
    cls = lax.broadcasted_iota(I32, (32, width), 0)
    member = jnp.where(cls == code, 1.0, 0.0)
    member_b = member.astype(BF16)
    stacked = jnp.concatenate([member_b[:, t * L:(t + 1) * L] for t in range(tiles)], axis=0)
    row_i = lax.broadcasted_iota(I32, (L, 256), 0)
    col_i = lax.broadcasted_iota(I32, (L, 256), 1)
    tri = jnp.where((row_i < col_i) | (col_i >= L), 1.0, 0.0).astype(BF16)
    pre = lax.dot_general(stacked, tri, NN, preferred_element_type=F32)
    carry = jnp.zeros((32, L), F32)
    if with_before:
        before_b = jnp.where(code < cls, 1.0, 0.0).astype(BF16)
        before_s = before_b[:, 0:L]
        tot = None
        ones = jnp.ones((L, L), BF16)
        for t in range(tiles):
            part = lax.dot_general(before_b[:, t * L:(t + 1) * L], ones, NN, preferred_element_type=F32)
            tot = part if tot is None else tot + part
        before = tot
        carry = before
    else:
        before = None
    places = []
    for t in range(tiles):
        within = pre[32 * t:32 * t + 32, 0:L] + carry
        places.append(jnp.sum(member[:, t * L:(t + 1) * L] * within, axis=0, keepdims=True))
        carry = carry + pre[32 * t:32 * t + 32, L:256]
    return jnp.concatenate(places, axis=1), before


def pad_lanes(x, width):
    return jnp.concatenate([x, jnp.zeros((x.shape[0], width - x.shape[1]), x.dtype)], axis=1)


def exchange_kernel(sizes, peers, slots, pos_hbm, vel_hbm, frc_hbm, id_hbm, ok_hbm, side_ref, srt_ref, gh_ref, ga_ref, pos_ref, vel_ref, frc_ref, id_ref, ok_ref, pkt, rcv, out3, new3, isem, psend, precv, gsend, grecv, asend, arecv):
    size_x, size_y, size_z = sizes
    me = (lax.axis_index("x"), lax.axis_index("y"), lax.axis_index("z"))

    def device_at(offset):
        return (lax.rem(me[2] + offset[2], size_z), lax.rem(me[1] + offset[1], size_y), lax.rem(me[0] + offset[0], size_x))

    loads = []
    for index, (src, dst) in enumerate(((ok_hbm, ok_ref), (id_hbm, id_ref), (pos_hbm, pos_ref), (vel_hbm, vel_ref), (frc_hbm, frc_ref))):
        load = pltpu.make_async_copy(src, dst, isem.at[index])
        load.start()
        loads.append(load)
    barrier = pltpu.get_barrier_semaphore()
    for offset in peers:
        pl.semaphore_signal(barrier, inc=1, device_id=device_at(offset), device_id_type=pl.DeviceIdType.MESH)

    n = pos_ref.shape[1]
    side = side_ref[0, 0]
    for load in loads:
        load.wait()
    owned = pad_lanes(jnp.reshape(ok_ref[...], (1, n)), slots) > 0
    half = vel_ref[...] + (0.5 * DT) * frc_ref[...]
    free = pos_ref[...] + DT * half
    half = pad_lanes(half, slots)
    free = pad_lanes(free, slots)
    ids = pad_lanes(jnp.reshape(id_ref[...], (1, n)), slots)
    code = jnp.zeros((1, slots), I32)
    moved = []
    low_side = []
    for axis in range(3):
        low = me[axis].astype(F32) * side
        high = (me[axis] + 1).astype(F32) * side
        box = side * float(sizes[axis])
        u = free[axis:axis + 1]
        step = jnp.where(u >= high, 1, 0) - jnp.where(u < low, 1, 0)
        code = code + (step + 1) * (1, 3, 9)[axis]
        moved.append(jnp.where(u < 0.0, u + box, jnp.where(u >= box, u - box, u)))
        low_side.append(low)
    code = jnp.where(owned, code, 31)
    id_hi = (ids >> 16).astype(F32)
    id_lo = (ids & 65535).astype(F32)
    okf = jnp.where(owned, 1.0, 0.0)
    data = jnp.concatenate(moved + [half, id_hi, id_lo, okf, jnp.zeros((7, slots), F32)], axis=0)

    place, _ = class_places(code, False)
    leaving = owned & (code != 13)
    way = jnp.where(leaving, code - jnp.where(code > 13, 1, 0), 31)
    member = jnp.where(lax.broadcasted_iota(I32, (32, slots), 0) == way, 1.0, 0.0).astype(BF16)
    fields = jnp.concatenate([jnp.where(place == float(k), data, 0.0) for k in range(PACK)], axis=0)
    packed = jnp.zeros((32, L), F32)
    for part in split3(fields):
        packed = packed + lax.dot_general(member, part, NT, preferred_element_type=F32)
    pkt[...] = packed

    def bins_of(pos):
        bins = []
        for axis in range(3):
            loc = pos[axis:axis + 1] - low_side[axis]
            bins.append(jnp.where(loc < NEAR, 0, jnp.where(loc > side - NEAR, 2, 1)))
        cx, cy, cz = bins
        return cz * 9 + cy * 3 + cx, cy * 9 + cx * 3 + cz, cx * 9 + cz * 3 + cy

    eye = lax.broadcasted_iota(I32, (32, L), 0) == lax.broadcasted_iota(I32, (32, L), 1)

    def sorted_block(cand, keys, kept):
        width = cand.shape[1]
        where_to, before = class_places(jnp.where(kept, keys, 28), True)
        arranged = scatter_lanes(cand, jnp.where(kept, where_to.astype(I32), -1), width)
        total = jnp.concatenate([before[27:28]] * (width // L), axis=1)
        lane = lax.broadcasted_iota(I32, (1, width), 1).astype(F32)
        counts = jnp.sum(jnp.where(eye, before, 0.0), axis=0, keepdims=True)
        return jnp.concatenate([jnp.where(lane < total, arranged[0:3], FAR), pad_lanes(counts, width)], axis=0)

    sent = []

    def send(src, dst, ssem, rsem, offset):
        copy = pltpu.make_async_remote_copy(
            src_ref=src, dst_ref=dst, send_sem=ssem, recv_sem=rsem,
            device_id=device_at(offset), device_id_type=pl.DeviceIdType.MESH)
        copy.start()
        sent.append(copy)
        return copy

    def send_blocks(block, dst, ssem, rsem, kind):
        out = []
        for index, offset in enumerate(peers):
            if order_of(tuple(0 if c == 0 else 1 for c in offset)) == kind:
                out.append(send(block.at[kind], dst.at[index], ssem.at[index], rsem.at[index], offset))
        return out

    staying = code == 13
    keys = bins_of(data)
    for kind in range(2):
        out3[kind] = sorted_block(data[0:8], keys[kind], staying)
    pl.semaphore_wait(barrier, len(peers))
    packets = []
    for index, d in enumerate(DIRS):
        row = pl.ds(index, 1)
        packets.append(send(pkt.at[row], rcv.at[row], psend.at[index], precv.at[index], (d[0] % size_x, d[1] % size_y, d[2] % size_z)))
    blocks = send_blocks(out3, gh_ref, gsend, grecv, 0) + send_blocks(out3, gh_ref, gsend, grecv, 1)
    out3[2] = sorted_block(data[0:8], keys[2], staying)
    blocks = blocks + send_blocks(out3, gh_ref, gsend, grecv, 2)
    for copy in packets:
        copy.wait_recv()

    came = jnp.concatenate([rcv[...], jnp.zeros((32 - 26, L), F32)], axis=0)
    came = jnp.concatenate([came] + [pltpu.roll(came, L - 16 * k, 1) for k in range(1, PACK)], axis=0)
    came_t = jnp.transpose(came)[0:16]
    came_ok = came_t[8:9] > 0.5
    keys = bins_of(came_t)
    for kind in range(3):
        new3[kind] = sorted_block(came_t[0:8], keys[kind], came_ok)
        blocks = blocks + send_blocks(new3, ga_ref, asend, arecv, kind)

    arr_ids = came[:, 6:7].astype(I32) * 65536 + came[:, 7:8].astype(I32)
    arr_ok = came[:, 8:9] > 0.5
    row_ids = jnp.concatenate([ids, came_t[6:7].astype(I32) * 65536 + came_t[7:8].astype(I32)], axis=1)
    less = jnp.where((arr_ids < row_ids) & arr_ok, 1.0, 0.0)
    arrivals_below = jnp.sum(less, axis=0, keepdims=True)
    above = jnp.where((arr_ids > row_ids[:, 0:slots]) & staying, 1.0, 0.0).astype(BF16)
    stay_below = lax.dot_general(jnp.ones((16, slots), BF16), above, NT, preferred_element_type=F32)[0:1]
    stay_place, _ = class_places(jnp.where(staying, 0, 31), False)
    rank = jnp.concatenate([stay_place, stay_below], axis=1) + arrivals_below
    dest = jnp.where(jnp.concatenate([staying, came_ok], axis=1), rank.astype(I32), -1)
    srt_ref[...] = scatter_lanes(jnp.concatenate([data, came_t], axis=1), dest, slots)

    for copy in blocks:
        copy.wait_recv()
    for copy in sent:
        copy.wait_send()


def force_kernel(sizes, peers, slots, srt_ref, gh_ref, ga_ref, offs_ref, side_ref, pos_ref, vel_ref, frc_ref, id_ref, ok_ref, en_ref, line, wide_line, own_cols, sums):
    size_x, size_y, size_z = sizes
    me = (lax.axis_index("x"), lax.axis_index("y"), lax.axis_index("z"))
    n = pos_ref.shape[1]
    side = side_ref[0, 0]
    okrow = srt_ref[8:9]
    good = okrow > 0.5
    count = jnp.sum(okrow).astype(I32)
    spread = side > 2.0 * NEAR
    span = slots + L

    parts = [part.astype(F32) for part in split3(jnp.where(good, srt_ref[0:3], -FAR))]
    parts = jnp.concatenate(parts + [jnp.zeros((7, slots), F32)], axis=0)
    row = lax.broadcasted_iota(I32, (16, 3 * L), 0)
    tile = lax.broadcasted_iota(I32, (16, 3 * L), 1) // L
    picks = jnp.where((row == tile) | (row == tile + 3) | (row == tile + 6), 1.0, 0.0).astype(BF16)
    own_cols[...] = lax.dot_general(jnp.transpose(parts).astype(BF16), picks, NN, preferred_element_type=F32)

    pad5 = jnp.zeros((5, slots), F32)
    away = jnp.full((8, L), FAR, F32)
    line[:, 0:span] = jnp.concatenate([jnp.concatenate([jnp.where(good, srt_ref[0:3], FAR), pad5], axis=0), away], axis=1)
    lane = lax.broadcasted_iota(I32, (8, span), 1)
    fill = count
    for d in DIRS:
        offset = (d[0] % size_x, d[1] % size_y, d[2] % size_z)
        back = ((-offset[0]) % size_x, (-offset[1]) % size_y, (-offset[2]) % size_z)
        index = peers.index(back)
        first, last = range_of(d)
        shifts = []
        for axis in range(3):
            box = side * float(sizes[axis])
            if d[axis] == 1:
                shifts.append(jnp.where(me[axis] == sizes[axis] - 1, box, 0.0))
            elif d[axis] == -1:
                shifts.append(jnp.where(me[axis] == 0, -box, 0.0))
            else:
                shifts.append(jnp.float32(0.0))
        for source, entry in ((gh_ref, index), (ga_ref, index + len(peers))):
            width = source.shape[2]
            begin = jnp.where(spread, offs_ref[entry, first], 0)
            end = jnp.where(spread, offs_ref[entry, last], offs_ref[entry, 27])
            block = jnp.concatenate([source[index, a:a + 1] + shifts[a] for a in range(3)] + [jnp.zeros((5, width), F32)], axis=0)
            block = jnp.concatenate([block, away], axis=1)
            head = fill & (L - 1)
            base = pl.multiple_of(fill - head, L)
            move = head - begin
            block = pltpu.roll(block, jnp.where(move < 0, move + (width + L), move), 1)
            block = jnp.where(lane[:, 0:width + L] < head + end - begin, block, FAR)
            line[:, pl.ds(base, L)] = jnp.where(lane[:, 0:L] < head, line[:, pl.ds(base, L)], block[:, 0:L])
            line[:, pl.ds(pl.multiple_of(base + L, L), width)] = block[:, L:]
            fill = fill + (end - begin)
    rest = pl.multiple_of(((fill + L - 1) // L) * L, L)
    line[:, pl.ds(rest, CHUNK * L)] = jnp.full((8, CHUNK * L), FAR, F32)
    self_chunks = (count + CHUNK * L - 1) // (CHUNK * L)
    chunks = (fill + CHUNK * L - 1) // (CHUNK * L)

    def widen(c, carry):
        for t in range(CHUNK):
            place = pl.ds(pl.multiple_of((c * CHUNK + t) * L, L), L)
            tile = line[:, place]
            for a in range(3):
                wide_line[a, :, place] = jnp.broadcast_to(tile[a:a + 1], (8, L))
        return carry

    lax.fori_loop(0, chunks, widen, 0)

    def own_step(q, energy):
        rows = [pl.ds(pl.multiple_of((q * GROUPS + g) * 8, 8), 8) for g in range(GROUPS)]
        own = [[own_cols[rows[g], a * L:a * L + L] for a in range(3)] for g in range(GROUPS)]

        def body(with_self, c, carry):
            force, en = [list(f) for f in carry[0]], carry[1]
            for t in range(CHUNK):
                place = pl.ds(pl.multiple_of((c * CHUNK + t) * L, L), L)
                near_xyz = [wide_line[a, :, place] for a in range(3)]
                for g in range(GROUPS):
                    dx, dy, dz = [own[g][a] - near_xyz[a] for a in range(3)]
                    d2 = dx * dx + dy * dy + dz * dz
                    near = d2 < RC * RC
                    if with_self:
                        near = near & (d2 > 0.0)
                    inv = jnp.where(near, lax.rsqrt(d2), 0.0)
                    s2 = inv * inv
                    s6 = s2 * s2 * s2
                    s12 = s6 * s6
                    p = s12 - s6
                    w = inv * (UPC / 24.0)
                    scale = (p + s12) * s2 + w
                    en = en + ((p + jnp.where(near, 0.25 * (RC * UPC - UCUT), 0.0)) - 6.0 * (w * d2))
                    force[g] = [force[g][0] + scale * dx, force[g][1] + scale * dy, force[g][2] + scale * dz]
            return tuple(tuple(f) for f in force), en

        zero = jnp.zeros((8, L), F32)
        carry = (((zero,) * 3,) * GROUPS, energy)
        carry = lax.fori_loop(0, self_chunks, functools.partial(body, True), carry)
        force, energy = lax.fori_loop(self_chunks, chunks, functools.partial(body, False), carry)
        for g in range(GROUPS):
            for a in range(3):
                sums[a, rows[g], :] = force[g][a]
        return energy

    own_steps = (count + 8 * GROUPS - 1) // (8 * GROUPS)
    energy = lax.fori_loop(0, own_steps, own_step, jnp.zeros((8, L), F32))
    en_ref[...] = 2.0 * jnp.sum(energy, axis=0, keepdims=True)

    col = lax.broadcasted_iota(I32, (L, L), 1)
    total = jnp.zeros((slots, L), F32)
    for a in range(3):
        pick = jnp.where(col == a, 1.0, 0.0).astype(BF16)
        for part in split3(sums[a]):
            total = total + lax.dot_general(part, pick, NN, preferred_element_type=F32)
    force = jnp.where(good, 24.0 * jnp.transpose(total)[0:3], 0.0)
    pos_ref[...] = srt_ref[0:3, 0:n]
    frc_ref[...] = force[:, 0:n]
    vel_ref[...] = (srt_ref[3:6] + (0.5 * DT) * force)[:, 0:n]
    id_ref[...] = jnp.reshape((srt_ref[6:7].astype(I32) * 65536 + srt_ref[7:8].astype(I32))[:, 0:n], (n,))
    ok_ref[...] = jnp.reshape(okrow[:, 0:n].astype(I32), (n,))


def total_kernel(sizes, part_ref, sum_ref, rows, ssem, rsem):
    size_x, size_y, size_z = sizes
    me = (lax.axis_index("x"), lax.axis_index("y"), lax.axis_index("z"))
    mine = (me[2] * size_y + me[1]) * size_x + me[0]
    others = [(dx, dy, dz) for dz in range(size_z) for dy in range(size_y) for dx in range(size_x) if dx + dy + dz > 0]

    def device_at(offset):
        return (lax.rem(me[2] + offset[2], size_z), lax.rem(me[1] + offset[1], size_y), lax.rem(me[0] + offset[0], size_x))

    barrier = pltpu.get_barrier_semaphore()
    for offset in others:
        pl.semaphore_signal(barrier, inc=1, device_id=device_at(offset), device_id_type=pl.DeviceIdType.MESH)
    rows[pl.ds(mine, 1)] = part_ref[...]
    pl.semaphore_wait(barrier, len(others))
    copies = []
    for index, offset in enumerate(others):
        copy = pltpu.make_async_remote_copy(
            src_ref=part_ref, dst_ref=rows.at[pl.ds(mine, 1)], send_sem=ssem.at[index], recv_sem=rsem.at[index],
            device_id=device_at(offset), device_id_type=pl.DeviceIdType.MESH)
        copy.start()
        copies.append(copy)
    for copy in copies:
        copy.wait_recv()
    sum_ref[0, 0] = jnp.sum(rows[...])
    for copy in copies:
        copy.wait_send()


def solution(mesh):
    sizes = (mesh.shape["x"], mesh.shape["y"], mesh.shape["z"])
    peers = sorted({(d[0] % sizes[0], d[1] % sizes[1], d[2] % sizes[2]) for d in DIRS} - {(0, 0, 0)})
    devices = sizes[0] * sizes[1] * sizes[2]

    def local_step(atom_pos, atom_vel, atom_frc, atom_id, atom_ok, brick_side):
        n = atom_pos.shape[0]
        slots = -(-n // L) * L
        side = jnp.reshape(brick_side, (1, 1))
        vmem = pl.BlockSpec(memory_space=pltpu.VMEM)
        smem = pl.BlockSpec(memory_space=pltpu.SMEM)
        srt, ghosts, fresh = pl.pallas_call(
            functools.partial(exchange_kernel, sizes, peers, slots),
            out_shape=(jax.ShapeDtypeStruct((16, slots), F32), jax.ShapeDtypeStruct((len(peers), 4, slots), F32), jax.ShapeDtypeStruct((len(peers), 4, NEW), F32)),
            in_specs=[pl.BlockSpec(memory_space=pltpu.HBM)] * 5 + [smem],
            out_specs=(vmem,) * 3,
            scratch_shapes=[
                pltpu.VMEM((3, n), F32), pltpu.VMEM((3, n), F32), pltpu.VMEM((3, n), F32), pltpu.VMEM((n,), I32), pltpu.VMEM((n,), I32),
                pltpu.VMEM((32, L), F32), pltpu.VMEM((26, L), F32), pltpu.VMEM((3, 4, slots), F32), pltpu.VMEM((3, 4, NEW), F32),
                pltpu.SemaphoreType.DMA((5,)), pltpu.SemaphoreType.DMA((26,)), pltpu.SemaphoreType.DMA((26,)),
            ] + [pltpu.SemaphoreType.DMA((len(peers),))] * 4,
            compiler_params=pltpu.CompilerParams(collective_id=0, has_side_effects=True, vmem_limit_bytes=40 * 2 ** 20),
            name="exchange",
        )(*[pltpu.with_memory_space_constraint(v, pltpu.HBM) for v in (atom_pos.T, atom_vel.T, atom_frc.T, atom_id, atom_ok)], side)
        offs = jnp.concatenate([ghosts[:, 3, 0:32], fresh[:, 3, 0:32]], axis=0).astype(I32)
        out_f = jax.ShapeDtypeStruct((3, n), F32)
        out_i = jax.ShapeDtypeStruct((n,), I32)
        new_pos, new_vel, new_frc, new_id, new_ok, energy = pl.pallas_call(
            functools.partial(force_kernel, sizes, peers, slots),
            out_shape=(out_f, out_f, out_f, out_i, out_i, jax.ShapeDtypeStruct((1, L), F32)),
            in_specs=[vmem] * 3 + [smem] * 2,
            out_specs=(vmem,) * 6,
            scratch_shapes=[pltpu.VMEM((8, 28 * slots + CHUNK * L), F32), pltpu.VMEM((3, 8, 28 * slots + CHUNK * L), F32), pltpu.VMEM((slots, 3 * L), F32), pltpu.VMEM((3, slots, L), F32)],
            compiler_params=pltpu.CompilerParams(vmem_limit_bytes=40 * 2 ** 20),
            name="forces",
        )(srt, ghosts, fresh, offs, side)
        energy = pl.pallas_call(
            functools.partial(total_kernel, sizes),
            out_shape=jax.ShapeDtypeStruct((1, 1), F32),
            in_specs=[vmem],
            out_specs=smem,
            scratch_shapes=[pltpu.VMEM((devices, L), F32), pltpu.SemaphoreType.DMA((devices,)), pltpu.SemaphoreType.DMA((devices,))],
            compiler_params=pltpu.CompilerParams(collective_id=1, has_side_effects=True),
            name="total",
        )(pltpu.with_memory_space_constraint(energy, pltpu.VMEM))[0, 0]
        return new_pos.T, new_vel.T, new_frc.T, new_id, new_ok, energy

    row_spec = P(MESH_AXES, None)
    id_spec = P(MESH_AXES)
    return jax.shard_map(local_step, mesh=mesh, in_specs=(row_spec, row_spec, row_spec, id_spec, id_spec, P()), out_specs=(row_spec, row_spec, row_spec, id_spec, id_spec, P()), check_vma=False)
```

```python
import functools

import jax
import jax.numpy as jnp
from jax import lax
from jax.experimental import pallas as pl
from jax.experimental.pallas import tpu as pltpu
from jax.sharding import PartitionSpec as P

DT = 0.005
RC = 2.5
FAR = 1.0e6
UCUT = 4.0 * (RC ** -12 - RC ** -6)
UPC = -48.0 * RC ** -13 + 24.0 * RC ** -7
MESH_AXES = ("z", "y", "x")
DIRS = [(dx, dy, dz) for dz in (-1, 0, 1) for dy in (-1, 0, 1) for dx in (-1, 0, 1) if (dx, dy, dz) != (0, 0, 0)]
NEAR = RC + 1.0e-3
PACK = 8
NEW = 256
CHUNK = 4
GROUPS = 4
L = 128
F32 = jnp.float32
BF16 = jnp.bfloat16
I32 = jnp.int32
NT = (((1,), (1,)), ((), ()))
NN = (((1,), (0,)), ((), ()))


def order_of(d):
    if d[2] == 0:
        return 1 if d[1] != 0 else 2
    return 2 if (d[1] == 0 and d[0] != 0) else 0


def range_of(d):
    cx, cy, cz = [(1, 0, 2)[c] for c in (d[0], d[1], d[2])]
    kind = order_of(d)
    if kind == 0:
        if d[0] == 0 and d[1] == 0:
            return cz * 9, cz * 9 + 9
        if d[0] == 0:
            return cz * 9 + cy * 3, cz * 9 + cy * 3 + 3
        return cz * 9 + cy * 3 + cx, cz * 9 + cy * 3 + cx + 1
    if kind == 1:
        if d[0] == 0:
            return cy * 9, cy * 9 + 9
        return cy * 9 + cx * 3, cy * 9 + cx * 3 + 3
    if d[2] == 0:
        return cx * 9, cx * 9 + 9
    return cx * 9 + cz * 3, cx * 9 + cz * 3 + 3


def split3(x):
    hi = x.astype(BF16)
    rest = x - hi.astype(F32)
    mid = rest.astype(BF16)
    low = (rest - mid.astype(F32)).astype(BF16)
    return hi, mid, low


def onehot_rows(dest, base, count):
    rows = lax.broadcasted_iota(I32, (count, dest.shape[1]), 0) + base
    return jnp.where(rows == dest, 1.0, 0.0).astype(BF16)


def scatter_lanes(data, dest, slots):
    rows = data.shape[0]
    parts = jnp.concatenate(split3(data), axis=0)
    out = []
    for base in range(0, slots, 256):
        hot = onehot_rows(dest, base, min(256, slots - base))
        got = lax.dot_general(parts, hot, NT, preferred_element_type=F32)
        out.append(got[0:rows] + got[rows:2 * rows] + got[2 * rows:3 * rows])
    return jnp.concatenate(out, axis=1)


def class_places(code, with_before):
    width = code.shape[1]
    tiles = width // L
    cls = lax.broadcasted_iota(I32, (32, width), 0)
    member = jnp.where(cls == code, 1.0, 0.0)
    member_b = member.astype(BF16)
    stacked = jnp.concatenate([member_b[:, t * L:(t + 1) * L] for t in range(tiles)], axis=0)
    row_i = lax.broadcasted_iota(I32, (L, 256), 0)
    col_i = lax.broadcasted_iota(I32, (L, 256), 1)
    tri = jnp.where((row_i < col_i) | (col_i >= L), 1.0, 0.0).astype(BF16)
    pre = lax.dot_general(stacked, tri, NN, preferred_element_type=F32)
    carry = jnp.zeros((32, L), F32)
    if with_before:
        before_b = jnp.where(code < cls, 1.0, 0.0).astype(BF16)
        before_s = before_b[:, 0:L]
        tot = None
        ones = jnp.ones((L, L), BF16)
        for t in range(tiles):
            part = lax.dot_general(before_b[:, t * L:(t + 1) * L], ones, NN, preferred_element_type=F32)
            tot = part if tot is None else tot + part
        before = tot
        carry = before
    else:
        before = None
    places = []
    for t in range(tiles):
        within = pre[32 * t:32 * t + 32, 0:L] + carry
        places.append(jnp.sum(member[:, t * L:(t + 1) * L] * within, axis=0, keepdims=True))
        carry = carry + pre[32 * t:32 * t + 32, L:256]
    return jnp.concatenate(places, axis=1), before


def pad_lanes(x, width):
    return jnp.concatenate([x, jnp.zeros((x.shape[0], width - x.shape[1]), x.dtype)], axis=1)


def exchange_kernel(sizes, peers, slots, pos_hbm, vel_hbm, frc_hbm, id_hbm, ok_hbm, side_ref, srt_ref, gh_ref, ga_ref, pos_ref, vel_ref, frc_ref, id_ref, ok_ref, pkt, rcv, out3, new3, isem, psend, precv, gsend, grecv, asend, arecv):
    size_x, size_y, size_z = sizes
    me = (lax.axis_index("x"), lax.axis_index("y"), lax.axis_index("z"))

    def device_at(offset):
        return (lax.rem(me[2] + offset[2], size_z), lax.rem(me[1] + offset[1], size_y), lax.rem(me[0] + offset[0], size_x))

    loads = []
    for index, (src, dst) in enumerate(((ok_hbm, ok_ref), (id_hbm, id_ref), (pos_hbm, pos_ref), (vel_hbm, vel_ref), (frc_hbm, frc_ref))):
        load = pltpu.make_async_copy(src, dst, isem.at[index])
        load.start()
        loads.append(load)
    barrier = pltpu.get_barrier_semaphore()
    for offset in peers:
        pl.semaphore_signal(barrier, inc=1, device_id=device_at(offset), device_id_type=pl.DeviceIdType.MESH)

    n = pos_ref.shape[1]
    side = side_ref[0, 0]
    for load in loads:
        load.wait()
    owned = pad_lanes(jnp.reshape(ok_ref[...], (1, n)), slots) > 0
    half = vel_ref[...] + (0.5 * DT) * frc_ref[...]
    free = pos_ref[...] + DT * half
    half = pad_lanes(half, slots)
    free = pad_lanes(free, slots)
    ids = pad_lanes(jnp.reshape(id_ref[...], (1, n)), slots)
    code = jnp.zeros((1, slots), I32)
    moved = []
    low_side = []
    for axis in range(3):
        low = me[axis].astype(F32) * side
        high = (me[axis] + 1).astype(F32) * side
        box = side * float(sizes[axis])
        u = free[axis:axis + 1]
        step = jnp.where(u >= high, 1, 0) - jnp.where(u < low, 1, 0)
        code = code + (step + 1) * (1, 3, 9)[axis]
        moved.append(jnp.where(u < 0.0, u + box, jnp.where(u >= box, u - box, u)))
        low_side.append(low)
    code = jnp.where(owned, code, 31)
    id_hi = (ids >> 16).astype(F32)
    id_lo = (ids & 65535).astype(F32)
    okf = jnp.where(owned, 1.0, 0.0)
    data = jnp.concatenate(moved + [half, id_hi, id_lo, okf, jnp.zeros((7, slots), F32)], axis=0)

    place, _ = class_places(code, False)
    leaving = owned & (code != 13)
    way = jnp.where(leaving, code - jnp.where(code > 13, 1, 0), 31)
    member = jnp.where(lax.broadcasted_iota(I32, (32, slots), 0) == way, 1.0, 0.0).astype(BF16)
    fields = jnp.concatenate([jnp.where(place == float(k), data, 0.0) for k in range(PACK)], axis=0)
    packed = jnp.zeros((32, L), F32)
    for part in split3(fields):
        packed = packed + lax.dot_general(member, part, NT, preferred_element_type=F32)
    pkt[...] = packed

    def bins_of(pos):
        bins = []
        for axis in range(3):
            loc = pos[axis:axis + 1] - low_side[axis]
            bins.append(jnp.where(loc < NEAR, 0, jnp.where(loc > side - NEAR, 2, 1)))
        cx, cy, cz = bins
        return cz * 9 + cy * 3 + cx, cy * 9 + cx * 3 + cz, cx * 9 + cz * 3 + cy

    eye = lax.broadcasted_iota(I32, (32, L), 0) == lax.broadcasted_iota(I32, (32, L), 1)

    def sorted_block(cand, keys, kept):
        width = cand.shape[1]
        where_to, before = class_places(jnp.where(kept, keys, 28), True)
        arranged = scatter_lanes(cand, jnp.where(kept, where_to.astype(I32), -1), width)
        total = jnp.concatenate([before[27:28]] * (width // L), axis=1)
        lane = lax.broadcasted_iota(I32, (1, width), 1).astype(F32)
        counts = jnp.sum(jnp.where(eye, before, 0.0), axis=0, keepdims=True)
        return jnp.concatenate([jnp.where(lane < total, arranged[0:3], FAR), pad_lanes(counts, width)], axis=0)

    sent = []

    def send(src, dst, ssem, rsem, offset):
        copy = pltpu.make_async_remote_copy(
            src_ref=src, dst_ref=dst, send_sem=ssem, recv_sem=rsem,
            device_id=device_at(offset), device_id_type=pl.DeviceIdType.MESH)
        copy.start()
        sent.append(copy)
        return copy

    def send_blocks(block, dst, ssem, rsem, kind):
        out = []
        for index, offset in enumerate(peers):
            if order_of(tuple(0 if c == 0 else 1 for c in offset)) == kind:
                out.append(send(block.at[kind], dst.at[index], ssem.at[index], rsem.at[index], offset))
        return out

    staying = code == 13
    keys = bins_of(data)
    for kind in range(3):
        out3[kind] = sorted_block(data[0:8], keys[kind], staying)
    pl.semaphore_wait(barrier, len(peers))
    packets = []
    for index, d in enumerate(DIRS):
        row = pl.ds(index, 1)
        packets.append(send(pkt.at[row], rcv.at[row], psend.at[index], precv.at[index], (d[0] % size_x, d[1] % size_y, d[2] % size_z)))
    blocks = []
    for kind in range(3):
        blocks = blocks + send_blocks(out3, gh_ref, gsend, grecv, kind)
    for copy in packets:
        copy.wait_recv()

    came = jnp.concatenate([rcv[...], jnp.zeros((32 - 26, L), F32)], axis=0)
    came = jnp.concatenate([came] + [pltpu.roll(came, L - 16 * k, 1) for k in range(1, PACK)], axis=0)
    came_t = jnp.transpose(came)[0:16]
    came_ok = came_t[8:9] > 0.5
    keys = bins_of(came_t)
    late = []
    for kind in range(3):
        new3[kind] = sorted_block(came_t[0:8], keys[kind], came_ok)
        late = late + send_blocks(new3, ga_ref, asend, arecv, kind)
    for copy in blocks:
        copy.wait_recv()

    arr_ids = came[:, 6:7].astype(I32) * 65536 + came[:, 7:8].astype(I32)
    arr_ok = came[:, 8:9] > 0.5
    row_ids = jnp.concatenate([ids, came_t[6:7].astype(I32) * 65536 + came_t[7:8].astype(I32)], axis=1)
    less = jnp.where((arr_ids < row_ids) & arr_ok, 1.0, 0.0)
    arrivals_below = jnp.sum(less, axis=0, keepdims=True)
    above = jnp.where((arr_ids > row_ids[:, 0:slots]) & staying, 1.0, 0.0).astype(BF16)
    stay_below = lax.dot_general(jnp.ones((16, slots), BF16), above, NT, preferred_element_type=F32)[0:1]
    stay_place, _ = class_places(jnp.where(staying, 0, 31), False)
    rank = jnp.concatenate([stay_place, stay_below], axis=1) + arrivals_below
    dest = jnp.where(jnp.concatenate([staying, came_ok], axis=1), rank.astype(I32), -1)
    srt_ref[...] = scatter_lanes(jnp.concatenate([data, came_t], axis=1), dest, slots)

    for copy in late:
        copy.wait_recv()
    for copy in sent:
        copy.wait_send()


def force_kernel(sizes, peers, slots, srt_ref, gh_ref, ga_ref, offs_ref, side_ref, pos_ref, vel_ref, frc_ref, id_ref, ok_ref, en_ref, line, wide_line, own_cols, sums):
    size_x, size_y, size_z = sizes
    me = (lax.axis_index("x"), lax.axis_index("y"), lax.axis_index("z"))
    n = pos_ref.shape[1]
    side = side_ref[0, 0]
    okrow = srt_ref[8:9]
    good = okrow > 0.5
    count = jnp.sum(okrow).astype(I32)
    spread = side > 2.0 * NEAR
    span = slots + L

    parts = [part.astype(F32) for part in split3(jnp.where(good, srt_ref[0:3], -FAR))]
    parts = jnp.concatenate(parts + [jnp.zeros((7, slots), F32)], axis=0)
    row = lax.broadcasted_iota(I32, (16, 3 * L), 0)
    tile = lax.broadcasted_iota(I32, (16, 3 * L), 1) // L
    picks = jnp.where((row == tile) | (row == tile + 3) | (row == tile + 6), 1.0, 0.0).astype(BF16)
    own_cols[...] = lax.dot_general(jnp.transpose(parts).astype(BF16), picks, NN, preferred_element_type=F32)

    pad5 = jnp.zeros((5, slots), F32)
    away = jnp.full((8, L), FAR, F32)
    line[:, 0:span] = jnp.concatenate([jnp.concatenate([jnp.where(good, srt_ref[0:3], FAR), pad5], axis=0), away], axis=1)
    lane = lax.broadcasted_iota(I32, (8, span), 1)
    fill = count
    for d in DIRS:
        offset = (d[0] % size_x, d[1] % size_y, d[2] % size_z)
        back = ((-offset[0]) % size_x, (-offset[1]) % size_y, (-offset[2]) % size_z)
        index = peers.index(back)
        first, last = range_of(d)
        shifts = []
        for axis in range(3):
            box = side * float(sizes[axis])
            if d[axis] == 1:
                shifts.append(jnp.where(me[axis] == sizes[axis] - 1, box, 0.0))
            elif d[axis] == -1:
                shifts.append(jnp.where(me[axis] == 0, -box, 0.0))
            else:
                shifts.append(jnp.float32(0.0))
        for source, entry in ((gh_ref, index), (ga_ref, index + len(peers))):
            width = source.shape[2]
            begin = jnp.where(spread, offs_ref[entry, first], 0)
            end = jnp.where(spread, offs_ref[entry, last], offs_ref[entry, 27])
            block = jnp.concatenate([source[index, a:a + 1] + shifts[a] for a in range(3)] + [jnp.zeros((5, width), F32)], axis=0)
            block = jnp.concatenate([block, away], axis=1)
            head = fill & (L - 1)
            base = pl.multiple_of(fill - head, L)
            move = head - begin
            block = pltpu.roll(block, jnp.where(move < 0, move + (width + L), move), 1)
            block = jnp.where(lane[:, 0:width + L] < head + end - begin, block, FAR)
            line[:, pl.ds(base, L)] = jnp.where(lane[:, 0:L] < head, line[:, pl.ds(base, L)], block[:, 0:L])
            line[:, pl.ds(pl.multiple_of(base + L, L), width)] = block[:, L:]
            fill = fill + (end - begin)
    rest = pl.multiple_of(((fill + L - 1) // L) * L, L)
    line[:, pl.ds(rest, CHUNK * L)] = jnp.full((8, CHUNK * L), FAR, F32)
    self_chunks = (count + CHUNK * L - 1) // (CHUNK * L)
    chunks = (fill + CHUNK * L - 1) // (CHUNK * L)

    def widen(c, carry):
        for t in range(CHUNK):
            place = pl.ds(pl.multiple_of((c * CHUNK + t) * L, L), L)
            tile = line[:, place]
            for a in range(3):
                wide_line[a, :, place] = jnp.broadcast_to(tile[a:a + 1], (8, L))
        return carry

    lax.fori_loop(0, chunks, widen, 0)

    def own_step(q, energy):
        rows = [pl.ds(pl.multiple_of((q * GROUPS + g) * 8, 8), 8) for g in range(GROUPS)]
        own = [[own_cols[rows[g], a * L:a * L + L] for a in range(3)] for g in range(GROUPS)]

        def body(with_self, c, carry):
            force, en = [list(f) for f in carry[0]], carry[1]
            for t in range(CHUNK):
                place = pl.ds(pl.multiple_of((c * CHUNK + t) * L, L), L)
                near_xyz = [wide_line[a, :, place] for a in range(3)]
                for g in range(GROUPS):
                    dx, dy, dz = [own[g][a] - near_xyz[a] for a in range(3)]
                    d2 = dx * dx + dy * dy + dz * dz
                    near = d2 < RC * RC
                    if with_self:
                        near = near & (d2 > 0.0)
                    inv = jnp.where(near, lax.rsqrt(d2), 0.0)
                    s2 = inv * inv
                    s6 = s2 * s2 * s2
                    s12 = s6 * s6
                    p = s12 - s6
                    w = inv * (UPC / 24.0)
                    scale = (p + s12) * s2 + w
                    en = en + ((p + jnp.where(near, 0.25 * (RC * UPC - UCUT), 0.0)) - 6.0 * (w * d2))
                    force[g] = [force[g][0] + scale * dx, force[g][1] + scale * dy, force[g][2] + scale * dz]
            return tuple(tuple(f) for f in force), en

        zero = jnp.zeros((8, L), F32)
        carry = (((zero,) * 3,) * GROUPS, energy)
        carry = lax.fori_loop(0, self_chunks, functools.partial(body, True), carry)
        force, energy = lax.fori_loop(self_chunks, chunks, functools.partial(body, False), carry)
        for g in range(GROUPS):
            for a in range(3):
                sums[a, rows[g], :] = force[g][a]
        return energy

    own_steps = (count + 8 * GROUPS - 1) // (8 * GROUPS)
    energy = lax.fori_loop(0, own_steps, own_step, jnp.zeros((8, L), F32))
    en_ref[...] = 2.0 * jnp.sum(energy, axis=0, keepdims=True)

    col = lax.broadcasted_iota(I32, (L, L), 1)
    total = jnp.zeros((slots, L), F32)
    for a in range(3):
        pick = jnp.where(col == a, 1.0, 0.0).astype(BF16)
        for part in split3(sums[a]):
            total = total + lax.dot_general(part, pick, NN, preferred_element_type=F32)
    force = jnp.where(good, 24.0 * jnp.transpose(total)[0:3], 0.0)
    pos_ref[...] = srt_ref[0:3, 0:n]
    frc_ref[...] = force[:, 0:n]
    vel_ref[...] = (srt_ref[3:6] + (0.5 * DT) * force)[:, 0:n]
    id_ref[...] = jnp.reshape((srt_ref[6:7].astype(I32) * 65536 + srt_ref[7:8].astype(I32))[:, 0:n], (n,))
    ok_ref[...] = jnp.reshape(okrow[:, 0:n].astype(I32), (n,))


def total_kernel(sizes, part_ref, sum_ref, rows, ssem, rsem):
    size_x, size_y, size_z = sizes
    me = (lax.axis_index("x"), lax.axis_index("y"), lax.axis_index("z"))
    mine = (me[2] * size_y + me[1]) * size_x + me[0]
    others = [(dx, dy, dz) for dz in range(size_z) for dy in range(size_y) for dx in range(size_x) if dx + dy + dz > 0]

    def device_at(offset):
        return (lax.rem(me[2] + offset[2], size_z), lax.rem(me[1] + offset[1], size_y), lax.rem(me[0] + offset[0], size_x))

    barrier = pltpu.get_barrier_semaphore()
    for offset in others:
        pl.semaphore_signal(barrier, inc=1, device_id=device_at(offset), device_id_type=pl.DeviceIdType.MESH)
    rows[pl.ds(mine, 1)] = part_ref[...]
    pl.semaphore_wait(barrier, len(others))
    copies = []
    for index, offset in enumerate(others):
        copy = pltpu.make_async_remote_copy(
            src_ref=part_ref, dst_ref=rows.at[pl.ds(mine, 1)], send_sem=ssem.at[index], recv_sem=rsem.at[index],
            device_id=device_at(offset), device_id_type=pl.DeviceIdType.MESH)
        copy.start()
        copies.append(copy)
    for copy in copies:
        copy.wait_recv()
    sum_ref[0, 0] = jnp.sum(rows[...])
    for copy in copies:
        copy.wait_send()


def solution(mesh):
    sizes = (mesh.shape["x"], mesh.shape["y"], mesh.shape["z"])
    peers = sorted({(d[0] % sizes[0], d[1] % sizes[1], d[2] % sizes[2]) for d in DIRS} - {(0, 0, 0)})
    devices = sizes[0] * sizes[1] * sizes[2]

    def local_step(atom_pos, atom_vel, atom_frc, atom_id, atom_ok, brick_side):
        n = atom_pos.shape[0]
        slots = -(-n // L) * L
        side = jnp.reshape(brick_side, (1, 1))
        vmem = pl.BlockSpec(memory_space=pltpu.VMEM)
        smem = pl.BlockSpec(memory_space=pltpu.SMEM)
        srt, ghosts, fresh = pl.pallas_call(
            functools.partial(exchange_kernel, sizes, peers, slots),
            out_shape=(jax.ShapeDtypeStruct((16, slots), F32), jax.ShapeDtypeStruct((len(peers), 4, slots), F32), jax.ShapeDtypeStruct((len(peers), 4, NEW), F32)),
            in_specs=[pl.BlockSpec(memory_space=pltpu.HBM)] * 5 + [smem],
            out_specs=(vmem,) * 3,
            scratch_shapes=[
                pltpu.VMEM((3, n), F32), pltpu.VMEM((3, n), F32), pltpu.VMEM((3, n), F32), pltpu.VMEM((n,), I32), pltpu.VMEM((n,), I32),
                pltpu.VMEM((32, L), F32), pltpu.VMEM((26, L), F32), pltpu.VMEM((3, 4, slots), F32), pltpu.VMEM((3, 4, NEW), F32),
                pltpu.SemaphoreType.DMA((5,)), pltpu.SemaphoreType.DMA((26,)), pltpu.SemaphoreType.DMA((26,)),
            ] + [pltpu.SemaphoreType.DMA((len(peers),))] * 4,
            compiler_params=pltpu.CompilerParams(collective_id=0, has_side_effects=True, vmem_limit_bytes=40 * 2 ** 20),
            name="exchange",
        )(*[pltpu.with_memory_space_constraint(v, pltpu.HBM) for v in (atom_pos.T, atom_vel.T, atom_frc.T, atom_id, atom_ok)], side)
        offs = jnp.concatenate([ghosts[:, 3, 0:32], fresh[:, 3, 0:32]], axis=0).astype(I32)
        out_f = jax.ShapeDtypeStruct((3, n), F32)
        out_i = jax.ShapeDtypeStruct((n,), I32)
        new_pos, new_vel, new_frc, new_id, new_ok, energy = pl.pallas_call(
            functools.partial(force_kernel, sizes, peers, slots),
            out_shape=(out_f, out_f, out_f, out_i, out_i, jax.ShapeDtypeStruct((1, L), F32)),
            in_specs=[vmem] * 3 + [smem] * 2,
            out_specs=(vmem,) * 6,
            scratch_shapes=[pltpu.VMEM((8, 28 * slots + CHUNK * L), F32), pltpu.VMEM((3, 8, 28 * slots + CHUNK * L), F32), pltpu.VMEM((slots, 3 * L), F32), pltpu.VMEM((3, slots, L), F32)],
            compiler_params=pltpu.CompilerParams(vmem_limit_bytes=40 * 2 ** 20),
            name="forces",
        )(srt, ghosts, fresh, offs, side)
        energy = pl.pallas_call(
            functools.partial(total_kernel, sizes),
            out_shape=jax.ShapeDtypeStruct((1, 1), F32),
            in_specs=[vmem],
            out_specs=smem,
            scratch_shapes=[pltpu.VMEM((devices, L), F32), pltpu.SemaphoreType.DMA((devices,)), pltpu.SemaphoreType.DMA((devices,))],
            compiler_params=pltpu.CompilerParams(collective_id=1, has_side_effects=True),
            name="total",
        )(pltpu.with_memory_space_constraint(energy, pltpu.VMEM))[0, 0]
        return new_pos.T, new_vel.T, new_frc.T, new_id, new_ok, energy

    row_spec = P(MESH_AXES, None)
    id_spec = P(MESH_AXES)
    return jax.shard_map(local_step, mesh=mesh, in_specs=(row_spec, row_spec, row_spec, id_spec, id_spec, P()), out_specs=(row_spec, row_spec, row_spec, id_spec, id_spec, P()), check_vma=False)
```

```python
import functools

import jax
import jax.numpy as jnp
from jax import lax
from jax.experimental import pallas as pl
from jax.experimental.pallas import tpu as pltpu
from jax.sharding import PartitionSpec as P

DT = 0.005
RC = 2.5
FAR = 1.0e6
UCUT = 4.0 * (RC ** -12 - RC ** -6)
UPC = -48.0 * RC ** -13 + 24.0 * RC ** -7
MESH_AXES = ("z", "y", "x")
DIRS = [(dx, dy, dz) for dz in (-1, 0, 1) for dy in (-1, 0, 1) for dx in (-1, 0, 1) if (dx, dy, dz) != (0, 0, 0)]
NEAR = RC + 1.0e-3
PACK = 8
NEW = 256
CHUNK = 3
GROUPS = 8
L = 128
F32 = jnp.float32
BF16 = jnp.bfloat16
I32 = jnp.int32
NT = (((1,), (1,)), ((), ()))
NN = (((1,), (0,)), ((), ()))


def order_of(d):
    if d[2] == 0:
        return 1 if d[1] != 0 else 2
    return 2 if (d[1] == 0 and d[0] != 0) else 0


def range_of(d):
    cx, cy, cz = [(1, 0, 2)[c] for c in (d[0], d[1], d[2])]
    kind = order_of(d)
    if kind == 0:
        if d[0] == 0 and d[1] == 0:
            return cz * 9, cz * 9 + 9
        if d[0] == 0:
            return cz * 9 + cy * 3, cz * 9 + cy * 3 + 3
        return cz * 9 + cy * 3 + cx, cz * 9 + cy * 3 + cx + 1
    if kind == 1:
        if d[0] == 0:
            return cy * 9, cy * 9 + 9
        return cy * 9 + cx * 3, cy * 9 + cx * 3 + 3
    if d[2] == 0:
        return cx * 9, cx * 9 + 9
    return cx * 9 + cz * 3, cx * 9 + cz * 3 + 3


def split3(x):
    hi = x.astype(BF16)
    rest = x - hi.astype(F32)
    mid = rest.astype(BF16)
    low = (rest - mid.astype(F32)).astype(BF16)
    return hi, mid, low


def onehot_rows(dest, base, count):
    rows = lax.broadcasted_iota(I32, (count, dest.shape[1]), 0) + base
    return jnp.where(rows == dest, 1.0, 0.0).astype(BF16)


def scatter_lanes(data, dest, slots):
    rows = data.shape[0]
    parts = jnp.concatenate(split3(data), axis=0)
    out = []
    for base in range(0, slots, 256):
        hot = onehot_rows(dest, base, min(256, slots - base))
        got = lax.dot_general(parts, hot, NT, preferred_element_type=F32)
        out.append(got[0:rows] + got[rows:2 * rows] + got[2 * rows:3 * rows])
    return jnp.concatenate(out, axis=1)


def class_places(code, with_before):
    width = code.shape[1]
    tiles = width // L
    cls = lax.broadcasted_iota(I32, (32, width), 0)
    member = jnp.where(cls == code, 1.0, 0.0)
    member_b = member.astype(BF16)
    stacked = jnp.concatenate([member_b[:, t * L:(t + 1) * L] for t in range(tiles)], axis=0)
    row_i = lax.broadcasted_iota(I32, (L, 256), 0)
    col_i = lax.broadcasted_iota(I32, (L, 256), 1)
    tri = jnp.where((row_i < col_i) | (col_i >= L), 1.0, 0.0).astype(BF16)
    pre = lax.dot_general(stacked, tri, NN, preferred_element_type=F32)
    carry = jnp.zeros((32, L), F32)
    if with_before:
        before_b = jnp.where(code < cls, 1.0, 0.0).astype(BF16)
        before_s = before_b[:, 0:L]
        tot = None
        ones = jnp.ones((L, L), BF16)
        for t in range(tiles):
            part = lax.dot_general(before_b[:, t * L:(t + 1) * L], ones, NN, preferred_element_type=F32)
            tot = part if tot is None else tot + part
        before = tot
        carry = before
    else:
        before = None
    places = []
    for t in range(tiles):
        within = pre[32 * t:32 * t + 32, 0:L] + carry
        places.append(jnp.sum(member[:, t * L:(t + 1) * L] * within, axis=0, keepdims=True))
        carry = carry + pre[32 * t:32 * t + 32, L:256]
    return jnp.concatenate(places, axis=1), before


def pad_lanes(x, width):
    return jnp.concatenate([x, jnp.zeros((x.shape[0], width - x.shape[1]), x.dtype)], axis=1)


def pair_loop(own_cols, near_lanes, q, first, last, with_self, carry):
    rows = [step_rows(q, g) for g in range(GROUPS)]
    own = [[own_cols[rows[g], a * L:(a + 1) * L] for a in range(3)] for g in range(GROUPS)]

    def body(c, carry):
        force, en = [list(f) for f in carry[0]], carry[1]
        for t in range(CHUNK):
            place = pl.ds(pl.multiple_of((c * CHUNK + t) * L, L), L)
            near_xyz = [near_lanes[a, :, place] for a in range(3)]
            for g in range(GROUPS):
                dx, dy, dz = [own[g][a] - near_xyz[a] for a in range(3)]
                d2 = dx * dx + dy * dy + dz * dz
                near = d2 < RC * RC
                if with_self:
                    near = near & (d2 > 0.0)
                inv = jnp.where(near, lax.rsqrt(d2), 0.0)
                s2 = inv * inv
                s6 = s2 * s2 * s2
                s12 = s6 * s6
                p = s12 - s6
                w = inv * (UPC / 24.0)
                scale = (p + s12) * s2 + w
                en = en + ((p + jnp.where(near, 0.25 * (RC * UPC - UCUT), 0.0)) - 6.0 * (w * d2))
                force[g] = [force[g][0] + scale * dx, force[g][1] + scale * dy, force[g][2] + scale * dz]
        return tuple(tuple(f) for f in force), en

    return lax.fori_loop(first, last, body, carry)


def step_rows(q, g):
    return pl.ds(pl.multiple_of((q * GROUPS + g) * 8, 8), 8)


def own_columns(xyz):
    slots = xyz.shape[1]
    parts = [part.astype(F32) for part in split3(xyz)]
    parts = jnp.concatenate(parts + [jnp.zeros((7, slots), F32)], axis=0)
    row = lax.broadcasted_iota(I32, (16, 3 * L), 0)
    tile = lax.broadcasted_iota(I32, (16, 3 * L), 1) // L
    picks = jnp.where((row == tile) | (row == tile + 3) | (row == tile + 6), 1.0, 0.0).astype(BF16)
    return lax.dot_general(jnp.transpose(parts).astype(BF16), picks, NN, preferred_element_type=F32)


def exchange_kernel(sizes, peers, slots, pos_hbm, vel_hbm, frc_hbm, id_hbm, ok_hbm, side_ref, srt_ref, gh_ref, ga_ref, own_ref, inner_ref, inner_en_ref, pos_ref, vel_ref, frc_ref, id_ref, ok_ref, pkt, rcv, out3, new3, lanes, isem, psend, precv, gsend, grecv, asend, arecv):
    size_x, size_y, size_z = sizes
    me = (lax.axis_index("x"), lax.axis_index("y"), lax.axis_index("z"))

    def device_at(offset):
        return (lax.rem(me[2] + offset[2], size_z), lax.rem(me[1] + offset[1], size_y), lax.rem(me[0] + offset[0], size_x))

    loads = []
    for index, (src, dst) in enumerate(((ok_hbm, ok_ref), (id_hbm, id_ref), (pos_hbm, pos_ref), (vel_hbm, vel_ref), (frc_hbm, frc_ref))):
        load = pltpu.make_async_copy(src, dst, isem.at[index])
        load.start()
        loads.append(load)
    barrier = pltpu.get_barrier_semaphore()
    for offset in peers:
        pl.semaphore_signal(barrier, inc=1, device_id=device_at(offset), device_id_type=pl.DeviceIdType.MESH)

    n = pos_ref.shape[1]
    side = side_ref[0, 0]
    for load in loads:
        load.wait()
    owned = pad_lanes(jnp.reshape(ok_ref[...], (1, n)), slots) > 0
    half = vel_ref[...] + (0.5 * DT) * frc_ref[...]
    free = pos_ref[...] + DT * half
    half = pad_lanes(half, slots)
    free = pad_lanes(free, slots)
    ids = pad_lanes(jnp.reshape(id_ref[...], (1, n)), slots)
    code = jnp.zeros((1, slots), I32)
    moved = []
    low_side = []
    for axis in range(3):
        low = me[axis].astype(F32) * side
        high = (me[axis] + 1).astype(F32) * side
        box = side * float(sizes[axis])
        u = free[axis:axis + 1]
        step = jnp.where(u >= high, 1, 0) - jnp.where(u < low, 1, 0)
        code = code + (step + 1) * (1, 3, 9)[axis]
        moved.append(jnp.where(u < 0.0, u + box, jnp.where(u >= box, u - box, u)))
        low_side.append(low)
    code = jnp.where(owned, code, 31)
    id_hi = (ids >> 16).astype(F32)
    id_lo = (ids & 65535).astype(F32)
    okf = jnp.where(owned, 1.0, 0.0)
    data = jnp.concatenate(moved + [half, id_hi, id_lo, okf, jnp.zeros((7, slots), F32)], axis=0)

    place, _ = class_places(code, False)
    leaving = owned & (code != 13)
    way = jnp.where(leaving, code - jnp.where(code > 13, 1, 0), 31)
    member = jnp.where(lax.broadcasted_iota(I32, (32, slots), 0) == way, 1.0, 0.0).astype(BF16)
    fields = jnp.concatenate([jnp.where(place == float(k), data, 0.0) for k in range(PACK)], axis=0)
    packed = jnp.zeros((32, L), F32)
    for part in split3(fields):
        packed = packed + lax.dot_general(member, part, NT, preferred_element_type=F32)
    pkt[...] = packed

    def bins_of(pos):
        bins = []
        for axis in range(3):
            loc = pos[axis:axis + 1] - low_side[axis]
            bins.append(jnp.where(loc < NEAR, 0, jnp.where(loc > side - NEAR, 2, 1)))
        cx, cy, cz = bins
        return cz * 9 + cy * 3 + cx, cy * 9 + cx * 3 + cz, cx * 9 + cz * 3 + cy

    eye = lax.broadcasted_iota(I32, (32, L), 0) == lax.broadcasted_iota(I32, (32, L), 1)

    def sorted_block(cand, keys, kept):
        width = cand.shape[1]
        where_to, before = class_places(jnp.where(kept, keys, 28), True)
        arranged = scatter_lanes(cand, jnp.where(kept, where_to.astype(I32), -1), width)
        total = jnp.concatenate([before[27:28]] * (width // L), axis=1)
        lane = lax.broadcasted_iota(I32, (1, width), 1).astype(F32)
        counts = jnp.sum(jnp.where(eye, before, 0.0), axis=0, keepdims=True)
        return jnp.concatenate([jnp.where(lane < total, arranged[0:3], FAR), pad_lanes(counts, width)], axis=0)

    sent = []

    def send(src, dst, ssem, rsem, offset):
        copy = pltpu.make_async_remote_copy(
            src_ref=src, dst_ref=dst, send_sem=ssem, recv_sem=rsem,
            device_id=device_at(offset), device_id_type=pl.DeviceIdType.MESH)
        copy.start()
        sent.append(copy)
        return copy

    def send_blocks(block, dst, ssem, rsem, kind):
        out = []
        for index, offset in enumerate(peers):
            if order_of(tuple(0 if c == 0 else 1 for c in offset)) == kind:
                out.append(send(block.at[kind], dst.at[index], ssem.at[index], rsem.at[index], offset))
        return out

    staying = code == 13
    keys = bins_of(data)
    for kind in range(3):
        out3[kind] = sorted_block(data[0:8], keys[kind], staying)
    pl.semaphore_wait(barrier, len(peers))
    packets = []
    for index, d in enumerate(DIRS):
        row = pl.ds(index, 1)
        packets.append(send(pkt.at[row], rcv.at[row], psend.at[index], precv.at[index], (d[0] % size_x, d[1] % size_y, d[2] % size_z)))
    blocks = []
    for kind in range(3):
        blocks = blocks + send_blocks(out3, gh_ref, gsend, grecv, kind)
    for copy in packets:
        copy.wait_recv()

    came = jnp.concatenate([rcv[...], jnp.zeros((32 - 26, L), F32)], axis=0)
    came = jnp.concatenate([came] + [pltpu.roll(came, L - 16 * k, 1) for k in range(1, PACK)], axis=0)
    came_t = jnp.transpose(came)[0:16]
    came_ok = came_t[8:9] > 0.5
    keys = bins_of(came_t)
    late = []
    for kind in range(3):
        new3[kind] = sorted_block(came_t[0:8], keys[kind], came_ok)
        late = late + send_blocks(new3, ga_ref, asend, arecv, kind)
    for copy in blocks:
        copy.wait_recv()

    arr_ids = came[:, 6:7].astype(I32) * 65536 + came[:, 7:8].astype(I32)
    arr_ok = came[:, 8:9] > 0.5
    row_ids = jnp.concatenate([ids, came_t[6:7].astype(I32) * 65536 + came_t[7:8].astype(I32)], axis=1)
    less = jnp.where((arr_ids < row_ids) & arr_ok, 1.0, 0.0)
    arrivals_below = jnp.sum(less, axis=0, keepdims=True)
    above = jnp.where((arr_ids > row_ids[:, 0:slots]) & staying, 1.0, 0.0).astype(BF16)
    stay_below = lax.dot_general(jnp.ones((16, slots), BF16), above, NT, preferred_element_type=F32)[0:1]
    stay_place, _ = class_places(jnp.where(staying, 0, 31), False)
    rank = jnp.concatenate([stay_place, stay_below], axis=1) + arrivals_below
    dest = jnp.where(jnp.concatenate([staying, came_ok], axis=1), rank.astype(I32), -1)
    merged = scatter_lanes(jnp.concatenate([data, came_t], axis=1), dest, slots)
    srt_ref[...] = merged

    good = merged[8:9] > 0.5
    own_ref[...] = own_columns(jnp.where(good, merged[0:3], -FAR))
    for a in range(3):
        lanes[a] = jnp.broadcast_to(jnp.where(good, merged[a:a + 1], FAR), (8, slots))
    zero = jnp.zeros((8, L), F32)

    def own_step(q, energy):
        force, energy = pair_loop(own_ref, lanes, q, 0, slots // (CHUNK * L), True, (((zero,) * 3,) * GROUPS, energy))
        for g in range(GROUPS):
            for a in range(3):
                inner_ref[a, step_rows(q, g), :] = force[g][a]
        return energy

    inner_en_ref[...] = lax.fori_loop(0, slots // (8 * GROUPS), own_step, zero)

    for copy in late:
        copy.wait_recv()
    for copy in sent:
        copy.wait_send()


def force_kernel(sizes, peers, slots, srt_ref, gh_ref, ga_ref, own_cols, inner_ref, inner_en_ref, offs_ref, side_ref, pos_ref, vel_ref, frc_ref, id_ref, ok_ref, en_ref, line, wide_line, sums):
    size_x, size_y, size_z = sizes
    me = (lax.axis_index("x"), lax.axis_index("y"), lax.axis_index("z"))
    n = pos_ref.shape[1]
    side = side_ref[0, 0]
    okrow = srt_ref[8:9]
    good = okrow > 0.5
    count = jnp.sum(okrow).astype(I32)
    spread = side > 2.0 * NEAR
    span = slots + L

    away = jnp.full((8, L), FAR, F32)
    line[:, 0:L] = away
    lane = lax.broadcasted_iota(I32, (8, span), 1)
    fill = jnp.int32(0)
    for d in DIRS:
        offset = (d[0] % size_x, d[1] % size_y, d[2] % size_z)
        back = ((-offset[0]) % size_x, (-offset[1]) % size_y, (-offset[2]) % size_z)
        index = peers.index(back)
        first, last = range_of(d)
        shifts = []
        for axis in range(3):
            box = side * float(sizes[axis])
            if d[axis] == 1:
                shifts.append(jnp.where(me[axis] == sizes[axis] - 1, box, 0.0))
            elif d[axis] == -1:
                shifts.append(jnp.where(me[axis] == 0, -box, 0.0))
            else:
                shifts.append(jnp.float32(0.0))
        for source, entry in ((gh_ref, index), (ga_ref, index + len(peers))):
            width = source.shape[2]
            begin = jnp.where(spread, offs_ref[entry, first], 0)
            end = jnp.where(spread, offs_ref[entry, last], offs_ref[entry, 27])
            block = jnp.concatenate([source[index, a:a + 1] + shifts[a] for a in range(3)] + [jnp.zeros((5, width), F32)], axis=0)
            block = jnp.concatenate([block, away], axis=1)
            head = fill & (L - 1)
            base = pl.multiple_of(fill - head, L)
            move = head - begin
            block = pltpu.roll(block, jnp.where(move < 0, move + (width + L), move), 1)
            block = jnp.where(lane[:, 0:width + L] < head + end - begin, block, FAR)
            line[:, pl.ds(base, L)] = jnp.where(lane[:, 0:L] < head, line[:, pl.ds(base, L)], block[:, 0:L])
            line[:, pl.ds(pl.multiple_of(base + L, L), width)] = block[:, L:]
            fill = fill + (end - begin)
    rest = pl.multiple_of(((fill + L - 1) // L) * L, L)
    line[:, pl.ds(rest, CHUNK * L)] = jnp.full((8, CHUNK * L), FAR, F32)
    chunks = (fill + CHUNK * L - 1) // (CHUNK * L)

    def widen(c, carry):
        for t in range(CHUNK):
            place = pl.ds(pl.multiple_of((c * CHUNK + t) * L, L), L)
            tile = line[:, place]
            for a in range(3):
                wide_line[a, :, place] = jnp.broadcast_to(tile[a:a + 1], (8, L))
        return carry

    lax.fori_loop(0, chunks, widen, 0)

    def own_step(q, energy):
        start = tuple(tuple(inner_ref[a, step_rows(q, g), :] for a in range(3)) for g in range(GROUPS))
        force, energy = pair_loop(own_cols, wide_line, q, 0, chunks, False, (start, energy))
        for g in range(GROUPS):
            for a in range(3):
                sums[a, step_rows(q, g), :] = force[g][a]
        return energy

    own_steps = (count + 8 * GROUPS - 1) // (8 * GROUPS)
    energy = lax.fori_loop(0, own_steps, own_step, inner_en_ref[...])
    en_ref[...] = 2.0 * jnp.sum(energy, axis=0, keepdims=True)

    col = lax.broadcasted_iota(I32, (L, L), 1)
    total = jnp.zeros((slots, L), F32)
    for a in range(3):
        pick = jnp.where(col == a, 1.0, 0.0).astype(BF16)
        for part in split3(sums[a]):
            total = total + lax.dot_general(part, pick, NN, preferred_element_type=F32)
    force = jnp.where(good, 24.0 * jnp.transpose(total)[0:3], 0.0)
    pos_ref[...] = srt_ref[0:3, 0:n]
    frc_ref[...] = force[:, 0:n]
    vel_ref[...] = (srt_ref[3:6] + (0.5 * DT) * force)[:, 0:n]
    id_ref[...] = jnp.reshape((srt_ref[6:7].astype(I32) * 65536 + srt_ref[7:8].astype(I32))[:, 0:n], (n,))
    ok_ref[...] = jnp.reshape(okrow[:, 0:n].astype(I32), (n,))


def total_kernel(sizes, part_ref, sum_ref, rows, ssem, rsem):
    size_x, size_y, size_z = sizes
    me = (lax.axis_index("x"), lax.axis_index("y"), lax.axis_index("z"))
    mine = (me[2] * size_y + me[1]) * size_x + me[0]
    others = [(dx, dy, dz) for dz in range(size_z) for dy in range(size_y) for dx in range(size_x) if dx + dy + dz > 0]

    def device_at(offset):
        return (lax.rem(me[2] + offset[2], size_z), lax.rem(me[1] + offset[1], size_y), lax.rem(me[0] + offset[0], size_x))

    barrier = pltpu.get_barrier_semaphore()
    for offset in others:
        pl.semaphore_signal(barrier, inc=1, device_id=device_at(offset), device_id_type=pl.DeviceIdType.MESH)
    rows[pl.ds(mine, 1)] = part_ref[...]
    pl.semaphore_wait(barrier, len(others))
    copies = []
    for index, offset in enumerate(others):
        copy = pltpu.make_async_remote_copy(
            src_ref=part_ref, dst_ref=rows.at[pl.ds(mine, 1)], send_sem=ssem.at[index], recv_sem=rsem.at[index],
            device_id=device_at(offset), device_id_type=pl.DeviceIdType.MESH)
        copy.start()
        copies.append(copy)
    for copy in copies:
        copy.wait_recv()
    sum_ref[0, 0] = jnp.sum(rows[...])
    for copy in copies:
        copy.wait_send()


def solution(mesh):
    sizes = (mesh.shape["x"], mesh.shape["y"], mesh.shape["z"])
    peers = sorted({(d[0] % sizes[0], d[1] % sizes[1], d[2] % sizes[2]) for d in DIRS} - {(0, 0, 0)})
    devices = sizes[0] * sizes[1] * sizes[2]

    def local_step(atom_pos, atom_vel, atom_frc, atom_id, atom_ok, brick_side):
        n = atom_pos.shape[0]
        slots = -(-n // L) * L
        side = jnp.reshape(brick_side, (1, 1))
        vmem = pl.BlockSpec(memory_space=pltpu.VMEM)
        smem = pl.BlockSpec(memory_space=pltpu.SMEM)
        srt, ghosts, fresh, own, inner, inner_en = pl.pallas_call(
            functools.partial(exchange_kernel, sizes, peers, slots),
            out_shape=(jax.ShapeDtypeStruct((16, slots), F32), jax.ShapeDtypeStruct((len(peers), 4, slots), F32), jax.ShapeDtypeStruct((len(peers), 4, NEW), F32),
                       jax.ShapeDtypeStruct((slots, 3 * L), F32), jax.ShapeDtypeStruct((3, slots, L), F32), jax.ShapeDtypeStruct((8, L), F32)),
            in_specs=[pl.BlockSpec(memory_space=pltpu.HBM)] * 5 + [smem],
            out_specs=(vmem,) * 6,
            scratch_shapes=[
                pltpu.VMEM((3, n), F32), pltpu.VMEM((3, n), F32), pltpu.VMEM((3, n), F32), pltpu.VMEM((n,), I32), pltpu.VMEM((n,), I32),
                pltpu.VMEM((32, L), F32), pltpu.VMEM((26, L), F32), pltpu.VMEM((3, 4, slots), F32), pltpu.VMEM((3, 4, NEW), F32), pltpu.VMEM((3, 8, slots), F32),
                pltpu.SemaphoreType.DMA((5,)), pltpu.SemaphoreType.DMA((26,)), pltpu.SemaphoreType.DMA((26,)),
            ] + [pltpu.SemaphoreType.DMA((len(peers),))] * 4,
            compiler_params=pltpu.CompilerParams(collective_id=0, has_side_effects=True, vmem_limit_bytes=40 * 2 ** 20),
            name="exchange",
        )(*[pltpu.with_memory_space_constraint(v, pltpu.HBM) for v in (atom_pos.T, atom_vel.T, atom_frc.T, atom_id, atom_ok)], side)
        offs = jnp.concatenate([ghosts[:, 3, 0:32], fresh[:, 3, 0:32]], axis=0).astype(I32)
        out_f = jax.ShapeDtypeStruct((3, n), F32)
        out_i = jax.ShapeDtypeStruct((n,), I32)
        new_pos, new_vel, new_frc, new_id, new_ok, energy = pl.pallas_call(
            functools.partial(force_kernel, sizes, peers, slots),
            out_shape=(out_f, out_f, out_f, out_i, out_i, jax.ShapeDtypeStruct((1, L), F32)),
            in_specs=[vmem] * 6 + [smem] * 2,
            out_specs=(vmem,) * 6,
            scratch_shapes=[pltpu.VMEM((8, 28 * slots + CHUNK * L), F32), pltpu.VMEM((3, 8, 28 * slots + CHUNK * L), F32), pltpu.VMEM((3, slots, L), F32)],
            compiler_params=pltpu.CompilerParams(vmem_limit_bytes=40 * 2 ** 20),
            name="forces",
        )(srt, ghosts, fresh, own, inner, inner_en, offs, side)
        energy = pl.pallas_call(
            functools.partial(total_kernel, sizes),
            out_shape=jax.ShapeDtypeStruct((1, 1), F32),
            in_specs=[vmem],
            out_specs=smem,
            scratch_shapes=[pltpu.VMEM((devices, L), F32), pltpu.SemaphoreType.DMA((devices,)), pltpu.SemaphoreType.DMA((devices,))],
            compiler_params=pltpu.CompilerParams(collective_id=1, has_side_effects=True),
            name="total",
        )(pltpu.with_memory_space_constraint(energy, pltpu.VMEM))[0, 0]
        return new_pos.T, new_vel.T, new_frc.T, new_id, new_ok, energy

    row_spec = P(MESH_AXES, None)
    id_spec = P(MESH_AXES)
    return jax.shard_map(local_step, mesh=mesh, in_specs=(row_spec, row_spec, row_spec, id_spec, id_spec, P()), out_specs=(row_spec, row_spec, row_spec, id_spec, id_spec, P()), check_vma=False)
```

```python
import functools

import jax
import jax.numpy as jnp
from jax import lax
from jax.experimental import pallas as pl
from jax.experimental.pallas import tpu as pltpu
from jax.sharding import PartitionSpec as P

DT = 0.005
RC = 2.5
FAR = 1.0e6
UCUT = 4.0 * (RC ** -12 - RC ** -6)
UPC = -48.0 * RC ** -13 + 24.0 * RC ** -7
MESH_AXES = ("z", "y", "x")
DIRS = [(dx, dy, dz) for dz in (-1, 0, 1) for dy in (-1, 0, 1) for dx in (-1, 0, 1) if (dx, dy, dz) != (0, 0, 0)]
NEAR = RC + 1.0e-3
MAJOR = ((2, 1, 0), (1, 0, 2), (0, 2, 1))
PACK = 8
NEW = 256
CHUNK = 3
GROUPS = 8
L = 128
TILE = (8, L)
F32 = jnp.float32
BF16 = jnp.bfloat16
I32 = jnp.int32
NT = (((1,), (1,)), ((), ()))
NN = (((1,), (0,)), ((), ()))


def order_of(d):
    if d[2] == 0:
        return 1 if d[1] != 0 else 2
    return 2 if (d[1] == 0 and d[0] != 0) else 0


def range_of(d):
    first, size = 0, 27
    for axis in MAJOR[order_of(d)]:
        if d[axis] == 0:
            break
        size = size // 3
        first = first + (1, 0, 2)[d[axis]] * size
    return first, first + size


def split3(x):
    hi = x.astype(BF16)
    rest = x - hi.astype(F32)
    mid = rest.astype(BF16)
    low = (rest - mid.astype(F32)).astype(BF16)
    return hi, mid, low


def onehot_rows(dest, base, count):
    rows = lax.broadcasted_iota(I32, (count, dest.shape[1]), 0) + base
    return jnp.where(rows == dest, 1.0, 0.0).astype(BF16)


def scatter_lanes(data, dest, slots):
    rows = data.shape[0]
    parts = jnp.concatenate(split3(data), axis=0)
    out = []
    for base in range(0, slots, 256):
        hot = onehot_rows(dest, base, min(256, slots - base))
        got = lax.dot_general(parts, hot, NT, preferred_element_type=F32)
        out.append(got[0:rows] + got[rows:2 * rows] + got[2 * rows:3 * rows])
    return jnp.concatenate(out, axis=1)


def class_places(code, with_before):
    width = code.shape[1]
    tiles = width // L
    cls = lax.broadcasted_iota(I32, (32, width), 0)
    member = jnp.where(cls == code, 1.0, 0.0)
    member_b = member.astype(BF16)
    stacked = jnp.concatenate([member_b[:, t * L:(t + 1) * L] for t in range(tiles)], axis=0)
    row_i = lax.broadcasted_iota(I32, (L, 256), 0)
    col_i = lax.broadcasted_iota(I32, (L, 256), 1)
    tri = jnp.where((row_i < col_i) | (col_i >= L), 1.0, 0.0).astype(BF16)
    pre = lax.dot_general(stacked, tri, NN, preferred_element_type=F32)
    carry = jnp.zeros((32, L), F32)
    if with_before:
        before_b = jnp.where(code < cls, 1.0, 0.0).astype(BF16)
        before_s = before_b[:, 0:L]
        tot = None
        ones = jnp.ones((L, L), BF16)
        for t in range(tiles):
            part = lax.dot_general(before_b[:, t * L:(t + 1) * L], ones, NN, preferred_element_type=F32)
            tot = part if tot is None else tot + part
        before = tot
        carry = before
    else:
        before = None
    places = []
    for t in range(tiles):
        within = pre[32 * t:32 * t + 32, 0:L] + carry
        places.append(jnp.sum(member[:, t * L:(t + 1) * L] * within, axis=0, keepdims=True))
        carry = carry + pre[32 * t:32 * t + 32, L:256]
    return jnp.concatenate(places, axis=1), before


def pad_lanes(x, width):
    return jnp.concatenate([x, jnp.zeros((x.shape[0], width - x.shape[1]), x.dtype)], axis=1)


def pair_loop(own_cols, near_lanes, q, first, last, with_self, carry):
    rows = [step_rows(q, g) for g in range(GROUPS)]
    own = [[own_cols[rows[g], a * L:(a + 1) * L] for a in range(3)] for g in range(GROUPS)]

    def body(c, carry):
        force, en = [list(f) for f in carry[0]], carry[1]
        for t in range(CHUNK):
            place = pl.ds(pl.multiple_of((c * CHUNK + t) * L, L), L)
            near_xyz = [near_lanes[a, :, place] for a in range(3)]
            for g in range(GROUPS):
                dx, dy, dz = [own[g][a] - near_xyz[a] for a in range(3)]
                d2 = dx * dx + dy * dy + dz * dz
                near = d2 < RC * RC
                if with_self:
                    near = near & (d2 > 0.0)
                inv = jnp.where(near, lax.rsqrt(d2), 0.0)
                s2 = inv * inv
                s6 = s2 * s2 * s2
                s12 = s6 * s6
                p = s12 - s6
                w = inv * (UPC / 24.0)
                scale = (p + s12) * s2 + w
                en = en + ((p + jnp.where(near, 0.25 * (RC * UPC - UCUT), 0.0)) - 6.0 * (w * d2))
                force[g] = [force[g][0] + scale * dx, force[g][1] + scale * dy, force[g][2] + scale * dz]
        return tuple(tuple(f) for f in force), en

    return lax.fori_loop(first, last, body, carry)


def step_rows(q, g):
    return pl.ds(pl.multiple_of((q * GROUPS + g) * 8, 8), 8)


def own_columns(xyz):
    slots = xyz.shape[1]
    parts = [part.astype(F32) for part in split3(xyz)]
    parts = jnp.concatenate(parts + [jnp.zeros((7, slots), F32)], axis=0)
    row = lax.broadcasted_iota(I32, (16, 3 * L), 0)
    tile = lax.broadcasted_iota(I32, (16, 3 * L), 1) // L
    picks = jnp.where((row == tile) | (row == tile + 3) | (row == tile + 6), 1.0, 0.0).astype(BF16)
    return lax.dot_general(jnp.transpose(parts).astype(BF16), picks, NN, preferred_element_type=F32)


def exchange_kernel(sizes, peers, slots, pos_hbm, vel_hbm, frc_hbm, id_hbm, ok_hbm, side_ref, srt_ref, gh_ref, ga_ref, own_ref, inner_ref, inner_en_ref, pos_ref, vel_ref, frc_ref, id_ref, ok_ref, pkt, rcv, out3, new3, lanes, isem, psend, precv, gsend, grecv, asend, arecv):
    size_x, size_y, size_z = sizes
    me = (lax.axis_index("x"), lax.axis_index("y"), lax.axis_index("z"))

    def device_at(offset):
        return (lax.rem(me[2] + offset[2], size_z), lax.rem(me[1] + offset[1], size_y), lax.rem(me[0] + offset[0], size_x))

    loads = []
    for index, (src, dst) in enumerate(((ok_hbm, ok_ref), (id_hbm, id_ref), (pos_hbm, pos_ref), (vel_hbm, vel_ref), (frc_hbm, frc_ref))):
        load = pltpu.make_async_copy(src, dst, isem.at[index])
        load.start()
        loads.append(load)
    barrier = pltpu.get_barrier_semaphore()
    for offset in peers:
        pl.semaphore_signal(barrier, inc=1, device_id=device_at(offset), device_id_type=pl.DeviceIdType.MESH)

    n = pos_ref.shape[1]
    side = side_ref[0, 0]
    for load in loads:
        load.wait()
    owned = pad_lanes(jnp.reshape(ok_ref[...], (1, n)), slots) > 0
    half = vel_ref[...] + (0.5 * DT) * frc_ref[...]
    free = pos_ref[...] + DT * half
    half = pad_lanes(half, slots)
    free = pad_lanes(free, slots)
    ids = pad_lanes(jnp.reshape(id_ref[...], (1, n)), slots)
    code = jnp.zeros((1, slots), I32)
    moved = []
    low_side = []
    for axis in range(3):
        low = me[axis].astype(F32) * side
        high = (me[axis] + 1).astype(F32) * side
        box = side * float(sizes[axis])
        u = free[axis:axis + 1]
        step = jnp.where(u >= high, 1, 0) - jnp.where(u < low, 1, 0)
        code = code + (step + 1) * (1, 3, 9)[axis]
        moved.append(jnp.where(u < 0.0, u + box, jnp.where(u >= box, u - box, u)))
        low_side.append(low)
    code = jnp.where(owned, code, 31)
    id_hi = (ids >> 16).astype(F32)
    id_lo = (ids & 65535).astype(F32)
    okf = jnp.where(owned, 1.0, 0.0)
    data = jnp.concatenate(moved + [half, id_hi, id_lo, okf, jnp.zeros((7, slots), F32)], axis=0)

    place, _ = class_places(code, False)
    leaving = owned & (code != 13)
    way = jnp.where(leaving, code - jnp.where(code > 13, 1, 0), 31)
    member = jnp.where(lax.broadcasted_iota(I32, (32, slots), 0) == way, 1.0, 0.0).astype(BF16)
    fields = jnp.concatenate([jnp.where(place == float(k), data, 0.0) for k in range(PACK)], axis=0)
    packed = jnp.zeros((32, L), F32)
    for part in split3(fields):
        packed = packed + lax.dot_general(member, part, NT, preferred_element_type=F32)
    pkt[...] = packed

    def bins_of(pos):
        bins = []
        for axis in range(3):
            loc = pos[axis:axis + 1] - low_side[axis]
            bins.append(jnp.where(loc < NEAR, 0, jnp.where(loc > side - NEAR, 2, 1)))
        return [(bins[i] * 3 + bins[j]) * 3 + bins[k] for i, j, k in MAJOR]

    eye = lax.broadcasted_iota(I32, (32, L), 0) == lax.broadcasted_iota(I32, (32, L), 1)

    def sorted_block(cand, keys, kept):
        width = cand.shape[1]
        where_to, before = class_places(jnp.where(kept, keys, 28), True)
        arranged = scatter_lanes(cand, jnp.where(kept, where_to.astype(I32), -1), width)
        total = jnp.concatenate([before[27:28]] * (width // L), axis=1)
        lane = lax.broadcasted_iota(I32, (1, width), 1).astype(F32)
        counts = jnp.sum(jnp.where(eye, before, 0.0), axis=0, keepdims=True)
        return jnp.concatenate([jnp.where(lane < total, arranged[0:3], FAR), pad_lanes(counts, width)], axis=0)

    sent = []

    def send(src, dst, ssem, rsem, offset):
        copy = pltpu.make_async_remote_copy(
            src_ref=src, dst_ref=dst, send_sem=ssem, recv_sem=rsem,
            device_id=device_at(offset), device_id_type=pl.DeviceIdType.MESH)
        copy.start()
        sent.append(copy)
        return copy

    def send_blocks(block, dst, ssem, rsem, kind):
        out = []
        for index, offset in enumerate(peers):
            if order_of(tuple(0 if c == 0 else 1 for c in offset)) == kind:
                out.append(send(block.at[kind], dst.at[index], ssem.at[index], rsem.at[index], offset))
        return out

    staying = code == 13
    keys = bins_of(data)
    for kind in range(3):
        out3[kind] = sorted_block(data[0:8], keys[kind], staying)
    pl.semaphore_wait(barrier, len(peers))
    packets = []
    for index, d in enumerate(DIRS):
        row = pl.ds(index, 1)
        packets.append(send(pkt.at[row], rcv.at[row], psend.at[index], precv.at[index], (d[0] % size_x, d[1] % size_y, d[2] % size_z)))
    blocks = []
    for kind in range(3):
        blocks = blocks + send_blocks(out3, gh_ref, gsend, grecv, kind)
    for copy in packets:
        copy.wait_recv()

    came = jnp.concatenate([rcv[...], jnp.zeros((32 - 26, L), F32)], axis=0)
    came = jnp.concatenate([came] + [pltpu.roll(came, L - 16 * k, 1) for k in range(1, PACK)], axis=0)
    came_t = jnp.transpose(came)[0:16]
    came_ok = came_t[8:9] > 0.5
    keys = bins_of(came_t)
    late = []
    for kind in range(3):
        new3[kind] = sorted_block(came_t[0:8], keys[kind], came_ok)
        late = late + send_blocks(new3, ga_ref, asend, arecv, kind)
    for copy in blocks:
        copy.wait_recv()

    arr_ids = came[:, 6:7].astype(I32) * 65536 + came[:, 7:8].astype(I32)
    arr_ok = came[:, 8:9] > 0.5
    row_ids = jnp.concatenate([ids, came_t[6:7].astype(I32) * 65536 + came_t[7:8].astype(I32)], axis=1)
    less = jnp.where((arr_ids < row_ids) & arr_ok, 1.0, 0.0)
    arrivals_below = jnp.sum(less, axis=0, keepdims=True)
    above = jnp.where((arr_ids > row_ids[:, 0:slots]) & staying, 1.0, 0.0).astype(BF16)
    stay_below = lax.dot_general(jnp.ones((16, slots), BF16), above, NT, preferred_element_type=F32)[0:1]
    stay_place, _ = class_places(jnp.where(staying, 0, 31), False)
    rank = jnp.concatenate([stay_place, stay_below], axis=1) + arrivals_below
    dest = jnp.where(jnp.concatenate([staying, came_ok], axis=1), rank.astype(I32), -1)
    merged = scatter_lanes(jnp.concatenate([data, came_t], axis=1), dest, slots)
    srt_ref[...] = merged

    good = merged[8:9] > 0.5
    own_ref[...] = own_columns(jnp.where(good, merged[0:3], -FAR))
    first = CHUNK * L
    for a in range(3):
        lanes[a] = jnp.broadcast_to(jnp.where(good, merged[a:a + 1], FAR)[:, 0:first], (8, first))
    zero = jnp.zeros(TILE, F32)

    def own_step(q, energy):
        force, energy = pair_loop(own_ref, lanes, q, 0, 1, True, (((zero,) * 3,) * GROUPS, energy))
        for g in range(GROUPS):
            for a in range(3):
                inner_ref[a, step_rows(q, g), :] = force[g][a]
        return energy

    inner_en_ref[...] = lax.fori_loop(0, slots // (8 * GROUPS), own_step, zero)

    for copy in late:
        copy.wait_recv()
    for copy in sent:
        copy.wait_send()


def force_kernel(sizes, peers, slots, srt_ref, gh_ref, ga_ref, own_cols, inner_ref, inner_en_ref, offs_ref, side_ref, pos_ref, vel_ref, frc_ref, id_ref, ok_ref, en_ref, line, wide_line, sums):
    size_x, size_y, size_z = sizes
    me = (lax.axis_index("x"), lax.axis_index("y"), lax.axis_index("z"))
    n = pos_ref.shape[1]
    side = side_ref[0, 0]
    okrow = srt_ref[8:9]
    good = okrow > 0.5
    count = jnp.sum(okrow).astype(I32)
    spread = side > 2.0 * NEAR
    span = slots + L

    away = jnp.full(TILE, FAR, F32)
    first = CHUNK * L
    line[:, 0:slots - first] = jnp.concatenate([jnp.where(good, srt_ref[0:3], FAR), jnp.full((5, slots), FAR, F32)], axis=0)[:, first:]
    lane = lax.broadcasted_iota(I32, (8, span), 1)
    fill = jnp.maximum(count - first, 0)
    for d in DIRS:
        offset = (d[0] % size_x, d[1] % size_y, d[2] % size_z)
        back = ((-offset[0]) % size_x, (-offset[1]) % size_y, (-offset[2]) % size_z)
        index = peers.index(back)
        low, high = range_of(d)
        shifts = []
        for axis in range(3):
            box = side * float(sizes[axis])
            if d[axis] == 1:
                shifts.append(jnp.where(me[axis] == sizes[axis] - 1, box, 0.0))
            elif d[axis] == -1:
                shifts.append(jnp.where(me[axis] == 0, -box, 0.0))
            else:
                shifts.append(jnp.float32(0.0))
        for source, entry in ((gh_ref, index), (ga_ref, index + len(peers))):
            width = source.shape[2]
            begin = jnp.where(spread, offs_ref[entry, low], 0)
            end = jnp.where(spread, offs_ref[entry, high], offs_ref[entry, 27])
            block = jnp.concatenate([source[index, a:a + 1] + shifts[a] for a in range(3)] + [jnp.zeros((5, width), F32)], axis=0)
            block = jnp.concatenate([block, away], axis=1)
            head = fill & (L - 1)
            base = pl.multiple_of(fill - head, L)
            move = head - begin
            block = pltpu.roll(block, jnp.where(move < 0, move + (width + L), move), 1)
            block = jnp.where(lane[:, 0:width + L] < head + end - begin, block, FAR)
            line[:, pl.ds(base, L)] = jnp.where(lane[:, 0:L] < head, line[:, pl.ds(base, L)], block[:, 0:L])
            line[:, pl.ds(pl.multiple_of(base + L, L), width)] = block[:, L:]
            fill = fill + (end - begin)
    rest = pl.multiple_of(((fill + L - 1) // L) * L, L)
    line[:, pl.ds(rest, CHUNK * L)] = jnp.full((8, CHUNK * L), FAR, F32)
    chunks = jnp.maximum((fill + CHUNK * L - 1) // (CHUNK * L), 1)

    def widen(c, carry):
        for t in range(CHUNK):
            place = pl.ds(pl.multiple_of((c * CHUNK + t) * L, L), L)
            tile = line[:, place]
            for a in range(3):
                wide_line[a, :, place] = jnp.broadcast_to(tile[a:a + 1], TILE)
        return carry

    lax.fori_loop(0, chunks, widen, 0)

    def own_step(q, energy):
        start = tuple(tuple(inner_ref[a, step_rows(q, g), :] for a in range(3)) for g in range(GROUPS))
        carry = pair_loop(own_cols, wide_line, q, 0, 1, True, (start, energy))
        force, energy = pair_loop(own_cols, wide_line, q, 1, chunks, False, carry)
        for g in range(GROUPS):
            for a in range(3):
                sums[a, step_rows(q, g), :] = force[g][a]
        return energy

    own_steps = (count + 8 * GROUPS - 1) // (8 * GROUPS)
    energy = lax.fori_loop(0, own_steps, own_step, inner_en_ref[...])
    en_ref[...] = 2.0 * jnp.sum(energy, axis=0, keepdims=True)

    col = lax.broadcasted_iota(I32, (L, L), 1)
    total = jnp.zeros((slots, L), F32)
    for a in range(3):
        pick = jnp.where(col == a, 1.0, 0.0).astype(BF16)
        for part in split3(sums[a]):
            total = total + lax.dot_general(part, pick, NN, preferred_element_type=F32)
    force = jnp.where(good, 24.0 * jnp.transpose(total)[0:3], 0.0)
    pos_ref[...] = srt_ref[0:3, 0:n]
    frc_ref[...] = force[:, 0:n]
    vel_ref[...] = (srt_ref[3:6] + (0.5 * DT) * force)[:, 0:n]
    id_ref[...] = jnp.reshape((srt_ref[6:7].astype(I32) * 65536 + srt_ref[7:8].astype(I32))[:, 0:n], (n,))
    ok_ref[...] = jnp.reshape(okrow[:, 0:n].astype(I32), (n,))


def total_kernel(sizes, part_ref, sum_ref, rows, ssem, rsem):
    size_x, size_y, size_z = sizes
    me = (lax.axis_index("x"), lax.axis_index("y"), lax.axis_index("z"))
    mine = (me[2] * size_y + me[1]) * size_x + me[0]
    others = [(dx, dy, dz) for dz in range(size_z) for dy in range(size_y) for dx in range(size_x) if dx + dy + dz > 0]

    def device_at(offset):
        return (lax.rem(me[2] + offset[2], size_z), lax.rem(me[1] + offset[1], size_y), lax.rem(me[0] + offset[0], size_x))

    barrier = pltpu.get_barrier_semaphore()
    for offset in others:
        pl.semaphore_signal(barrier, inc=1, device_id=device_at(offset), device_id_type=pl.DeviceIdType.MESH)
    rows[pl.ds(mine, 1)] = part_ref[...]
    pl.semaphore_wait(barrier, len(others))
    copies = []
    for index, offset in enumerate(others):
        copy = pltpu.make_async_remote_copy(
            src_ref=part_ref, dst_ref=rows.at[pl.ds(mine, 1)], send_sem=ssem.at[index], recv_sem=rsem.at[index],
            device_id=device_at(offset), device_id_type=pl.DeviceIdType.MESH)
        copy.start()
        copies.append(copy)
    for copy in copies:
        copy.wait_recv()
    sum_ref[0, 0] = jnp.sum(rows[...])
    for copy in copies:
        copy.wait_send()


def solution(mesh):
    sizes = (mesh.shape["x"], mesh.shape["y"], mesh.shape["z"])
    peers = sorted({(d[0] % sizes[0], d[1] % sizes[1], d[2] % sizes[2]) for d in DIRS} - {(0, 0, 0)})
    devices = sizes[0] * sizes[1] * sizes[2]

    def local_step(atom_pos, atom_vel, atom_frc, atom_id, atom_ok, brick_side):
        n = atom_pos.shape[0]
        slots = -(-n // L) * L
        side = jnp.reshape(brick_side, (1, 1))
        vmem = pl.BlockSpec(memory_space=pltpu.VMEM)
        smem = pl.BlockSpec(memory_space=pltpu.SMEM)
        srt, ghosts, fresh, own, inner, inner_en = pl.pallas_call(
            functools.partial(exchange_kernel, sizes, peers, slots),
            out_shape=(jax.ShapeDtypeStruct((16, slots), F32), jax.ShapeDtypeStruct((len(peers), 4, slots), F32), jax.ShapeDtypeStruct((len(peers), 4, NEW), F32),
                       jax.ShapeDtypeStruct((slots, 3 * L), F32), jax.ShapeDtypeStruct((3, slots, L), F32), jax.ShapeDtypeStruct(TILE, F32)),
            in_specs=[pl.BlockSpec(memory_space=pltpu.HBM)] * 5 + [smem],
            out_specs=(vmem,) * 6,
            scratch_shapes=[
                pltpu.VMEM((3, n), F32), pltpu.VMEM((3, n), F32), pltpu.VMEM((3, n), F32), pltpu.VMEM((n,), I32), pltpu.VMEM((n,), I32),
                pltpu.VMEM((32, L), F32), pltpu.VMEM((26, L), F32), pltpu.VMEM((3, 4, slots), F32), pltpu.VMEM((3, 4, NEW), F32), pltpu.VMEM((3, 8, CHUNK * L), F32),
                pltpu.SemaphoreType.DMA((5,)), pltpu.SemaphoreType.DMA((26,)), pltpu.SemaphoreType.DMA((26,)),
            ] + [pltpu.SemaphoreType.DMA((len(peers),))] * 4,
            compiler_params=pltpu.CompilerParams(collective_id=0, has_side_effects=True, vmem_limit_bytes=40 * 2 ** 20),
            name="exchange",
        )(*[pltpu.with_memory_space_constraint(v, pltpu.HBM) for v in (atom_pos.T, atom_vel.T, atom_frc.T, atom_id, atom_ok)], side)
        offs = jnp.concatenate([ghosts[:, 3, 0:32], fresh[:, 3, 0:32]], axis=0).astype(I32)
        out_f = jax.ShapeDtypeStruct((3, n), F32)
        out_i = jax.ShapeDtypeStruct((n,), I32)
        new_pos, new_vel, new_frc, new_id, new_ok, energy = pl.pallas_call(
            functools.partial(force_kernel, sizes, peers, slots),
            out_shape=(out_f, out_f, out_f, out_i, out_i, jax.ShapeDtypeStruct((1, L), F32)),
            in_specs=[vmem] * 6 + [smem] * 2,
            out_specs=(vmem,) * 6,
            scratch_shapes=[pltpu.VMEM((8, 28 * slots + CHUNK * L), F32), pltpu.VMEM((3, 8, 28 * slots + CHUNK * L), F32), pltpu.VMEM((3, slots, L), F32)],
            compiler_params=pltpu.CompilerParams(vmem_limit_bytes=40 * 2 ** 20),
            name="forces",
        )(srt, ghosts, fresh, own, inner, inner_en, offs, side)
        energy = pl.pallas_call(
            functools.partial(total_kernel, sizes),
            out_shape=jax.ShapeDtypeStruct((1, 1), F32),
            in_specs=[vmem],
            out_specs=smem,
            scratch_shapes=[pltpu.VMEM((devices, L), F32), pltpu.SemaphoreType.DMA((devices,)), pltpu.SemaphoreType.DMA((devices,))],
            compiler_params=pltpu.CompilerParams(collective_id=1, has_side_effects=True),
            name="total",
        )(pltpu.with_memory_space_constraint(energy, pltpu.VMEM))[0, 0]
        return new_pos.T, new_vel.T, new_frc.T, new_id, new_ok, energy

    row_spec = P(MESH_AXES, None)
    id_spec = P(MESH_AXES)
    return jax.shard_map(local_step, mesh=mesh, in_specs=(row_spec, row_spec, row_spec, id_spec, id_spec, P()), out_specs=(row_spec, row_spec, row_spec, id_spec, id_spec, P()), check_vma=False)
```

```python
import functools

import jax
import jax.numpy as jnp
from jax import lax
from jax.experimental import pallas as pl
from jax.experimental.pallas import tpu as pltpu
from jax.sharding import PartitionSpec as P

DT = 0.005
RC = 2.5
FAR = 1.0e6
UCUT = 4.0 * (RC ** -12 - RC ** -6)
UPC = -48.0 * RC ** -13 + 24.0 * RC ** -7
MESH_AXES = ("z", "y", "x")
DIRS = [(dx, dy, dz) for dz in (-1, 0, 1) for dy in (-1, 0, 1) for dx in (-1, 0, 1) if (dx, dy, dz) != (0, 0, 0)]
NEAR = RC + 1.0e-3
MAJOR = ((2, 1, 0), (1, 0, 2), (0, 2, 1))
PACK = 8
NEW = 256
CHUNK = 3
GROUPS = 8
L = 128
TILE = (8, L)
F32 = jnp.float32
BF16 = jnp.bfloat16
I32 = jnp.int32
NT = (((1,), (1,)), ((), ()))
NN = (((1,), (0,)), ((), ()))


def order_of(d):
    if d[2] == 0:
        return 1 if d[1] != 0 else 2
    return 2 if (d[1] == 0 and d[0] != 0) else 0


def range_of(d):
    first, size = 0, 27
    for axis in MAJOR[order_of(d)]:
        if d[axis] == 0:
            break
        size = size // 3
        first = first + (1, 0, 2)[d[axis]] * size
    return first, first + size


def split3(x):
    hi = x.astype(BF16)
    rest = x - hi.astype(F32)
    mid = rest.astype(BF16)
    low = (rest - mid.astype(F32)).astype(BF16)
    return hi, mid, low


def onehot_rows(dest, base, count):
    rows = lax.broadcasted_iota(I32, (count, dest.shape[1]), 0) + base
    return jnp.where(rows == dest, 1.0, 0.0).astype(BF16)


def scatter_lanes(data, dest, slots):
    rows = data.shape[0]
    parts = jnp.concatenate(split3(data), axis=0)
    out = []
    for base in range(0, slots, 256):
        hot = onehot_rows(dest, base, min(256, slots - base))
        got = lax.dot_general(parts, hot, NT, preferred_element_type=F32)
        out.append(got[0:rows] + got[rows:2 * rows] + got[2 * rows:3 * rows])
    return jnp.concatenate(out, axis=1)


def class_places(code, with_before):
    width = code.shape[1]
    tiles = width // L
    cls = lax.broadcasted_iota(I32, (32, width), 0)
    member = jnp.where(cls == code, 1.0, 0.0)
    member_b = member.astype(BF16)
    stacked = jnp.concatenate([member_b[:, t * L:(t + 1) * L] for t in range(tiles)], axis=0)
    row_i = lax.broadcasted_iota(I32, (L, 256), 0)
    col_i = lax.broadcasted_iota(I32, (L, 256), 1)
    tri = jnp.where((row_i < col_i) | (col_i >= L), 1.0, 0.0).astype(BF16)
    pre = lax.dot_general(stacked, tri, NN, preferred_element_type=F32)
    carry = jnp.zeros((32, L), F32)
    if with_before:
        before_b = jnp.where(code < cls, 1.0, 0.0).astype(BF16)
        before_s = before_b[:, 0:L]
        tot = None
        ones = jnp.ones((L, L), BF16)
        for t in range(tiles):
            part = lax.dot_general(before_b[:, t * L:(t + 1) * L], ones, NN, preferred_element_type=F32)
            tot = part if tot is None else tot + part
        before = tot
        carry = before
    else:
        before = None
    places = []
    for t in range(tiles):
        within = pre[32 * t:32 * t + 32, 0:L] + carry
        places.append(jnp.sum(member[:, t * L:(t + 1) * L] * within, axis=0, keepdims=True))
        carry = carry + pre[32 * t:32 * t + 32, L:256]
    return jnp.concatenate(places, axis=1), before


def pad_lanes(x, width):
    return jnp.concatenate([x, jnp.zeros((x.shape[0], width - x.shape[1]), x.dtype)], axis=1)


def pair_loop(own_cols, near_lanes, q, first, last, with_self, carry):
    rows = [step_rows(q, g) for g in range(GROUPS)]
    own = [[own_cols[rows[g], a * L:(a + 1) * L] for a in range(3)] for g in range(GROUPS)]

    def body(c, carry):
        force, en = [list(f) for f in carry[0]], carry[1]
        for t in range(CHUNK):
            place = pl.ds(pl.multiple_of((c * CHUNK + t) * L, L), L)
            near_xyz = [near_lanes[a, :, place] for a in range(3)]
            for g in range(GROUPS):
                dx, dy, dz = [own[g][a] - near_xyz[a] for a in range(3)]
                d2 = dx * dx + dy * dy + dz * dz
                near = d2 < RC * RC
                if with_self:
                    near = near & (d2 > 0.0)
                inv = jnp.where(near, lax.rsqrt(d2), 0.0)
                s2 = inv * inv
                s6 = s2 * s2 * s2
                s12 = s6 * s6
                p = s12 - s6
                w = inv * (UPC / 24.0)
                scale = (p + s12) * s2 + w
                en = en + ((p + jnp.where(near, 0.25 * (RC * UPC - UCUT), 0.0)) - 6.0 * (w * d2))
                force[g] = [force[g][0] + scale * dx, force[g][1] + scale * dy, force[g][2] + scale * dz]
        return tuple(tuple(f) for f in force), en

    return lax.fori_loop(first, last, body, carry)


def step_rows(q, g):
    return pl.ds(pl.multiple_of((q * GROUPS + g) * 8, 8), 8)


def own_columns(xyz):
    slots = xyz.shape[1]
    parts = [part.astype(F32) for part in split3(xyz)]
    parts = jnp.concatenate(parts + [jnp.zeros((7, slots), F32)], axis=0)
    row = lax.broadcasted_iota(I32, (16, 3 * L), 0)
    tile = lax.broadcasted_iota(I32, (16, 3 * L), 1) // L
    picks = jnp.where((row == tile) | (row == tile + 3) | (row == tile + 6), 1.0, 0.0).astype(BF16)
    return lax.dot_general(jnp.transpose(parts).astype(BF16), picks, NN, preferred_element_type=F32)


def exchange_kernel(sizes, peers, slots, pos_hbm, vel_hbm, frc_hbm, id_hbm, ok_hbm, side_ref, srt_ref, gh_ref, ga_ref, own_ref, inner_ref, inner_en_ref, pos_ref, vel_ref, frc_ref, id_ref, ok_ref, pkt, rcv, out3, new3, lanes, isem, psend, precv, gsend, grecv, asend, arecv):
    size_x, size_y, size_z = sizes
    me = (lax.axis_index("x"), lax.axis_index("y"), lax.axis_index("z"))

    def device_at(offset):
        return (lax.rem(me[2] + offset[2], size_z), lax.rem(me[1] + offset[1], size_y), lax.rem(me[0] + offset[0], size_x))

    loads = []
    for index, (src, dst) in enumerate(((ok_hbm, ok_ref), (id_hbm, id_ref), (pos_hbm, pos_ref), (vel_hbm, vel_ref), (frc_hbm, frc_ref))):
        load = pltpu.make_async_copy(src, dst, isem.at[index])
        load.start()
        loads.append(load)
    barrier = pltpu.get_barrier_semaphore()
    for offset in peers:
        pl.semaphore_signal(barrier, inc=1, device_id=device_at(offset), device_id_type=pl.DeviceIdType.MESH)

    n = pos_ref.shape[1]
    side = side_ref[0, 0]
    for load in loads:
        load.wait()
    owned = pad_lanes(jnp.reshape(ok_ref[...], (1, n)), slots) > 0
    half = vel_ref[...] + (0.5 * DT) * frc_ref[...]
    free = pos_ref[...] + DT * half
    half = pad_lanes(half, slots)
    free = pad_lanes(free, slots)
    ids = pad_lanes(jnp.reshape(id_ref[...], (1, n)), slots)
    code = jnp.zeros((1, slots), I32)
    moved = []
    low_side = []
    for axis in range(3):
        low = me[axis].astype(F32) * side
        high = (me[axis] + 1).astype(F32) * side
        box = side * float(sizes[axis])
        u = free[axis:axis + 1]
        step = jnp.where(u >= high, 1, 0) - jnp.where(u < low, 1, 0)
        code = code + (step + 1) * (1, 3, 9)[axis]
        moved.append(jnp.where(u < 0.0, u + box, jnp.where(u >= box, u - box, u)))
        low_side.append(low)
    code = jnp.where(owned, code, 31)
    id_hi = (ids >> 16).astype(F32)
    id_lo = (ids & 65535).astype(F32)
    okf = jnp.where(owned, 1.0, 0.0)
    data = jnp.concatenate(moved + [half, id_hi, id_lo, okf, jnp.zeros((7, slots), F32)], axis=0)

    place, _ = class_places(code, False)
    leaving = owned & (code != 13)
    way = jnp.where(leaving, code - jnp.where(code > 13, 1, 0), 31)
    member = jnp.where(lax.broadcasted_iota(I32, (32, slots), 0) == way, 1.0, 0.0).astype(BF16)
    fields = jnp.concatenate([jnp.where(place == float(k), data, 0.0) for k in range(PACK)], axis=0)
    packed = jnp.zeros((32, L), F32)
    for part in split3(fields):
        packed = packed + lax.dot_general(member, part, NT, preferred_element_type=F32)
    pkt[...] = packed

    def bins_of(pos):
        bins = []
        for axis in range(3):
            loc = pos[axis:axis + 1] - low_side[axis]
            bins.append(jnp.where(loc < NEAR, 0, jnp.where(loc > side - NEAR, 2, 1)))
        return [(bins[i] * 3 + bins[j]) * 3 + bins[k] for i, j, k in MAJOR]

    eye = lax.broadcasted_iota(I32, (32, L), 0) == lax.broadcasted_iota(I32, (32, L), 1)

    def sorted_block(cand, keys, kept):
        width = cand.shape[1]
        where_to, before = class_places(jnp.where(kept, keys, 28), True)
        arranged = scatter_lanes(cand, jnp.where(kept, where_to.astype(I32), -1), width)
        total = jnp.concatenate([before[27:28]] * (width // L), axis=1)
        lane = lax.broadcasted_iota(I32, (1, width), 1).astype(F32)
        counts = jnp.sum(jnp.where(eye, before, 0.0), axis=0, keepdims=True)
        return jnp.concatenate([jnp.where(lane < total, arranged[0:3], FAR), pad_lanes(counts, width)], axis=0)

    def send(src, dst, ssem, rsem, offset):
        copy = pltpu.make_async_remote_copy(
            src_ref=src, dst_ref=dst, send_sem=ssem, recv_sem=rsem,
            device_id=device_at(offset), device_id_type=pl.DeviceIdType.MESH)
        copy.start()
        return copy

    def send_blocks(block, dst, ssem, rsem, kind):
        out = []
        for index, offset in enumerate(peers):
            if order_of(tuple(0 if c == 0 else 1 for c in offset)) == kind:
                out.append(send(block.at[kind], dst.at[index], ssem.at[index], rsem.at[index], offset))
        return out

    staying = code == 13
    keys = bins_of(data)
    for kind in range(3):
        out3[kind] = sorted_block(data[0:8], keys[kind], staying)
    pl.semaphore_wait(barrier, len(peers))
    packets = []
    for index, d in enumerate(DIRS):
        row = pl.ds(index, 1)
        packets.append(send(pkt.at[row], rcv.at[row], psend.at[index], precv.at[index], (d[0] % size_x, d[1] % size_y, d[2] % size_z)))
    blocks = []
    for kind in range(3):
        blocks = blocks + send_blocks(out3, gh_ref, gsend, grecv, kind)
    for copy in packets:
        copy.wait_recv()

    came = jnp.concatenate([rcv[...], jnp.zeros((32 - 26, L), F32)], axis=0)
    came = jnp.concatenate([came] + [pltpu.roll(came, L - 16 * k, 1) for k in range(1, PACK)], axis=0)
    came_t = jnp.transpose(came)[0:16]
    came_ok = came_t[8:9] > 0.5
    keys = bins_of(came_t)
    late = []
    for kind in range(3):
        new3[kind] = sorted_block(came_t[0:8], keys[kind], came_ok)
        late = late + send_blocks(new3, ga_ref, asend, arecv, kind)
    for copy in packets:
        copy.wait_send()

    arr_ids = came[:, 6:7].astype(I32) * 65536 + came[:, 7:8].astype(I32)
    arr_ok = came[:, 8:9] > 0.5
    row_ids = jnp.concatenate([ids, came_t[6:7].astype(I32) * 65536 + came_t[7:8].astype(I32)], axis=1)
    less = jnp.where((arr_ids < row_ids) & arr_ok, 1.0, 0.0)
    arrivals_below = jnp.sum(less, axis=0, keepdims=True)
    above = jnp.where((arr_ids > row_ids[:, 0:slots]) & staying, 1.0, 0.0).astype(BF16)
    stay_below = lax.dot_general(jnp.ones((16, slots), BF16), above, NT, preferred_element_type=F32)[0:1]
    stay_place, _ = class_places(jnp.where(staying, 0, 31), False)
    rank = jnp.concatenate([stay_place, stay_below], axis=1) + arrivals_below
    dest = jnp.where(jnp.concatenate([staying, came_ok], axis=1), rank.astype(I32), -1)
    merged = scatter_lanes(jnp.concatenate([data, came_t], axis=1), dest, slots)
    srt_ref[...] = merged

    good = merged[8:9] > 0.5
    own_ref[...] = own_columns(jnp.where(good, merged[0:3], -FAR))
    first = CHUNK * L
    for a in range(3):
        lanes[a] = jnp.broadcast_to(jnp.where(good, merged[a:a + 1], FAR)[:, 0:first], (8, first))
    zero = jnp.zeros(TILE, F32)

    def own_step(q, energy):
        force, energy = pair_loop(own_ref, lanes, q, 0, 1, True, (((zero,) * 3,) * GROUPS, energy))
        for g in range(GROUPS):
            for a in range(3):
                inner_ref[a, step_rows(q, g), :] = force[g][a]
        return energy

    inner_en_ref[...] = lax.fori_loop(0, slots // (8 * GROUPS), own_step, zero)

    for copy in blocks + late:
        copy.wait()


def force_kernel(sizes, peers, slots, srt_ref, gh_ref, ga_ref, own_cols, inner_ref, inner_en_ref, offs_ref, side_ref, pos_ref, vel_ref, frc_ref, id_ref, ok_ref, en_ref, line, wide_line, sums):
    size_x, size_y, size_z = sizes
    me = (lax.axis_index("x"), lax.axis_index("y"), lax.axis_index("z"))
    n = pos_ref.shape[1]
    side = side_ref[0, 0]
    okrow = srt_ref[8:9]
    good = okrow > 0.5
    count = jnp.sum(okrow).astype(I32)
    spread = side > 2.0 * NEAR
    span = slots + L

    away = jnp.full(TILE, FAR, F32)
    first = CHUNK * L
    line[:, 0:slots - first] = jnp.concatenate([jnp.where(good, srt_ref[0:3], FAR), jnp.full((5, slots), FAR, F32)], axis=0)[:, first:]
    lane = lax.broadcasted_iota(I32, (8, span), 1)
    fill = jnp.maximum(count - first, 0)
    for d in DIRS:
        offset = (d[0] % size_x, d[1] % size_y, d[2] % size_z)
        back = ((-offset[0]) % size_x, (-offset[1]) % size_y, (-offset[2]) % size_z)
        index = peers.index(back)
        low, high = range_of(d)
        shifts = []
        for axis in range(3):
            box = side * float(sizes[axis])
            if d[axis] == 1:
                shifts.append(jnp.where(me[axis] == sizes[axis] - 1, box, 0.0))
            elif d[axis] == -1:
                shifts.append(jnp.where(me[axis] == 0, -box, 0.0))
            else:
                shifts.append(jnp.float32(0.0))
        for source, entry in ((gh_ref, index), (ga_ref, index + len(peers))):
            width = source.shape[2]
            begin = jnp.where(spread, offs_ref[entry, low], 0)
            end = jnp.where(spread, offs_ref[entry, high], offs_ref[entry, 27])
            block = jnp.concatenate([source[index, a:a + 1] + shifts[a] for a in range(3)] + [jnp.zeros((5, width), F32)], axis=0)
            block = jnp.concatenate([block, away], axis=1)
            head = fill & (L - 1)
            base = pl.multiple_of(fill - head, L)
            move = head - begin
            block = pltpu.roll(block, jnp.where(move < 0, move + (width + L), move), 1)
            block = jnp.where(lane[:, 0:width + L] < head + end - begin, block, FAR)
            line[:, pl.ds(base, L)] = jnp.where(lane[:, 0:L] < head, line[:, pl.ds(base, L)], block[:, 0:L])
            line[:, pl.ds(pl.multiple_of(base + L, L), width)] = block[:, L:]
            fill = fill + (end - begin)
    rest = pl.multiple_of(((fill + L - 1) // L) * L, L)
    line[:, pl.ds(rest, CHUNK * L)] = jnp.full((8, CHUNK * L), FAR, F32)
    chunks = jnp.maximum((fill + CHUNK * L - 1) // (CHUNK * L), 1)

    def widen(c, carry):
        for t in range(CHUNK):
            place = pl.ds(pl.multiple_of((c * CHUNK + t) * L, L), L)
            tile = line[:, place]
            for a in range(3):
                wide_line[a, :, place] = jnp.broadcast_to(tile[a:a + 1], TILE)
        return carry

    lax.fori_loop(0, chunks, widen, 0)

    def own_step(q, energy):
        start = tuple(tuple(inner_ref[a, step_rows(q, g), :] for a in range(3)) for g in range(GROUPS))
        carry = pair_loop(own_cols, wide_line, q, 0, 1, True, (start, energy))
        force, energy = pair_loop(own_cols, wide_line, q, 1, chunks, False, carry)
        for g in range(GROUPS):
            for a in range(3):
                sums[a, step_rows(q, g), :] = force[g][a]
        return energy

    own_steps = (count + 8 * GROUPS - 1) // (8 * GROUPS)
    energy = lax.fori_loop(0, own_steps, own_step, inner_en_ref[...])
    en_ref[...] = 2.0 * jnp.sum(energy, axis=0, keepdims=True)

    col = lax.broadcasted_iota(I32, (L, L), 1)
    total = jnp.zeros((slots, L), F32)
    for a in range(3):
        pick = jnp.where(col == a, 1.0, 0.0).astype(BF16)
        for part in split3(sums[a]):
            total = total + lax.dot_general(part, pick, NN, preferred_element_type=F32)
    force = jnp.where(good, 24.0 * jnp.transpose(total)[0:3], 0.0)
    pos_ref[...] = srt_ref[0:3, 0:n]
    frc_ref[...] = force[:, 0:n]
    vel_ref[...] = (srt_ref[3:6] + (0.5 * DT) * force)[:, 0:n]
    id_ref[...] = jnp.reshape((srt_ref[6:7].astype(I32) * 65536 + srt_ref[7:8].astype(I32))[:, 0:n], (n,))
    ok_ref[...] = jnp.reshape(okrow[:, 0:n].astype(I32), (n,))


def total_kernel(sizes, part_ref, sum_ref, rows, ssem, rsem):
    size_x, size_y, size_z = sizes
    me = (lax.axis_index("x"), lax.axis_index("y"), lax.axis_index("z"))
    mine = (me[2] * size_y + me[1]) * size_x + me[0]
    others = [(dx, dy, dz) for dz in range(size_z) for dy in range(size_y) for dx in range(size_x) if dx + dy + dz > 0]
    others.sort(key=lambda o: -(2 * min(o[2], size_z - o[2]) + 2 * o[1] + min(o[0], size_x - o[0])))

    def device_at(offset):
        return (lax.rem(me[2] + offset[2], size_z), lax.rem(me[1] + offset[1], size_y), lax.rem(me[0] + offset[0], size_x))

    barrier = pltpu.get_barrier_semaphore()
    for offset in others:
        pl.semaphore_signal(barrier, inc=1, device_id=device_at(offset), device_id_type=pl.DeviceIdType.MESH)
    rows[pl.ds(mine, 1)] = part_ref[...]
    pl.semaphore_wait(barrier, len(others))
    copies = []
    for index, offset in enumerate(others):
        copy = pltpu.make_async_remote_copy(
            src_ref=part_ref, dst_ref=rows.at[pl.ds(mine, 1)], send_sem=ssem.at[index], recv_sem=rsem.at[index],
            device_id=device_at(offset), device_id_type=pl.DeviceIdType.MESH)
        copy.start()
        copies.append(copy)
    for copy in copies:
        copy.wait_recv()
    sum_ref[0, 0] = jnp.sum(rows[...])
    for copy in copies:
        copy.wait_send()


def solution(mesh):
    sizes = (mesh.shape["x"], mesh.shape["y"], mesh.shape["z"])
    peers = sorted({(d[0] % sizes[0], d[1] % sizes[1], d[2] % sizes[2]) for d in DIRS} - {(0, 0, 0)})
    devices = sizes[0] * sizes[1] * sizes[2]

    def local_step(atom_pos, atom_vel, atom_frc, atom_id, atom_ok, brick_side):
        n = atom_pos.shape[0]
        slots = -(-n // L) * L
        side = jnp.reshape(brick_side, (1, 1))
        vmem = pl.BlockSpec(memory_space=pltpu.VMEM)
        smem = pl.BlockSpec(memory_space=pltpu.SMEM)
        srt, ghosts, fresh, own, inner, inner_en = pl.pallas_call(
            functools.partial(exchange_kernel, sizes, peers, slots),
            out_shape=(jax.ShapeDtypeStruct((16, slots), F32), jax.ShapeDtypeStruct((len(peers), 4, slots), F32), jax.ShapeDtypeStruct((len(peers), 4, NEW), F32),
                       jax.ShapeDtypeStruct((slots, 3 * L), F32), jax.ShapeDtypeStruct((3, slots, L), F32), jax.ShapeDtypeStruct(TILE, F32)),
            in_specs=[pl.BlockSpec(memory_space=pltpu.HBM)] * 5 + [smem],
            out_specs=(vmem,) * 6,
            scratch_shapes=[
                pltpu.VMEM((3, n), F32), pltpu.VMEM((3, n), F32), pltpu.VMEM((3, n), F32), pltpu.VMEM((n,), I32), pltpu.VMEM((n,), I32),
                pltpu.VMEM((32, L), F32), pltpu.VMEM((26, L), F32), pltpu.VMEM((3, 4, slots), F32), pltpu.VMEM((3, 4, NEW), F32), pltpu.VMEM((3, 8, CHUNK * L), F32),
                pltpu.SemaphoreType.DMA((5,)), pltpu.SemaphoreType.DMA((26,)), pltpu.SemaphoreType.DMA((26,)),
            ] + [pltpu.SemaphoreType.DMA((len(peers),))] * 4,
            compiler_params=pltpu.CompilerParams(collective_id=0, has_side_effects=True, vmem_limit_bytes=40 * 2 ** 20),
            name="exchange",
        )(*[pltpu.with_memory_space_constraint(v, pltpu.HBM) for v in (atom_pos.T, atom_vel.T, atom_frc.T, atom_id, atom_ok)], side)
        offs = jnp.concatenate([ghosts[:, 3, 0:32], fresh[:, 3, 0:32]], axis=0).astype(I32)
        out_f = jax.ShapeDtypeStruct((3, n), F32)
        out_i = jax.ShapeDtypeStruct((n,), I32)
        new_pos, new_vel, new_frc, new_id, new_ok, energy = pl.pallas_call(
            functools.partial(force_kernel, sizes, peers, slots),
            out_shape=(out_f, out_f, out_f, out_i, out_i, jax.ShapeDtypeStruct((1, L), F32)),
            in_specs=[vmem] * 6 + [smem] * 2,
            out_specs=(vmem,) * 6,
            scratch_shapes=[pltpu.VMEM((8, 28 * slots + CHUNK * L), F32), pltpu.VMEM((3, 8, 28 * slots + CHUNK * L), F32), pltpu.VMEM((3, slots, L), F32)],
            compiler_params=pltpu.CompilerParams(vmem_limit_bytes=40 * 2 ** 20),
            name="forces",
        )(srt, ghosts, fresh, own, inner, inner_en, offs, side)
        energy = pl.pallas_call(
            functools.partial(total_kernel, sizes),
            out_shape=jax.ShapeDtypeStruct((1, 1), F32),
            in_specs=[vmem],
            out_specs=smem,
            scratch_shapes=[pltpu.VMEM((devices, L), F32), pltpu.SemaphoreType.DMA((devices,)), pltpu.SemaphoreType.DMA((devices,))],
            compiler_params=pltpu.CompilerParams(collective_id=1, has_side_effects=True),
            name="total",
        )(pltpu.with_memory_space_constraint(energy, pltpu.VMEM))[0, 0]
        return new_pos.T, new_vel.T, new_frc.T, new_id, new_ok, energy

    row_spec = P(MESH_AXES, None)
    id_spec = P(MESH_AXES)
    return jax.shard_map(local_step, mesh=mesh, in_specs=(row_spec, row_spec, row_spec, id_spec, id_spec, P()), out_specs=(row_spec, row_spec, row_spec, id_spec, id_spec, P()), check_vma=False)
```

```python
import functools

import jax
import jax.numpy as jnp
from jax import lax
from jax.experimental import pallas as pl
from jax.experimental.pallas import tpu as pltpu
from jax.sharding import PartitionSpec as P

DT = 0.005
RC = 2.5
FAR = 1.0e6
UCUT = 4.0 * (RC ** -12 - RC ** -6)
UPC = -48.0 * RC ** -13 + 24.0 * RC ** -7
MESH_AXES = ("z", "y", "x")
DIRS = [(dx, dy, dz) for dz in (-1, 0, 1) for dy in (-1, 0, 1) for dx in (-1, 0, 1) if (dx, dy, dz) != (0, 0, 0)]
NEAR = RC + 1.0e-3
MAJOR = ((2, 1, 0), (1, 0, 2), (0, 2, 1))
PACK = 8
NEW = 256
CHUNK = 3
GROUPS = 8
L = 128
TILE = (8, L)
F32 = jnp.float32
BF16 = jnp.bfloat16
I32 = jnp.int32
NT = (((1,), (1,)), ((), ()))
NN = (((1,), (0,)), ((), ()))


def order_of(d):
    if d[2] == 0:
        return 1 if d[1] != 0 else 2
    return 2 if (d[1] == 0 and d[0] != 0) else 0


def range_of(d):
    first, size = 0, 27
    for axis in MAJOR[order_of(d)]:
        if d[axis] == 0:
            break
        size = size // 3
        first = first + (1, 0, 2)[d[axis]] * size
    return first, first + size


def split3(x):
    hi = x.astype(BF16)
    rest = x - hi.astype(F32)
    mid = rest.astype(BF16)
    low = (rest - mid.astype(F32)).astype(BF16)
    return hi, mid, low


def onehot_rows(dest, base, count):
    rows = lax.broadcasted_iota(I32, (count, dest.shape[1]), 0) + base
    return jnp.where(rows == dest, 1.0, 0.0).astype(BF16)


def scatter_lanes(data, dest, slots):
    rows = data.shape[0]
    parts = jnp.concatenate(split3(data), axis=0)
    out = []
    for base in range(0, slots, 256):
        hot = onehot_rows(dest, base, min(256, slots - base))
        got = lax.dot_general(parts, hot, NT, preferred_element_type=F32)
        out.append(got[0:rows] + got[rows:2 * rows] + got[2 * rows:3 * rows])
    return jnp.concatenate(out, axis=1)


def class_places(code, with_before):
    width = code.shape[1]
    tiles = width // L
    cls = lax.broadcasted_iota(I32, (32, width), 0)
    member = jnp.where(cls == code, 1.0, 0.0)
    member_b = member.astype(BF16)
    stacked = jnp.concatenate([member_b[:, t * L:(t + 1) * L] for t in range(tiles)], axis=0)
    row_i = lax.broadcasted_iota(I32, (L, 256), 0)
    col_i = lax.broadcasted_iota(I32, (L, 256), 1)
    tri = jnp.where((row_i < col_i) | (col_i >= L), 1.0, 0.0).astype(BF16)
    pre = lax.dot_general(stacked, tri, NN, preferred_element_type=F32)
    carry = jnp.zeros((32, L), F32)
    if with_before:
        before_b = jnp.where(code < cls, 1.0, 0.0).astype(BF16)
        before_s = before_b[:, 0:L]
        tot = None
        ones = jnp.ones((L, L), BF16)
        for t in range(tiles):
            part = lax.dot_general(before_b[:, t * L:(t + 1) * L], ones, NN, preferred_element_type=F32)
            tot = part if tot is None else tot + part
        before = tot
        carry = before
    else:
        before = None
    places = []
    for t in range(tiles):
        within = pre[32 * t:32 * t + 32, 0:L] + carry
        places.append(jnp.sum(member[:, t * L:(t + 1) * L] * within, axis=0, keepdims=True))
        carry = carry + pre[32 * t:32 * t + 32, L:256]
    return jnp.concatenate(places, axis=1), before


def pad_lanes(x, width):
    return jnp.concatenate([x, jnp.zeros((x.shape[0], width - x.shape[1]), x.dtype)], axis=1)


def pair_loop(own_cols, near_lanes, q, first, last, with_self, carry):
    rows = [step_rows(q, g) for g in range(GROUPS)]
    own = [[own_cols[rows[g], a * L:(a + 1) * L] for a in range(3)] for g in range(GROUPS)]

    def body(c, carry):
        force, en = [list(f) for f in carry[0]], carry[1]
        for t in range(CHUNK):
            place = pl.ds(pl.multiple_of((c * CHUNK + t) * L, L), L)
            near_xyz = [near_lanes[a, :, place] for a in range(3)]
            for g in range(GROUPS):
                dx, dy, dz = [own[g][a] - near_xyz[a] for a in range(3)]
                d2 = dx * dx + dy * dy + dz * dz
                near = d2 < RC * RC
                if with_self:
                    near = near & (d2 > 0.0)
                inv = jnp.where(near, lax.rsqrt(d2), 0.0)
                s2 = inv * inv
                s6 = s2 * s2 * s2
                s12 = s6 * s6
                p = s12 - s6
                w = inv * (UPC / 24.0)
                scale = (p + s12) * s2 + w
                en = en + ((p + jnp.where(near, 0.25 * (RC * UPC - UCUT), 0.0)) - 6.0 * (w * d2))
                force[g] = [force[g][0] + scale * dx, force[g][1] + scale * dy, force[g][2] + scale * dz]
        return tuple(tuple(f) for f in force), en

    return lax.fori_loop(first, last, body, carry)


def step_rows(q, g):
    return pl.ds(pl.multiple_of((q * GROUPS + g) * 8, 8), 8)


def own_columns(xyz):
    slots = xyz.shape[1]
    parts = [part.astype(F32) for part in split3(xyz)]
    parts = jnp.concatenate(parts + [jnp.zeros((7, slots), F32)], axis=0)
    row = lax.broadcasted_iota(I32, (16, 3 * L), 0)
    tile = lax.broadcasted_iota(I32, (16, 3 * L), 1) // L
    picks = jnp.where((row == tile) | (row == tile + 3) | (row == tile + 6), 1.0, 0.0).astype(BF16)
    return lax.dot_general(jnp.transpose(parts).astype(BF16), picks, NN, preferred_element_type=F32)


def exchange_kernel(sizes, peers, slots, pos_hbm, vel_hbm, frc_hbm, id_hbm, ok_hbm, side_ref, srt_ref, gh_ref, ga_ref, own_ref, inner_ref, inner_en_ref, pos_ref, vel_ref, frc_ref, id_ref, ok_ref, pkt, rcv, out3, new3, lanes, isem, psend, precv, gsend, grecv, asend, arecv):
    size_x, size_y, size_z = sizes
    me = (lax.axis_index("x"), lax.axis_index("y"), lax.axis_index("z"))

    def device_at(offset):
        return (lax.rem(me[2] + offset[2], size_z), lax.rem(me[1] + offset[1], size_y), lax.rem(me[0] + offset[0], size_x))

    loads = []
    for index, (src, dst) in enumerate(((ok_hbm, ok_ref), (id_hbm, id_ref), (pos_hbm, pos_ref), (vel_hbm, vel_ref), (frc_hbm, frc_ref))):
        load = pltpu.make_async_copy(src, dst, isem.at[index])
        load.start()
        loads.append(load)
    barrier = pltpu.get_barrier_semaphore()
    for offset in peers:
        pl.semaphore_signal(barrier, inc=1, device_id=device_at(offset), device_id_type=pl.DeviceIdType.MESH)

    n = pos_ref.shape[1]
    for load in loads:
        load.wait()
    side = side_ref[0, 0]
    owned = pad_lanes(jnp.reshape(ok_ref[...], (1, n)), slots) > 0
    half = vel_ref[...] + (0.5 * DT) * frc_ref[...]
    free = pos_ref[...] + DT * half
    half = pad_lanes(half, slots)
    free = pad_lanes(free, slots)
    ids = pad_lanes(jnp.reshape(id_ref[...], (1, n)), slots)
    code = jnp.zeros((1, slots), I32)
    moved = []
    low_side = []
    for axis in range(3):
        low = me[axis].astype(F32) * side
        high = (me[axis] + 1).astype(F32) * side
        box = side * float(sizes[axis])
        u = free[axis:axis + 1]
        step = jnp.where(u >= high, 1, 0) - jnp.where(u < low, 1, 0)
        code = code + (step + 1) * (1, 3, 9)[axis]
        moved.append(jnp.where(u < 0.0, u + box, jnp.where(u >= box, u - box, u)))
        low_side.append(low)
    code = jnp.where(owned, code, 31)
    id_hi = (ids >> 16).astype(F32)
    id_lo = (ids & 65535).astype(F32)
    okf = jnp.where(owned, 1.0, 0.0)
    data = jnp.concatenate(moved + [half, id_hi, id_lo, okf, jnp.zeros((7, slots), F32)], axis=0)

    place, _ = class_places(code, False)
    leaving = owned & (code != 13)
    way = jnp.where(leaving, code - jnp.where(code > 13, 1, 0), 31)
    member = jnp.where(lax.broadcasted_iota(I32, (32, slots), 0) == way, 1.0, 0.0).astype(BF16)
    fields = jnp.concatenate([jnp.where(place == float(k), data, 0.0) for k in range(PACK)], axis=0)
    packed = jnp.zeros((32, L), F32)
    for part in split3(fields):
        packed = packed + lax.dot_general(member, part, NT, preferred_element_type=F32)
    pkt[...] = packed

    def bins_of(pos):
        bins = []
        for axis in range(3):
            loc = pos[axis:axis + 1] - low_side[axis]
            bins.append(jnp.where(loc < NEAR, 0, jnp.where(loc > side - NEAR, 2, 1)))
        return [(bins[i] * 3 + bins[j]) * 3 + bins[k] for i, j, k in MAJOR]

    wide = side > 2.0 * NEAR
    eye = lax.broadcasted_iota(I32, (32, L), 0) == lax.broadcasted_iota(I32, (32, L), 1)

    def sorted_block(cand, keys, kept):
        width = cand.shape[1]
        where_to, before = class_places(jnp.where(kept, keys, 28), True)
        arranged = scatter_lanes(cand, jnp.where(kept, where_to.astype(I32), -1), width)
        total = jnp.concatenate([before[27:28]] * (width // L), axis=1)
        lane = lax.broadcasted_iota(I32, (1, width), 1).astype(F32)
        begins = jnp.sum(jnp.where(eye, before, 0.0), axis=0, keepdims=True)
        ends = jnp.where(wide, begins, before[27:28])
        counts = jnp.concatenate([jnp.where(wide, begins, 0.0)[:, 0:32], ends[:, 0:32], jnp.zeros((1, L - 64), F32)], axis=1)
        return jnp.concatenate([jnp.where(lane < total, arranged[0:3], FAR), pad_lanes(counts, width)], axis=0)

    def send(src, dst, ssem, rsem, offset):
        copy = pltpu.make_async_remote_copy(
            src_ref=src, dst_ref=dst, send_sem=ssem, recv_sem=rsem,
            device_id=device_at(offset), device_id_type=pl.DeviceIdType.MESH)
        copy.start()
        return copy

    def send_blocks(block, dst, ssem, rsem, kind):
        out = []
        for index, offset in enumerate(peers):
            if order_of(tuple(0 if c == 0 else 1 for c in offset)) == kind:
                out.append(send(block.at[kind], dst.at[index], ssem.at[index], rsem.at[index], offset))
        return out

    staying = code == 13
    keys = bins_of(data)
    for kind in range(3):
        out3[kind] = sorted_block(data[0:8], keys[kind], staying)
    pl.semaphore_wait(barrier, len(peers))
    packets = []
    for index, d in enumerate(DIRS):
        row = pl.ds(index, 1)
        packets.append(send(pkt.at[row], rcv.at[row], psend.at[index], precv.at[index], (d[0] % size_x, d[1] % size_y, d[2] % size_z)))
    blocks = []
    for kind in range(3):
        blocks = blocks + send_blocks(out3, gh_ref, gsend, grecv, kind)
    for copy in packets:
        copy.wait_recv()

    came = jnp.concatenate([rcv[...], jnp.zeros((32 - 26, L), F32)], axis=0)
    came = jnp.concatenate([came] + [pltpu.roll(came, L - 16 * k, 1) for k in range(1, PACK)], axis=0)
    came_t = jnp.transpose(came)[0:16]
    came_ok = came_t[8:9] > 0.5
    keys = bins_of(came_t)
    late = []
    for kind in range(3):
        new3[kind] = sorted_block(came_t[0:8], keys[kind], came_ok)
        late = late + send_blocks(new3, ga_ref, asend, arecv, kind)
    for copy in packets:
        copy.wait_send()

    arr_ids = came[:, 6:7].astype(I32) * 65536 + came[:, 7:8].astype(I32)
    arr_ok = came[:, 8:9] > 0.5
    row_ids = jnp.concatenate([ids, came_t[6:7].astype(I32) * 65536 + came_t[7:8].astype(I32)], axis=1)
    less = jnp.where((arr_ids < row_ids) & arr_ok, 1.0, 0.0)
    arrivals_below = jnp.sum(less, axis=0, keepdims=True)
    above = jnp.where((arr_ids > row_ids[:, 0:slots]) & staying, 1.0, 0.0).astype(BF16)
    stay_below = lax.dot_general(jnp.ones((16, slots), BF16), above, NT, preferred_element_type=F32)[0:1]
    stay_place, _ = class_places(jnp.where(staying, 0, 31), False)
    rank = jnp.concatenate([stay_place, stay_below], axis=1) + arrivals_below
    dest = jnp.where(jnp.concatenate([staying, came_ok], axis=1), rank.astype(I32), -1)
    merged = scatter_lanes(jnp.concatenate([data, came_t], axis=1), dest, slots)
    srt_ref[...] = jnp.where(lax.broadcasted_iota(I32, (16, slots), 0) == 9, side, merged)

    good = merged[8:9] > 0.5
    own_ref[...] = own_columns(jnp.where(good, merged[0:3], -FAR))
    first = CHUNK * L
    for a in range(3):
        lanes[a] = jnp.broadcast_to(jnp.where(good, merged[a:a + 1], FAR)[:, 0:first], (8, first))
    zero = jnp.zeros(TILE, F32)

    def own_step(q, energy):
        force, energy = pair_loop(own_ref, lanes, q, 0, 1, True, (((zero,) * 3,) * GROUPS, energy))
        for g in range(GROUPS):
            for a in range(3):
                inner_ref[a, step_rows(q, g), :] = force[g][a]
        return energy

    inner_en_ref[...] = lax.fori_loop(0, slots // (8 * GROUPS), own_step, zero)

    for copy in blocks + late:
        copy.wait()


def force_kernel(sizes, peers, slots, srt_ref, gh_ref, ga_ref, own_cols, inner_ref, inner_en_ref, offs_ref, pos_ref, vel_ref, frc_ref, id_ref, ok_ref, en_ref, line, wide_line, sums):
    size_x, size_y, size_z = sizes
    me = (lax.axis_index("x"), lax.axis_index("y"), lax.axis_index("z"))
    n = pos_ref.shape[1]
    side = srt_ref[9:10, 0:1]
    okrow = srt_ref[8:9]
    good = okrow > 0.5
    count = jnp.sum(okrow).astype(I32)
    span = slots + L

    away = jnp.full(TILE, FAR, F32)
    first = CHUNK * L
    line[:, 0:slots - first] = jnp.concatenate([jnp.where(good, srt_ref[0:3], FAR), jnp.full((5, slots), FAR, F32)], axis=0)[:, first:]
    lane = lax.broadcasted_iota(I32, (8, span), 1)
    fill = jnp.maximum(count - first, 0)
    for d in DIRS:
        offset = (d[0] % size_x, d[1] % size_y, d[2] % size_z)
        back = ((-offset[0]) % size_x, (-offset[1]) % size_y, (-offset[2]) % size_z)
        index = peers.index(back)
        low, high = range_of(d)
        shifts = []
        for axis in range(3):
            box = side * float(sizes[axis])
            if d[axis] == 1:
                shifts.append(jnp.where(me[axis] == sizes[axis] - 1, box, 0.0))
            elif d[axis] == -1:
                shifts.append(jnp.where(me[axis] == 0, -box, 0.0))
            else:
                shifts.append(jnp.zeros((1, 1), F32))
        for source, entry in ((gh_ref, index), (ga_ref, index + len(peers))):
            width = source.shape[2]
            begin = offs_ref[entry, low]
            end = offs_ref[entry, 32 + high]
            block = jnp.concatenate([source[index, a:a + 1] + shifts[a] for a in range(3)] + [jnp.zeros((5, width), F32)], axis=0)
            block = jnp.concatenate([block, away], axis=1)
            head = fill & (L - 1)
            base = pl.multiple_of(fill - head, L)
            move = head - begin
            block = pltpu.roll(block, jnp.where(move < 0, move + (width + L), move), 1)
            block = jnp.where(lane[:, 0:width + L] < head + end - begin, block, FAR)
            line[:, pl.ds(base, L)] = jnp.where(lane[:, 0:L] < head, line[:, pl.ds(base, L)], block[:, 0:L])
            line[:, pl.ds(pl.multiple_of(base + L, L), width)] = block[:, L:]
            fill = fill + (end - begin)
    rest = pl.multiple_of(((fill + L - 1) // L) * L, L)
    line[:, pl.ds(rest, CHUNK * L)] = jnp.full((8, CHUNK * L), FAR, F32)
    chunks = jnp.maximum((fill + CHUNK * L - 1) // (CHUNK * L), 1)

    def widen(c, carry):
        for t in range(CHUNK):
            place = pl.ds(pl.multiple_of((c * CHUNK + t) * L, L), L)
            tile = line[:, place]
            for a in range(3):
                wide_line[a, :, place] = jnp.broadcast_to(tile[a:a + 1], TILE)
        return carry

    lax.fori_loop(0, chunks, widen, 0)

    def own_step(q, energy):
        start = tuple(tuple(inner_ref[a, step_rows(q, g), :] for a in range(3)) for g in range(GROUPS))
        carry = pair_loop(own_cols, wide_line, q, 0, 1, True, (start, energy))
        force, energy = pair_loop(own_cols, wide_line, q, 1, chunks, False, carry)
        for g in range(GROUPS):
            for a in range(3):
                sums[a, step_rows(q, g), :] = force[g][a]
        return energy

    own_steps = (count + 8 * GROUPS - 1) // (8 * GROUPS)
    energy = lax.fori_loop(0, own_steps, own_step, inner_en_ref[...])
    en_ref[...] = 2.0 * jnp.sum(energy, axis=0, keepdims=True)

    col = lax.broadcasted_iota(I32, (L, L), 1)
    total = jnp.zeros((slots, L), F32)
    for a in range(3):
        pick = jnp.where(col == a, 1.0, 0.0).astype(BF16)
        for part in split3(sums[a]):
            total = total + lax.dot_general(part, pick, NN, preferred_element_type=F32)
    force = jnp.where(good, 24.0 * jnp.transpose(total)[0:3], 0.0)
    pos_ref[...] = srt_ref[0:3, 0:n]
    frc_ref[...] = force[:, 0:n]
    vel_ref[...] = (srt_ref[3:6] + (0.5 * DT) * force)[:, 0:n]
    id_ref[...] = jnp.reshape((srt_ref[6:7].astype(I32) * 65536 + srt_ref[7:8].astype(I32))[:, 0:n], (n,))
    ok_ref[...] = jnp.reshape(okrow[:, 0:n].astype(I32), (n,))


def total_kernel(sizes, part_ref, sum_ref, rows, ssem, rsem):
    size_x, size_y, size_z = sizes
    me = (lax.axis_index("x"), lax.axis_index("y"), lax.axis_index("z"))
    mine = (me[2] * size_y + me[1]) * size_x + me[0]
    others = [(dx, dy, dz) for dz in range(size_z) for dy in range(size_y) for dx in range(size_x) if dx + dy + dz > 0]
    others.sort(key=lambda o: -(2 * min(o[2], size_z - o[2]) + 2 * o[1] + min(o[0], size_x - o[0])))

    def device_at(offset):
        return (lax.rem(me[2] + offset[2], size_z), lax.rem(me[1] + offset[1], size_y), lax.rem(me[0] + offset[0], size_x))

    barrier = pltpu.get_barrier_semaphore()
    for offset in others:
        pl.semaphore_signal(barrier, inc=1, device_id=device_at(offset), device_id_type=pl.DeviceIdType.MESH)
    rows[pl.ds(mine, 1)] = part_ref[...]
    pl.semaphore_wait(barrier, len(others))
    copies = []
    for index, offset in enumerate(others):
        copy = pltpu.make_async_remote_copy(
            src_ref=part_ref, dst_ref=rows.at[pl.ds(mine, 1)], send_sem=ssem.at[index], recv_sem=rsem.at[index],
            device_id=device_at(offset), device_id_type=pl.DeviceIdType.MESH)
        copy.start()
        copies.append(copy)
    for copy in copies:
        copy.wait_recv()
    sum_ref[...] = jnp.sum(rows[...], axis=0, keepdims=True)
    for copy in copies:
        copy.wait_send()


def solution(mesh):
    sizes = (mesh.shape["x"], mesh.shape["y"], mesh.shape["z"])
    peers = sorted({(d[0] % sizes[0], d[1] % sizes[1], d[2] % sizes[2]) for d in DIRS} - {(0, 0, 0)})
    devices = sizes[0] * sizes[1] * sizes[2]

    def local_step(atom_pos, atom_vel, atom_frc, atom_id, atom_ok, brick_side):
        n = atom_pos.shape[0]
        slots = -(-n // L) * L
        side = jnp.reshape(brick_side, (1, 1))
        vmem = pl.BlockSpec(memory_space=pltpu.VMEM)
        smem = pl.BlockSpec(memory_space=pltpu.SMEM)
        srt, ghosts, fresh, own, inner, inner_en = pl.pallas_call(
            functools.partial(exchange_kernel, sizes, peers, slots),
            out_shape=(jax.ShapeDtypeStruct((16, slots), F32), jax.ShapeDtypeStruct((len(peers), 4, slots), F32), jax.ShapeDtypeStruct((len(peers), 4, NEW), F32),
                       jax.ShapeDtypeStruct((slots, 3 * L), F32), jax.ShapeDtypeStruct((3, slots, L), F32), jax.ShapeDtypeStruct(TILE, F32)),
            in_specs=[pl.BlockSpec(memory_space=pltpu.HBM)] * 5 + [smem],
            out_specs=(vmem,) * 6,
            scratch_shapes=[
                pltpu.VMEM((3, n), F32), pltpu.VMEM((3, n), F32), pltpu.VMEM((3, n), F32), pltpu.VMEM((n,), I32), pltpu.VMEM((n,), I32),
                pltpu.VMEM((32, L), F32), pltpu.VMEM((26, L), F32), pltpu.VMEM((3, 4, slots), F32), pltpu.VMEM((3, 4, NEW), F32), pltpu.VMEM((3, 8, CHUNK * L), F32),
                pltpu.SemaphoreType.DMA((5,)), pltpu.SemaphoreType.DMA((26,)), pltpu.SemaphoreType.DMA((26,)),
            ] + [pltpu.SemaphoreType.DMA((len(peers),))] * 4,
            compiler_params=pltpu.CompilerParams(collective_id=0, has_side_effects=True, vmem_limit_bytes=40 * 2 ** 20),
            name="exchange",
        )(*[pltpu.with_memory_space_constraint(v, pltpu.HBM) for v in (atom_pos.T, atom_vel.T, atom_frc.T, atom_id, atom_ok)], side)
        offs = jnp.concatenate([ghosts[:, 3, 0:64], fresh[:, 3, 0:64]], axis=0).astype(I32)
        out_f = jax.ShapeDtypeStruct((3, n), F32)
        out_i = jax.ShapeDtypeStruct((n,), I32)
        new_pos, new_vel, new_frc, new_id, new_ok, energy = pl.pallas_call(
            functools.partial(force_kernel, sizes, peers, slots),
            out_shape=(out_f, out_f, out_f, out_i, out_i, jax.ShapeDtypeStruct((1, L), F32)),
            in_specs=[vmem] * 6 + [smem],
            out_specs=(vmem,) * 6,
            scratch_shapes=[pltpu.VMEM((8, 28 * slots + CHUNK * L), F32), pltpu.VMEM((3, 8, 28 * slots + CHUNK * L), F32), pltpu.VMEM((3, slots, L), F32)],
            compiler_params=pltpu.CompilerParams(vmem_limit_bytes=40 * 2 ** 20),
            name="forces",
        )(srt, ghosts, fresh, own, inner, inner_en, offs)
        energy = pl.pallas_call(
            functools.partial(total_kernel, sizes),
            out_shape=jax.ShapeDtypeStruct((1, L), F32),
            in_specs=[vmem],
            out_specs=vmem,
            scratch_shapes=[pltpu.VMEM((devices, L), F32), pltpu.SemaphoreType.DMA((devices,)), pltpu.SemaphoreType.DMA((devices,))],
            compiler_params=pltpu.CompilerParams(collective_id=1, has_side_effects=True),
            name="total",
        )(pltpu.with_memory_space_constraint(energy, pltpu.VMEM))
        return new_pos.T, new_vel.T, new_frc.T, new_id, new_ok, jnp.sum(energy)

    row_spec = P(MESH_AXES, None)
    id_spec = P(MESH_AXES)
    return jax.shard_map(local_step, mesh=mesh, in_specs=(row_spec, row_spec, row_spec, id_spec, id_spec, P()), out_specs=(row_spec, row_spec, row_spec, id_spec, id_spec, P()), check_vma=False)
```

```python
import functools

import jax
import jax.numpy as jnp
from jax import lax
from jax.experimental import pallas as pl
from jax.experimental.pallas import tpu as pltpu
from jax.sharding import PartitionSpec as P

DT = 0.005
RC = 2.5
FAR = 1.0e6
UCUT = 4.0 * (RC ** -12 - RC ** -6)
UPC = -48.0 * RC ** -13 + 24.0 * RC ** -7
MESH_AXES = ("z", "y", "x")
DIRS = [(dx, dy, dz) for dz in (-1, 0, 1) for dy in (-1, 0, 1) for dx in (-1, 0, 1) if (dx, dy, dz) != (0, 0, 0)]
NEAR = RC + 1.0e-3
MAJOR = ((2, 1, 0), (1, 0, 2), (0, 2, 1))
PACK = 8
NEW = 256
CHUNK = 3
GROUPS = 8
L = 128
TILE = (8, L)
F32 = jnp.float32
BF16 = jnp.bfloat16
I32 = jnp.int32
NT = (((1,), (1,)), ((), ()))
NN = (((1,), (0,)), ((), ()))


def order_of(d):
    if d[2] == 0:
        return 1 if d[1] != 0 else 2
    return 2 if (d[1] == 0 and d[0] != 0) else 0


def range_of(d):
    first, size = 0, 27
    for axis in MAJOR[order_of(d)]:
        if d[axis] == 0:
            break
        size = size // 3
        first = first + (1, 0, 2)[d[axis]] * size
    return first, first + size


def split3(x):
    hi = x.astype(BF16)
    rest = x - hi.astype(F32)
    mid = rest.astype(BF16)
    low = (rest - mid.astype(F32)).astype(BF16)
    return hi, mid, low


def onehot_rows(dest, base, count):
    rows = lax.broadcasted_iota(I32, (count, dest.shape[1]), 0) + base
    return jnp.where(rows == dest, 1.0, 0.0).astype(BF16)


def scatter_lanes(data, dest, slots):
    rows = data.shape[0]
    parts = jnp.concatenate(split3(data), axis=0)
    out = []
    for base in range(0, slots, 256):
        hot = onehot_rows(dest, base, min(256, slots - base))
        got = lax.dot_general(parts, hot, NT, preferred_element_type=F32)
        out.append(got[0:rows] + got[rows:2 * rows] + got[2 * rows:3 * rows])
    return jnp.concatenate(out, axis=1)


def class_places(code, with_before):
    width = code.shape[1]
    tiles = width // L
    cls = lax.broadcasted_iota(I32, (32, width), 0)
    member = jnp.where(cls == code, 1.0, 0.0)
    member_b = member.astype(BF16)
    stacked = jnp.concatenate([member_b[:, t * L:(t + 1) * L] for t in range(tiles)], axis=0)
    row_i = lax.broadcasted_iota(I32, (L, 256), 0)
    col_i = lax.broadcasted_iota(I32, (L, 256), 1)
    tri = jnp.where((row_i < col_i) | (col_i >= L), 1.0, 0.0).astype(BF16)
    pre = lax.dot_general(stacked, tri, NN, preferred_element_type=F32)
    carry = jnp.zeros((32, L), F32)
    if with_before:
        before_b = jnp.where(code < cls, 1.0, 0.0).astype(BF16)
        before_s = before_b[:, 0:L]
        tot = None
        ones = jnp.ones((L, L), BF16)
        for t in range(tiles):
            part = lax.dot_general(before_b[:, t * L:(t + 1) * L], ones, NN, preferred_element_type=F32)
            tot = part if tot is None else tot + part
        before = tot
        carry = before
    else:
        before = None
    places = []
    for t in range(tiles):
        within = pre[32 * t:32 * t + 32, 0:L] + carry
        places.append(jnp.sum(member[:, t * L:(t + 1) * L] * within, axis=0, keepdims=True))
        carry = carry + pre[32 * t:32 * t + 32, L:256]
    return jnp.concatenate(places, axis=1), before


def pad_lanes(x, width):
    return jnp.concatenate([x, jnp.zeros((x.shape[0], width - x.shape[1]), x.dtype)], axis=1)


def pair_loop(own_cols, near_lanes, q, first, last, with_self, carry):
    rows = [step_rows(q, g) for g in range(GROUPS)]
    own = [[own_cols[rows[g], a * L:(a + 1) * L] for a in range(3)] for g in range(GROUPS)]

    def body(c, carry):
        force, en = [list(f) for f in carry[0]], carry[1]
        for t in range(CHUNK):
            place = pl.ds(pl.multiple_of((c * CHUNK + t) * L, L), L)
            near_xyz = [near_lanes[a, :, place] for a in range(3)]
            for g in range(GROUPS):
                dx, dy, dz = [own[g][a] - near_xyz[a] for a in range(3)]
                d2 = dx * dx + dy * dy + dz * dz
                near = d2 < RC * RC
                if with_self:
                    near = near & (d2 > 0.0)
                inv = jnp.where(near, lax.rsqrt(d2), 0.0)
                s2 = inv * inv
                s6 = s2 * s2 * s2
                s12 = s6 * s6
                p = s12 - s6
                w = inv * (UPC / 24.0)
                scale = (p + s12) * s2 + w
                en = en + ((p + jnp.where(near, 0.25 * (RC * UPC - UCUT), 0.0)) - 6.0 * (w * d2))
                force[g] = [force[g][0] + scale * dx, force[g][1] + scale * dy, force[g][2] + scale * dz]
        return tuple(tuple(f) for f in force), en

    return lax.fori_loop(first, last, body, carry)


def step_rows(q, g):
    return pl.ds(pl.multiple_of((q * GROUPS + g) * 8, 8), 8)


def own_columns(xyz):
    slots = xyz.shape[1]
    parts = [part.astype(F32) for part in split3(xyz)]
    parts = jnp.concatenate(parts + [jnp.zeros((7, slots), F32)], axis=0)
    row = lax.broadcasted_iota(I32, (16, 3 * L), 0)
    tile = lax.broadcasted_iota(I32, (16, 3 * L), 1) // L
    picks = jnp.where((row == tile) | (row == tile + 3) | (row == tile + 6), 1.0, 0.0).astype(BF16)
    return lax.dot_general(jnp.transpose(parts).astype(BF16), picks, NN, preferred_element_type=F32)


def exchange_kernel(sizes, peers, slots, pos_hbm, vel_hbm, frc_hbm, id_hbm, ok_hbm, side_ref, srt_ref, gh_ref, ga_ref, own_ref, inner_ref, inner_en_ref, pos_ref, vel_ref, frc_ref, id_ref, ok_ref, pkt, rcv, out3, new3, lanes, isem, psend, precv, gsend, grecv, asend, arecv):
    size_x, size_y, size_z = sizes
    me = (lax.axis_index("x"), lax.axis_index("y"), lax.axis_index("z"))

    def device_at(offset):
        return (lax.rem(me[2] + offset[2], size_z), lax.rem(me[1] + offset[1], size_y), lax.rem(me[0] + offset[0], size_x))

    loads = []
    for index, (src, dst) in enumerate(((ok_hbm, ok_ref), (id_hbm, id_ref), (pos_hbm, pos_ref), (vel_hbm, vel_ref), (frc_hbm, frc_ref))):
        load = pltpu.make_async_copy(src, dst, isem.at[index])
        load.start()
        loads.append(load)
    barrier = pltpu.get_barrier_semaphore()
    for offset in peers:
        pl.semaphore_signal(barrier, inc=1, device_id=device_at(offset), device_id_type=pl.DeviceIdType.MESH)

    n = pos_ref.shape[1]
    for load in loads:
        load.wait()
    side = side_ref[0, 0]
    owned = pad_lanes(jnp.reshape(ok_ref[...], (1, n)), slots) > 0
    half = vel_ref[...] + (0.5 * DT) * frc_ref[...]
    free = pos_ref[...] + DT * half
    half = pad_lanes(half, slots)
    free = pad_lanes(free, slots)
    ids = pad_lanes(jnp.reshape(id_ref[...], (1, n)), slots)
    code = jnp.zeros((1, slots), I32)
    moved = []
    low_side = []
    for axis in range(3):
        low = me[axis].astype(F32) * side
        high = (me[axis] + 1).astype(F32) * side
        box = side * float(sizes[axis])
        u = free[axis:axis + 1]
        step = jnp.where(u >= high, 1, 0) - jnp.where(u < low, 1, 0)
        code = code + (step + 1) * (1, 3, 9)[axis]
        moved.append(jnp.where(u < 0.0, u + box, jnp.where(u >= box, u - box, u)))
        low_side.append(low)
    code = jnp.where(owned, code, 31)
    id_hi = (ids >> 16).astype(F32)
    id_lo = (ids & 65535).astype(F32)
    okf = jnp.where(owned, 1.0, 0.0)
    data = jnp.concatenate(moved + [half, id_hi, id_lo, okf, jnp.zeros((7, slots), F32)], axis=0)

    place, _ = class_places(code, False)
    leaving = owned & (code != 13)
    way = jnp.where(leaving, code - jnp.where(code > 13, 1, 0), 31)
    member = jnp.where(lax.broadcasted_iota(I32, (32, slots), 0) == way, 1.0, 0.0).astype(BF16)
    fields = jnp.concatenate([jnp.where(place == float(k), data, 0.0) for k in range(PACK)], axis=0)
    packed = jnp.zeros((32, L), F32)
    for part in split3(fields):
        packed = packed + lax.dot_general(member, part, NT, preferred_element_type=F32)
    pkt[...] = packed

    def bins_of(pos):
        bins = []
        for axis in range(3):
            loc = pos[axis:axis + 1] - low_side[axis]
            bins.append(jnp.where(loc < NEAR, 0, jnp.where(loc > side - NEAR, 2, 1)))
        return [(bins[i] * 3 + bins[j]) * 3 + bins[k] for i, j, k in MAJOR]

    wide = side > 2.0 * NEAR
    eye = lax.broadcasted_iota(I32, (32, L), 0) == lax.broadcasted_iota(I32, (32, L), 1)

    def sorted_block(cand, keys, kept):
        width = cand.shape[1]
        where_to, before = class_places(jnp.where(kept, keys, 28), True)
        arranged = scatter_lanes(cand, jnp.where(kept, where_to.astype(I32), -1), width)
        total = jnp.concatenate([before[27:28]] * (width // L), axis=1)
        lane = lax.broadcasted_iota(I32, (1, width), 1).astype(F32)
        begins = jnp.sum(jnp.where(eye, before, 0.0), axis=0, keepdims=True)
        ends = jnp.where(wide, begins, before[27:28])
        counts = jnp.concatenate([jnp.where(wide, begins, 0.0)[:, 0:32], ends[:, 0:32], jnp.zeros((1, L - 64), F32)], axis=1)
        return jnp.concatenate([jnp.where(lane < total, arranged[0:3], FAR), pad_lanes(counts, width)], axis=0)

    def send(src, dst, ssem, rsem, offset):
        copy = pltpu.make_async_remote_copy(
            src_ref=src, dst_ref=dst, send_sem=ssem, recv_sem=rsem,
            device_id=device_at(offset), device_id_type=pl.DeviceIdType.MESH)
        copy.start()
        return copy

    def send_blocks(block, dst, ssem, rsem, kind):
        out = []
        for index, offset in enumerate(peers):
            if order_of(tuple(0 if c == 0 else 1 for c in offset)) == kind:
                out.append(send(block.at[kind], dst.at[index], ssem.at[index], rsem.at[index], offset))
        return out

    staying = code == 13
    keys = bins_of(data)
    for kind in range(3):
        out3[kind] = sorted_block(data[0:8], keys[kind], staying)
    pl.semaphore_wait(barrier, len(peers))
    packets = []
    for index, d in enumerate(DIRS):
        row = pl.ds(index, 1)
        packets.append(send(pkt.at[row], rcv.at[row], psend.at[index], precv.at[index], (d[0] % size_x, d[1] % size_y, d[2] % size_z)))
    blocks = []
    for kind in range(3):
        blocks = blocks + send_blocks(out3, gh_ref, gsend, grecv, kind)
    for copy in packets:
        copy.wait_recv()

    came = jnp.concatenate([rcv[...], jnp.zeros((32 - 26, L), F32)], axis=0)
    came = jnp.concatenate([came] + [pltpu.roll(came, L - 16 * k, 1) for k in range(1, PACK)], axis=0)
    came_t = jnp.transpose(came)[0:16]
    came_ok = came_t[8:9] > 0.5
    keys = bins_of(came_t)
    late = []
    for kind in range(3):
        new3[kind] = sorted_block(came_t[0:8], keys[kind], came_ok)
        late = late + send_blocks(new3, ga_ref, asend, arecv, kind)
    for copy in packets:
        copy.wait_send()

    arr_ids = came[:, 6:7].astype(I32) * 65536 + came[:, 7:8].astype(I32)
    arr_ok = came[:, 8:9] > 0.5
    row_ids = jnp.concatenate([ids, came_t[6:7].astype(I32) * 65536 + came_t[7:8].astype(I32)], axis=1)
    less = jnp.where((arr_ids < row_ids) & arr_ok, 1.0, 0.0)
    arrivals_below = jnp.sum(less, axis=0, keepdims=True)
    above = jnp.where((arr_ids > row_ids[:, 0:slots]) & staying, 1.0, 0.0).astype(BF16)
    stay_below = lax.dot_general(jnp.ones((16, slots), BF16), above, NT, preferred_element_type=F32)[0:1]
    stay_place, _ = class_places(jnp.where(staying, 0, 31), False)
    rank = jnp.concatenate([stay_place, stay_below], axis=1) + arrivals_below
    dest = jnp.where(jnp.concatenate([staying, came_ok], axis=1), rank.astype(I32), -1)
    merged = scatter_lanes(jnp.concatenate([data, came_t], axis=1), dest, slots)
    srt_ref[...] = jnp.where(lax.broadcasted_iota(I32, (16, slots), 0) == 9, side, merged)

    good = merged[8:9] > 0.5
    own_ref[...] = own_columns(jnp.where(good, merged[0:3], -FAR))
    for a in range(3):
        lanes[a] = jnp.broadcast_to(jnp.where(good, merged[a:a + 1], FAR), (8, slots))
    zero = jnp.zeros(TILE, F32)

    def own_step(q, energy):
        force, energy = pair_loop(own_ref, lanes, q, 0, slots // (CHUNK * L), True, (((zero,) * 3,) * GROUPS, energy))
        for g in range(GROUPS):
            for a in range(3):
                inner_ref[a, step_rows(q, g), :] = force[g][a]
        return energy

    inner_en_ref[...] = lax.fori_loop(0, slots // (8 * GROUPS), own_step, zero)

    for copy in blocks + late:
        copy.wait()


def force_kernel(sizes, peers, slots, srt_ref, gh_ref, ga_ref, own_cols, inner_ref, inner_en_ref, offs_ref, pos_ref, vel_ref, frc_ref, id_ref, ok_ref, en_ref, line, wide_line, sums):
    size_x, size_y, size_z = sizes
    me = (lax.axis_index("x"), lax.axis_index("y"), lax.axis_index("z"))
    n = pos_ref.shape[1]
    side = srt_ref[9:10, 0:1]
    okrow = srt_ref[8:9]
    good = okrow > 0.5
    count = jnp.sum(okrow).astype(I32)
    span = slots + L

    away = jnp.full(TILE, FAR, F32)
    line[:, 0:L] = away
    lane = lax.broadcasted_iota(I32, (8, span), 1)
    fill = jnp.int32(0)
    for d in DIRS:
        offset = (d[0] % size_x, d[1] % size_y, d[2] % size_z)
        back = ((-offset[0]) % size_x, (-offset[1]) % size_y, (-offset[2]) % size_z)
        index = peers.index(back)
        low, high = range_of(d)
        shifts = []
        for axis in range(3):
            box = side * float(sizes[axis])
            if d[axis] == 1:
                shifts.append(jnp.where(me[axis] == sizes[axis] - 1, box, 0.0))
            elif d[axis] == -1:
                shifts.append(jnp.where(me[axis] == 0, -box, 0.0))
            else:
                shifts.append(jnp.zeros((1, 1), F32))
        for source, entry in ((gh_ref, index), (ga_ref, index + len(peers))):
            width = source.shape[2]
            begin = offs_ref[entry, low]
            end = offs_ref[entry, 32 + high]
            block = jnp.concatenate([source[index, a:a + 1] + shifts[a] for a in range(3)] + [jnp.zeros((5, width), F32)], axis=0)
            block = jnp.concatenate([block, away], axis=1)
            head = fill & (L - 1)
            base = pl.multiple_of(fill - head, L)
            move = head - begin
            block = pltpu.roll(block, jnp.where(move < 0, move + (width + L), move), 1)
            block = jnp.where(lane[:, 0:width + L] < head + end - begin, block, FAR)
            line[:, pl.ds(base, L)] = jnp.where(lane[:, 0:L] < head, line[:, pl.ds(base, L)], block[:, 0:L])
            line[:, pl.ds(pl.multiple_of(base + L, L), width)] = block[:, L:]
            fill = fill + (end - begin)
    rest = pl.multiple_of(((fill + L - 1) // L) * L, L)
    line[:, pl.ds(rest, CHUNK * L)] = jnp.full((8, CHUNK * L), FAR, F32)
    chunks = jnp.maximum((fill + CHUNK * L - 1) // (CHUNK * L), 1)

    def widen(c, carry):
        for t in range(CHUNK):
            place = pl.ds(pl.multiple_of((c * CHUNK + t) * L, L), L)
            tile = line[:, place]
            for a in range(3):
                wide_line[a, :, place] = jnp.broadcast_to(tile[a:a + 1], TILE)
        return carry

    lax.fori_loop(0, chunks, widen, 0)

    def own_step(q, energy):
        start = tuple(tuple(inner_ref[a, step_rows(q, g), :] for a in range(3)) for g in range(GROUPS))
        force, energy = pair_loop(own_cols, wide_line, q, 0, chunks, False, (start, energy))
        for g in range(GROUPS):
            for a in range(3):
                sums[a, step_rows(q, g), :] = force[g][a]
        return energy

    own_steps = (count + 8 * GROUPS - 1) // (8 * GROUPS)
    energy = lax.fori_loop(0, own_steps, own_step, inner_en_ref[...])
    en_ref[...] = 2.0 * jnp.sum(energy, axis=0, keepdims=True)

    col = lax.broadcasted_iota(I32, (L, L), 1)
    total = jnp.zeros((slots, L), F32)
    for a in range(3):
        pick = jnp.where(col == a, 1.0, 0.0).astype(BF16)
        for part in split3(sums[a]):
            total = total + lax.dot_general(part, pick, NN, preferred_element_type=F32)
    force = jnp.where(good, 24.0 * jnp.transpose(total)[0:3], 0.0)
    pos_ref[...] = srt_ref[0:3, 0:n]
    frc_ref[...] = force[:, 0:n]
    vel_ref[...] = (srt_ref[3:6] + (0.5 * DT) * force)[:, 0:n]
    id_ref[...] = jnp.reshape((srt_ref[6:7].astype(I32) * 65536 + srt_ref[7:8].astype(I32))[:, 0:n], (n,))
    ok_ref[...] = jnp.reshape(okrow[:, 0:n].astype(I32), (n,))


def total_kernel(sizes, part_ref, sum_ref, rows, ssem, rsem):
    size_x, size_y, size_z = sizes
    me = (lax.axis_index("x"), lax.axis_index("y"), lax.axis_index("z"))
    mine = (me[2] * size_y + me[1]) * size_x + me[0]
    others = [(dx, dy, dz) for dz in range(size_z) for dy in range(size_y) for dx in range(size_x) if dx + dy + dz > 0]
    others.sort(key=lambda o: -(2 * min(o[2], size_z - o[2]) + 2 * o[1] + min(o[0], size_x - o[0])))

    def device_at(offset):
        return (lax.rem(me[2] + offset[2], size_z), lax.rem(me[1] + offset[1], size_y), lax.rem(me[0] + offset[0], size_x))

    barrier = pltpu.get_barrier_semaphore()
    for offset in others:
        pl.semaphore_signal(barrier, inc=1, device_id=device_at(offset), device_id_type=pl.DeviceIdType.MESH)
    rows[pl.ds(mine, 1)] = part_ref[...]
    pl.semaphore_wait(barrier, len(others))
    copies = []
    for index, offset in enumerate(others):
        copy = pltpu.make_async_remote_copy(
            src_ref=part_ref, dst_ref=rows.at[pl.ds(mine, 1)], send_sem=ssem.at[index], recv_sem=rsem.at[index],
            device_id=device_at(offset), device_id_type=pl.DeviceIdType.MESH)
        copy.start()
        copies.append(copy)
    for copy in copies:
        copy.wait_recv()
    sum_ref[...] = jnp.sum(rows[...], axis=0, keepdims=True)
    for copy in copies:
        copy.wait_send()


def solution(mesh):
    sizes = (mesh.shape["x"], mesh.shape["y"], mesh.shape["z"])
    peers = sorted({(d[0] % sizes[0], d[1] % sizes[1], d[2] % sizes[2]) for d in DIRS} - {(0, 0, 0)})
    devices = sizes[0] * sizes[1] * sizes[2]

    def local_step(atom_pos, atom_vel, atom_frc, atom_id, atom_ok, brick_side):
        n = atom_pos.shape[0]
        slots = -(-n // L) * L
        side = jnp.reshape(brick_side, (1, 1))
        vmem = pl.BlockSpec(memory_space=pltpu.VMEM)
        smem = pl.BlockSpec(memory_space=pltpu.SMEM)
        srt, ghosts, fresh, own, inner, inner_en = pl.pallas_call(
            functools.partial(exchange_kernel, sizes, peers, slots),
            out_shape=(jax.ShapeDtypeStruct((16, slots), F32), jax.ShapeDtypeStruct((len(peers), 4, slots), F32), jax.ShapeDtypeStruct((len(peers), 4, NEW), F32),
                       jax.ShapeDtypeStruct((slots, 3 * L), F32), jax.ShapeDtypeStruct((3, slots, L), F32), jax.ShapeDtypeStruct(TILE, F32)),
            in_specs=[pl.BlockSpec(memory_space=pltpu.HBM)] * 5 + [smem],
            out_specs=(vmem,) * 6,
            scratch_shapes=[
                pltpu.VMEM((3, n), F32), pltpu.VMEM((3, n), F32), pltpu.VMEM((3, n), F32), pltpu.VMEM((n,), I32), pltpu.VMEM((n,), I32),
                pltpu.VMEM((32, L), F32), pltpu.VMEM((26, L), F32), pltpu.VMEM((3, 4, slots), F32), pltpu.VMEM((3, 4, NEW), F32), pltpu.VMEM((3, 8, slots), F32),
                pltpu.SemaphoreType.DMA((5,)), pltpu.SemaphoreType.DMA((26,)), pltpu.SemaphoreType.DMA((26,)),
            ] + [pltpu.SemaphoreType.DMA((len(peers),))] * 4,
            compiler_params=pltpu.CompilerParams(collective_id=0, has_side_effects=True, vmem_limit_bytes=40 * 2 ** 20),
            name="exchange",
        )(*[pltpu.with_memory_space_constraint(v, pltpu.HBM) for v in (atom_pos.T, atom_vel.T, atom_frc.T, atom_id, atom_ok)], side)
        offs = jnp.concatenate([ghosts[:, 3, 0:64], fresh[:, 3, 0:64]], axis=0).astype(I32)
        out_f = jax.ShapeDtypeStruct((3, n), F32)
        out_i = jax.ShapeDtypeStruct((n,), I32)
        new_pos, new_vel, new_frc, new_id, new_ok, energy = pl.pallas_call(
            functools.partial(force_kernel, sizes, peers, slots),
            out_shape=(out_f, out_f, out_f, out_i, out_i, jax.ShapeDtypeStruct((1, L), F32)),
            in_specs=[vmem] * 6 + [smem],
            out_specs=(vmem,) * 6,
            scratch_shapes=[pltpu.VMEM((8, 28 * slots + CHUNK * L), F32), pltpu.VMEM((3, 8, 28 * slots + CHUNK * L), F32), pltpu.VMEM((3, slots, L), F32)],
            compiler_params=pltpu.CompilerParams(vmem_limit_bytes=40 * 2 ** 20),
            name="forces",
        )(srt, ghosts, fresh, own, inner, inner_en, offs)
        energy = pl.pallas_call(
            functools.partial(total_kernel, sizes),
            out_shape=jax.ShapeDtypeStruct((1, L), F32),
            in_specs=[vmem],
            out_specs=vmem,
            scratch_shapes=[pltpu.VMEM((devices, L), F32), pltpu.SemaphoreType.DMA((devices,)), pltpu.SemaphoreType.DMA((devices,))],
            compiler_params=pltpu.CompilerParams(collective_id=1, has_side_effects=True, vmem_limit_bytes=4 * 2 ** 20),
            name="total",
        )(pltpu.with_memory_space_constraint(energy, pltpu.VMEM))
        return new_pos.T, new_vel.T, new_frc.T, new_id, new_ok, jnp.sum(energy)

    row_spec = P(MESH_AXES, None)
    id_spec = P(MESH_AXES)
    return jax.shard_map(local_step, mesh=mesh, in_specs=(row_spec, row_spec, row_spec, id_spec, id_spec, P()), out_specs=(row_spec, row_spec, row_spec, id_spec, id_spec, P()), check_vma=False)
```

```python
import functools

import jax
import jax.numpy as jnp
from jax import lax
from jax.experimental import pallas as pl
from jax.experimental.pallas import tpu as pltpu
from jax.sharding import PartitionSpec as P

DT = 0.005
RC = 2.5
FAR = 1.0e6
UCUT = 4.0 * (RC ** -12 - RC ** -6)
UPC = -48.0 * RC ** -13 + 24.0 * RC ** -7
MESH_AXES = ("z", "y", "x")
DIRS = [(dx, dy, dz) for dz in (-1, 0, 1) for dy in (-1, 0, 1) for dx in (-1, 0, 1) if (dx, dy, dz) != (0, 0, 0)]
NEAR = RC + 1.0e-3
MAJOR = ((2, 1, 0), (1, 0, 2), (0, 2, 1))
PACK = 8
NEW = 256
CHUNK = 3
GROUPS = 8
L = 128
TILE = (8, L)
F32 = jnp.float32
BF16 = jnp.bfloat16
I32 = jnp.int32
NT = (((1,), (1,)), ((), ()))
NN = (((1,), (0,)), ((), ()))


def device_of(sizes, me, offset):
    return tuple(lax.rem(me[axis] + offset[axis], sizes[axis]) for axis in (2, 1, 0))


def offset_of(sizes, d):
    return tuple(c % size for c, size in zip(d, sizes))


def order_of(d):
    if d[2] == 0:
        return 1 if d[1] != 0 else 2
    return 2 if (d[1] == 0 and d[0] != 0) else 0


def range_of(d):
    first, size = 0, 27
    for axis in MAJOR[order_of(d)]:
        if d[axis] == 0:
            break
        size = size // 3
        first = first + (1, 0, 2)[d[axis]] * size
    return first, first + size


def split3(x):
    hi = x.astype(BF16)
    rest = x - hi.astype(F32)
    mid = rest.astype(BF16)
    low = (rest - mid.astype(F32)).astype(BF16)
    return hi, mid, low


def onehot_rows(dest, base, count):
    rows = lax.broadcasted_iota(I32, (count, dest.shape[1]), 0) + base
    return jnp.where(rows == dest, 1.0, 0.0).astype(BF16)


def scatter_lanes(data, dest, slots):
    rows = data.shape[0]
    parts = jnp.concatenate(split3(data), axis=0)
    out = []
    for base in range(0, slots, 256):
        hot = onehot_rows(dest, base, min(256, slots - base))
        got = lax.dot_general(parts, hot, NT, preferred_element_type=F32)
        out.append(got[0:rows] + got[rows:2 * rows] + got[2 * rows:3 * rows])
    return jnp.concatenate(out, axis=1)


def class_places(code, with_before):
    width = code.shape[1]
    tiles = width // L
    cls = lax.broadcasted_iota(I32, (32, width), 0)
    member = jnp.where(cls == code, 1.0, 0.0)
    member_b = member.astype(BF16)
    stacked = jnp.concatenate([member_b[:, t * L:(t + 1) * L] for t in range(tiles)], axis=0)
    row_i = lax.broadcasted_iota(I32, (L, 256), 0)
    col_i = lax.broadcasted_iota(I32, (L, 256), 1)
    tri = jnp.where((row_i < col_i) | (col_i >= L), 1.0, 0.0).astype(BF16)
    pre = lax.dot_general(stacked, tri, NN, preferred_element_type=F32)
    carry = jnp.zeros((32, L), F32)
    if with_before:
        before_b = jnp.where(code < cls, 1.0, 0.0).astype(BF16)
        before_s = before_b[:, 0:L]
        tot = None
        ones = jnp.ones((L, L), BF16)
        for t in range(tiles):
            part = lax.dot_general(before_b[:, t * L:(t + 1) * L], ones, NN, preferred_element_type=F32)
            tot = part if tot is None else tot + part
        before = tot
        carry = before
    else:
        before = None
    places = []
    for t in range(tiles):
        within = pre[32 * t:32 * t + 32, 0:L] + carry
        places.append(jnp.sum(member[:, t * L:(t + 1) * L] * within, axis=0, keepdims=True))
        carry = carry + pre[32 * t:32 * t + 32, L:256]
    return jnp.concatenate(places, axis=1), before


def pad_lanes(x, width):
    return jnp.concatenate([x, jnp.zeros((x.shape[0], width - x.shape[1]), x.dtype)], axis=1)


def pair_loop(own_cols, near_lanes, q, first, last, with_self, carry):
    rows = [step_rows(q, g) for g in range(GROUPS)]
    own = [[own_cols[rows[g], a * L:(a + 1) * L] for a in range(3)] for g in range(GROUPS)]

    def body(c, carry):
        force, en = [list(f) for f in carry[0]], list(carry[1])
        for t in range(CHUNK):
            place = pl.ds(pl.multiple_of((c * CHUNK + t) * L, L), L)
            near_xyz = [near_lanes[a, :, place] for a in range(3)]
            for g in range(GROUPS):
                dx, dy, dz = [own[g][a] - near_xyz[a] for a in range(3)]
                d2 = dx * dx + dy * dy + dz * dz
                near = d2 < RC * RC
                if with_self:
                    near = near & (d2 > 0.0)
                inv = jnp.where(near, lax.rsqrt(d2), 0.0)
                s2 = inv * inv
                s6 = s2 * s2 * s2
                s12 = s6 * s6
                p = s12 - s6
                w = inv * (UPC / 24.0)
                scale = (p + s12) * s2 + w
                en = [en[0] + p, en[1] + w * d2, en[2] + jnp.where(near, 1.0, 0.0)]
                force[g] = [force[g][0] + scale * dx, force[g][1] + scale * dy, force[g][2] + scale * dz]
        return tuple(tuple(f) for f in force), tuple(en)

    return lax.fori_loop(first, last, body, carry)


def step_rows(q, g):
    return pl.ds(pl.multiple_of((q * GROUPS + g) * 8, 8), 8)


def own_columns(xyz):
    slots = xyz.shape[1]
    parts = [part.astype(F32) for part in split3(xyz)]
    parts = jnp.concatenate(parts + [jnp.zeros((7, slots), F32)], axis=0)
    row = lax.broadcasted_iota(I32, (16, 3 * L), 0)
    tile = lax.broadcasted_iota(I32, (16, 3 * L), 1) // L
    picks = jnp.where((row == tile) | (row == tile + 3) | (row == tile + 6), 1.0, 0.0).astype(BF16)
    return lax.dot_general(jnp.transpose(parts).astype(BF16), picks, NN, preferred_element_type=F32)


def exchange_kernel(sizes, peers, slots, pos_hbm, vel_hbm, frc_hbm, id_hbm, ok_hbm, side_ref, srt_ref, gh_ref, ga_ref, own_ref, inner_ref, inner_en_ref, pos_ref, vel_ref, frc_ref, id_ref, ok_ref, pkt, rcv, out3, new3, lanes, isem, psend, precv, gsend, grecv, asend, arecv):
    me = [lax.axis_index(name) for name in "xyz"]

    device_at = functools.partial(device_of, sizes, me)

    loads = []
    for index, (src, dst) in enumerate(((ok_hbm, ok_ref), (id_hbm, id_ref), (pos_hbm, pos_ref), (vel_hbm, vel_ref), (frc_hbm, frc_ref))):
        load = pltpu.make_async_copy(src, dst, isem.at[index])
        load.start()
        loads.append(load)
    barrier = pltpu.get_barrier_semaphore()
    for offset in peers:
        pl.semaphore_signal(barrier, inc=1, device_id=device_at(offset), device_id_type=pl.DeviceIdType.MESH)

    n = pos_ref.shape[1]
    for load in loads:
        load.wait()
    side = side_ref[0, 0]
    owned = pad_lanes(jnp.reshape(ok_ref[...], (1, n)), slots) > 0
    half = vel_ref[...] + (0.5 * DT) * frc_ref[...]
    free = pos_ref[...] + DT * half
    half = pad_lanes(half, slots)
    free = pad_lanes(free, slots)
    ids = pad_lanes(jnp.reshape(id_ref[...], (1, n)), slots)
    code = jnp.zeros((1, slots), I32)
    moved = []
    low_side = []
    for axis in range(3):
        low = me[axis].astype(F32) * side
        high = (me[axis] + 1).astype(F32) * side
        box = side * float(sizes[axis])
        u = free[axis:axis + 1]
        step = jnp.where(u >= high, 1, 0) - jnp.where(u < low, 1, 0)
        code = code + (step + 1) * (1, 3, 9)[axis]
        moved.append(jnp.where(u < 0.0, u + box, jnp.where(u >= box, u - box, u)))
        low_side.append(low)
    code = jnp.where(owned, code, 31)
    id_hi = (ids >> 16).astype(F32)
    id_lo = (ids & 65535).astype(F32)
    okf = jnp.where(owned, 1.0, 0.0)
    data = jnp.concatenate(moved + [half, id_hi, id_lo, okf, jnp.zeros((7, slots), F32)], axis=0)

    place, _ = class_places(code, False)
    leaving = owned & (code != 13)
    way = jnp.where(leaving, code - jnp.where(code > 13, 1, 0), 31)
    member = jnp.where(lax.broadcasted_iota(I32, (32, slots), 0) == way, 1.0, 0.0).astype(BF16)
    fields = jnp.concatenate([jnp.where(place == float(k), data, 0.0) for k in range(PACK)], axis=0)
    packed = jnp.zeros((32, L), F32)
    for part in split3(fields):
        packed = packed + lax.dot_general(member, part, NT, preferred_element_type=F32)
    pkt[...] = packed

    def bins_of(pos):
        bins = []
        for axis in range(3):
            loc = pos[axis:axis + 1] - low_side[axis]
            bins.append(jnp.where(loc < NEAR, 0, jnp.where(loc > side - NEAR, 2, 1)))
        return [(bins[i] * 3 + bins[j]) * 3 + bins[k] for i, j, k in MAJOR]

    wide = side > 2.0 * NEAR
    eye = lax.broadcasted_iota(I32, (32, L), 0) == lax.broadcasted_iota(I32, (32, L), 1)

    def sorted_block(cand, keys, kept):
        width = cand.shape[1]
        where_to, before = class_places(jnp.where(kept, keys, 28), True)
        arranged = scatter_lanes(cand, jnp.where(kept, where_to.astype(I32), -1), width)
        total = jnp.concatenate([before[27:28]] * (width // L), axis=1)
        lane = lax.broadcasted_iota(I32, (1, width), 1).astype(F32)
        begins = jnp.sum(jnp.where(eye, before, 0.0), axis=0, keepdims=True)
        ends = jnp.where(wide, begins, before[27:28])
        counts = jnp.concatenate([jnp.where(wide, begins, 0.0)[:, 0:32], ends[:, 0:32], jnp.zeros((1, L - 64), F32)], axis=1)
        return jnp.concatenate([jnp.where(lane < total, arranged[0:3], FAR), pad_lanes(counts, width)], axis=0)

    def send(src, dst, ssem, rsem, offset):
        copy = pltpu.make_async_remote_copy(
            src_ref=src, dst_ref=dst, send_sem=ssem, recv_sem=rsem,
            device_id=device_at(offset), device_id_type=pl.DeviceIdType.MESH)
        copy.start()
        return copy

    def send_blocks(block, dst, ssem, rsem, kind):
        out = []
        for index, offset in enumerate(peers):
            if order_of(tuple(0 if c == 0 else 1 for c in offset)) == kind:
                out.append(send(block.at[kind], dst.at[index], ssem.at[index], rsem.at[index], offset))
        return out

    staying = code == 13
    keys = bins_of(data)
    for kind in range(3):
        out3[kind] = sorted_block(data[0:8], keys[kind], staying)
    pl.semaphore_wait(barrier, len(peers))
    packets = []
    for index, d in enumerate(DIRS):
        row = pl.ds(index, 1)
        packets.append(send(pkt.at[row], rcv.at[row], psend.at[index], precv.at[index], offset_of(sizes, d)))
    blocks = []
    for kind in range(3):
        blocks = blocks + send_blocks(out3, gh_ref, gsend, grecv, kind)
    for copy in packets:
        copy.wait_recv()

    came = jnp.concatenate([rcv[...], jnp.zeros((32 - 26, L), F32)], axis=0)
    came = jnp.concatenate([came] + [pltpu.roll(came, L - 16 * k, 1) for k in range(1, PACK)], axis=0)
    came_t = jnp.transpose(came)[0:16]
    came_ok = came_t[8:9] > 0.5
    keys = bins_of(came_t)
    late = []
    for kind in range(3):
        new3[kind] = sorted_block(came_t[0:8], keys[kind], came_ok)
        late = late + send_blocks(new3, ga_ref, asend, arecv, kind)
    for copy in packets:
        copy.wait_send()

    arr_ids = came[:, 6:7].astype(I32) * 65536 + came[:, 7:8].astype(I32)
    arr_ok = came[:, 8:9] > 0.5
    row_ids = jnp.concatenate([ids, came_t[6:7].astype(I32) * 65536 + came_t[7:8].astype(I32)], axis=1)
    less = jnp.where((arr_ids < row_ids) & arr_ok, 1.0, 0.0)
    arrivals_below = jnp.sum(less, axis=0, keepdims=True)
    above = jnp.where((arr_ids > row_ids[:, 0:slots]) & staying, 1.0, 0.0).astype(BF16)
    stay_below = lax.dot_general(jnp.ones((16, slots), BF16), above, NT, preferred_element_type=F32)[0:1]
    stay_place, _ = class_places(jnp.where(staying, 0, 31), False)
    rank = jnp.concatenate([stay_place, stay_below], axis=1) + arrivals_below
    dest = jnp.where(jnp.concatenate([staying, came_ok], axis=1), rank.astype(I32), -1)
    merged = scatter_lanes(jnp.concatenate([data, came_t], axis=1), dest, slots)
    srt_ref[...] = jnp.where(lax.broadcasted_iota(I32, (16, slots), 0) == 9, side, merged)

    good = merged[8:9] > 0.5
    own_ref[...] = own_columns(jnp.where(good, merged[0:3], -FAR))
    first = CHUNK * L
    for a in range(3):
        lanes[a] = jnp.broadcast_to(jnp.where(good, merged[a:a + 1], FAR)[:, 0:first], (8, first))
    zero = jnp.zeros(TILE, F32)

    def own_step(q, energy):
        force, energy = pair_loop(own_ref, lanes, q, 0, 1, True, (((zero,) * 3,) * GROUPS, energy))
        for g in range(GROUPS):
            for a in range(3):
                inner_ref[a, step_rows(q, g), :] = force[g][a]
        return energy

    for k, part in enumerate(lax.fori_loop(0, slots // (8 * GROUPS), own_step, (zero,) * 3)):
        inner_en_ref[k] = part

    for copy in blocks + late:
        copy.wait()


def force_kernel(sizes, peers, slots, srt_ref, gh_ref, ga_ref, own_cols, inner_ref, inner_en_ref, offs_ref, pos_ref, vel_ref, frc_ref, id_ref, ok_ref, en_ref, line, wide_line, sums, added):
    me = [lax.axis_index(name) for name in "xyz"]
    n = pos_ref.shape[1]
    side = srt_ref[9:10, 0:1]
    okrow = srt_ref[8:9]
    good = okrow > 0.5
    count = jnp.sum(okrow).astype(I32)
    span = slots + L

    away = jnp.full(TILE, FAR, F32)
    first = CHUNK * L
    line[:, 0:slots - first] = jnp.concatenate([jnp.where(good, srt_ref[0:3], FAR), jnp.full((5, slots), FAR, F32)], axis=0)[:, first:]
    lane = lax.broadcasted_iota(I32, (8, span), 1)
    fill = jnp.maximum(count - first, 0)
    for d in DIRS:
        index = peers.index(offset_of(sizes, [-c for c in d]))
        low, high = range_of(d)
        shifts = []
        for axis in range(3):
            box = side * float(sizes[axis])
            if d[axis] == 1:
                shifts.append(jnp.where(me[axis] == sizes[axis] - 1, box, 0.0))
            elif d[axis] == -1:
                shifts.append(jnp.where(me[axis] == 0, -box, 0.0))
            else:
                shifts.append(jnp.zeros((1, 1), F32))
        for source, entry in ((gh_ref, index), (ga_ref, index + len(peers))):
            width = source.shape[2]
            begin = offs_ref[entry, low]
            end = offs_ref[entry, 32 + high]
            block = jnp.concatenate([source[index, a:a + 1] + shifts[a] for a in range(3)] + [jnp.zeros((5, width), F32)], axis=0)
            block = jnp.concatenate([block, away], axis=1)
            head = fill & (L - 1)
            base = pl.multiple_of(fill - head, L)
            move = head - begin
            block = pltpu.roll(block, jnp.where(move < 0, move + (width + L), move), 1)
            block = jnp.where(lane[:, 0:width + L] < head + end - begin, block, FAR)
            line[:, pl.ds(base, L)] = jnp.where(lane[:, 0:L] < head, line[:, pl.ds(base, L)], block[:, 0:L])
            line[:, pl.ds(pl.multiple_of(base + L, L), width)] = block[:, L:]
            fill = fill + (end - begin)
    rest = pl.multiple_of(((fill + L - 1) // L) * L, L)
    line[:, pl.ds(rest, CHUNK * L)] = jnp.full((8, CHUNK * L), FAR, F32)
    chunks = jnp.maximum((fill + CHUNK * L - 1) // (CHUNK * L), 1)

    def widen(c, carry):
        for t in range(CHUNK):
            place = pl.ds(pl.multiple_of((c * CHUNK + t) * L, L), L)
            tile = line[:, place]
            for a in range(3):
                wide_line[a, :, place] = jnp.broadcast_to(tile[a:a + 1], TILE)
        return carry

    lax.fori_loop(0, chunks, widen, 0)

    def own_step(q, energy):
        start = tuple(tuple(inner_ref[a, step_rows(q, g), :] for a in range(3)) for g in range(GROUPS))
        carry = pair_loop(own_cols, wide_line, q, 0, 1, True, (start, energy))
        force, energy = pair_loop(own_cols, wide_line, q, 1, chunks, False, carry)
        for g in range(GROUPS):
            for a in range(3):
                sums[a, step_rows(q, g), :] = force[g][a]
        return energy

    own_steps = (count + 8 * GROUPS - 1) // (8 * GROUPS)
    energy = lax.fori_loop(0, own_steps, own_step, tuple(inner_en_ref[k] for k in range(3)))
    en_ref[...] = jnp.sum(2.0 * energy[0] - 12.0 * energy[1] + 0.5 * (RC * UPC - UCUT) * energy[2], axis=0, keepdims=True)

    col = lax.broadcasted_iota(I32, (L, L), 1)
    picks = [jnp.where(col == a, 1.0, 0.0).astype(BF16) for a in range(3)]

    def add_up(base):
        total = jnp.zeros((2 * L, L), F32)
        for a in range(3):
            for part in split3(sums[a, base:base + 2 * L, :]):
                total = total + lax.dot_general(part, picks[a], NN, preferred_element_type=F32)
        added[:, base:base + 2 * L] = jnp.transpose(total)[0:8]

    for base in range(0, slots, 2 * L):
        pl.when(count > base)(functools.partial(add_up, base))
    force = jnp.where(good, 24.0 * added[0:3], 0.0)
    pos_ref[...] = srt_ref[0:3, 0:n]
    frc_ref[...] = force[:, 0:n]
    vel_ref[...] = (srt_ref[3:6] + (0.5 * DT) * force)[:, 0:n]
    id_ref[...] = jnp.reshape((srt_ref[6:7].astype(I32) * 65536 + srt_ref[7:8].astype(I32))[:, 0:n], (n,))
    ok_ref[...] = jnp.reshape(okrow[:, 0:n].astype(I32), (n,))


def total_kernel(sizes, part_ref, sum_ref, rows, ssem, rsem):
    me = [lax.axis_index(name) for name in "xyz"]
    size_x, size_y, size_z = sizes
    mine = (me[2] * size_y + me[1]) * size_x + me[0]
    others = [(dx, dy, dz) for dz in range(size_z) for dy in range(size_y) for dx in range(size_x) if dx + dy + dz > 0]
    others.sort(key=lambda o: -(2 * min(o[2], size_z - o[2]) + 2 * o[1] + min(o[0], size_x - o[0])))

    device_at = functools.partial(device_of, sizes, me)

    barrier = pltpu.get_barrier_semaphore()
    for offset in others:
        pl.semaphore_signal(barrier, inc=1, device_id=device_at(offset), device_id_type=pl.DeviceIdType.MESH)
    rows[pl.ds(mine, 1)] = part_ref[...]
    pl.semaphore_wait(barrier, len(others))
    copies = []
    for index, offset in enumerate(others):
        copy = pltpu.make_async_remote_copy(
            src_ref=part_ref, dst_ref=rows.at[pl.ds(mine, 1)], send_sem=ssem.at[index], recv_sem=rsem.at[index],
            device_id=device_at(offset), device_id_type=pl.DeviceIdType.MESH)
        copy.start()
        copies.append(copy)
    for copy in copies:
        copy.wait_recv()
    sum_ref[...] = jnp.sum(rows[...], axis=0, keepdims=True)
    for copy in copies:
        copy.wait_send()


def solution(mesh):
    sizes = (mesh.shape["x"], mesh.shape["y"], mesh.shape["z"])
    peers = sorted({offset_of(sizes, d) for d in DIRS} - {(0, 0, 0)})
    devices = sizes[0] * sizes[1] * sizes[2]

    def local_step(atom_pos, atom_vel, atom_frc, atom_id, atom_ok, brick_side):
        n = atom_pos.shape[0]
        slots = -(-n // L) * L
        side = jnp.reshape(brick_side, (1, 1))
        vmem = pl.BlockSpec(memory_space=pltpu.VMEM)
        smem = pl.BlockSpec(memory_space=pltpu.SMEM)
        srt, ghosts, fresh, own, inner, inner_en = pl.pallas_call(
            functools.partial(exchange_kernel, sizes, peers, slots),
            out_shape=(jax.ShapeDtypeStruct((16, slots), F32), jax.ShapeDtypeStruct((len(peers), 4, slots), F32), jax.ShapeDtypeStruct((len(peers), 4, NEW), F32),
                       jax.ShapeDtypeStruct((slots, 3 * L), F32), jax.ShapeDtypeStruct((3, slots, L), F32), jax.ShapeDtypeStruct((3,) + TILE, F32)),
            in_specs=[pl.BlockSpec(memory_space=pltpu.HBM)] * 5 + [smem],
            out_specs=(vmem,) * 6,
            scratch_shapes=[
                pltpu.VMEM((3, n), F32), pltpu.VMEM((3, n), F32), pltpu.VMEM((3, n), F32), pltpu.VMEM((n,), I32), pltpu.VMEM((n,), I32),
                pltpu.VMEM((32, L), F32), pltpu.VMEM((26, L), F32), pltpu.VMEM((3, 4, slots), F32), pltpu.VMEM((3, 4, NEW), F32), pltpu.VMEM((3, 8, CHUNK * L), F32),
                pltpu.SemaphoreType.DMA((5,)), pltpu.SemaphoreType.DMA((26,)), pltpu.SemaphoreType.DMA((26,)),
            ] + [pltpu.SemaphoreType.DMA((len(peers),))] * 4,
            compiler_params=pltpu.CompilerParams(collective_id=0, has_side_effects=True, vmem_limit_bytes=40 * 2 ** 20),
            name="exchange",
        )(*[pltpu.with_memory_space_constraint(v, pltpu.HBM) for v in (atom_pos.T, atom_vel.T, atom_frc.T, atom_id, atom_ok)], side)
        offs = jnp.concatenate([ghosts[:, 3, 0:64], fresh[:, 3, 0:64]], axis=0).astype(I32)
        out_f = jax.ShapeDtypeStruct((3, n), F32)
        out_i = jax.ShapeDtypeStruct((n,), I32)
        new_pos, new_vel, new_frc, new_id, new_ok, energy = pl.pallas_call(
            functools.partial(force_kernel, sizes, peers, slots),
            out_shape=(out_f, out_f, out_f, out_i, out_i, jax.ShapeDtypeStruct((1, L), F32)),
            in_specs=[vmem] * 6 + [smem],
            out_specs=(vmem,) * 6,
            scratch_shapes=[pltpu.VMEM((8, 28 * slots + CHUNK * L), F32), pltpu.VMEM((3, 8, 28 * slots + CHUNK * L), F32), pltpu.VMEM((3, slots, L), F32), pltpu.VMEM((8, slots), F32)],
            compiler_params=pltpu.CompilerParams(vmem_limit_bytes=40 * 2 ** 20),
            name="forces",
        )(srt, ghosts, fresh, own, inner, inner_en, offs)
        energy = pl.pallas_call(
            functools.partial(total_kernel, sizes),
            out_shape=jax.ShapeDtypeStruct((1, L), F32),
            in_specs=[vmem],
            out_specs=vmem,
            scratch_shapes=[pltpu.VMEM((devices, L), F32), pltpu.SemaphoreType.DMA((devices,)), pltpu.SemaphoreType.DMA((devices,))],
            compiler_params=pltpu.CompilerParams(collective_id=1, has_side_effects=True, vmem_limit_bytes=4 * 2 ** 20),
            name="total",
        )(pltpu.with_memory_space_constraint(energy, pltpu.VMEM))
        return new_pos.T, new_vel.T, new_frc.T, new_id, new_ok, jnp.sum(energy)

    row_spec = P(MESH_AXES, None)
    id_spec = P(MESH_AXES)
    return jax.shard_map(local_step, mesh=mesh, in_specs=(row_spec, row_spec, row_spec, id_spec, id_spec, P()), out_specs=(row_spec, row_spec, row_spec, id_spec, id_spec, P()), check_vma=False)
```

```python
import functools

import jax
import jax.numpy as jnp
from jax import lax
from jax.experimental import pallas as pl
from jax.experimental.pallas import tpu as pltpu
from jax.sharding import PartitionSpec as P

DT = 0.005
RC = 2.5
FAR = 1.0e6
UCUT = 4.0 * (RC ** -12 - RC ** -6)
UPC = -48.0 * RC ** -13 + 24.0 * RC ** -7
MESH_AXES = ("z", "y", "x")
DIRS = [(dx, dy, dz) for dz in (-1, 0, 1) for dy in (-1, 0, 1) for dx in (-1, 0, 1) if (dx, dy, dz) != (0, 0, 0)]
NEAR = RC + 1.0e-3
MAJOR = ((2, 1, 0), (1, 0, 2), (0, 2, 1))
PACK = 8
NEW = 256
CHUNK = 3
GROUPS = 8
L = 128
TILE = (8, L)
F32 = jnp.float32
BF16 = jnp.bfloat16
I32 = jnp.int32
NT = (((1,), (1,)), ((), ()))
NN = (((1,), (0,)), ((), ()))


def device_of(sizes, me, offset):
    return tuple(lax.rem(me[axis] + offset[axis], sizes[axis]) for axis in (2, 1, 0))


def offset_of(sizes, d):
    return tuple(c % size for c, size in zip(d, sizes))


def order_of(d):
    if d[2] == 0:
        return 1 if d[1] != 0 else 2
    return 2 if (d[1] == 0 and d[0] != 0) else 0


def range_of(d):
    first, size = 0, 27
    for axis in MAJOR[order_of(d)]:
        if d[axis] == 0:
            break
        size = size // 3
        first = first + (1, 0, 2)[d[axis]] * size
    return first, first + size


def split3(x):
    hi = x.astype(BF16)
    rest = x - hi.astype(F32)
    mid = rest.astype(BF16)
    low = (rest - mid.astype(F32)).astype(BF16)
    return hi, mid, low


def onehot_rows(dest, base, count):
    rows = lax.broadcasted_iota(I32, (count, dest.shape[1]), 0) + base
    return jnp.where(rows == dest, 1.0, 0.0).astype(BF16)


def scatter_lanes(data, dest, slots):
    rows = data.shape[0]
    parts = jnp.concatenate(split3(data), axis=0)
    out = []
    for base in range(0, slots, 256):
        hot = onehot_rows(dest, base, min(256, slots - base))
        got = lax.dot_general(parts, hot, NT, preferred_element_type=F32)
        out.append(got[0:rows] + got[rows:2 * rows] + got[2 * rows:3 * rows])
    return jnp.concatenate(out, axis=1)


def class_places(code, with_before):
    width = code.shape[1]
    tiles = width // L
    cls = lax.broadcasted_iota(I32, (32, width), 0)
    member = jnp.where(cls == code, 1.0, 0.0)
    member_b = member.astype(BF16)
    stacked = jnp.concatenate([member_b[:, t * L:(t + 1) * L] for t in range(tiles)], axis=0)
    row_i = lax.broadcasted_iota(I32, (L, 256), 0)
    col_i = lax.broadcasted_iota(I32, (L, 256), 1)
    tri = jnp.where((row_i < col_i) | (col_i >= L), 1.0, 0.0).astype(BF16)
    pre = lax.dot_general(stacked, tri, NN, preferred_element_type=F32)
    carry = jnp.zeros((32, L), F32)
    if with_before:
        before_b = jnp.where(code < cls, 1.0, 0.0).astype(BF16)
        before_s = before_b[:, 0:L]
        tot = None
        ones = jnp.ones((L, L), BF16)
        for t in range(tiles):
            part = lax.dot_general(before_b[:, t * L:(t + 1) * L], ones, NN, preferred_element_type=F32)
            tot = part if tot is None else tot + part
        before = tot
        carry = before
    else:
        before = None
    places = []
    for t in range(tiles):
        within = pre[32 * t:32 * t + 32, 0:L] + carry
        places.append(jnp.sum(member[:, t * L:(t + 1) * L] * within, axis=0, keepdims=True))
        carry = carry + pre[32 * t:32 * t + 32, L:256]
    return jnp.concatenate(places, axis=1), before


def pad_lanes(x, width):
    return jnp.concatenate([x, jnp.zeros((x.shape[0], width - x.shape[1]), x.dtype)], axis=1)


def pair_loop(own_cols, near_lanes, q, first, last, with_self, carry):
    rows = [step_rows(q, g) for g in range(GROUPS)]
    own = [[own_cols[rows[g], a * L:(a + 1) * L] for a in range(3)] for g in range(GROUPS)]

    def body(c, carry):
        force, en = [list(f) for f in carry[0]], list(carry[1])
        for t in range(CHUNK):
            place = pl.ds(pl.multiple_of((c * CHUNK + t) * L, L), L)
            near_xyz = [near_lanes[a, :, place] for a in range(3)]
            for g in range(GROUPS):
                dx, dy, dz = [own[g][a] - near_xyz[a] for a in range(3)]
                d2 = dx * dx + dy * dy + dz * dz
                near = d2 < RC * RC
                if with_self:
                    near = near & (d2 > 0.0)
                inv = jnp.where(near, lax.rsqrt(d2), 0.0)
                s2 = inv * inv
                s6 = s2 * s2 * s2
                s12 = s6 * s6
                p = s12 - s6
                w = inv * (UPC / 24.0)
                scale = (p + s12) * s2 + w
                en = [en[0] + p, en[1] + w * d2, en[2] + jnp.where(near, 1.0, 0.0)]
                force[g] = [force[g][0] + scale * dx, force[g][1] + scale * dy, force[g][2] + scale * dz]
        return tuple(tuple(f) for f in force), tuple(en)

    return lax.fori_loop(first, last, body, carry)


def step_rows(q, g):
    return pl.ds(pl.multiple_of((q * GROUPS + g) * 8, 8), 8)


def own_columns(xyz):
    slots = xyz.shape[1]
    parts = [part.astype(F32) for part in split3(xyz)]
    parts = jnp.concatenate(parts + [jnp.zeros((7, slots), F32)], axis=0)
    row = lax.broadcasted_iota(I32, (16, 3 * L), 0)
    tile = lax.broadcasted_iota(I32, (16, 3 * L), 1) // L
    picks = jnp.where((row == tile) | (row == tile + 3) | (row == tile + 6), 1.0, 0.0).astype(BF16)
    return lax.dot_general(jnp.transpose(parts).astype(BF16), picks, NN, preferred_element_type=F32)


def exchange_kernel(sizes, peers, slots, pos_hbm, vel_hbm, frc_hbm, id_hbm, ok_hbm, side_ref, srt_ref, gh_ref, ga_ref, own_ref, inner_ref, inner_en_ref, pos_ref, vel_ref, frc_ref, id_ref, ok_ref, pkt, rcv, out3, new3, lanes, isem, psend, precv, gsend, grecv, asend, arecv):
    me = [lax.axis_index(name) for name in "xyz"]

    device_at = functools.partial(device_of, sizes, me)

    loads = []
    for index, (src, dst) in enumerate(((ok_hbm, ok_ref), (id_hbm, id_ref), (pos_hbm, pos_ref), (vel_hbm, vel_ref), (frc_hbm, frc_ref))):
        load = pltpu.make_async_copy(src, dst, isem.at[index])
        load.start()
        loads.append(load)
    barrier = pltpu.get_barrier_semaphore()
    for offset in peers:
        pl.semaphore_signal(barrier, inc=1, device_id=device_at(offset), device_id_type=pl.DeviceIdType.MESH)

    n = pos_ref.shape[1]
    for load in loads:
        load.wait()
    side = side_ref[0, 0]
    owned = pad_lanes(jnp.reshape(ok_ref[...], (1, n)), slots) > 0
    half = vel_ref[...] + (0.5 * DT) * frc_ref[...]
    free = pos_ref[...] + DT * half
    half = pad_lanes(half, slots)
    free = pad_lanes(free, slots)
    ids = pad_lanes(jnp.reshape(id_ref[...], (1, n)), slots)
    code = jnp.zeros((1, slots), I32)
    moved = []
    low_side = []
    for axis in range(3):
        low = me[axis].astype(F32) * side
        high = (me[axis] + 1).astype(F32) * side
        box = side * float(sizes[axis])
        u = free[axis:axis + 1]
        step = jnp.where(u >= high, 1, 0) - jnp.where(u < low, 1, 0)
        code = code + (step + 1) * (1, 3, 9)[axis]
        moved.append(jnp.where(u < 0.0, u + box, jnp.where(u >= box, u - box, u)))
        low_side.append(low)
    code = jnp.where(owned, code, 31)
    id_hi = (ids >> 16).astype(F32)
    id_lo = (ids & 65535).astype(F32)
    okf = jnp.where(owned, 1.0, 0.0)
    data = jnp.concatenate(moved + [half, id_hi, id_lo, okf, jnp.zeros((7, slots), F32)], axis=0)

    place, _ = class_places(code, False)
    leaving = owned & (code != 13)
    way = jnp.where(leaving, code - jnp.where(code > 13, 1, 0), 31)
    member = jnp.where(lax.broadcasted_iota(I32, (32, slots), 0) == way, 1.0, 0.0).astype(BF16)
    fields = jnp.concatenate([jnp.where(place == float(k), data, 0.0) for k in range(PACK)], axis=0)
    packed = jnp.zeros((32, L), F32)
    for part in split3(fields):
        packed = packed + lax.dot_general(member, part, NT, preferred_element_type=F32)
    pkt[...] = packed

    def bins_of(pos):
        bins = []
        for axis in range(3):
            loc = pos[axis:axis + 1] - low_side[axis]
            bins.append(jnp.where(loc < NEAR, 0, jnp.where(loc > side - NEAR, 2, 1)))
        return [(bins[i] * 3 + bins[j]) * 3 + bins[k] for i, j, k in MAJOR]

    wide = side > 2.0 * NEAR
    eye = lax.broadcasted_iota(I32, (32, L), 0) == lax.broadcasted_iota(I32, (32, L), 1)

    def sorted_block(cand, keys, kept):
        width = cand.shape[1]
        where_to, before = class_places(jnp.where(kept, keys, 28), True)
        arranged = scatter_lanes(cand, jnp.where(kept, where_to.astype(I32), -1), width)
        total = jnp.concatenate([before[27:28]] * (width // L), axis=1)
        lane = lax.broadcasted_iota(I32, (1, width), 1).astype(F32)
        begins = jnp.sum(jnp.where(eye, before, 0.0), axis=0, keepdims=True)
        ends = jnp.where(wide, begins, before[27:28])
        counts = jnp.concatenate([jnp.where(wide, begins, 0.0)[:, 0:32], ends[:, 0:32], jnp.zeros((1, L - 64), F32)], axis=1)
        return jnp.where(lane < total, arranged[0:3], FAR), counts

    def send(src, dst, ssem, rsem, offset):
        copy = pltpu.make_async_remote_copy(
            src_ref=src, dst_ref=dst, send_sem=ssem, recv_sem=rsem,
            device_id=device_at(offset), device_id_type=pl.DeviceIdType.MESH)
        copy.start()
        return copy

    def store_block(ref, kind, xyz, counts):
        tiles = xyz.shape[1] // L
        for a in range(3):
            for t in range(tiles):
                ref[kind, pl.ds(a * tiles + t, 1)] = xyz[a:a + 1, t * L:(t + 1) * L]
        ref[kind, pl.ds(3 * tiles, 1)] = counts

    def send_blocks(block, dst, ssem, rsem, kind):
        out = []
        for index, offset in enumerate(peers):
            if order_of(tuple(0 if c == 0 else 1 for c in offset)) == kind:
                out.append(send(block.at[kind], dst.at[index], ssem.at[index], rsem.at[index], offset))
        return out

    staying = code == 13
    keys = bins_of(data)
    for kind in range(3):
        store_block(out3, kind, *sorted_block(data[0:8], keys[kind], staying))
    pl.semaphore_wait(barrier, len(peers))
    packets = []
    for index, d in enumerate(DIRS):
        row = pl.ds(index, 1)
        packets.append(send(pkt.at[row], rcv.at[row], psend.at[index], precv.at[index], offset_of(sizes, d)))
    blocks = []
    for kind in range(3):
        blocks = blocks + send_blocks(out3, gh_ref, gsend, grecv, kind)
    for copy in packets:
        copy.wait_recv()

    came = jnp.concatenate([rcv[...], jnp.zeros((32 - 26, L), F32)], axis=0)
    came = jnp.concatenate([came] + [pltpu.roll(came, L - 16 * k, 1) for k in range(1, PACK)], axis=0)
    came_t = jnp.transpose(came)[0:16]
    came_ok = came_t[8:9] > 0.5
    keys = bins_of(came_t)
    late = []
    for kind in range(3):
        store_block(new3, kind, *sorted_block(came_t[0:8], keys[kind], came_ok))
        late = late + send_blocks(new3, ga_ref, asend, arecv, kind)
    for copy in packets:
        copy.wait_send()

    arr_ids = came[:, 6:7].astype(I32) * 65536 + came[:, 7:8].astype(I32)
    arr_ok = came[:, 8:9] > 0.5
    row_ids = jnp.concatenate([ids, came_t[6:7].astype(I32) * 65536 + came_t[7:8].astype(I32)], axis=1)
    less = jnp.where((arr_ids < row_ids) & arr_ok, 1.0, 0.0)
    arrivals_below = jnp.sum(less, axis=0, keepdims=True)
    above = jnp.where((arr_ids > row_ids[:, 0:slots]) & staying, 1.0, 0.0).astype(BF16)
    stay_below = lax.dot_general(jnp.ones((16, slots), BF16), above, NT, preferred_element_type=F32)[0:1]
    stay_place, _ = class_places(jnp.where(staying, 0, 31), False)
    rank = jnp.concatenate([stay_place, stay_below], axis=1) + arrivals_below
    dest = jnp.where(jnp.concatenate([staying, came_ok], axis=1), rank.astype(I32), -1)
    merged = scatter_lanes(jnp.concatenate([data, came_t], axis=1), dest, slots)
    srt_ref[...] = jnp.where(lax.broadcasted_iota(I32, (16, slots), 0) == 9, side, merged)

    good = merged[8:9] > 0.5
    own_ref[...] = own_columns(jnp.where(good, merged[0:3], -FAR))
    first = CHUNK * L
    for a in range(3):
        lanes[a] = jnp.broadcast_to(jnp.where(good, merged[a:a + 1], FAR)[:, 0:first], (8, first))
    zero = jnp.zeros(TILE, F32)

    def own_step(q, energy):
        force, energy = pair_loop(own_ref, lanes, q, 0, 1, True, (((zero,) * 3,) * GROUPS, energy))
        for g in range(GROUPS):
            for a in range(3):
                inner_ref[a, step_rows(q, g), :] = force[g][a]
        return energy

    for k, part in enumerate(lax.fori_loop(0, slots // (8 * GROUPS), own_step, (zero,) * 3)):
        inner_en_ref[k] = part

    for copy in blocks + late:
        copy.wait()


def force_kernel(sizes, peers, slots, srt_ref, gh_ref, ga_ref, own_cols, inner_ref, inner_en_ref, offs_ref, pos_ref, vel_ref, frc_ref, id_ref, ok_ref, en_ref, line, wide_line, sums, added):
    me = [lax.axis_index(name) for name in "xyz"]
    n = pos_ref.shape[1]
    side = srt_ref[9:10, 0:1]
    okrow = srt_ref[8:9]
    good = okrow > 0.5
    count = jnp.sum(okrow).astype(I32)
    span = slots + L

    away = jnp.full(TILE, FAR, F32)
    first = CHUNK * L
    line[:, 0:slots - first] = jnp.concatenate([jnp.where(good, srt_ref[0:3], FAR), jnp.full((5, slots), FAR, F32)], axis=0)[:, first:]
    lane = lax.broadcasted_iota(I32, (8, span), 1)
    fill = jnp.maximum(count - first, 0)
    for d in DIRS:
        index = peers.index(offset_of(sizes, [-c for c in d]))
        low, high = range_of(d)
        shifts = []
        for axis in range(3):
            box = side * float(sizes[axis])
            if d[axis] == 1:
                shifts.append(jnp.where(me[axis] == sizes[axis] - 1, box, 0.0))
            elif d[axis] == -1:
                shifts.append(jnp.where(me[axis] == 0, -box, 0.0))
            else:
                shifts.append(jnp.zeros((1, 1), F32))
        shift = jnp.concatenate(shifts, axis=0)
        for source, entry in ((gh_ref, index), (ga_ref, index + len(peers))):
            tiles = source.shape[1] // 3
            width = tiles * L
            begin = offs_ref[entry, low]
            end = offs_ref[entry, 32 + high]
            block = jnp.concatenate([source[index, pl.ds(t, 3, stride=tiles), :] for t in range(tiles)], axis=1) + shift
            block = jnp.concatenate([block, jnp.zeros((5, width), F32)], axis=0)
            block = jnp.concatenate([block, away], axis=1)
            head = fill & (L - 1)
            base = pl.multiple_of(fill - head, L)
            move = head - begin
            block = pltpu.roll(block, jnp.where(move < 0, move + (width + L), move), 1)
            block = jnp.where(lane[:, 0:width + L] < head + end - begin, block, FAR)
            line[:, pl.ds(base, L)] = jnp.where(lane[:, 0:L] < head, line[:, pl.ds(base, L)], block[:, 0:L])
            line[:, pl.ds(pl.multiple_of(base + L, L), width)] = block[:, L:]
            fill = fill + (end - begin)
    rest = pl.multiple_of(((fill + L - 1) // L) * L, L)
    line[:, pl.ds(rest, CHUNK * L)] = jnp.full((8, CHUNK * L), FAR, F32)
    chunks = jnp.maximum((fill + CHUNK * L - 1) // (CHUNK * L), 1)

    def widen(c, carry):
        for t in range(CHUNK):
            place = pl.ds(pl.multiple_of((c * CHUNK + t) * L, L), L)
            tile = line[:, place]
            for a in range(3):
                wide_line[a, :, place] = jnp.broadcast_to(tile[a:a + 1], TILE)
        return carry

    lax.fori_loop(0, chunks, widen, 0)

    def own_step(q, energy):
        start = tuple(tuple(inner_ref[a, step_rows(q, g), :] for a in range(3)) for g in range(GROUPS))
        carry = pair_loop(own_cols, wide_line, q, 0, 1, True, (start, energy))
        force, energy = pair_loop(own_cols, wide_line, q, 1, chunks, False, carry)
        for g in range(GROUPS):
            for a in range(3):
                sums[a, step_rows(q, g), :] = force[g][a]
        return energy

    own_steps = (count + 8 * GROUPS - 1) // (8 * GROUPS)
    energy = lax.fori_loop(0, own_steps, own_step, tuple(inner_en_ref[k] for k in range(3)))
    en_ref[...] = jnp.sum(2.0 * energy[0] - 12.0 * energy[1] + 0.5 * (RC * UPC - UCUT) * energy[2], axis=0, keepdims=True)

    col = lax.broadcasted_iota(I32, (L, L), 1)
    picks = [jnp.where(col == a, 1.0, 0.0).astype(BF16) for a in range(3)]

    def add_up(base):
        total = jnp.zeros((2 * L, L), F32)
        for a in range(3):
            for part in split3(sums[a, base:base + 2 * L, :]):
                total = total + lax.dot_general(part, picks[a], NN, preferred_element_type=F32)
        added[:, base:base + 2 * L] = jnp.transpose(total)[0:8]

    for base in range(0, slots, 2 * L):
        pl.when(count > base)(functools.partial(add_up, base))
    force = jnp.where(good, 24.0 * added[0:3], 0.0)
    pos_ref[...] = srt_ref[0:3, 0:n]
    frc_ref[...] = force[:, 0:n]
    vel_ref[...] = (srt_ref[3:6] + (0.5 * DT) * force)[:, 0:n]
    id_ref[...] = jnp.reshape((srt_ref[6:7].astype(I32) * 65536 + srt_ref[7:8].astype(I32))[:, 0:n], (n,))
    ok_ref[...] = jnp.reshape(okrow[:, 0:n].astype(I32), (n,))


def total_kernel(sizes, part_ref, sum_ref, rows, ssem, rsem):
    me = [lax.axis_index(name) for name in "xyz"]
    size_x, size_y, size_z = sizes
    mine = (me[2] * size_y + me[1]) * size_x + me[0]
    others = [(dx, dy, dz) for dz in range(size_z) for dy in range(size_y) for dx in range(size_x) if dx + dy + dz > 0]
    others.sort(key=lambda o: -(2 * min(o[2], size_z - o[2]) + 2 * o[1] + min(o[0], size_x - o[0])))

    device_at = functools.partial(device_of, sizes, me)

    barrier = pltpu.get_barrier_semaphore()
    for offset in others:
        pl.semaphore_signal(barrier, inc=1, device_id=device_at(offset), device_id_type=pl.DeviceIdType.MESH)
    rows[pl.ds(mine, 1)] = part_ref[...]
    pl.semaphore_wait(barrier, len(others))
    copies = []
    for index, offset in enumerate(others):
        copy = pltpu.make_async_remote_copy(
            src_ref=part_ref, dst_ref=rows.at[pl.ds(mine, 1)], send_sem=ssem.at[index], recv_sem=rsem.at[index],
            device_id=device_at(offset), device_id_type=pl.DeviceIdType.MESH)
        copy.start()
        copies.append(copy)
    for copy in copies:
        copy.wait_recv()
    sum_ref[...] = jnp.sum(rows[...], axis=0, keepdims=True)
    for copy in copies:
        copy.wait_send()


def solution(mesh):
    sizes = (mesh.shape["x"], mesh.shape["y"], mesh.shape["z"])
    peers = sorted({offset_of(sizes, d) for d in DIRS} - {(0, 0, 0)})
    devices = sizes[0] * sizes[1] * sizes[2]

    def local_step(atom_pos, atom_vel, atom_frc, atom_id, atom_ok, brick_side):
        n = atom_pos.shape[0]
        slots = -(-n // L) * L
        side = jnp.reshape(brick_side, (1, 1))
        old_rows, new_rows = [3 * (width // L) + 1 for width in (slots, NEW)]
        vmem = pl.BlockSpec(memory_space=pltpu.VMEM)
        smem = pl.BlockSpec(memory_space=pltpu.SMEM)
        srt, ghosts, fresh, own, inner, inner_en = pl.pallas_call(
            functools.partial(exchange_kernel, sizes, peers, slots),
            out_shape=(jax.ShapeDtypeStruct((16, slots), F32), jax.ShapeDtypeStruct((len(peers), old_rows, L), F32), jax.ShapeDtypeStruct((len(peers), new_rows, L), F32),
                       jax.ShapeDtypeStruct((slots, 3 * L), F32), jax.ShapeDtypeStruct((3, slots, L), F32), jax.ShapeDtypeStruct((3,) + TILE, F32)),
            in_specs=[pl.BlockSpec(memory_space=pltpu.HBM)] * 5 + [smem],
            out_specs=(vmem,) * 6,
            scratch_shapes=[
                pltpu.VMEM((3, n), F32), pltpu.VMEM((3, n), F32), pltpu.VMEM((3, n), F32), pltpu.VMEM((n,), I32), pltpu.VMEM((n,), I32),
                pltpu.VMEM((32, L), F32), pltpu.VMEM((26, L), F32), pltpu.VMEM((3, old_rows, L), F32), pltpu.VMEM((3, new_rows, L), F32), pltpu.VMEM((3, 8, CHUNK * L), F32),
                pltpu.SemaphoreType.DMA((5,)), pltpu.SemaphoreType.DMA((26,)), pltpu.SemaphoreType.DMA((26,)),
            ] + [pltpu.SemaphoreType.DMA((len(peers),))] * 4,
            compiler_params=pltpu.CompilerParams(collective_id=0, has_side_effects=True, vmem_limit_bytes=40 * 2 ** 20),
            name="exchange",
        )(*[pltpu.with_memory_space_constraint(v, pltpu.HBM) for v in (atom_pos.T, atom_vel.T, atom_frc.T, atom_id, atom_ok)], side)
        offs = jnp.concatenate([ghosts[:, -1, 0:64], fresh[:, -1, 0:64]], axis=0).astype(I32)
        out_f = jax.ShapeDtypeStruct((3, n), F32)
        out_i = jax.ShapeDtypeStruct((n,), I32)
        new_pos, new_vel, new_frc, new_id, new_ok, energy = pl.pallas_call(
            functools.partial(force_kernel, sizes, peers, slots),
            out_shape=(out_f, out_f, out_f, out_i, out_i, jax.ShapeDtypeStruct((1, L), F32)),
            in_specs=[vmem] * 6 + [smem],
            out_specs=(vmem,) * 6,
            scratch_shapes=[pltpu.VMEM((8, 28 * slots + CHUNK * L), F32), pltpu.VMEM((3, 8, 28 * slots + CHUNK * L), F32), pltpu.VMEM((3, slots, L), F32), pltpu.VMEM((8, slots), F32)],
            compiler_params=pltpu.CompilerParams(vmem_limit_bytes=40 * 2 ** 20),
            name="forces",
        )(srt, ghosts, fresh, own, inner, inner_en, offs)
        energy = pl.pallas_call(
            functools.partial(total_kernel, sizes),
            out_shape=jax.ShapeDtypeStruct((1, L), F32),
            in_specs=[vmem],
            out_specs=vmem,
            scratch_shapes=[pltpu.VMEM((devices, L), F32), pltpu.SemaphoreType.DMA((devices,)), pltpu.SemaphoreType.DMA((devices,))],
            compiler_params=pltpu.CompilerParams(collective_id=1, has_side_effects=True, vmem_limit_bytes=4 * 2 ** 20),
            name="total",
        )(pltpu.with_memory_space_constraint(energy, pltpu.VMEM))
        return new_pos.T, new_vel.T, new_frc.T, new_id, new_ok, jnp.sum(energy)

    row_spec = P(MESH_AXES, None)
    id_spec = P(MESH_AXES)
    return jax.shard_map(local_step, mesh=mesh, in_specs=(row_spec, row_spec, row_spec, id_spec, id_spec, P()), out_specs=(row_spec, row_spec, row_spec, id_spec, id_spec, P()), check_vma=False)
```

```python
import functools

import jax
import jax.numpy as jnp
from jax import lax
from jax.experimental import pallas as pl
from jax.experimental.pallas import tpu as pltpu
from jax.sharding import PartitionSpec as P

DT = 0.005
RC = 2.5
FAR = 1.0e6
UCUT = 4.0 * (RC ** -12 - RC ** -6)
UPC = -48.0 * RC ** -13 + 24.0 * RC ** -7
MESH_AXES = ("z", "y", "x")
DIRS = [(dx, dy, dz) for dz in (-1, 0, 1) for dy in (-1, 0, 1) for dx in (-1, 0, 1) if (dx, dy, dz) != (0, 0, 0)]
NEAR = RC + 1.0e-3
MAJOR = ((2, 1, 0), (1, 0, 2), (0, 2, 1))
PACK = 8
NEW = 256
CHUNK = 4
GROUPS = 8
L = 128
TILE = (8, L)
F32 = jnp.float32
BF16 = jnp.bfloat16
I32 = jnp.int32
NT = (((1,), (1,)), ((), ()))
NN = (((1,), (0,)), ((), ()))


def device_of(sizes, me, offset):
    return tuple(lax.rem(me[axis] + offset[axis], sizes[axis]) for axis in (2, 1, 0))


def offset_of(sizes, d):
    return tuple(c % size for c, size in zip(d, sizes))


def order_of(d):
    if d[2] == 0:
        return 1 if d[1] != 0 else 2
    return 2 if (d[1] == 0 and d[0] != 0) else 0


def range_of(d):
    first, size = 0, 27
    for axis in MAJOR[order_of(d)]:
        if d[axis] == 0:
            break
        size = size // 3
        first = first + (1, 0, 2)[d[axis]] * size
    return first, first + size


def split3(x):
    hi = x.astype(BF16)
    rest = x - hi.astype(F32)
    mid = rest.astype(BF16)
    low = (rest - mid.astype(F32)).astype(BF16)
    return hi, mid, low


def onehot_rows(dest, base, count):
    rows = lax.broadcasted_iota(I32, (count, dest.shape[1]), 0) + base
    return jnp.where(rows == dest, 1.0, 0.0).astype(BF16)


def scatter_lanes(data, dest, slots):
    rows = data.shape[0]
    parts = jnp.concatenate(split3(data), axis=0)
    out = []
    for base in range(0, slots, 256):
        hot = onehot_rows(dest, base, min(256, slots - base))
        got = lax.dot_general(parts, hot, NT, preferred_element_type=F32)
        out.append(got[0:rows] + got[rows:2 * rows] + got[2 * rows:3 * rows])
    return jnp.concatenate(out, axis=1)


def class_places(code, with_before):
    width = code.shape[1]
    tiles = width // L
    cls = lax.broadcasted_iota(I32, (32, width), 0)
    member = jnp.where(cls == code, 1.0, 0.0)
    member_b = member.astype(BF16)
    stacked = jnp.concatenate([member_b[:, t * L:(t + 1) * L] for t in range(tiles)], axis=0)
    row_i = lax.broadcasted_iota(I32, (L, 256), 0)
    col_i = lax.broadcasted_iota(I32, (L, 256), 1)
    tri = jnp.where((row_i < col_i) | (col_i >= L), 1.0, 0.0).astype(BF16)
    pre = lax.dot_general(stacked, tri, NN, preferred_element_type=F32)
    carry = jnp.zeros((32, L), F32)
    if with_before:
        before_b = jnp.where(code < cls, 1.0, 0.0).astype(BF16)
        before_s = before_b[:, 0:L]
        tot = None
        ones = jnp.ones((L, L), BF16)
        for t in range(tiles):
            part = lax.dot_general(before_b[:, t * L:(t + 1) * L], ones, NN, preferred_element_type=F32)
            tot = part if tot is None else tot + part
        before = tot
        carry = before
    else:
        before = None
    places = []
    for t in range(tiles):
        within = pre[32 * t:32 * t + 32, 0:L] + carry
        places.append(jnp.sum(member[:, t * L:(t + 1) * L] * within, axis=0, keepdims=True))
        carry = carry + pre[32 * t:32 * t + 32, L:256]
    return jnp.concatenate(places, axis=1), before


def pad_lanes(x, width):
    return jnp.concatenate([x, jnp.zeros((x.shape[0], width - x.shape[1]), x.dtype)], axis=1)


def pair_loop(own_cols, near_lanes, q, first, last, with_self, carry):
    rows = [step_rows(q, g) for g in range(GROUPS)]
    own = [[own_cols[rows[g], a * L:(a + 1) * L] for a in range(3)] for g in range(GROUPS)]

    def body(c, carry):
        force, en = [list(f) for f in carry[0]], list(carry[1])
        for t in range(CHUNK):
            place = pl.ds(pl.multiple_of((c * CHUNK + t) * L, L), L)
            near_xyz = [near_lanes[a, :, place] for a in range(3)]
            for g in range(GROUPS):
                dx, dy, dz = [own[g][a] - near_xyz[a] for a in range(3)]
                d2 = dx * dx + dy * dy + dz * dz
                near = d2 < RC * RC
                if with_self:
                    near = near & (d2 > 0.0)
                inv = jnp.where(near, lax.rsqrt(d2), 0.0)
                s2 = inv * inv
                s6 = s2 * s2 * s2
                s12 = s6 * s6
                p = s12 - s6
                w = inv * (UPC / 24.0)
                scale = (p + s12) * s2 + w
                en = [en[0] + p, en[1] + w * d2, en[2] + jnp.where(near, 1.0, 0.0)]
                force[g] = [force[g][0] + scale * dx, force[g][1] + scale * dy, force[g][2] + scale * dz]
        return tuple(tuple(f) for f in force), tuple(en)

    return lax.fori_loop(first, last, body, carry)


def step_rows(q, g):
    return pl.ds(pl.multiple_of((q * GROUPS + g) * 8, 8), 8)


def own_columns(xyz):
    slots = xyz.shape[1]
    parts = [part.astype(F32) for part in split3(xyz)]
    parts = jnp.concatenate(parts + [jnp.zeros((7, slots), F32)], axis=0)
    row = lax.broadcasted_iota(I32, (16, 3 * L), 0)
    tile = lax.broadcasted_iota(I32, (16, 3 * L), 1) // L
    picks = jnp.where((row == tile) | (row == tile + 3) | (row == tile + 6), 1.0, 0.0).astype(BF16)
    return lax.dot_general(jnp.transpose(parts).astype(BF16), picks, NN, preferred_element_type=F32)


def exchange_kernel(sizes, peers, slots, pos_hbm, vel_hbm, frc_hbm, id_hbm, ok_hbm, side_ref, srt_ref, gh_ref, ga_ref, own_ref, inner_ref, inner_en_ref, pos_ref, vel_ref, frc_ref, id_ref, ok_ref, pkt, rcv, out3, new3, lanes, isem, psend, precv, gsend, grecv, asend, arecv):
    me = [lax.axis_index(name) for name in "xyz"]

    device_at = functools.partial(device_of, sizes, me)

    loads = []
    for index, (src, dst) in enumerate(((ok_hbm, ok_ref), (id_hbm, id_ref), (pos_hbm, pos_ref), (vel_hbm, vel_ref), (frc_hbm, frc_ref))):
        load = pltpu.make_async_copy(src, dst, isem.at[index])
        load.start()
        loads.append(load)
    barrier = pltpu.get_barrier_semaphore()
    for offset in peers:
        pl.semaphore_signal(barrier, inc=1, device_id=device_at(offset), device_id_type=pl.DeviceIdType.MESH)

    n = pos_ref.shape[1]
    for load in loads:
        load.wait()
    side = side_ref[0, 0]
    owned = pad_lanes(jnp.reshape(ok_ref[...], (1, n)), slots) > 0
    half = vel_ref[...] + (0.5 * DT) * frc_ref[...]
    free = pos_ref[...] + DT * half
    half = pad_lanes(half, slots)
    free = pad_lanes(free, slots)
    ids = pad_lanes(jnp.reshape(id_ref[...], (1, n)), slots)
    code = jnp.zeros((1, slots), I32)
    moved = []
    low_side = []
    for axis in range(3):
        low = me[axis].astype(F32) * side
        high = (me[axis] + 1).astype(F32) * side
        box = side * float(sizes[axis])
        u = free[axis:axis + 1]
        step = jnp.where(u >= high, 1, 0) - jnp.where(u < low, 1, 0)
        code = code + (step + 1) * (1, 3, 9)[axis]
        moved.append(jnp.where(u < 0.0, u + box, jnp.where(u >= box, u - box, u)))
        low_side.append(low)
    code = jnp.where(owned, code, 31)
    id_hi = (ids >> 16).astype(F32)
    id_lo = (ids & 65535).astype(F32)
    okf = jnp.where(owned, 1.0, 0.0)
    data = jnp.concatenate(moved + [half, id_hi, id_lo, okf, jnp.zeros((7, slots), F32)], axis=0)

    place, _ = class_places(code, False)
    leaving = owned & (code != 13)
    way = jnp.where(leaving, code - jnp.where(code > 13, 1, 0), 31)
    member = jnp.where(lax.broadcasted_iota(I32, (32, slots), 0) == way, 1.0, 0.0).astype(BF16)
    fields = jnp.concatenate([jnp.where(place == float(k), data, 0.0) for k in range(PACK)], axis=0)
    packed = jnp.zeros((32, L), F32)
    for part in split3(fields):
        packed = packed + lax.dot_general(member, part, NT, preferred_element_type=F32)
    pkt[...] = packed

    def bins_of(pos):
        bins = []
        for axis in range(3):
            loc = pos[axis:axis + 1] - low_side[axis]
            bins.append(jnp.where(loc < NEAR, 0, jnp.where(loc > side - NEAR, 2, 1)))
        return [(bins[i] * 3 + bins[j]) * 3 + bins[k] for i, j, k in MAJOR]

    wide = side > 2.0 * NEAR
    eye = lax.broadcasted_iota(I32, (32, L), 0) == lax.broadcasted_iota(I32, (32, L), 1)

    def sorted_block(cand, keys, kept):
        width = cand.shape[1]
        where_to, before = class_places(jnp.where(kept, keys, 28), True)
        arranged = scatter_lanes(cand, jnp.where(kept, where_to.astype(I32), -1), width)
        total = jnp.concatenate([before[27:28]] * (width // L), axis=1)
        lane = lax.broadcasted_iota(I32, (1, width), 1).astype(F32)
        begins = jnp.sum(jnp.where(eye, before, 0.0), axis=0, keepdims=True)
        ends = jnp.where(wide, begins, before[27:28])
        counts = jnp.concatenate([jnp.where(wide, begins, 0.0)[:, 0:32], ends[:, 0:32], jnp.zeros((1, L - 64), F32)], axis=1)
        return jnp.where(lane < total, arranged[0:3], FAR), counts

    def send(src, dst, ssem, rsem, offset):
        copy = pltpu.make_async_remote_copy(
            src_ref=src, dst_ref=dst, send_sem=ssem, recv_sem=rsem,
            device_id=device_at(offset), device_id_type=pl.DeviceIdType.MESH)
        copy.start()
        return copy

    def store_block(ref, kind, xyz, counts):
        tiles = xyz.shape[1] // L
        for a in range(3):
            for t in range(tiles):
                ref[kind, pl.ds(a * tiles + t, 1)] = xyz[a:a + 1, t * L:(t + 1) * L]
        ref[kind, pl.ds(3 * tiles, 1)] = counts

    def send_blocks(block, dst, ssem, rsem, kind):
        out = []
        for index, offset in enumerate(peers):
            if order_of(tuple(0 if c == 0 else 1 for c in offset)) == kind:
                out.append(send(block.at[kind], dst.at[index], ssem.at[index], rsem.at[index], offset))
        return out

    staying = code == 13
    keys = bins_of(data)
    for kind in range(3):
        store_block(out3, kind, *sorted_block(data[0:8], keys[kind], staying))
    pl.semaphore_wait(barrier, len(peers))
    packets = []
    for index, d in enumerate(DIRS):
        row = pl.ds(index, 1)
        packets.append(send(pkt.at[row], rcv.at[row], psend.at[index], precv.at[index], offset_of(sizes, d)))
    blocks = []
    for kind in range(3):
        blocks = blocks + send_blocks(out3, gh_ref, gsend, grecv, kind)
    for copy in packets:
        copy.wait_recv()

    came = jnp.concatenate([rcv[...], jnp.zeros((32 - 26, L), F32)], axis=0)
    came = jnp.concatenate([came] + [pltpu.roll(came, L - 16 * k, 1) for k in range(1, PACK)], axis=0)
    came_t = jnp.transpose(came)[0:16]
    came_ok = came_t[8:9] > 0.5
    keys = bins_of(came_t)
    late = []
    for kind in range(3):
        store_block(new3, kind, *sorted_block(came_t[0:8], keys[kind], came_ok))
        late = late + send_blocks(new3, ga_ref, asend, arecv, kind)
    for copy in packets:
        copy.wait_send()

    arr_ids = came[:, 6:7].astype(I32) * 65536 + came[:, 7:8].astype(I32)
    arr_ok = came[:, 8:9] > 0.5
    row_ids = jnp.concatenate([ids, came_t[6:7].astype(I32) * 65536 + came_t[7:8].astype(I32)], axis=1)
    less = jnp.where((arr_ids < row_ids) & arr_ok, 1.0, 0.0)
    arrivals_below = jnp.sum(less, axis=0, keepdims=True)
    above = jnp.where((arr_ids > row_ids[:, 0:slots]) & staying, 1.0, 0.0).astype(BF16)
    stay_below = lax.dot_general(jnp.ones((16, slots), BF16), above, NT, preferred_element_type=F32)[0:1]
    stay_place, _ = class_places(jnp.where(staying, 0, 31), False)
    rank = jnp.concatenate([stay_place, stay_below], axis=1) + arrivals_below
    dest = jnp.where(jnp.concatenate([staying, came_ok], axis=1), rank.astype(I32), -1)
    merged = scatter_lanes(jnp.concatenate([data, came_t], axis=1), dest, slots)
    srt_ref[...] = jnp.where(lax.broadcasted_iota(I32, (16, slots), 0) == 9, side, merged)

    good = merged[8:9] > 0.5
    own_ref[...] = own_columns(jnp.where(good, merged[0:3], -FAR))
    first = CHUNK * L
    for a in range(3):
        lanes[a] = jnp.broadcast_to(jnp.where(good, merged[a:a + 1], FAR)[:, 0:first], (8, first))
    zero = jnp.zeros(TILE, F32)

    def own_step(q, energy):
        force, energy = pair_loop(own_ref, lanes, q, 0, 1, True, (((zero,) * 3,) * GROUPS, energy))
        for g in range(GROUPS):
            for a in range(3):
                inner_ref[a, step_rows(q, g), :] = force[g][a]
        return energy

    for k, part in enumerate(lax.fori_loop(0, slots // (8 * GROUPS), own_step, (zero,) * 3)):
        inner_en_ref[k] = part

    for copy in blocks + late:
        copy.wait()


def force_kernel(sizes, peers, slots, srt_ref, gh_ref, ga_ref, own_cols, inner_ref, inner_en_ref, offs_ref, pos_ref, vel_ref, frc_ref, id_ref, ok_ref, en_ref, line, wide_line, sums, added):
    me = [lax.axis_index(name) for name in "xyz"]
    n = pos_ref.shape[1]
    side = srt_ref[9:10, 0:1]
    okrow = srt_ref[8:9]
    good = okrow > 0.5
    count = jnp.sum(okrow).astype(I32)
    span = slots + L

    away = jnp.full(TILE, FAR, F32)
    first = CHUNK * L
    line[:, 0:slots - first] = jnp.concatenate([jnp.where(good, srt_ref[0:3], FAR), jnp.full((5, slots), FAR, F32)], axis=0)[:, first:]
    lane = lax.broadcasted_iota(I32, (8, span), 1)
    fill = jnp.maximum(count - first, 0)
    for d in DIRS:
        index = peers.index(offset_of(sizes, [-c for c in d]))
        low, high = range_of(d)
        shifts = []
        for axis in range(3):
            box = side * float(sizes[axis])
            if d[axis] == 1:
                shifts.append(jnp.where(me[axis] == sizes[axis] - 1, box, 0.0))
            elif d[axis] == -1:
                shifts.append(jnp.where(me[axis] == 0, -box, 0.0))
            else:
                shifts.append(jnp.zeros((1, 1), F32))
        shift = jnp.concatenate(shifts, axis=0)
        for source, entry in ((gh_ref, index), (ga_ref, index + len(peers))):
            tiles = source.shape[1] // 3
            width = tiles * L
            begin = offs_ref[entry, low]
            end = offs_ref[entry, 32 + high]
            block = jnp.concatenate([source[index, pl.ds(t, 3, stride=tiles), :] for t in range(tiles)], axis=1) + shift
            block = jnp.concatenate([block, jnp.zeros((5, width), F32)], axis=0)
            block = jnp.concatenate([block, away], axis=1)
            head = fill & (L - 1)
            base = pl.multiple_of(fill - head, L)
            move = head - begin
            block = pltpu.roll(block, jnp.where(move < 0, move + (width + L), move), 1)
            block = jnp.where(lane[:, 0:width + L] < head + end - begin, block, FAR)
            line[:, pl.ds(base, L)] = jnp.where(lane[:, 0:L] < head, line[:, pl.ds(base, L)], block[:, 0:L])
            line[:, pl.ds(pl.multiple_of(base + L, L), width)] = block[:, L:]
            fill = fill + (end - begin)
    rest = pl.multiple_of(((fill + L - 1) // L) * L, L)
    line[:, pl.ds(rest, CHUNK * L)] = jnp.full((8, CHUNK * L), FAR, F32)
    chunks = jnp.maximum((fill + CHUNK * L - 1) // (CHUNK * L), 1)

    def widen(c, carry):
        for t in range(CHUNK):
            place = pl.ds(pl.multiple_of((c * CHUNK + t) * L, L), L)
            tile = line[:, place]
            for a in range(3):
                wide_line[a, :, place] = jnp.broadcast_to(tile[a:a + 1], TILE)
        return carry

    lax.fori_loop(0, chunks, widen, 0)

    def own_step(q, energy):
        start = tuple(tuple(inner_ref[a, step_rows(q, g), :] for a in range(3)) for g in range(GROUPS))
        carry = pair_loop(own_cols, wide_line, q, 0, 1, True, (start, energy))
        force, energy = pair_loop(own_cols, wide_line, q, 1, chunks, False, carry)
        for g in range(GROUPS):
            for a in range(3):
                sums[a, step_rows(q, g), :] = force[g][a]
        return energy

    own_steps = (count + 8 * GROUPS - 1) // (8 * GROUPS)
    energy = lax.fori_loop(0, own_steps, own_step, tuple(inner_en_ref[k] for k in range(3)))
    en_ref[...] = jnp.sum(2.0 * energy[0] - 12.0 * energy[1] + 0.5 * (RC * UPC - UCUT) * energy[2], axis=0, keepdims=True)

    col = lax.broadcasted_iota(I32, (L, L), 1)
    picks = [jnp.where(col == a, 1.0, 0.0).astype(BF16) for a in range(3)]

    def add_up(base):
        total = jnp.zeros((2 * L, L), F32)
        for a in range(3):
            for part in split3(sums[a, base:base + 2 * L, :]):
                total = total + lax.dot_general(part, picks[a], NN, preferred_element_type=F32)
        added[:, base:base + 2 * L] = jnp.transpose(total)[0:8]

    for base in range(0, slots, 2 * L):
        pl.when(count > base)(functools.partial(add_up, base))
    force = jnp.where(good, 24.0 * added[0:3], 0.0)
    pos_ref[...] = srt_ref[0:3, 0:n]
    frc_ref[...] = force[:, 0:n]
    vel_ref[...] = (srt_ref[3:6] + (0.5 * DT) * force)[:, 0:n]
    id_ref[...] = jnp.reshape((srt_ref[6:7].astype(I32) * 65536 + srt_ref[7:8].astype(I32))[:, 0:n], (n,))
    ok_ref[...] = jnp.reshape(okrow[:, 0:n].astype(I32), (n,))


def total_kernel(sizes, part_ref, sum_ref, rows, ssem, rsem):
    me = [lax.axis_index(name) for name in "xyz"]
    size_x, size_y, size_z = sizes
    mine = (me[2] * size_y + me[1]) * size_x + me[0]
    others = [(dx, dy, dz) for dz in range(size_z) for dy in range(size_y) for dx in range(size_x) if dx + dy + dz > 0]
    others.sort(key=lambda o: -(2 * min(o[2], size_z - o[2]) + 2 * o[1] + min(o[0], size_x - o[0])))

    device_at = functools.partial(device_of, sizes, me)

    barrier = pltpu.get_barrier_semaphore()
    for offset in others:
        pl.semaphore_signal(barrier, inc=1, device_id=device_at(offset), device_id_type=pl.DeviceIdType.MESH)
    rows[pl.ds(mine, 1)] = part_ref[...]
    pl.semaphore_wait(barrier, len(others))
    copies = []
    for index, offset in enumerate(others):
        copy = pltpu.make_async_remote_copy(
            src_ref=part_ref, dst_ref=rows.at[pl.ds(mine, 1)], send_sem=ssem.at[index], recv_sem=rsem.at[index],
            device_id=device_at(offset), device_id_type=pl.DeviceIdType.MESH)
        copy.start()
        copies.append(copy)
    for copy in copies:
        copy.wait_recv()
    sum_ref[...] = jnp.sum(rows[...], axis=0, keepdims=True)
    for copy in copies:
        copy.wait_send()


def solution(mesh):
    sizes = (mesh.shape["x"], mesh.shape["y"], mesh.shape["z"])
    peers = sorted({offset_of(sizes, d) for d in DIRS} - {(0, 0, 0)})
    devices = sizes[0] * sizes[1] * sizes[2]

    def local_step(atom_pos, atom_vel, atom_frc, atom_id, atom_ok, brick_side):
        n = atom_pos.shape[0]
        slots = -(-n // L) * L
        side = jnp.reshape(brick_side, (1, 1))
        old_rows, new_rows = [3 * (width // L) + 1 for width in (slots, NEW)]
        vmem = pl.BlockSpec(memory_space=pltpu.VMEM)
        smem = pl.BlockSpec(memory_space=pltpu.SMEM)
        srt, ghosts, fresh, own, inner, inner_en = pl.pallas_call(
            functools.partial(exchange_kernel, sizes, peers, slots),
            out_shape=(jax.ShapeDtypeStruct((16, slots), F32), jax.ShapeDtypeStruct((len(peers), old_rows, L), F32), jax.ShapeDtypeStruct((len(peers), new_rows, L), F32),
                       jax.ShapeDtypeStruct((slots, 3 * L), F32), jax.ShapeDtypeStruct((3, slots, L), F32), jax.ShapeDtypeStruct((3,) + TILE, F32)),
            in_specs=[pl.BlockSpec(memory_space=pltpu.HBM)] * 5 + [smem],
            out_specs=(vmem,) * 6,
            scratch_shapes=[
                pltpu.VMEM((3, n), F32), pltpu.VMEM((3, n), F32), pltpu.VMEM((3, n), F32), pltpu.VMEM((n,), I32), pltpu.VMEM((n,), I32),
                pltpu.VMEM((32, L), F32), pltpu.VMEM((26, L), F32), pltpu.VMEM((3, old_rows, L), F32), pltpu.VMEM((3, new_rows, L), F32), pltpu.VMEM((3, 8, CHUNK * L), F32),
                pltpu.SemaphoreType.DMA((5,)), pltpu.SemaphoreType.DMA((26,)), pltpu.SemaphoreType.DMA((26,)),
            ] + [pltpu.SemaphoreType.DMA((len(peers),))] * 4,
            compiler_params=pltpu.CompilerParams(collective_id=0, has_side_effects=True, vmem_limit_bytes=40 * 2 ** 20),
            name="exchange",
        )(*[pltpu.with_memory_space_constraint(v, pltpu.HBM) for v in (atom_pos.T, atom_vel.T, atom_frc.T, atom_id, atom_ok)], side)
        offs = jnp.concatenate([ghosts[:, -1, 0:64], fresh[:, -1, 0:64]], axis=0).astype(I32)
        out_f = jax.ShapeDtypeStruct((3, n), F32)
        out_i = jax.ShapeDtypeStruct((n,), I32)
        new_pos, new_vel, new_frc, new_id, new_ok, energy = pl.pallas_call(
            functools.partial(force_kernel, sizes, peers, slots),
            out_shape=(out_f, out_f, out_f, out_i, out_i, jax.ShapeDtypeStruct((1, L), F32)),
            in_specs=[vmem] * 6 + [smem],
            out_specs=(vmem,) * 6,
            scratch_shapes=[pltpu.VMEM((8, 28 * slots + CHUNK * L), F32), pltpu.VMEM((3, 8, 28 * slots + CHUNK * L), F32), pltpu.VMEM((3, slots, L), F32), pltpu.VMEM((8, slots), F32)],
            compiler_params=pltpu.CompilerParams(vmem_limit_bytes=40 * 2 ** 20),
            name="forces",
        )(srt, ghosts, fresh, own, inner, inner_en, offs)
        energy = pl.pallas_call(
            functools.partial(total_kernel, sizes),
            out_shape=jax.ShapeDtypeStruct((1, L), F32),
            in_specs=[vmem],
            out_specs=vmem,
            scratch_shapes=[pltpu.VMEM((devices, L), F32), pltpu.SemaphoreType.DMA((devices,)), pltpu.SemaphoreType.DMA((devices,))],
            compiler_params=pltpu.CompilerParams(collective_id=1, has_side_effects=True, vmem_limit_bytes=4 * 2 ** 20),
            name="total",
        )(pltpu.with_memory_space_constraint(energy, pltpu.VMEM))
        return new_pos.T, new_vel.T, new_frc.T, new_id, new_ok, jnp.sum(energy)

    row_spec = P(MESH_AXES, None)
    id_spec = P(MESH_AXES)
    return jax.shard_map(local_step, mesh=mesh, in_specs=(row_spec, row_spec, row_spec, id_spec, id_spec, P()), out_specs=(row_spec, row_spec, row_spec, id_spec, id_spec, P()), check_vma=False)
```

```python
import functools

import jax
import jax.numpy as jnp
from jax import lax
from jax.experimental import pallas as pl
from jax.experimental.pallas import tpu as pltpu
from jax.sharding import PartitionSpec as P

DT = 0.005
RC = 2.5
FAR = 1.0e6
UCUT = 4.0 * (RC ** -12 - RC ** -6)
UPC = -48.0 * RC ** -13 + 24.0 * RC ** -7
MESH_AXES = ("z", "y", "x")
DIRS = [(dx, dy, dz) for dz in (-1, 0, 1) for dy in (-1, 0, 1) for dx in (-1, 0, 1) if (dx, dy, dz) != (0, 0, 0)]
NEAR = RC + 1.0e-3
MAJOR = ((2, 1, 0), (1, 0, 2), (0, 2, 1))
PACK = 8
NEW = 256
CHUNK = 4
GROUPS = 8
L = 128
TILE = (8, L)
F32 = jnp.float32
BF16 = jnp.bfloat16
I32 = jnp.int32
NT = (((1,), (1,)), ((), ()))
NN = (((1,), (0,)), ((), ()))


def device_of(sizes, me, offset):
    return tuple(lax.rem(me[axis] + offset[axis], sizes[axis]) for axis in (2, 1, 0))


def offset_of(sizes, d):
    return tuple(c % size for c, size in zip(d, sizes))


def order_of(d):
    if d[2] == 0:
        return 1 if d[1] != 0 else 2
    return 2 if (d[1] == 0 and d[0] != 0) else 0


def range_of(d):
    first, size = 0, 27
    for axis in MAJOR[order_of(d)]:
        if d[axis] == 0:
            break
        size = size // 3
        first = first + (1, 0, 2)[d[axis]] * size
    return first, first + size


def split3(x):
    hi = x.astype(BF16)
    rest = x - hi.astype(F32)
    mid = rest.astype(BF16)
    low = (rest - mid.astype(F32)).astype(BF16)
    return hi, mid, low


def onehot_rows(dest, base, count):
    rows = lax.broadcasted_iota(I32, (count, dest.shape[1]), 0) + base
    return jnp.where(rows == dest, 1.0, 0.0).astype(BF16)


def scatter_lanes(data, dest, slots):
    rows = data.shape[0]
    parts = jnp.concatenate(split3(data), axis=0)
    out = []
    for base in range(0, slots, 256):
        hot = onehot_rows(dest, base, min(256, slots - base))
        got = lax.dot_general(parts, hot, NT, preferred_element_type=F32)
        out.append(got[0:rows] + got[rows:2 * rows] + got[2 * rows:3 * rows])
    return jnp.concatenate(out, axis=1)


def class_places(code, with_before):
    width = code.shape[1]
    tiles = width // L
    cls = lax.broadcasted_iota(I32, (32, width), 0)
    member = jnp.where(cls == code, 1.0, 0.0)
    member_b = member.astype(BF16)
    stacked = jnp.concatenate([member_b[:, t * L:(t + 1) * L] for t in range(tiles)], axis=0)
    row_i = lax.broadcasted_iota(I32, (L, 256), 0)
    col_i = lax.broadcasted_iota(I32, (L, 256), 1)
    tri = jnp.where((row_i < col_i) | (col_i >= L), 1.0, 0.0).astype(BF16)
    pre = lax.dot_general(stacked, tri, NN, preferred_element_type=F32)
    carry = jnp.zeros((32, L), F32)
    if with_before:
        before_b = jnp.where(code < cls, 1.0, 0.0).astype(BF16)
        before_s = before_b[:, 0:L]
        tot = None
        ones = jnp.ones((L, L), BF16)
        for t in range(tiles):
            part = lax.dot_general(before_b[:, t * L:(t + 1) * L], ones, NN, preferred_element_type=F32)
            tot = part if tot is None else tot + part
        before = tot
        carry = before
    else:
        before = None
    places = []
    for t in range(tiles):
        within = pre[32 * t:32 * t + 32, 0:L] + carry
        places.append(jnp.sum(member[:, t * L:(t + 1) * L] * within, axis=0, keepdims=True))
        carry = carry + pre[32 * t:32 * t + 32, L:256]
    return jnp.concatenate(places, axis=1), before


def pad_lanes(x, width):
    return jnp.concatenate([x, jnp.zeros((x.shape[0], width - x.shape[1]), x.dtype)], axis=1)


def pair_loop(own_cols, near_lanes, q, first, last, with_self, carry):
    rows = [step_rows(q, g) for g in range(GROUPS)]
    own = [[own_cols[rows[g], a * L:(a + 1) * L] for a in range(3)] for g in range(GROUPS)]

    def body(c, carry):
        force, en = [list(f) for f in carry[0]], list(carry[1])
        for t in range(CHUNK):
            place = pl.ds(pl.multiple_of((c * CHUNK + t) * L, L), L)
            near_xyz = [near_lanes[a, :, place] for a in range(3)]
            for g in range(GROUPS):
                dx, dy, dz = [own[g][a] - near_xyz[a] for a in range(3)]
                d2 = dx * dx + dy * dy + dz * dz
                near = d2 < RC * RC
                if with_self:
                    near = near & (d2 > 0.0)
                inv = jnp.where(near, lax.rsqrt(d2), 0.0)
                s2 = inv * inv
                s6 = s2 * s2 * s2
                s12 = s6 * s6
                p = s12 - s6
                w = inv * (UPC / 24.0)
                scale = (p + s12) * s2 + w
                en = [en[0] + p, en[1] + w * d2, en[2] + jnp.where(near, 1.0, 0.0)]
                force[g] = [force[g][0] + scale * dx, force[g][1] + scale * dy, force[g][2] + scale * dz]
        return tuple(tuple(f) for f in force), tuple(en)

    return lax.fori_loop(first, last, body, carry)


def step_rows(q, g):
    return pl.ds(pl.multiple_of((q * GROUPS + g) * 8, 8), 8)


def own_columns(xyz):
    slots = xyz.shape[1]
    parts = [part.astype(F32) for part in split3(xyz)]
    parts = jnp.concatenate(parts + [jnp.zeros((7, slots), F32)], axis=0)
    row = lax.broadcasted_iota(I32, (16, 3 * L), 0)
    tile = lax.broadcasted_iota(I32, (16, 3 * L), 1) // L
    picks = jnp.where((row == tile) | (row == tile + 3) | (row == tile + 6), 1.0, 0.0).astype(BF16)
    return lax.dot_general(jnp.transpose(parts).astype(BF16), picks, NN, preferred_element_type=F32)


def exchange_kernel(sizes, peers, slots, pos_hbm, vel_hbm, frc_hbm, id_hbm, ok_hbm, side_ref, srt_ref, gh_ref, ga_ref, own_ref, inner_ref, inner_en_ref, pos_ref, vel_ref, frc_ref, id_ref, ok_ref, pkt, rcv, out3, new3, lanes, isem, psend, precv, gsend, grecv, asend, arecv):
    me = [lax.axis_index(name) for name in "xyz"]

    device_at = functools.partial(device_of, sizes, me)

    loads = []
    for index, (src, dst) in enumerate(((ok_hbm, ok_ref), (id_hbm, id_ref), (pos_hbm, pos_ref), (vel_hbm, vel_ref), (frc_hbm, frc_ref))):
        load = pltpu.make_async_copy(src, dst, isem.at[index])
        load.start()
        loads.append(load)
    barrier = pltpu.get_barrier_semaphore()
    for offset in peers:
        pl.semaphore_signal(barrier, inc=1, device_id=device_at(offset), device_id_type=pl.DeviceIdType.MESH)

    n = pos_ref.shape[1]
    for load in loads:
        load.wait()
    side = side_ref[0, 0]
    owned = pad_lanes(jnp.reshape(ok_ref[...], (1, n)), slots) > 0
    half = vel_ref[...] + (0.5 * DT) * frc_ref[...]
    free = pos_ref[...] + DT * half
    half = pad_lanes(half, slots)
    free = pad_lanes(free, slots)
    ids = pad_lanes(jnp.reshape(id_ref[...], (1, n)), slots)
    code = jnp.zeros((1, slots), I32)
    moved = []
    low_side = []
    for axis in range(3):
        low = me[axis].astype(F32) * side
        high = (me[axis] + 1).astype(F32) * side
        box = side * float(sizes[axis])
        u = free[axis:axis + 1]
        step = jnp.where(u >= high, 1, 0) - jnp.where(u < low, 1, 0)
        code = code + (step + 1) * (1, 3, 9)[axis]
        moved.append(jnp.where(u < 0.0, u + box, jnp.where(u >= box, u - box, u)))
        low_side.append(low)
    code = jnp.where(owned, code, 31)
    id_hi = (ids >> 16).astype(F32)
    id_lo = (ids & 65535).astype(F32)
    okf = jnp.where(owned, 1.0, 0.0)
    data = jnp.concatenate(moved + [half, id_hi, id_lo, okf, jnp.zeros((7, slots), F32)], axis=0)

    place, _ = class_places(code, False)
    leaving = owned & (code != 13)
    way = jnp.where(leaving, code - jnp.where(code > 13, 1, 0), 31)
    member = jnp.where(lax.broadcasted_iota(I32, (32, slots), 0) == way, 1.0, 0.0).astype(BF16)
    fields = jnp.concatenate([jnp.where(place == float(k), data, 0.0) for k in range(PACK)], axis=0)
    packed = jnp.zeros((32, L), F32)
    for part in split3(fields):
        packed = packed + lax.dot_general(member, part, NT, preferred_element_type=F32)
    pkt[...] = packed

    def bins_of(pos):
        bins = []
        for axis in range(3):
            loc = pos[axis:axis + 1] - low_side[axis]
            bins.append(jnp.where(loc < NEAR, 0, jnp.where(loc > side - NEAR, 2, 1)))
        return [(bins[i] * 3 + bins[j]) * 3 + bins[k] for i, j, k in MAJOR]

    wide = side > 2.0 * NEAR
    eye = lax.broadcasted_iota(I32, (32, L), 0) == lax.broadcasted_iota(I32, (32, L), 1)

    def sorted_block(cand, keys, kept):
        width = cand.shape[1]
        where_to, before = class_places(jnp.where(kept, keys, 28), True)
        arranged = scatter_lanes(cand, jnp.where(kept, where_to.astype(I32), -1), width)
        total = jnp.concatenate([before[27:28]] * (width // L), axis=1)
        lane = lax.broadcasted_iota(I32, (1, width), 1).astype(F32)
        begins = jnp.sum(jnp.where(eye, before, 0.0), axis=0, keepdims=True)
        ends = jnp.where(wide, begins, before[27:28])
        counts = jnp.concatenate([jnp.where(wide, begins, 0.0)[:, 0:32], ends[:, 0:32], jnp.zeros((1, L - 64), F32)], axis=1)
        return jnp.where(lane < total, arranged[0:3], FAR), counts

    def send(src, dst, ssem, rsem, offset):
        copy = pltpu.make_async_remote_copy(
            src_ref=src, dst_ref=dst, send_sem=ssem, recv_sem=rsem,
            device_id=device_at(offset), device_id_type=pl.DeviceIdType.MESH)
        copy.start()
        return copy

    def store_block(ref, kind, xyz, counts):
        tiles = xyz.shape[1] // L
        for a in range(3):
            for t in range(tiles):
                ref[kind, pl.ds(a * tiles + t, 1)] = xyz[a:a + 1, t * L:(t + 1) * L]
        ref[kind, pl.ds(3 * tiles, 1)] = counts

    def send_blocks(block, dst, ssem, rsem, kind):
        out = []
        for index, offset in enumerate(peers):
            if order_of(tuple(0 if c == 0 else 1 for c in offset)) == kind:
                out.append(send(block.at[kind], dst.at[index], ssem.at[index], rsem.at[index], offset))
        return out

    pl.semaphore_wait(barrier, len(peers))
    packets = []
    for index, d in enumerate(DIRS):
        row = pl.ds(index, 1)
        packets.append(send(pkt.at[row], rcv.at[row], psend.at[index], precv.at[index], offset_of(sizes, d)))
    blocks = []
    staying = code == 13
    keys = bins_of(data)
    for kind in range(3):
        store_block(out3, kind, *sorted_block(data[0:8], keys[kind], staying))
        blocks = blocks + send_blocks(out3, gh_ref, gsend, grecv, kind)
    for copy in packets:
        copy.wait_recv()

    came = jnp.concatenate([rcv[...], jnp.zeros((32 - 26, L), F32)], axis=0)
    came = jnp.concatenate([came] + [pltpu.roll(came, L - 16 * k, 1) for k in range(1, PACK)], axis=0)
    came_t = jnp.transpose(came)[0:16]
    came_ok = came_t[8:9] > 0.5
    keys = bins_of(came_t)
    late = []
    for kind in range(3):
        store_block(new3, kind, *sorted_block(came_t[0:8], keys[kind], came_ok))
        late = late + send_blocks(new3, ga_ref, asend, arecv, kind)
    for copy in packets:
        copy.wait_send()

    arr_ids = came[:, 6:7].astype(I32) * 65536 + came[:, 7:8].astype(I32)
    arr_ok = came[:, 8:9] > 0.5
    row_ids = jnp.concatenate([ids, came_t[6:7].astype(I32) * 65536 + came_t[7:8].astype(I32)], axis=1)
    less = jnp.where((arr_ids < row_ids) & arr_ok, 1.0, 0.0)
    arrivals_below = jnp.sum(less, axis=0, keepdims=True)
    above = jnp.where((arr_ids > row_ids[:, 0:slots]) & staying, 1.0, 0.0).astype(BF16)
    stay_below = lax.dot_general(jnp.ones((16, slots), BF16), above, NT, preferred_element_type=F32)[0:1]
    stay_place, _ = class_places(jnp.where(staying, 0, 31), False)
    rank = jnp.concatenate([stay_place, stay_below], axis=1) + arrivals_below
    dest = jnp.where(jnp.concatenate([staying, came_ok], axis=1), rank.astype(I32), -1)
    merged = scatter_lanes(jnp.concatenate([data, came_t], axis=1), dest, slots)
    srt_ref[...] = jnp.where(lax.broadcasted_iota(I32, (16, slots), 0) == 9, side, merged)

    good = merged[8:9] > 0.5
    own_ref[...] = own_columns(jnp.where(good, merged[0:3], -FAR))
    first = CHUNK * L
    for a in range(3):
        lanes[a] = jnp.broadcast_to(jnp.where(good, merged[a:a + 1], FAR)[:, 0:first], (8, first))
    zero = jnp.zeros(TILE, F32)

    def own_step(q, energy):
        force, energy = pair_loop(own_ref, lanes, q, 0, 1, True, (((zero,) * 3,) * GROUPS, energy))
        for g in range(GROUPS):
            for a in range(3):
                inner_ref[a, step_rows(q, g), :] = force[g][a]
        return energy

    for k, part in enumerate(lax.fori_loop(0, slots // (8 * GROUPS), own_step, (zero,) * 3)):
        inner_en_ref[k] = part

    for copy in blocks + late:
        copy.wait()


def force_kernel(sizes, peers, slots, srt_ref, gh_ref, ga_ref, own_cols, inner_ref, inner_en_ref, offs_ref, pos_ref, vel_ref, frc_ref, id_ref, ok_ref, en_ref, line, wide_line, sums, added):
    me = [lax.axis_index(name) for name in "xyz"]
    n = pos_ref.shape[1]
    side = srt_ref[9:10, 0:1]
    okrow = srt_ref[8:9]
    good = okrow > 0.5
    count = jnp.sum(okrow).astype(I32)
    span = slots + L

    away = jnp.full(TILE, FAR, F32)
    first = CHUNK * L
    line[:, 0:slots - first] = jnp.concatenate([jnp.where(good, srt_ref[0:3], FAR), jnp.full((5, slots), FAR, F32)], axis=0)[:, first:]
    lane = lax.broadcasted_iota(I32, (8, span), 1)
    fill = jnp.maximum(count - first, 0)
    for d in DIRS:
        index = peers.index(offset_of(sizes, [-c for c in d]))
        low, high = range_of(d)
        shifts = []
        for axis in range(3):
            box = side * float(sizes[axis])
            if d[axis] == 1:
                shifts.append(jnp.where(me[axis] == sizes[axis] - 1, box, 0.0))
            elif d[axis] == -1:
                shifts.append(jnp.where(me[axis] == 0, -box, 0.0))
            else:
                shifts.append(jnp.zeros((1, 1), F32))
        shift = jnp.concatenate(shifts, axis=0)
        for source, entry in ((gh_ref, index), (ga_ref, index + len(peers))):
            tiles = source.shape[1] // 3
            width = tiles * L
            begin = offs_ref[entry, low]
            end = offs_ref[entry, 32 + high]
            block = jnp.concatenate([source[index, pl.ds(t, 3, stride=tiles), :] for t in range(tiles)], axis=1) + shift
            block = jnp.concatenate([block, jnp.zeros((5, width), F32)], axis=0)
            block = jnp.concatenate([block, away], axis=1)
            head = fill & (L - 1)
            base = pl.multiple_of(fill - head, L)
            move = head - begin
            block = pltpu.roll(block, jnp.where(move < 0, move + (width + L), move), 1)
            block = jnp.where(lane[:, 0:width + L] < head + end - begin, block, FAR)
            line[:, pl.ds(base, L)] = jnp.where(lane[:, 0:L] < head, line[:, pl.ds(base, L)], block[:, 0:L])
            line[:, pl.ds(pl.multiple_of(base + L, L), width)] = block[:, L:]
            fill = fill + (end - begin)
    rest = pl.multiple_of(((fill + L - 1) // L) * L, L)
    line[:, pl.ds(rest, CHUNK * L)] = jnp.full((8, CHUNK * L), FAR, F32)
    chunks = jnp.maximum((fill + CHUNK * L - 1) // (CHUNK * L), 1)

    def widen(c, carry):
        for t in range(CHUNK):
            place = pl.ds(pl.multiple_of((c * CHUNK + t) * L, L), L)
            tile = line[:, place]
            for a in range(3):
                wide_line[a, :, place] = jnp.broadcast_to(tile[a:a + 1], TILE)
        return carry

    lax.fori_loop(0, chunks, widen, 0)

    def own_step(q, energy):
        start = tuple(tuple(inner_ref[a, step_rows(q, g), :] for a in range(3)) for g in range(GROUPS))
        carry = pair_loop(own_cols, wide_line, q, 0, 1, True, (start, energy))
        force, energy = pair_loop(own_cols, wide_line, q, 1, chunks, False, carry)
        for g in range(GROUPS):
            for a in range(3):
                sums[a, step_rows(q, g), :] = force[g][a]
        return energy

    own_steps = (count + 8 * GROUPS - 1) // (8 * GROUPS)
    energy = lax.fori_loop(0, own_steps, own_step, tuple(inner_en_ref[k] for k in range(3)))
    en_ref[...] = jnp.sum(2.0 * energy[0] - 12.0 * energy[1] + 0.5 * (RC * UPC - UCUT) * energy[2], axis=0, keepdims=True)

    col = lax.broadcasted_iota(I32, (L, L), 1)
    picks = [jnp.where(col == a, 1.0, 0.0).astype(BF16) for a in range(3)]

    def add_up(base):
        total = jnp.zeros((2 * L, L), F32)
        for a in range(3):
            for part in split3(sums[a, base:base + 2 * L, :]):
                total = total + lax.dot_general(part, picks[a], NN, preferred_element_type=F32)
        added[:, base:base + 2 * L] = jnp.transpose(total)[0:8]

    for base in range(0, slots, 2 * L):
        pl.when(count > base)(functools.partial(add_up, base))
    force = jnp.where(good, 24.0 * added[0:3], 0.0)
    pos_ref[...] = srt_ref[0:3, 0:n]
    frc_ref[...] = force[:, 0:n]
    vel_ref[...] = (srt_ref[3:6] + (0.5 * DT) * force)[:, 0:n]
    id_ref[...] = jnp.reshape((srt_ref[6:7].astype(I32) * 65536 + srt_ref[7:8].astype(I32))[:, 0:n], (n,))
    ok_ref[...] = jnp.reshape(okrow[:, 0:n].astype(I32), (n,))


def total_kernel(sizes, part_ref, sum_ref, rows, ssem, rsem):
    me = [lax.axis_index(name) for name in "xyz"]
    size_x, size_y, size_z = sizes
    mine = (me[2] * size_y + me[1]) * size_x + me[0]
    others = [(dx, dy, dz) for dz in range(size_z) for dy in range(size_y) for dx in range(size_x) if dx + dy + dz > 0]
    others.sort(key=lambda o: -(2 * min(o[2], size_z - o[2]) + 2 * o[1] + min(o[0], size_x - o[0])))

    device_at = functools.partial(device_of, sizes, me)

    barrier = pltpu.get_barrier_semaphore()
    for offset in others:
        pl.semaphore_signal(barrier, inc=1, device_id=device_at(offset), device_id_type=pl.DeviceIdType.MESH)
    rows[pl.ds(mine, 1)] = part_ref[...]
    pl.semaphore_wait(barrier, len(others))
    copies = []
    for index, offset in enumerate(others):
        copy = pltpu.make_async_remote_copy(
            src_ref=part_ref, dst_ref=rows.at[pl.ds(mine, 1)], send_sem=ssem.at[index], recv_sem=rsem.at[index],
            device_id=device_at(offset), device_id_type=pl.DeviceIdType.MESH)
        copy.start()
        copies.append(copy)
    for copy in copies:
        copy.wait_recv()
    sum_ref[...] = jnp.sum(rows[...], axis=0, keepdims=True)
    for copy in copies:
        copy.wait_send()


def solution(mesh):
    sizes = (mesh.shape["x"], mesh.shape["y"], mesh.shape["z"])
    peers = sorted({offset_of(sizes, d) for d in DIRS} - {(0, 0, 0)})
    devices = sizes[0] * sizes[1] * sizes[2]

    def local_step(atom_pos, atom_vel, atom_frc, atom_id, atom_ok, brick_side):
        n = atom_pos.shape[0]
        slots = -(-n // L) * L
        side = jnp.reshape(brick_side, (1, 1))
        old_rows, new_rows = [3 * (width // L) + 1 for width in (slots, NEW)]
        vmem = pl.BlockSpec(memory_space=pltpu.VMEM)
        smem = pl.BlockSpec(memory_space=pltpu.SMEM)
        srt, ghosts, fresh, own, inner, inner_en = pl.pallas_call(
            functools.partial(exchange_kernel, sizes, peers, slots),
            out_shape=(jax.ShapeDtypeStruct((16, slots), F32), jax.ShapeDtypeStruct((len(peers), old_rows, L), F32), jax.ShapeDtypeStruct((len(peers), new_rows, L), F32),
                       jax.ShapeDtypeStruct((slots, 3 * L), F32), jax.ShapeDtypeStruct((3, slots, L), F32), jax.ShapeDtypeStruct((3,) + TILE, F32)),
            in_specs=[pl.BlockSpec(memory_space=pltpu.HBM)] * 5 + [smem],
            out_specs=(vmem,) * 6,
            scratch_shapes=[
                pltpu.VMEM((3, n), F32), pltpu.VMEM((3, n), F32), pltpu.VMEM((3, n), F32), pltpu.VMEM((n,), I32), pltpu.VMEM((n,), I32),
                pltpu.VMEM((32, L), F32), pltpu.VMEM((26, L), F32), pltpu.VMEM((3, old_rows, L), F32), pltpu.VMEM((3, new_rows, L), F32), pltpu.VMEM((3, 8, CHUNK * L), F32),
                pltpu.SemaphoreType.DMA((5,)), pltpu.SemaphoreType.DMA((26,)), pltpu.SemaphoreType.DMA((26,)),
            ] + [pltpu.SemaphoreType.DMA((len(peers),))] * 4,
            compiler_params=pltpu.CompilerParams(collective_id=0, has_side_effects=True, vmem_limit_bytes=40 * 2 ** 20),
            name="exchange",
        )(*[pltpu.with_memory_space_constraint(v, pltpu.HBM) for v in (atom_pos.T, atom_vel.T, atom_frc.T, atom_id, atom_ok)], side)
        offs = jnp.concatenate([ghosts[:, -1, 0:64], fresh[:, -1, 0:64]], axis=0).astype(I32)
        out_f = jax.ShapeDtypeStruct((3, n), F32)
        out_i = jax.ShapeDtypeStruct((n,), I32)
        new_pos, new_vel, new_frc, new_id, new_ok, energy = pl.pallas_call(
            functools.partial(force_kernel, sizes, peers, slots),
            out_shape=(out_f, out_f, out_f, out_i, out_i, jax.ShapeDtypeStruct((1, L), F32)),
            in_specs=[vmem] * 6 + [smem],
            out_specs=(vmem,) * 6,
            scratch_shapes=[pltpu.VMEM((8, 28 * slots + CHUNK * L), F32), pltpu.VMEM((3, 8, 28 * slots + CHUNK * L), F32), pltpu.VMEM((3, slots, L), F32), pltpu.VMEM((8, slots), F32)],
            compiler_params=pltpu.CompilerParams(vmem_limit_bytes=40 * 2 ** 20),
            name="forces",
        )(srt, ghosts, fresh, own, inner, inner_en, offs)
        energy = pl.pallas_call(
            functools.partial(total_kernel, sizes),
            out_shape=jax.ShapeDtypeStruct((1, L), F32),
            in_specs=[vmem],
            out_specs=vmem,
            scratch_shapes=[pltpu.VMEM((devices, L), F32), pltpu.SemaphoreType.DMA((devices,)), pltpu.SemaphoreType.DMA((devices,))],
            compiler_params=pltpu.CompilerParams(collective_id=1, has_side_effects=True, vmem_limit_bytes=4 * 2 ** 20),
            name="total",
        )(pltpu.with_memory_space_constraint(energy, pltpu.VMEM))
        return new_pos.T, new_vel.T, new_frc.T, new_id, new_ok, jnp.sum(energy)

    row_spec = P(MESH_AXES, None)
    id_spec = P(MESH_AXES)
    return jax.shard_map(local_step, mesh=mesh, in_specs=(row_spec, row_spec, row_spec, id_spec, id_spec, P()), out_specs=(row_spec, row_spec, row_spec, id_spec, id_spec, P()), check_vma=False)
```

```python
import functools

import jax
import jax.numpy as jnp
from jax import lax
from jax.experimental import pallas as pl
from jax.experimental.pallas import tpu as pltpu
from jax.sharding import PartitionSpec as P

DT = 0.005
RC = 2.5
FAR = 1.0e6
UCUT = 4.0 * (RC ** -12 - RC ** -6)
UPC = -48.0 * RC ** -13 + 24.0 * RC ** -7
MESH_AXES = ("z", "y", "x")
DIRS = [(dx, dy, dz) for dz in (-1, 0, 1) for dy in (-1, 0, 1) for dx in (-1, 0, 1) if (dx, dy, dz) != (0, 0, 0)]
NEAR = RC + 1.0e-3
MAJOR = ((2, 1, 0), (1, 0, 2), (0, 2, 1))
PACK = 8
NEW = 256
CHUNK = 4
GROUPS = 8
L = 128
TILE = (8, L)
F32 = jnp.float32
BF16 = jnp.bfloat16
I32 = jnp.int32
NT = (((1,), (1,)), ((), ()))
NN = (((1,), (0,)), ((), ()))


def device_of(sizes, me, offset):
    return tuple(lax.rem(me[axis] + offset[axis], sizes[axis]) for axis in (2, 1, 0))


def offset_of(sizes, d):
    return tuple(c % size for c, size in zip(d, sizes))


def far_first(d):
    return sum(c == 0 for c in d)


def order_of(d):
    if d[2] == 0:
        return 1 if d[1] != 0 else 2
    return 2 if (d[1] == 0 and d[0] != 0) else 0


def range_of(d):
    first, size = 0, 27
    for axis in MAJOR[order_of(d)]:
        if d[axis] == 0:
            break
        size = size // 3
        first = first + (1, 0, 2)[d[axis]] * size
    return first, first + size


def split3(x):
    hi = x.astype(BF16)
    rest = x - hi.astype(F32)
    mid = rest.astype(BF16)
    low = (rest - mid.astype(F32)).astype(BF16)
    return hi, mid, low


def onehot_rows(dest, base, count):
    rows = lax.broadcasted_iota(I32, (count, dest.shape[1]), 0) + base
    return jnp.where(rows == dest, 1.0, 0.0).astype(BF16)


def scatter_lanes(data, dest, slots):
    rows = data.shape[0]
    parts = jnp.concatenate(split3(data), axis=0)
    out = []
    for base in range(0, slots, 256):
        hot = onehot_rows(dest, base, min(256, slots - base))
        got = lax.dot_general(parts, hot, NT, preferred_element_type=F32)
        out.append(got[0:rows] + got[rows:2 * rows] + got[2 * rows:3 * rows])
    return jnp.concatenate(out, axis=1)


def class_places(code, with_before):
    width = code.shape[1]
    tiles = width // L
    cls = lax.broadcasted_iota(I32, (32, width), 0)
    member = jnp.where(cls == code, 1.0, 0.0)
    member_b = member.astype(BF16)
    stacked = jnp.concatenate([member_b[:, t * L:(t + 1) * L] for t in range(tiles)], axis=0)
    row_i = lax.broadcasted_iota(I32, (L, 256), 0)
    col_i = lax.broadcasted_iota(I32, (L, 256), 1)
    tri = jnp.where((row_i < col_i) | (col_i >= L), 1.0, 0.0).astype(BF16)
    pre = lax.dot_general(stacked, tri, NN, preferred_element_type=F32)
    carry = jnp.zeros((32, L), F32)
    if with_before:
        before_b = jnp.where(code < cls, 1.0, 0.0).astype(BF16)
        before_s = before_b[:, 0:L]
        tot = None
        ones = jnp.ones((L, L), BF16)
        for t in range(tiles):
            part = lax.dot_general(before_b[:, t * L:(t + 1) * L], ones, NN, preferred_element_type=F32)
            tot = part if tot is None else tot + part
        before = tot
        carry = before
    else:
        before = None
    places = []
    for t in range(tiles):
        within = pre[32 * t:32 * t + 32, 0:L] + carry
        places.append(jnp.sum(member[:, t * L:(t + 1) * L] * within, axis=0, keepdims=True))
        carry = carry + pre[32 * t:32 * t + 32, L:256]
    return jnp.concatenate(places, axis=1), before


def pad_lanes(x, width):
    return jnp.concatenate([x, jnp.zeros((x.shape[0], width - x.shape[1]), x.dtype)], axis=1)


def pair_loop(own_cols, near_lanes, q, first, last, with_self, carry):
    rows = [step_rows(q, g) for g in range(GROUPS)]
    own = [[own_cols[rows[g], a * L:(a + 1) * L] for a in range(3)] for g in range(GROUPS)]

    def body(c, carry):
        force, en = [list(f) for f in carry[0]], list(carry[1])
        for t in range(CHUNK):
            place = pl.ds(pl.multiple_of((c * CHUNK + t) * L, L), L)
            near_xyz = [near_lanes[a, :, place] for a in range(3)]
            for g in range(GROUPS):
                dx, dy, dz = [own[g][a] - near_xyz[a] for a in range(3)]
                d2 = dx * dx + dy * dy + dz * dz
                near = d2 < RC * RC
                if with_self:
                    near = near & (d2 > 0.0)
                inv = jnp.where(near, lax.rsqrt(d2), 0.0)
                s2 = inv * inv
                s6 = s2 * s2 * s2
                s12 = s6 * s6
                p = s12 - s6
                w = inv * (UPC / 24.0)
                scale = (p + s12) * s2 + w
                en = [en[0] + p, en[1] + w * d2, en[2] + jnp.where(near, 1.0, 0.0)]
                force[g] = [force[g][0] + scale * dx, force[g][1] + scale * dy, force[g][2] + scale * dz]
        return tuple(tuple(f) for f in force), tuple(en)

    return lax.fori_loop(first, last, body, carry)


def step_rows(q, g):
    return pl.ds(pl.multiple_of((q * GROUPS + g) * 8, 8), 8)


def own_columns(xyz):
    slots = xyz.shape[1]
    parts = [part.astype(F32) for part in split3(xyz)]
    parts = jnp.concatenate(parts + [jnp.zeros((7, slots), F32)], axis=0)
    row = lax.broadcasted_iota(I32, (16, 3 * L), 0)
    tile = lax.broadcasted_iota(I32, (16, 3 * L), 1) // L
    picks = jnp.where((row == tile) | (row == tile + 3) | (row == tile + 6), 1.0, 0.0).astype(BF16)
    return lax.dot_general(jnp.transpose(parts).astype(BF16), picks, NN, preferred_element_type=F32)


def exchange_kernel(sizes, peers, slots, pos_hbm, vel_hbm, frc_hbm, id_hbm, ok_hbm, side_ref, srt_ref, gh_ref, ga_ref, own_ref, inner_ref, inner_en_ref, pos_ref, vel_ref, frc_ref, id_ref, ok_ref, pkt, rcv, out3, new3, lanes, isem, psend, precv, gsend, grecv, asend, arecv):
    me = [lax.axis_index(name) for name in "xyz"]

    device_at = functools.partial(device_of, sizes, me)

    loads = []
    for index, (src, dst) in enumerate(((ok_hbm, ok_ref), (id_hbm, id_ref), (pos_hbm, pos_ref), (vel_hbm, vel_ref), (frc_hbm, frc_ref))):
        load = pltpu.make_async_copy(src, dst, isem.at[index])
        load.start()
        loads.append(load)
    barrier = pltpu.get_barrier_semaphore()
    for offset in sorted(peers, key=far_first):
        pl.semaphore_signal(barrier, inc=1, device_id=device_at(offset), device_id_type=pl.DeviceIdType.MESH)

    n = pos_ref.shape[1]
    for load in loads:
        load.wait()
    side = side_ref[0, 0]
    owned = pad_lanes(jnp.reshape(ok_ref[...], (1, n)), slots) > 0
    half = vel_ref[...] + (0.5 * DT) * frc_ref[...]
    free = pos_ref[...] + DT * half
    half = pad_lanes(half, slots)
    free = pad_lanes(free, slots)
    ids = pad_lanes(jnp.reshape(id_ref[...], (1, n)), slots)
    code = jnp.zeros((1, slots), I32)
    moved = []
    low_side = []
    for axis in range(3):
        low = me[axis].astype(F32) * side
        high = (me[axis] + 1).astype(F32) * side
        box = side * float(sizes[axis])
        u = free[axis:axis + 1]
        step = jnp.where(u >= high, 1, 0) - jnp.where(u < low, 1, 0)
        code = code + (step + 1) * (1, 3, 9)[axis]
        moved.append(jnp.where(u < 0.0, u + box, jnp.where(u >= box, u - box, u)))
        low_side.append(low)
    code = jnp.where(owned, code, 31)
    id_hi = (ids >> 16).astype(F32)
    id_lo = (ids & 65535).astype(F32)
    okf = jnp.where(owned, 1.0, 0.0)
    data = jnp.concatenate(moved + [half, id_hi, id_lo, okf, jnp.zeros((7, slots), F32)], axis=0)

    place, _ = class_places(code, False)
    leaving = owned & (code != 13)
    way = jnp.where(leaving, code - jnp.where(code > 13, 1, 0), 31)
    member = jnp.where(lax.broadcasted_iota(I32, (32, slots), 0) == way, 1.0, 0.0).astype(BF16)
    fields = jnp.concatenate([jnp.where(place == float(k), data, 0.0) for k in range(PACK)], axis=0)
    packed = jnp.zeros((32, L), F32)
    for part in split3(fields):
        packed = packed + lax.dot_general(member, part, NT, preferred_element_type=F32)
    pkt[...] = packed

    def bins_of(pos):
        bins = []
        for axis in range(3):
            loc = pos[axis:axis + 1] - low_side[axis]
            bins.append(jnp.where(loc < NEAR, 0, jnp.where(loc > side - NEAR, 2, 1)))
        return [(bins[i] * 3 + bins[j]) * 3 + bins[k] for i, j, k in MAJOR]

    wide = side > 2.0 * NEAR
    eye = lax.broadcasted_iota(I32, (32, L), 0) == lax.broadcasted_iota(I32, (32, L), 1)

    def sorted_block(cand, keys, kept):
        width = cand.shape[1]
        where_to, before = class_places(jnp.where(kept, keys, 28), True)
        arranged = scatter_lanes(cand, jnp.where(kept, where_to.astype(I32), -1), width)
        total = jnp.concatenate([before[27:28]] * (width // L), axis=1)
        lane = lax.broadcasted_iota(I32, (1, width), 1).astype(F32)
        begins = jnp.sum(jnp.where(eye, before, 0.0), axis=0, keepdims=True)
        ends = jnp.where(wide, begins, before[27:28])
        counts = jnp.concatenate([jnp.where(wide, begins, 0.0)[:, 0:32], ends[:, 0:32], jnp.zeros((1, L - 64), F32)], axis=1)
        return jnp.where(lane < total, arranged[0:3], FAR), counts

    def send(src, dst, ssem, rsem, offset):
        copy = pltpu.make_async_remote_copy(
            src_ref=src, dst_ref=dst, send_sem=ssem, recv_sem=rsem,
            device_id=device_at(offset), device_id_type=pl.DeviceIdType.MESH)
        copy.start()
        return copy

    def store_block(ref, kind, xyz, counts):
        tiles = xyz.shape[1] // L
        for a in range(3):
            for t in range(tiles):
                ref[kind, pl.ds(a * tiles + t, 1)] = xyz[a:a + 1, t * L:(t + 1) * L]
        ref[kind, pl.ds(3 * tiles, 1)] = counts

    def send_blocks(block, dst, ssem, rsem, kind):
        out = []
        for offset in sorted(peers, key=far_first):
            index = peers.index(offset)
            if order_of(tuple(0 if c == 0 else 1 for c in offset)) == kind:
                out.append(send(block.at[kind], dst.at[index], ssem.at[index], rsem.at[index], offset))
        return out

    staying = code == 13
    keys = bins_of(data)
    for kind in range(3):
        store_block(out3, kind, *sorted_block(data[0:8], keys[kind], staying))
    pl.semaphore_wait(barrier, len(peers))
    packets = []
    for d in sorted(DIRS, key=far_first):
        index = DIRS.index(d)
        row = pl.ds(index, 1)
        packets.append(send(pkt.at[row], rcv.at[row], psend.at[index], precv.at[index], offset_of(sizes, d)))
    blocks = []
    for kind in range(3):
        blocks = blocks + send_blocks(out3, gh_ref, gsend, grecv, kind)
    for copy in packets:
        copy.wait_recv()

    came = jnp.concatenate([rcv[...], jnp.zeros((32 - 26, L), F32)], axis=0)
    came = jnp.concatenate([came] + [pltpu.roll(came, L - 16 * k, 1) for k in range(1, PACK)], axis=0)
    came_t = jnp.transpose(came)[0:16]
    came_ok = came_t[8:9] > 0.5
    keys = bins_of(came_t)
    late = []
    for kind in range(3):
        store_block(new3, kind, *sorted_block(came_t[0:8], keys[kind], came_ok))
        late = late + send_blocks(new3, ga_ref, asend, arecv, kind)
    for copy in packets:
        copy.wait_send()

    arr_ids = came[:, 6:7].astype(I32) * 65536 + came[:, 7:8].astype(I32)
    arr_ok = came[:, 8:9] > 0.5
    row_ids = jnp.concatenate([ids, came_t[6:7].astype(I32) * 65536 + came_t[7:8].astype(I32)], axis=1)
    less = jnp.where((arr_ids < row_ids) & arr_ok, 1.0, 0.0)
    arrivals_below = jnp.sum(less, axis=0, keepdims=True)
    above = jnp.where((arr_ids > row_ids[:, 0:slots]) & staying, 1.0, 0.0).astype(BF16)
    stay_below = lax.dot_general(jnp.ones((16, slots), BF16), above, NT, preferred_element_type=F32)[0:1]
    stay_place, _ = class_places(jnp.where(staying, 0, 31), False)
    rank = jnp.concatenate([stay_place, stay_below], axis=1) + arrivals_below
    dest = jnp.where(jnp.concatenate([staying, came_ok], axis=1), rank.astype(I32), -1)
    merged = scatter_lanes(jnp.concatenate([data, came_t], axis=1), dest, slots)
    srt_ref[...] = jnp.where(lax.broadcasted_iota(I32, (16, slots), 0) == 9, side, merged)

    good = merged[8:9] > 0.5
    own_ref[...] = own_columns(jnp.where(good, merged[0:3], -FAR))
    first = CHUNK * L
    for a in range(3):
        lanes[a] = jnp.broadcast_to(jnp.where(good, merged[a:a + 1], FAR)[:, 0:first], (8, first))
    zero = jnp.zeros(TILE, F32)

    def own_step(q, energy):
        force, energy = pair_loop(own_ref, lanes, q, 0, 1, True, (((zero,) * 3,) * GROUPS, energy))
        for g in range(GROUPS):
            for a in range(3):
                inner_ref[a, step_rows(q, g), :] = force[g][a]
        return energy

    for k, part in enumerate(lax.fori_loop(0, slots // (8 * GROUPS), own_step, (zero,) * 3)):
        inner_en_ref[k] = part

    for copy in blocks + late:
        copy.wait()


def force_kernel(sizes, peers, slots, srt_ref, gh_ref, ga_ref, own_cols, inner_ref, inner_en_ref, offs_ref, pos_ref, vel_ref, frc_ref, id_ref, ok_ref, en_ref, line, wide_line, sums, added):
    me = [lax.axis_index(name) for name in "xyz"]
    n = pos_ref.shape[1]
    side = srt_ref[9:10, 0:1]
    okrow = srt_ref[8:9]
    good = okrow > 0.5
    count = jnp.sum(okrow).astype(I32)
    span = slots + L

    away = jnp.full(TILE, FAR, F32)
    first = CHUNK * L
    line[:, 0:slots - first] = jnp.concatenate([jnp.where(good, srt_ref[0:3], FAR), jnp.full((5, slots), FAR, F32)], axis=0)[:, first:]
    lane = lax.broadcasted_iota(I32, (8, span), 1)
    fill = jnp.maximum(count - first, 0)
    for d in DIRS:
        index = peers.index(offset_of(sizes, [-c for c in d]))
        low, high = range_of(d)
        shifts = []
        for axis in range(3):
            box = side * float(sizes[axis])
            if d[axis] == 1:
                shifts.append(jnp.where(me[axis] == sizes[axis] - 1, box, 0.0))
            elif d[axis] == -1:
                shifts.append(jnp.where(me[axis] == 0, -box, 0.0))
            else:
                shifts.append(jnp.zeros((1, 1), F32))
        shift = jnp.concatenate(shifts, axis=0)
        for source, entry in ((gh_ref, index), (ga_ref, index + len(peers))):
            tiles = source.shape[1] // 3
            width = tiles * L
            begin = offs_ref[entry, low]
            end = offs_ref[entry, 32 + high]
            block = jnp.concatenate([source[index, pl.ds(t, 3, stride=tiles), :] for t in range(tiles)], axis=1) + shift
            block = jnp.concatenate([block, jnp.zeros((5, width), F32)], axis=0)
            block = jnp.concatenate([block, away], axis=1)
            head = fill & (L - 1)
            base = pl.multiple_of(fill - head, L)
            move = head - begin
            block = pltpu.roll(block, jnp.where(move < 0, move + (width + L), move), 1)
            block = jnp.where(lane[:, 0:width + L] < head + end - begin, block, FAR)
            line[:, pl.ds(base, L)] = jnp.where(lane[:, 0:L] < head, line[:, pl.ds(base, L)], block[:, 0:L])
            line[:, pl.ds(pl.multiple_of(base + L, L), width)] = block[:, L:]
            fill = fill + (end - begin)
    rest = pl.multiple_of(((fill + L - 1) // L) * L, L)
    line[:, pl.ds(rest, CHUNK * L)] = jnp.full((8, CHUNK * L), FAR, F32)
    chunks = jnp.maximum((fill + CHUNK * L - 1) // (CHUNK * L), 1)

    def widen(c, carry):
        for t in range(CHUNK):
            place = pl.ds(pl.multiple_of((c * CHUNK + t) * L, L), L)
            tile = line[:, place]
            for a in range(3):
                wide_line[a, :, place] = jnp.broadcast_to(tile[a:a + 1], TILE)
        return carry

    lax.fori_loop(0, chunks, widen, 0)

    def own_step(q, energy):
        start = tuple(tuple(inner_ref[a, step_rows(q, g), :] for a in range(3)) for g in range(GROUPS))
        carry = pair_loop(own_cols, wide_line, q, 0, 1, True, (start, energy))
        force, energy = pair_loop(own_cols, wide_line, q, 1, chunks, False, carry)
        for g in range(GROUPS):
            for a in range(3):
                sums[a, step_rows(q, g), :] = force[g][a]
        return energy

    own_steps = (count + 8 * GROUPS - 1) // (8 * GROUPS)
    energy = lax.fori_loop(0, own_steps, own_step, tuple(inner_en_ref[k] for k in range(3)))
    en_ref[...] = jnp.sum(2.0 * energy[0] - 12.0 * energy[1] + 0.5 * (RC * UPC - UCUT) * energy[2], axis=0, keepdims=True)

    col = lax.broadcasted_iota(I32, (L, L), 1)
    picks = [jnp.where(col == a, 1.0, 0.0).astype(BF16) for a in range(3)]

    def add_up(base):
        total = jnp.zeros((2 * L, L), F32)
        for a in range(3):
            for part in split3(sums[a, base:base + 2 * L, :]):
                total = total + lax.dot_general(part, picks[a], NN, preferred_element_type=F32)
        added[:, base:base + 2 * L] = jnp.transpose(total)[0:8]

    for base in range(0, slots, 2 * L):
        pl.when(count > base)(functools.partial(add_up, base))
    force = jnp.where(good, 24.0 * added[0:3], 0.0)
    pos_ref[...] = srt_ref[0:3, 0:n]
    frc_ref[...] = force[:, 0:n]
    vel_ref[...] = (srt_ref[3:6] + (0.5 * DT) * force)[:, 0:n]
    id_ref[...] = jnp.reshape((srt_ref[6:7].astype(I32) * 65536 + srt_ref[7:8].astype(I32))[:, 0:n], (n,))
    ok_ref[...] = jnp.reshape(okrow[:, 0:n].astype(I32), (n,))


def total_kernel(sizes, part_ref, sum_ref, rows, ssem, rsem):
    me = [lax.axis_index(name) for name in "xyz"]
    size_x, size_y, size_z = sizes
    mine = (me[2] * size_y + me[1]) * size_x + me[0]
    others = [(dx, dy, dz) for dz in range(size_z) for dy in range(size_y) for dx in range(size_x) if dx + dy + dz > 0]
    others.sort(key=lambda o: -(2 * min(o[2], size_z - o[2]) + 2 * o[1] + min(o[0], size_x - o[0])))

    device_at = functools.partial(device_of, sizes, me)

    barrier = pltpu.get_barrier_semaphore()
    for offset in others:
        pl.semaphore_signal(barrier, inc=1, device_id=device_at(offset), device_id_type=pl.DeviceIdType.MESH)
    rows[pl.ds(mine, 1)] = part_ref[...]
    pl.semaphore_wait(barrier, len(others))
    copies = []
    for index, offset in enumerate(others):
        copy = pltpu.make_async_remote_copy(
            src_ref=part_ref, dst_ref=rows.at[pl.ds(mine, 1)], send_sem=ssem.at[index], recv_sem=rsem.at[index],
            device_id=device_at(offset), device_id_type=pl.DeviceIdType.MESH)
        copy.start()
        copies.append(copy)
    for copy in copies:
        copy.wait_recv()
    sum_ref[...] = jnp.sum(rows[...], axis=0, keepdims=True)
    for copy in copies:
        copy.wait_send()


def solution(mesh):
    sizes = (mesh.shape["x"], mesh.shape["y"], mesh.shape["z"])
    peers = sorted({offset_of(sizes, d) for d in DIRS} - {(0, 0, 0)})
    devices = sizes[0] * sizes[1] * sizes[2]

    def local_step(atom_pos, atom_vel, atom_frc, atom_id, atom_ok, brick_side):
        n = atom_pos.shape[0]
        slots = -(-n // L) * L
        side = jnp.reshape(brick_side, (1, 1))
        old_rows, new_rows = [3 * (width // L) + 1 for width in (slots, NEW)]
        vmem = pl.BlockSpec(memory_space=pltpu.VMEM)
        smem = pl.BlockSpec(memory_space=pltpu.SMEM)
        srt, ghosts, fresh, own, inner, inner_en = pl.pallas_call(
            functools.partial(exchange_kernel, sizes, peers, slots),
            out_shape=(jax.ShapeDtypeStruct((16, slots), F32), jax.ShapeDtypeStruct((len(peers), old_rows, L), F32), jax.ShapeDtypeStruct((len(peers), new_rows, L), F32),
                       jax.ShapeDtypeStruct((slots, 3 * L), F32), jax.ShapeDtypeStruct((3, slots, L), F32), jax.ShapeDtypeStruct((3,) + TILE, F32)),
            in_specs=[pl.BlockSpec(memory_space=pltpu.HBM)] * 5 + [smem],
            out_specs=(vmem,) * 6,
            scratch_shapes=[
                pltpu.VMEM((3, n), F32), pltpu.VMEM((3, n), F32), pltpu.VMEM((3, n), F32), pltpu.VMEM((n,), I32), pltpu.VMEM((n,), I32),
                pltpu.VMEM((32, L), F32), pltpu.VMEM((26, L), F32), pltpu.VMEM((3, old_rows, L), F32), pltpu.VMEM((3, new_rows, L), F32), pltpu.VMEM((3, 8, CHUNK * L), F32),
                pltpu.SemaphoreType.DMA((5,)), pltpu.SemaphoreType.DMA((26,)), pltpu.SemaphoreType.DMA((26,)),
            ] + [pltpu.SemaphoreType.DMA((len(peers),))] * 4,
            compiler_params=pltpu.CompilerParams(collective_id=0, has_side_effects=True, vmem_limit_bytes=40 * 2 ** 20),
            name="exchange",
        )(*[pltpu.with_memory_space_constraint(v, pltpu.HBM) for v in (atom_pos.T, atom_vel.T, atom_frc.T, atom_id, atom_ok)], side)
        offs = jnp.concatenate([ghosts[:, -1, 0:64], fresh[:, -1, 0:64]], axis=0).astype(I32)
        out_f = jax.ShapeDtypeStruct((3, n), F32)
        out_i = jax.ShapeDtypeStruct((n,), I32)
        new_pos, new_vel, new_frc, new_id, new_ok, energy = pl.pallas_call(
            functools.partial(force_kernel, sizes, peers, slots),
            out_shape=(out_f, out_f, out_f, out_i, out_i, jax.ShapeDtypeStruct((1, L), F32)),
            in_specs=[vmem] * 6 + [smem],
            out_specs=(vmem,) * 6,
            scratch_shapes=[pltpu.VMEM((8, 28 * slots + CHUNK * L), F32), pltpu.VMEM((3, 8, 28 * slots + CHUNK * L), F32), pltpu.VMEM((3, slots, L), F32), pltpu.VMEM((8, slots), F32)],
            compiler_params=pltpu.CompilerParams(vmem_limit_bytes=40 * 2 ** 20),
            name="forces",
        )(srt, ghosts, fresh, own, inner, inner_en, offs)
        energy = pl.pallas_call(
            functools.partial(total_kernel, sizes),
            out_shape=jax.ShapeDtypeStruct((1, L), F32),
            in_specs=[vmem],
            out_specs=vmem,
            scratch_shapes=[pltpu.VMEM((devices, L), F32), pltpu.SemaphoreType.DMA((devices,)), pltpu.SemaphoreType.DMA((devices,))],
            compiler_params=pltpu.CompilerParams(collective_id=1, has_side_effects=True, vmem_limit_bytes=4 * 2 ** 20),
            name="total",
        )(pltpu.with_memory_space_constraint(energy, pltpu.VMEM))
        return new_pos.T, new_vel.T, new_frc.T, new_id, new_ok, jnp.sum(energy)

    row_spec = P(MESH_AXES, None)
    id_spec = P(MESH_AXES)
    return jax.shard_map(local_step, mesh=mesh, in_specs=(row_spec, row_spec, row_spec, id_spec, id_spec, P()), out_specs=(row_spec, row_spec, row_spec, id_spec, id_spec, P()), check_vma=False)
```

```python
import functools

import jax
import jax.numpy as jnp
from jax import lax
from jax.experimental import pallas as pl
from jax.experimental.pallas import tpu as pltpu
from jax.sharding import PartitionSpec as P

DT = 0.005
RC = 2.5
FAR = 1.0e6
UCUT = 4.0 * (RC ** -12 - RC ** -6)
UPC = -48.0 * RC ** -13 + 24.0 * RC ** -7
MESH_AXES = ("z", "y", "x")
DIRS = [(dx, dy, dz) for dz in (-1, 0, 1) for dy in (-1, 0, 1) for dx in (-1, 0, 1) if (dx, dy, dz) != (0, 0, 0)]
NEAR = RC + 1.0e-3
MAJOR = ((2, 1, 0), (1, 0, 2), (0, 2, 1))
PACK = 8
NEW = 256
CHUNK = 4
GROUPS = 8
L = 128
TILE = (8, L)
F32 = jnp.float32
BF16 = jnp.bfloat16
I32 = jnp.int32
NT = (((1,), (1,)), ((), ()))
NN = (((1,), (0,)), ((), ()))


def device_of(sizes, me, offset):
    return tuple(lax.rem(me[axis] + offset[axis], sizes[axis]) for axis in (2, 1, 0))


def offset_of(sizes, d):
    return tuple(c % size for c, size in zip(d, sizes))


def far_first(d):
    return sum(c == 0 for c in d)


def order_of(d):
    if d[2] == 0:
        return 1 if d[1] != 0 else 2
    return 2 if (d[1] == 0 and d[0] != 0) else 0


def range_of(d):
    first, size = 0, 27
    for axis in MAJOR[order_of(d)]:
        if d[axis] == 0:
            break
        size = size // 3
        first = first + (1, 0, 2)[d[axis]] * size
    return first, first + size


def split3(x):
    hi = x.astype(BF16)
    rest = x - hi.astype(F32)
    mid = rest.astype(BF16)
    low = (rest - mid.astype(F32)).astype(BF16)
    return hi, mid, low


def onehot_rows(dest, base, count):
    rows = lax.broadcasted_iota(I32, (count, dest.shape[1]), 0) + base
    return jnp.where(rows == dest, 1.0, 0.0).astype(BF16)


def scatter_lanes(data, dest, slots):
    rows = data.shape[0]
    parts = jnp.concatenate(split3(data), axis=0)
    out = []
    for base in range(0, slots, 256):
        hot = onehot_rows(dest, base, min(256, slots - base))
        got = lax.dot_general(parts, hot, NT, preferred_element_type=F32)
        out.append(got[0:rows] + got[rows:2 * rows] + got[2 * rows:3 * rows])
    return jnp.concatenate(out, axis=1)


def class_places(code, with_before):
    width = code.shape[1]
    tiles = width // L
    cls = lax.broadcasted_iota(I32, (32, width), 0)
    member = jnp.where(cls == code, 1.0, 0.0)
    member_b = member.astype(BF16)
    stacked = jnp.concatenate([member_b[:, t * L:(t + 1) * L] for t in range(tiles)], axis=0)
    row_i = lax.broadcasted_iota(I32, (L, 256), 0)
    col_i = lax.broadcasted_iota(I32, (L, 256), 1)
    tri = jnp.where((row_i < col_i) | (col_i >= L), 1.0, 0.0).astype(BF16)
    pre = lax.dot_general(stacked, tri, NN, preferred_element_type=F32)
    carry = jnp.zeros((32, L), F32)
    if with_before:
        before_b = jnp.where(code < cls, 1.0, 0.0).astype(BF16)
        before_s = before_b[:, 0:L]
        tot = None
        ones = jnp.ones((L, L), BF16)
        for t in range(tiles):
            part = lax.dot_general(before_b[:, t * L:(t + 1) * L], ones, NN, preferred_element_type=F32)
            tot = part if tot is None else tot + part
        before = tot
        carry = before
    else:
        before = None
    places = []
    for t in range(tiles):
        within = pre[32 * t:32 * t + 32, 0:L] + carry
        places.append(jnp.sum(member[:, t * L:(t + 1) * L] * within, axis=0, keepdims=True))
        carry = carry + pre[32 * t:32 * t + 32, L:256]
    return jnp.concatenate(places, axis=1), before


def pad_lanes(x, width):
    return jnp.concatenate([x, jnp.zeros((x.shape[0], width - x.shape[1]), x.dtype)], axis=1)


def pair_loop(own_cols, near_lanes, q, first, last, with_self, carry):
    rows = [step_rows(q, g) for g in range(GROUPS)]
    own = [[own_cols[rows[g], a * L:(a + 1) * L] for a in range(3)] for g in range(GROUPS)]

    def body(c, carry):
        force, en = [list(f) for f in carry[0]], list(carry[1])
        for t in range(CHUNK):
            place = pl.ds(pl.multiple_of((c * CHUNK + t) * L, L), L)
            near_xyz = [near_lanes[a, :, place] for a in range(3)]
            for g in range(GROUPS):
                dx, dy, dz = [own[g][a] - near_xyz[a] for a in range(3)]
                d2 = dx * dx + dy * dy + dz * dz
                near = d2 < RC * RC
                if with_self:
                    near = near & (d2 > 0.0)
                inv = jnp.where(near, lax.rsqrt(d2), 0.0)
                s2 = inv * inv
                s6 = s2 * s2 * s2
                s12 = s6 * s6
                p = s12 - s6
                w = inv * (UPC / 24.0)
                scale = (p + s12) * s2 + w
                en = [en[0] + p, en[1] + w * d2, en[2] + jnp.where(near, 1.0, 0.0)]
                force[g] = [force[g][0] + scale * dx, force[g][1] + scale * dy, force[g][2] + scale * dz]
        return tuple(tuple(f) for f in force), tuple(en)

    return lax.fori_loop(first, last, body, carry)


def step_rows(q, g):
    return pl.ds(pl.multiple_of((q * GROUPS + g) * 8, 8), 8)


def own_columns(xyz):
    slots = xyz.shape[1]
    parts = [part.astype(F32) for part in split3(xyz)]
    parts = jnp.concatenate(parts + [jnp.zeros((7, slots), F32)], axis=0)
    row = lax.broadcasted_iota(I32, (16, 3 * L), 0)
    tile = lax.broadcasted_iota(I32, (16, 3 * L), 1) // L
    picks = jnp.where((row == tile) | (row == tile + 3) | (row == tile + 6), 1.0, 0.0).astype(BF16)
    return lax.dot_general(jnp.transpose(parts).astype(BF16), picks, NN, preferred_element_type=F32)


def exchange_kernel(sizes, peers, slots, pos_hbm, vel_hbm, frc_hbm, id_hbm, ok_hbm, side_ref, srt_ref, gh_ref, ga_ref, own_ref, inner_ref, inner_en_ref, pos_ref, vel_ref, frc_ref, id_ref, ok_ref, pkt, rcv, out3, new3, lanes, isem, psend, precv, gsend, grecv, asend, arecv):
    me = [lax.axis_index(name) for name in "xyz"]

    device_at = functools.partial(device_of, sizes, me)

    loads = []
    for index, (src, dst) in enumerate(((ok_hbm, ok_ref), (id_hbm, id_ref), (pos_hbm, pos_ref), (vel_hbm, vel_ref), (frc_hbm, frc_ref))):
        load = pltpu.make_async_copy(src, dst, isem.at[index])
        load.start()
        loads.append(load)
    barrier = pltpu.get_barrier_semaphore()
    for offset in sorted(peers, key=far_first):
        pl.semaphore_signal(barrier, inc=1, device_id=device_at(offset), device_id_type=pl.DeviceIdType.MESH)

    n = pos_ref.shape[1]
    for load in loads:
        load.wait()
    side = side_ref[0, 0]
    owned = pad_lanes(jnp.reshape(ok_ref[...], (1, n)), slots) > 0
    half = vel_ref[...] + (0.5 * DT) * frc_ref[...]
    free = pos_ref[...] + DT * half
    half = pad_lanes(half, slots)
    free = pad_lanes(free, slots)
    ids = pad_lanes(jnp.reshape(id_ref[...], (1, n)), slots)
    code = jnp.zeros((1, slots), I32)
    moved = []
    low_side = []
    for axis in range(3):
        low = me[axis].astype(F32) * side
        high = (me[axis] + 1).astype(F32) * side
        box = side * float(sizes[axis])
        u = free[axis:axis + 1]
        step = jnp.where(u >= high, 1, 0) - jnp.where(u < low, 1, 0)
        code = code + (step + 1) * (1, 3, 9)[axis]
        moved.append(jnp.where(u < 0.0, u + box, jnp.where(u >= box, u - box, u)))
        low_side.append(low)
    code = jnp.where(owned, code, 31)
    id_hi = (ids >> 16).astype(F32)
    id_lo = (ids & 65535).astype(F32)
    okf = jnp.where(owned, 1.0, 0.0)
    data = jnp.concatenate(moved + [half, id_hi, id_lo, okf, jnp.zeros((7, slots), F32)], axis=0)

    place, _ = class_places(code, False)
    leaving = owned & (code != 13)
    way = jnp.where(leaving, code - jnp.where(code > 13, 1, 0), 31)
    member = jnp.where(lax.broadcasted_iota(I32, (32, slots), 0) == way, 1.0, 0.0).astype(BF16)
    fields = jnp.concatenate([jnp.where(place == float(k), data, 0.0) for k in range(PACK)], axis=0)
    packed = jnp.zeros((32, L), F32)
    for part in split3(fields):
        packed = packed + lax.dot_general(member, part, NT, preferred_element_type=F32)
    pkt[...] = packed

    def bins_of(pos):
        bins = []
        for axis in range(3):
            loc = pos[axis:axis + 1] - low_side[axis]
            bins.append(jnp.where(loc < NEAR, 0, jnp.where(loc > side - NEAR, 2, 1)))
        return [(bins[i] * 3 + bins[j]) * 3 + bins[k] for i, j, k in MAJOR]

    wide = side > 2.0 * NEAR
    eye = lax.broadcasted_iota(I32, (32, L), 0) == lax.broadcasted_iota(I32, (32, L), 1)

    def sorted_block(cand, keys, kept):
        width = cand.shape[1]
        where_to, before = class_places(jnp.where(kept, keys, 28), True)
        arranged = scatter_lanes(cand, jnp.where(kept, where_to.astype(I32), -1), width)
        total = jnp.concatenate([before[27:28]] * (width // L), axis=1)
        lane = lax.broadcasted_iota(I32, (1, width), 1).astype(F32)
        begins = jnp.sum(jnp.where(eye, before, 0.0), axis=0, keepdims=True)
        ends = jnp.where(wide, begins, before[27:28])
        counts = jnp.concatenate([jnp.where(wide, begins, 0.0)[:, 0:32], ends[:, 0:32], jnp.zeros((1, L - 64), F32)], axis=1)
        return jnp.where(lane < total, arranged[0:3], FAR), counts

    def send(src, dst, ssem, rsem, offset):
        copy = pltpu.make_async_remote_copy(
            src_ref=src, dst_ref=dst, send_sem=ssem, recv_sem=rsem,
            device_id=device_at(offset), device_id_type=pl.DeviceIdType.MESH)
        copy.start()
        return copy

    def store_block(ref, kind, xyz, counts):
        tiles = xyz.shape[1] // L
        for a in range(3):
            for t in range(tiles):
                ref[kind, pl.ds(a * tiles + t, 1)] = xyz[a:a + 1, t * L:(t + 1) * L]
        ref[kind, pl.ds(3 * tiles, 1)] = counts

    def send_blocks(block, dst, ssem, rsem, kind):
        out = []
        for offset in sorted(peers, key=far_first):
            index = peers.index(offset)
            if order_of(tuple(0 if c == 0 else 1 for c in offset)) == kind:
                out.append(send(block.at[kind], dst.at[index], ssem.at[index], rsem.at[index], offset))
        return out

    staying = code == 13
    keys = bins_of(data)
    for kind in range(3):
        store_block(out3, kind, *sorted_block(data[0:8], keys[kind], staying))
    pl.semaphore_wait(barrier, len(peers))
    packets = []
    for d in sorted(DIRS, key=far_first):
        index = DIRS.index(d)
        row = pl.ds(index, 1)
        packets.append(send(pkt.at[row], rcv.at[row], psend.at[index], precv.at[index], offset_of(sizes, d)))
    blocks = []
    for kind in range(3):
        blocks = blocks + send_blocks(out3, gh_ref, gsend, grecv, kind)
    for copy in packets:
        copy.wait_recv()

    came = jnp.concatenate([rcv[...], jnp.zeros((32 - 26, L), F32)], axis=0)
    came = jnp.concatenate([came] + [pltpu.roll(came, L - 16 * k, 1) for k in range(1, PACK)], axis=0)
    came_t = jnp.transpose(came)[0:16]
    came_ok = came_t[8:9] > 0.5
    keys = bins_of(came_t)
    late = []
    for kind in range(3):
        store_block(new3, kind, *sorted_block(came_t[0:8], keys[kind], came_ok))
        late = late + send_blocks(new3, ga_ref, asend, arecv, kind)
    for copy in packets:
        copy.wait_send()

    arr_ids = came[:, 6:7].astype(I32) * 65536 + came[:, 7:8].astype(I32)
    arr_ok = came[:, 8:9] > 0.5
    row_ids = jnp.concatenate([ids, came_t[6:7].astype(I32) * 65536 + came_t[7:8].astype(I32)], axis=1)
    less = jnp.where((arr_ids < row_ids) & arr_ok, 1.0, 0.0)
    arrivals_below = jnp.sum(less, axis=0, keepdims=True)
    above = jnp.where((arr_ids > row_ids[:, 0:slots]) & staying, 1.0, 0.0).astype(BF16)
    stay_below = lax.dot_general(jnp.ones((16, slots), BF16), above, NT, preferred_element_type=F32)[0:1]
    stay_place, _ = class_places(jnp.where(staying, 0, 31), False)
    rank = jnp.concatenate([stay_place, stay_below], axis=1) + arrivals_below
    dest = jnp.where(jnp.concatenate([staying, came_ok], axis=1), rank.astype(I32), -1)
    merged = scatter_lanes(jnp.concatenate([data, came_t], axis=1), dest, slots)
    srt_ref[...] = jnp.where(lax.broadcasted_iota(I32, (16, slots), 0) == 9, side, merged)

    good = merged[8:9] > 0.5
    own_ref[...] = own_columns(jnp.where(good, merged[0:3], -FAR))
    first = CHUNK * L
    for a in range(3):
        lanes[a] = jnp.broadcast_to(jnp.where(good, merged[a:a + 1], FAR)[:, 0:first], (8, first))
    zero = jnp.zeros(TILE, F32)

    def own_step(q, energy):
        force, energy = pair_loop(own_ref, lanes, q, 0, 1, True, (((zero,) * 3,) * GROUPS, energy))
        for g in range(GROUPS):
            for a in range(3):
                inner_ref[a, step_rows(q, g), :] = force[g][a]
        return energy

    for k, part in enumerate(lax.fori_loop(0, slots // (8 * GROUPS), own_step, (zero,) * 3)):
        inner_en_ref[k] = part

    for copy in blocks + late:
        copy.wait()


def force_kernel(sizes, peers, slots, srt_ref, gh_ref, ga_ref, own_cols, inner_ref, inner_en_ref, offs_ref, pos_ref, vel_ref, frc_ref, id_ref, ok_ref, en_ref, line, wide_line, sums, added):
    me = [lax.axis_index(name) for name in "xyz"]
    n = pos_ref.shape[1]
    side = srt_ref[9:10, 0:1]
    okrow = srt_ref[8:9]
    good = okrow > 0.5
    count = jnp.sum(okrow).astype(I32)
    span = slots + L

    away = jnp.full(TILE, FAR, F32)
    first = CHUNK * L
    line[:, 0:slots - first] = jnp.concatenate([jnp.where(good, srt_ref[0:3], FAR), jnp.full((5, slots), FAR, F32)], axis=0)[:, first:]
    lane = lax.broadcasted_iota(I32, (8, span), 1)
    fill = jnp.maximum(count - first, 0)
    for d in DIRS:
        index = peers.index(offset_of(sizes, [-c for c in d]))
        low, high = range_of(d)
        shifts = []
        for axis in range(3):
            box = side * float(sizes[axis])
            if d[axis] == 1:
                shifts.append(jnp.where(me[axis] == sizes[axis] - 1, box, 0.0))
            elif d[axis] == -1:
                shifts.append(jnp.where(me[axis] == 0, -box, 0.0))
            else:
                shifts.append(jnp.zeros((1, 1), F32))
        shift = jnp.concatenate(shifts, axis=0)
        for source, entry in ((gh_ref, index), (ga_ref, index + len(peers))):
            tiles = source.shape[1] // 3
            width = tiles * L
            begin = offs_ref[entry, low]
            end = offs_ref[entry, 32 + high]
            block = jnp.concatenate([source[index, pl.ds(t, 3, stride=tiles), :] for t in range(tiles)], axis=1) + shift
            block = jnp.concatenate([block, jnp.zeros((5, width), F32)], axis=0)
            block = jnp.concatenate([block, away], axis=1)
            head = fill & (L - 1)
            base = pl.multiple_of(fill - head, L)
            move = head - begin
            block = pltpu.roll(block, jnp.where(move < 0, move + (width + L), move), 1)
            block = jnp.where(lane[:, 0:width + L] < head + end - begin, block, FAR)
            line[:, pl.ds(base, L)] = jnp.where(lane[:, 0:L] < head, line[:, pl.ds(base, L)], block[:, 0:L])
            line[:, pl.ds(pl.multiple_of(base + L, L), width)] = block[:, L:]
            fill = fill + (end - begin)
    rest = pl.multiple_of(((fill + L - 1) // L) * L, L)
    line[:, pl.ds(rest, CHUNK * L)] = jnp.full((8, CHUNK * L), FAR, F32)
    chunks = jnp.maximum((fill + CHUNK * L - 1) // (CHUNK * L), 1)

    def widen(c, carry):
        for t in range(CHUNK):
            place = pl.ds(pl.multiple_of((c * CHUNK + t) * L, L), L)
            tile = line[:, place]
            for a in range(3):
                wide_line[a, :, place] = jnp.broadcast_to(tile[a:a + 1], TILE)
        return carry

    lax.fori_loop(0, chunks, widen, 0)

    def own_step(q, energy):
        start = tuple(tuple(inner_ref[a, step_rows(q, g), :] for a in range(3)) for g in range(GROUPS))
        carry = pair_loop(own_cols, wide_line, q, 0, own_chunks, True, (start, energy))
        force, energy = pair_loop(own_cols, wide_line, q, own_chunks, chunks, False, carry)
        for g in range(GROUPS):
            for a in range(3):
                sums[a, step_rows(q, g), :] = force[g][a]
        return energy

    own_chunks = jnp.where(count > first, 1, 0)
    own_steps = (count + 8 * GROUPS - 1) // (8 * GROUPS)
    energy = lax.fori_loop(0, own_steps, own_step, tuple(inner_en_ref[k] for k in range(3)))
    en_ref[...] = jnp.sum(2.0 * energy[0] - 12.0 * energy[1] + 0.5 * (RC * UPC - UCUT) * energy[2], axis=0, keepdims=True)

    col = lax.broadcasted_iota(I32, (L, L), 1)
    picks = [jnp.where(col == a, 1.0, 0.0).astype(BF16) for a in range(3)]

    def add_up(base):
        total = jnp.zeros((2 * L, L), F32)
        for a in range(3):
            for part in split3(sums[a, base:base + 2 * L, :]):
                total = total + lax.dot_general(part, picks[a], NN, preferred_element_type=F32)
        added[:, base:base + 2 * L] = jnp.transpose(total)[0:8]

    for base in range(0, slots, 2 * L):
        pl.when(count > base)(functools.partial(add_up, base))
    force = jnp.where(good, 24.0 * added[0:3], 0.0)
    pos_ref[...] = srt_ref[0:3, 0:n]
    frc_ref[...] = force[:, 0:n]
    vel_ref[...] = (srt_ref[3:6] + (0.5 * DT) * force)[:, 0:n]
    id_ref[...] = jnp.reshape((srt_ref[6:7].astype(I32) * 65536 + srt_ref[7:8].astype(I32))[:, 0:n], (n,))
    ok_ref[...] = jnp.reshape(okrow[:, 0:n].astype(I32), (n,))


def total_kernel(sizes, part_ref, sum_ref, rows, ssem, rsem):
    me = [lax.axis_index(name) for name in "xyz"]
    size_x, size_y, size_z = sizes
    mine = (me[2] * size_y + me[1]) * size_x + me[0]
    others = [(dx, dy, dz) for dz in range(size_z) for dy in range(size_y) for dx in range(size_x) if dx + dy + dz > 0]
    others.sort(key=lambda o: -(2 * min(o[2], size_z - o[2]) + 2 * o[1] + min(o[0], size_x - o[0])))

    device_at = functools.partial(device_of, sizes, me)

    barrier = pltpu.get_barrier_semaphore()
    for offset in others:
        pl.semaphore_signal(barrier, inc=1, device_id=device_at(offset), device_id_type=pl.DeviceIdType.MESH)
    rows[pl.ds(mine, 1)] = part_ref[...]
    pl.semaphore_wait(barrier, len(others))
    copies = []
    for index, offset in enumerate(others):
        copy = pltpu.make_async_remote_copy(
            src_ref=part_ref, dst_ref=rows.at[pl.ds(mine, 1)], send_sem=ssem.at[index], recv_sem=rsem.at[index],
            device_id=device_at(offset), device_id_type=pl.DeviceIdType.MESH)
        copy.start()
        copies.append(copy)
    for copy in copies:
        copy.wait_recv()
    sum_ref[...] = jnp.sum(rows[...], axis=0, keepdims=True)
    for copy in copies:
        copy.wait_send()


def solution(mesh):
    sizes = (mesh.shape["x"], mesh.shape["y"], mesh.shape["z"])
    peers = sorted({offset_of(sizes, d) for d in DIRS} - {(0, 0, 0)})
    devices = sizes[0] * sizes[1] * sizes[2]

    def local_step(atom_pos, atom_vel, atom_frc, atom_id, atom_ok, brick_side):
        n = atom_pos.shape[0]
        slots = -(-n // L) * L
        side = jnp.reshape(brick_side, (1, 1))
        old_rows, new_rows = [3 * (width // L) + 1 for width in (slots, NEW)]
        vmem = pl.BlockSpec(memory_space=pltpu.VMEM)
        smem = pl.BlockSpec(memory_space=pltpu.SMEM)
        srt, ghosts, fresh, own, inner, inner_en = pl.pallas_call(
            functools.partial(exchange_kernel, sizes, peers, slots),
            out_shape=(jax.ShapeDtypeStruct((16, slots), F32), jax.ShapeDtypeStruct((len(peers), old_rows, L), F32), jax.ShapeDtypeStruct((len(peers), new_rows, L), F32),
                       jax.ShapeDtypeStruct((slots, 3 * L), F32), jax.ShapeDtypeStruct((3, slots, L), F32), jax.ShapeDtypeStruct((3,) + TILE, F32)),
            in_specs=[pl.BlockSpec(memory_space=pltpu.HBM)] * 5 + [smem],
            out_specs=(vmem,) * 6,
            scratch_shapes=[
                pltpu.VMEM((3, n), F32), pltpu.VMEM((3, n), F32), pltpu.VMEM((3, n), F32), pltpu.VMEM((n,), I32), pltpu.VMEM((n,), I32),
                pltpu.VMEM((32, L), F32), pltpu.VMEM((26, L), F32), pltpu.VMEM((3, old_rows, L), F32), pltpu.VMEM((3, new_rows, L), F32), pltpu.VMEM((3, 8, CHUNK * L), F32),
                pltpu.SemaphoreType.DMA((5,)), pltpu.SemaphoreType.DMA((26,)), pltpu.SemaphoreType.DMA((26,)),
            ] + [pltpu.SemaphoreType.DMA((len(peers),))] * 4,
            compiler_params=pltpu.CompilerParams(collective_id=0, has_side_effects=True, vmem_limit_bytes=40 * 2 ** 20),
            name="exchange",
        )(*[pltpu.with_memory_space_constraint(v, pltpu.HBM) for v in (atom_pos.T, atom_vel.T, atom_frc.T, atom_id, atom_ok)], side)
        offs = jnp.concatenate([ghosts[:, -1, 0:64], fresh[:, -1, 0:64]], axis=0).astype(I32)
        out_f = jax.ShapeDtypeStruct((3, n), F32)
        out_i = jax.ShapeDtypeStruct((n,), I32)
        new_pos, new_vel, new_frc, new_id, new_ok, energy = pl.pallas_call(
            functools.partial(force_kernel, sizes, peers, slots),
            out_shape=(out_f, out_f, out_f, out_i, out_i, jax.ShapeDtypeStruct((1, L), F32)),
            in_specs=[vmem] * 6 + [smem],
            out_specs=(vmem,) * 6,
            scratch_shapes=[pltpu.VMEM((8, 28 * slots + CHUNK * L), F32), pltpu.VMEM((3, 8, 28 * slots + CHUNK * L), F32), pltpu.VMEM((3, slots, L), F32), pltpu.VMEM((8, slots), F32)],
            compiler_params=pltpu.CompilerParams(vmem_limit_bytes=40 * 2 ** 20),
            name="forces",
        )(srt, ghosts, fresh, own, inner, inner_en, offs)
        energy = pl.pallas_call(
            functools.partial(total_kernel, sizes),
            out_shape=jax.ShapeDtypeStruct((1, L), F32),
            in_specs=[vmem],
            out_specs=vmem,
            scratch_shapes=[pltpu.VMEM((devices, L), F32), pltpu.SemaphoreType.DMA((devices,)), pltpu.SemaphoreType.DMA((devices,))],
            compiler_params=pltpu.CompilerParams(collective_id=1, has_side_effects=True, vmem_limit_bytes=4 * 2 ** 20),
            name="total",
        )(pltpu.with_memory_space_constraint(energy, pltpu.VMEM))
        return new_pos.T, new_vel.T, new_frc.T, new_id, new_ok, jnp.sum(energy)

    row_spec = P(MESH_AXES, None)
    id_spec = P(MESH_AXES)
    return jax.shard_map(local_step, mesh=mesh, in_specs=(row_spec, row_spec, row_spec, id_spec, id_spec, P()), out_specs=(row_spec, row_spec, row_spec, id_spec, id_spec, P()), check_vma=False)
```

```python
import functools

import jax
import jax.numpy as jnp
from jax import lax
from jax.experimental import pallas as pl
from jax.experimental.pallas import tpu as pltpu
from jax.sharding import PartitionSpec as P

DT = 0.005
RC = 2.5
FAR = 1.0e6
UCUT = 4.0 * (RC ** -12 - RC ** -6)
UPC = -48.0 * RC ** -13 + 24.0 * RC ** -7
MESH_AXES = ("z", "y", "x")
DIRS = [(dx, dy, dz) for dz in (-1, 0, 1) for dy in (-1, 0, 1) for dx in (-1, 0, 1) if (dx, dy, dz) != (0, 0, 0)]
NEAR = RC + 1.0e-3
MAJOR = ((2, 1, 0), (1, 0, 2), (0, 2, 1))
PACK = 8
NEW = 256
CHUNK = 4
GROUPS = 8
L = 128
TILE = (8, L)
F32 = jnp.float32
BF16 = jnp.bfloat16
I32 = jnp.int32
NT = (((1,), (1,)), ((), ()))
NN = (((1,), (0,)), ((), ()))


def device_of(sizes, me, offset):
    return tuple(lax.rem(me[axis] + offset[axis], sizes[axis]) for axis in (2, 1, 0))


def offset_of(sizes, d):
    return tuple(c % size for c, size in zip(d, sizes))


def far_first(d):
    return sum(c == 0 for c in d)


def order_of(d):
    if d[2] == 0:
        return 1 if d[1] != 0 else 2
    return 2 if (d[1] == 0 and d[0] != 0) else 0


def range_of(d):
    first, size = 0, 27
    for axis in MAJOR[order_of(d)]:
        if d[axis] == 0:
            break
        size = size // 3
        first = first + (1, 0, 2)[d[axis]] * size
    return first, first + size


def split3(x):
    hi = x.astype(BF16)
    rest = x - hi.astype(F32)
    mid = rest.astype(BF16)
    low = (rest - mid.astype(F32)).astype(BF16)
    return hi, mid, low


def onehot_rows(dest, base, count):
    rows = lax.broadcasted_iota(I32, (count, dest.shape[1]), 0) + base
    return jnp.where(rows == dest, 1.0, 0.0).astype(BF16)


def scatter_lanes(data, dest, slots):
    rows = data.shape[0]
    parts = jnp.concatenate(split3(data), axis=0)
    out = []
    for base in range(0, slots, 256):
        hot = onehot_rows(dest, base, min(256, slots - base))
        got = lax.dot_general(parts, hot, NT, preferred_element_type=F32)
        out.append(got[0:rows] + got[rows:2 * rows] + got[2 * rows:3 * rows])
    return jnp.concatenate(out, axis=1)


def class_places(code, with_before):
    width = code.shape[1]
    tiles = width // L
    cls = lax.broadcasted_iota(I32, (32, width), 0)
    member = jnp.where(cls == code, 1.0, 0.0)
    member_b = member.astype(BF16)
    stacked = jnp.concatenate([member_b[:, t * L:(t + 1) * L] for t in range(tiles)], axis=0)
    row_i = lax.broadcasted_iota(I32, (L, 256), 0)
    col_i = lax.broadcasted_iota(I32, (L, 256), 1)
    tri = jnp.where((row_i < col_i) | (col_i >= L), 1.0, 0.0).astype(BF16)
    pre = lax.dot_general(stacked, tri, NN, preferred_element_type=F32)
    carry = jnp.zeros((32, L), F32)
    if with_before:
        before_b = jnp.where(code < cls, 1.0, 0.0).astype(BF16)
        before_s = before_b[:, 0:L]
        tot = None
        ones = jnp.ones((L, L), BF16)
        for t in range(tiles):
            part = lax.dot_general(before_b[:, t * L:(t + 1) * L], ones, NN, preferred_element_type=F32)
            tot = part if tot is None else tot + part
        before = tot
        carry = before
    else:
        before = None
    places = []
    for t in range(tiles):
        within = pre[32 * t:32 * t + 32, 0:L] + carry
        places.append(jnp.sum(member[:, t * L:(t + 1) * L] * within, axis=0, keepdims=True))
        carry = carry + pre[32 * t:32 * t + 32, L:256]
    return jnp.concatenate(places, axis=1), before


def pad_lanes(x, width):
    return jnp.concatenate([x, jnp.zeros((x.shape[0], width - x.shape[1]), x.dtype)], axis=1)


def pair_loop(own_cols, near_lanes, q, first, last, with_self, carry):
    rows = [step_rows(q, g) for g in range(GROUPS)]
    own = [[own_cols[rows[g], a * L:(a + 1) * L] for a in range(3)] for g in range(GROUPS)]

    def body(c, carry):
        force, en = [list(f) for f in carry[0]], list(carry[1])
        for t in range(CHUNK):
            place = pl.ds(pl.multiple_of((c * CHUNK + t) * L, L), L)
            near_xyz = [near_lanes[a, :, place] for a in range(3)]
            for g in range(GROUPS):
                dx, dy, dz = [own[g][a] - near_xyz[a] for a in range(3)]
                d2 = dx * dx + dy * dy + dz * dz
                near = d2 < RC * RC
                if with_self:
                    near = near & (d2 > 0.0)
                inv = jnp.where(near, lax.rsqrt(d2), 0.0)
                s2 = inv * inv
                s6 = s2 * s2 * s2
                s12 = s6 * s6
                p = s12 - s6
                w = inv * (UPC / 24.0)
                scale = (p + s12) * s2 + w
                en = [en[0] + p, en[1] + w * d2, en[2] + jnp.where(near, 1.0, 0.0)]
                force[g] = [force[g][0] + scale * dx, force[g][1] + scale * dy, force[g][2] + scale * dz]
        return tuple(tuple(f) for f in force), tuple(en)

    return lax.fori_loop(first, last, body, carry)


def step_rows(q, g):
    return pl.ds(pl.multiple_of((q * GROUPS + g) * 8, 8), 8)


def own_columns(xyz):
    slots = xyz.shape[1]
    parts = [part.astype(F32) for part in split3(xyz)]
    parts = jnp.concatenate(parts + [jnp.zeros((7, slots), F32)], axis=0)
    row = lax.broadcasted_iota(I32, (16, 3 * L), 0)
    tile = lax.broadcasted_iota(I32, (16, 3 * L), 1) // L
    picks = jnp.where((row == tile) | (row == tile + 3) | (row == tile + 6), 1.0, 0.0).astype(BF16)
    return lax.dot_general(jnp.transpose(parts).astype(BF16), picks, NN, preferred_element_type=F32)


def exchange_kernel(sizes, peers, slots, pos_hbm, vel_hbm, frc_hbm, id_hbm, ok_hbm, side_ref, srt_ref, gh_ref, ga_ref, own_ref, inner_ref, inner_en_ref, pos_ref, vel_ref, frc_ref, id_ref, ok_ref, pkt, rcv, out3, new3, lanes, isem, psend, precv, gsend, grecv, asend, arecv):
    me = [lax.axis_index(name) for name in "xyz"]

    device_at = functools.partial(device_of, sizes, me)

    loads = []
    for index, (src, dst) in enumerate(((ok_hbm, ok_ref), (id_hbm, id_ref), (pos_hbm, pos_ref), (vel_hbm, vel_ref), (frc_hbm, frc_ref))):
        load = pltpu.make_async_copy(src, dst, isem.at[index])
        load.start()
        loads.append(load)
    barrier = pltpu.get_barrier_semaphore()
    for offset in sorted(peers, key=far_first):
        pl.semaphore_signal(barrier, inc=1, device_id=device_at(offset), device_id_type=pl.DeviceIdType.MESH)

    n = pos_ref.shape[1]
    for load in loads:
        load.wait()
    side = side_ref[0, 0]
    owned = pad_lanes(jnp.reshape(ok_ref[...], (1, n)), slots) > 0
    half = vel_ref[...] + (0.5 * DT) * frc_ref[...]
    free = pos_ref[...] + DT * half
    half = pad_lanes(half, slots)
    free = pad_lanes(free, slots)
    ids = pad_lanes(jnp.reshape(id_ref[...], (1, n)), slots)
    code = jnp.zeros((1, slots), I32)
    moved = []
    low_side = []
    for axis in range(3):
        low = me[axis].astype(F32) * side
        high = (me[axis] + 1).astype(F32) * side
        box = side * float(sizes[axis])
        u = free[axis:axis + 1]
        step = jnp.where(u >= high, 1, 0) - jnp.where(u < low, 1, 0)
        code = code + (step + 1) * (1, 3, 9)[axis]
        moved.append(jnp.where(u < 0.0, u + box, jnp.where(u >= box, u - box, u)))
        low_side.append(low)
    code = jnp.where(owned, code, 31)
    id_hi = (ids >> 16).astype(F32)
    id_lo = (ids & 65535).astype(F32)
    okf = jnp.where(owned, 1.0, 0.0)
    data = jnp.concatenate(moved + [half, id_hi, id_lo, okf, jnp.zeros((7, slots), F32)], axis=0)

    place, _ = class_places(code, False)
    leaving = owned & (code != 13)
    way = jnp.where(leaving, code - jnp.where(code > 13, 1, 0), 31)
    member = jnp.where(lax.broadcasted_iota(I32, (32, slots), 0) == way, 1.0, 0.0).astype(BF16)
    fields = jnp.concatenate([jnp.where(place == float(k), data, 0.0) for k in range(PACK)], axis=0)
    packed = jnp.zeros((32, L), F32)
    for part in split3(fields):
        packed = packed + lax.dot_general(member, part, NT, preferred_element_type=F32)
    pkt[...] = packed

    def bins_of(pos):
        bins = []
        for axis in range(3):
            loc = pos[axis:axis + 1] - low_side[axis]
            bins.append(jnp.where(loc < NEAR, 0, jnp.where(loc > side - NEAR, 2, 1)))
        return [(bins[i] * 3 + bins[j]) * 3 + bins[k] for i, j, k in MAJOR]

    wide = side > 2.0 * NEAR
    eye = lax.broadcasted_iota(I32, (32, L), 0) == lax.broadcasted_iota(I32, (32, L), 1)

    def sorted_block(cand, keys, kept):
        width = cand.shape[1]
        where_to, before = class_places(jnp.where(kept, keys, 28), True)
        arranged = scatter_lanes(cand, jnp.where(kept, where_to.astype(I32), -1), width)
        total = jnp.concatenate([before[27:28]] * (width // L), axis=1)
        lane = lax.broadcasted_iota(I32, (1, width), 1).astype(F32)
        begins = jnp.sum(jnp.where(eye, before, 0.0), axis=0, keepdims=True)
        ends = jnp.where(wide, begins, before[27:28])
        counts = jnp.concatenate([jnp.where(wide, begins, 0.0)[:, 0:32], ends[:, 0:32], jnp.zeros((1, L - 64), F32)], axis=1)
        return jnp.where(lane < total, arranged[0:3], FAR), counts

    def send(src, dst, ssem, rsem, offset):
        copy = pltpu.make_async_remote_copy(
            src_ref=src, dst_ref=dst, send_sem=ssem, recv_sem=rsem,
            device_id=device_at(offset), device_id_type=pl.DeviceIdType.MESH)
        copy.start()
        return copy

    def store_block(ref, kind, xyz, counts):
        tiles = xyz.shape[1] // L
        for a in range(3):
            for t in range(tiles):
                ref[kind, pl.ds(a * tiles + t, 1)] = xyz[a:a + 1, t * L:(t + 1) * L]
        ref[kind, pl.ds(3 * tiles, 1)] = counts

    def send_blocks(block, dst, ssem, rsem, kind):
        out = []
        for offset in sorted(peers, key=far_first):
            index = peers.index(offset)
            if order_of(tuple(0 if c == 0 else 1 for c in offset)) == kind:
                out.append(send(block.at[kind], dst.at[index], ssem.at[index], rsem.at[index], offset))
        return out

    staying = code == 13
    keys = bins_of(data)
    for kind in range(3):
        store_block(out3, kind, *sorted_block(data[0:8], keys[kind], staying))
    pl.semaphore_wait(barrier, len(peers))
    packets = []
    for d in sorted(DIRS, key=far_first):
        index = DIRS.index(d)
        row = pl.ds(index, 1)
        packets.append(send(pkt.at[row], rcv.at[row], psend.at[index], precv.at[index], offset_of(sizes, d)))
    blocks = []
    for kind in range(3):
        blocks = blocks + send_blocks(out3, gh_ref, gsend, grecv, kind)
    for copy in packets:
        copy.wait_recv()

    came = jnp.concatenate([rcv[...], jnp.zeros((32 - 26, L), F32)], axis=0)
    came = jnp.concatenate([came] + [pltpu.roll(came, L - 16 * k, 1) for k in range(1, PACK)], axis=0)
    came_t = jnp.transpose(came)[0:16]
    came_ok = came_t[8:9] > 0.5
    keys = bins_of(came_t)
    late = []
    for kind in range(3):
        store_block(new3, kind, *sorted_block(came_t[0:8], keys[kind], came_ok))
        late = late + send_blocks(new3, ga_ref, asend, arecv, kind)
    for copy in packets:
        copy.wait_send()

    arr_ids = came[:, 6:7].astype(I32) * 65536 + came[:, 7:8].astype(I32)
    arr_ok = came[:, 8:9] > 0.5
    row_ids = jnp.concatenate([ids, came_t[6:7].astype(I32) * 65536 + came_t[7:8].astype(I32)], axis=1)
    less = jnp.where((arr_ids < row_ids) & arr_ok, 1.0, 0.0)
    arrivals_below = jnp.sum(less, axis=0, keepdims=True)
    above = jnp.where((arr_ids > row_ids[:, 0:slots]) & staying, 1.0, 0.0).astype(BF16)
    stay_below = lax.dot_general(jnp.ones((16, slots), BF16), above, NT, preferred_element_type=F32)[0:1]
    stay_place, _ = class_places(jnp.where(staying, 0, 31), False)
    rank = jnp.concatenate([stay_place, stay_below], axis=1) + arrivals_below
    dest = jnp.where(jnp.concatenate([staying, came_ok], axis=1), rank.astype(I32), -1)
    merged = scatter_lanes(jnp.concatenate([data, came_t], axis=1), dest, slots)
    srt_ref[...] = jnp.where(lax.broadcasted_iota(I32, (16, slots), 0) == 9, side, merged)

    good = merged[8:9] > 0.5
    own_ref[...] = own_columns(jnp.where(good, merged[0:3], -FAR))
    first = CHUNK * L
    for a in range(3):
        lanes[a] = jnp.broadcast_to(jnp.where(good, merged[a:a + 1], FAR)[:, 0:first], (8, first))
    zero = jnp.zeros(TILE, F32)

    def own_step(q, energy):
        force, energy = pair_loop(own_ref, lanes, q, 0, 1, True, (((zero,) * 3,) * GROUPS, energy))
        for g in range(GROUPS):
            for a in range(3):
                inner_ref[a, step_rows(q, g), :] = force[g][a]
        return energy

    for k, part in enumerate(lax.fori_loop(0, slots // (8 * GROUPS), own_step, (zero,) * 3)):
        inner_en_ref[k] = part

    for copy in blocks + late:
        copy.wait()


def force_kernel(sizes, peers, slots, srt_ref, gh_ref, ga_ref, own_cols, inner_ref, inner_en_ref, offs_ref, pos_ref, vel_ref, frc_ref, id_ref, ok_ref, en_ref, line, wide_line, sums, added):
    me = [lax.axis_index(name) for name in "xyz"]
    n = pos_ref.shape[1]
    side = srt_ref[9:10, 0:1]
    okrow = srt_ref[8:9]
    good = okrow > 0.5
    count = jnp.sum(okrow).astype(I32)
    span = slots + L

    away = jnp.full(TILE, FAR, F32)
    first = CHUNK * L
    line[:, 0:slots - first] = jnp.concatenate([jnp.where(good, srt_ref[0:3], FAR), jnp.full((5, slots), FAR, F32)], axis=0)[:, first:]
    lane = lax.broadcasted_iota(I32, (8, span), 1)
    fill = jnp.maximum(count - first, 0)
    for d in DIRS:
        index = peers.index(offset_of(sizes, [-c for c in d]))
        low, high = range_of(d)
        shifts = []
        for axis in range(3):
            box = side * float(sizes[axis])
            if d[axis] == 1:
                shifts.append(jnp.where(me[axis] == sizes[axis] - 1, box, 0.0))
            elif d[axis] == -1:
                shifts.append(jnp.where(me[axis] == 0, -box, 0.0))
            else:
                shifts.append(jnp.zeros((1, 1), F32))
        shift = jnp.concatenate(shifts, axis=0)
        for source, entry in ((gh_ref, index), (ga_ref, index + len(peers))):
            tiles = source.shape[1] // 3
            width = tiles * L
            begin = offs_ref[entry, low]
            end = offs_ref[entry, 32 + high]
            block = jnp.concatenate([source[index, pl.ds(t, 3, stride=tiles), :] for t in range(tiles)], axis=1) + shift
            block = jnp.concatenate([block, jnp.zeros((5, width), F32)], axis=0)
            block = jnp.concatenate([block, away], axis=1)
            head = fill & (L - 1)
            base = pl.multiple_of(fill - head, L)
            move = head - begin
            block = pltpu.roll(block, jnp.where(move < 0, move + (width + L), move), 1)
            block = jnp.where(lane[:, 0:width + L] < head + end - begin, block, FAR)
            line[:, pl.ds(base, L)] = jnp.where(lane[:, 0:L] < head, line[:, pl.ds(base, L)], block[:, 0:L])
            line[:, pl.ds(pl.multiple_of(base + L, L), width)] = block[:, L:]
            fill = fill + (end - begin)
    rest = pl.multiple_of(((fill + L - 1) // L) * L, L)
    line[:, pl.ds(rest, CHUNK * L)] = jnp.full((8, CHUNK * L), FAR, F32)
    chunks = jnp.maximum((fill + CHUNK * L - 1) // (CHUNK * L), 1)

    def widen(c, carry):
        for t in range(CHUNK):
            place = pl.ds(pl.multiple_of((c * CHUNK + t) * L, L), L)
            tile = line[:, place]
            for a in range(3):
                wide_line[a, :, place] = jnp.broadcast_to(tile[a:a + 1], TILE)
        return carry

    lax.fori_loop(0, chunks, widen, 0)

    def own_step(q, energy):
        start = tuple(tuple(inner_ref[a, step_rows(q, g), :] for a in range(3)) for g in range(GROUPS))
        carry = pair_loop(own_cols, wide_line, q, 0, own_chunks, True, (start, energy))
        force, energy = pair_loop(own_cols, wide_line, q, own_chunks, chunks, False, carry)
        for g in range(GROUPS):
            for a in range(3):
                sums[a, step_rows(q, g), :] = force[g][a]
        return energy

    own_chunks = jnp.where(count > first, 1, 0)
    own_steps = (count + 8 * GROUPS - 1) // (8 * GROUPS)
    energy = lax.fori_loop(0, own_steps, own_step, tuple(inner_en_ref[k] for k in range(3)))
    en_ref[...] = jnp.sum(2.0 * energy[0] - 12.0 * energy[1] + 0.5 * (RC * UPC - UCUT) * energy[2], axis=0, keepdims=True)

    col = lax.broadcasted_iota(I32, (L, L), 1)
    picks = [jnp.where(col == a, 1.0, 0.0).astype(BF16) for a in range(3)]

    def add_up(base):
        total = jnp.zeros((2 * L, L), F32)
        for a in range(3):
            for part in split3(sums[a, base:base + 2 * L, :]):
                total = total + lax.dot_general(part, picks[a], NN, preferred_element_type=F32)
        added[:, base:base + 2 * L] = jnp.transpose(total)[0:8]

    for base in range(0, slots, 2 * L):
        if base < 4 * L:
            add_up(base)
        else:
            pl.when(count > base)(functools.partial(add_up, base))
    force = jnp.where(good, 24.0 * added[0:3], 0.0)
    pos_ref[...] = srt_ref[0:3, 0:n]
    frc_ref[...] = force[:, 0:n]
    vel_ref[...] = (srt_ref[3:6] + (0.5 * DT) * force)[:, 0:n]
    id_ref[...] = jnp.reshape((srt_ref[6:7].astype(I32) * 65536 + srt_ref[7:8].astype(I32))[:, 0:n], (n,))
    ok_ref[...] = jnp.reshape(okrow[:, 0:n].astype(I32), (n,))


def total_kernel(sizes, part_ref, sum_ref, rows, ssem, rsem):
    me = [lax.axis_index(name) for name in "xyz"]
    size_x, size_y, size_z = sizes
    mine = (me[2] * size_y + me[1]) * size_x + me[0]
    others = [(dx, dy, dz) for dz in range(size_z) for dy in range(size_y) for dx in range(size_x) if dx + dy + dz > 0]
    others.sort(key=lambda o: -(2 * min(o[2], size_z - o[2]) + 2 * o[1] + min(o[0], size_x - o[0])))

    device_at = functools.partial(device_of, sizes, me)

    barrier = pltpu.get_barrier_semaphore()
    for offset in others:
        pl.semaphore_signal(barrier, inc=1, device_id=device_at(offset), device_id_type=pl.DeviceIdType.MESH)
    rows[pl.ds(mine, 1)] = part_ref[...]
    pl.semaphore_wait(barrier, len(others))
    copies = []
    for index, offset in enumerate(others):
        copy = pltpu.make_async_remote_copy(
            src_ref=part_ref, dst_ref=rows.at[pl.ds(mine, 1)], send_sem=ssem.at[index], recv_sem=rsem.at[index],
            device_id=device_at(offset), device_id_type=pl.DeviceIdType.MESH)
        copy.start()
        copies.append(copy)
    for copy in copies:
        copy.wait_recv()
    sum_ref[...] = jnp.sum(rows[...], axis=0, keepdims=True)
    for copy in copies:
        copy.wait_send()


def solution(mesh):
    sizes = (mesh.shape["x"], mesh.shape["y"], mesh.shape["z"])
    peers = sorted({offset_of(sizes, d) for d in DIRS} - {(0, 0, 0)})
    devices = sizes[0] * sizes[1] * sizes[2]

    def local_step(atom_pos, atom_vel, atom_frc, atom_id, atom_ok, brick_side):
        n = atom_pos.shape[0]
        slots = -(-n // L) * L
        side = jnp.reshape(brick_side, (1, 1))
        old_rows, new_rows = [3 * (width // L) + 1 for width in (slots, NEW)]
        vmem = pl.BlockSpec(memory_space=pltpu.VMEM)
        smem = pl.BlockSpec(memory_space=pltpu.SMEM)
        srt, ghosts, fresh, own, inner, inner_en = pl.pallas_call(
            functools.partial(exchange_kernel, sizes, peers, slots),
            out_shape=(jax.ShapeDtypeStruct((16, slots), F32), jax.ShapeDtypeStruct((len(peers), old_rows, L), F32), jax.ShapeDtypeStruct((len(peers), new_rows, L), F32),
                       jax.ShapeDtypeStruct((slots, 3 * L), F32), jax.ShapeDtypeStruct((3, slots, L), F32), jax.ShapeDtypeStruct((3,) + TILE, F32)),
            in_specs=[pl.BlockSpec(memory_space=pltpu.HBM)] * 5 + [smem],
            out_specs=(vmem,) * 6,
            scratch_shapes=[
                pltpu.VMEM((3, n), F32), pltpu.VMEM((3, n), F32), pltpu.VMEM((3, n), F32), pltpu.VMEM((n,), I32), pltpu.VMEM((n,), I32),
                pltpu.VMEM((32, L), F32), pltpu.VMEM((26, L), F32), pltpu.VMEM((3, old_rows, L), F32), pltpu.VMEM((3, new_rows, L), F32), pltpu.VMEM((3, 8, CHUNK * L), F32),
                pltpu.SemaphoreType.DMA((5,)), pltpu.SemaphoreType.DMA((26,)), pltpu.SemaphoreType.DMA((26,)),
            ] + [pltpu.SemaphoreType.DMA((len(peers),))] * 4,
            compiler_params=pltpu.CompilerParams(collective_id=0, has_side_effects=True, vmem_limit_bytes=40 * 2 ** 20),
            name="exchange",
        )(*[pltpu.with_memory_space_constraint(v, pltpu.HBM) for v in (atom_pos.T, atom_vel.T, atom_frc.T, atom_id, atom_ok)], side)
        offs = jnp.concatenate([ghosts[:, -1, 0:64], fresh[:, -1, 0:64]], axis=0).astype(I32)
        out_f = jax.ShapeDtypeStruct((3, n), F32)
        out_i = jax.ShapeDtypeStruct((n,), I32)
        new_pos, new_vel, new_frc, new_id, new_ok, energy = pl.pallas_call(
            functools.partial(force_kernel, sizes, peers, slots),
            out_shape=(out_f, out_f, out_f, out_i, out_i, jax.ShapeDtypeStruct((1, L), F32)),
            in_specs=[vmem] * 6 + [smem],
            out_specs=(vmem,) * 6,
            scratch_shapes=[pltpu.VMEM((8, 28 * slots + CHUNK * L), F32), pltpu.VMEM((3, 8, 28 * slots + CHUNK * L), F32), pltpu.VMEM((3, slots, L), F32), pltpu.VMEM((8, slots), F32)],
            compiler_params=pltpu.CompilerParams(vmem_limit_bytes=40 * 2 ** 20),
            name="forces",
        )(srt, ghosts, fresh, own, inner, inner_en, offs)
        energy = pl.pallas_call(
            functools.partial(total_kernel, sizes),
            out_shape=jax.ShapeDtypeStruct((1, L), F32),
            in_specs=[vmem],
            out_specs=vmem,
            scratch_shapes=[pltpu.VMEM((devices, L), F32), pltpu.SemaphoreType.DMA((devices,)), pltpu.SemaphoreType.DMA((devices,))],
            compiler_params=pltpu.CompilerParams(collective_id=1, has_side_effects=True, vmem_limit_bytes=4 * 2 ** 20),
            name="total",
        )(pltpu.with_memory_space_constraint(energy, pltpu.VMEM))
        return new_pos.T, new_vel.T, new_frc.T, new_id, new_ok, jnp.sum(energy)

    row_spec = P(MESH_AXES, None)
    id_spec = P(MESH_AXES)
    return jax.shard_map(local_step, mesh=mesh, in_specs=(row_spec, row_spec, row_spec, id_spec, id_spec, P()), out_specs=(row_spec, row_spec, row_spec, id_spec, id_spec, P()), check_vma=False)
```
